32 devices in a mesh: row: 4 (over y, x), col: 8 (over z, core).
Axes of the slice: x: 2, y: 2, z: 4, core: 2. Of those that a mesh axis runs over, the one named last changes fastest.
Arguments:
- layer_input: bfloat16 [8192, 2048], P(('col', 'row')), may hold values from -6 to 6
- cotangent: bfloat16 [8192, 2048], P(('col', 'row')), may hold values from -6 to 6
- expert_index: int32 [8192, 8], P(('col', 'row')), may hold values from 0 to 63, all different within a row; in each aligned block of 256 rows (0 to 255, 256 to 511, ...) at most 36 rows name the same one
- attention_gain: bfloat16 [2048], P('col'), may hold values from 0.5 to 1.5
- query_gain: bfloat16 [2048], P(('row', 'col')), may hold values from 0.5 to 1.5
- key_gain: bfloat16 [2048], P(('row', 'col')), may hold values from 0.5 to 1.5
- query_weight: bfloat16 [2048, 2048], P('col', 'row'), may hold values from -1 to 1
- key_weight: bfloat16 [2048, 2048], P('col', 'row'), may hold values from -1 to 1
- value_weight: bfloat16 [2048, 2048], P('col', 'row'), may hold values from -0.125 to 0.125
- output_weight: bfloat16 [2048, 2048], P('row', 'col'), may hold values from -1 to 1
- feed_gain: bfloat16 [2048], P('col'), may hold values from 0.5 to 1.5
- router_weight: bfloat16 [2048, 64], P('col'), may hold values from -1 to 1
- gate_weight: bfloat16 [64, 2048, 1024], P('col', None, 'row'), may hold values from -0.125 to 0.125
- up_weight: bfloat16 [64, 2048, 1024], P('col', None, 'row'), may hold values from -0.125 to 0.125
- down_weight: bfloat16 [64, 1024, 2048], P('col', 'row'), may hold values from -1.5 to 1.5
Outputs:
- layer_output: float32 [8192, 2048], P(('col', 'row'))
- input_grad: float32 [8192, 2048], P(('col', 'row'))
- grad_attention_gain: float32 [2048], P('col')
- grad_query_gain: float32 [2048], P(('row', 'col'))
- grad_key_gain: float32 [2048], P(('row', 'col'))
- grad_query_weight: float32 [2048, 2048], P('col', 'row')
- grad_key_weight: float32 [2048, 2048], P('col', 'row')
- grad_value_weight: float32 [2048, 2048], P('col', 'row')
- grad_output_weight: float32 [2048, 2048], P('row', 'col')
- grad_feed_gain: float32 [2048], P('col')
- grad_router_weight: float32 [2048, 64], P('col')
- grad_gate_weight: float32 [64, 2048, 1024], P('col', None, 'row')
- grad_up_weight: float32 [64, 2048, 1024], P('col', None, 'row')
- grad_down_weight: float32 [64, 1024, 2048], P('col', 'row')
The draws below stay inside these ranges and needn't reach their ends.
Inputs may be any that keep to these rules, and one draw needn't show every extreme that they name: `expert_index`: each row names 8 different experts; among the rows of one device no expert is named more than 36 times, and one expert is named exactly 36 times on some device.
All inputs are finite; a program needn't handle non-finite values.
Results may differ from the reference program's by a relative error of at most 0.022.
Values may be sent and summed in bfloat16 or wider, within the bound.
A program may use at most 448 MiB of HBM per device.

```python
import math
import jax
import jax.numpy as jnp
import numpy as np
from jax import lax

D = 2048
HEADS = 16
HD = 128
FF = 1024
EXPERTS = 64
TOP = 8
TOK_DEV = 256
TOKENS = 8192
CAP = 36
N_ROW = 4
N_COL = 8


def clipped_normal(key, shape):
    return jnp.clip(jax.random.normal(key, shape, jnp.float32), -4.0, 4.0)


def draw_query_weight(key, part):
    base = clipped_normal(jax.random.fold_in(key, 17), (D, D))
    return (base * D ** (-0.5)).astype(jnp.bfloat16)


def draw_key_weight(key, part):
    own = clipped_normal(jax.random.fold_in(key, 29), (D, D))
    return (own * D ** (-0.5)).astype(jnp.bfloat16)


def gain_values(key):
    unit = jax.random.uniform(key, (D,), jnp.float32)
    return 0.6 + 0.8 * unit


def draw_query_gain(key, part):
    return gain_values(jax.random.fold_in(key, 41)).astype(jnp.bfloat16)


def draw_key_gain(key, part):
    return gain_values(jax.random.fold_in(key, 43)).astype(jnp.bfloat16)


def draw_router_weight(key, part):
    base = clipped_normal(jax.random.fold_in(key, 53), (D, EXPERTS)) * D ** (-0.5)
    return base.astype(jnp.bfloat16)


def steps_of(stream_key, extent, cuts, least, high):
    loudness, own = 1.0, jax.random.fold_in(stream_key, 6)
    for dim, shards_of in cuts:
        heights = jnp.exp(jax.random.uniform(jax.random.fold_in(own, dim), (shards_of,), jnp.float32, least / len(cuts), high / len(cuts)))
        loudness = loudness * jnp.repeat(heights, extent[dim] // shards_of).reshape([-1 if axis == dim else 1 for axis in range(len(extent))])
    return loudness


def deal_out(stream_key, own, number, rows, amount, top, bound, lean):
    order = jax.random.permutation(stream_key, amount)
    crowded, ordinary = shares(amount, rows * top, bound, lean, True), shares(amount, rows * top, bound, lean, False)
    places = jnp.arange(amount)

    def named(sizes, offset_by):
        used = int((sizes > 0).sum())
        fixed = max(1, used // 4)
        moved = fixed + (places - fixed + offset_by * (used - fixed)) % max(1, amount - fixed)
        return jnp.zeros((amount,), jnp.int32).at[order[jnp.where(places < fixed, places, moved)]].set(jnp.asarray(sizes, jnp.int32))

    sizes = jnp.where(number % 4 == 0, named(crowded, number // 4), named(ordinary, number - number // 4 - 1))
    mixed = jax.random.permutation(jax.random.fold_in(own, 3), amount)
    donor, taker = mixed[0:amount // 2 * 2:2], mixed[1:amount // 2 * 2:2]
    room = jnp.minimum(sizes[donor] - 1, bound - sizes[taker]) // 2
    room = jnp.where((donor == order[0]) | (taker == order[0]) | (sizes[taker] == 0), 0, jnp.maximum(room, 0))
    moved = jax.random.randint(jax.random.fold_in(own, 4), (amount // 2,), 0, 1 << 20) % (room + 1)
    sizes = sizes.at[donor].add(-moved).at[taker].add(moved)
    members = jnp.searchsorted(jnp.cumsum(sizes), jnp.arange(rows * top), side="right").astype(jnp.int32)
    table = members.reshape(top, rows).T
    table = table[jax.random.permutation(jax.random.fold_in(own, 1), rows)]
    offset_by = jax.random.randint(jax.random.fold_in(own, 2), (rows, 1), 0, top)
    return jnp.take_along_axis(table, (jnp.arange(top)[None, :] + offset_by) % top, axis=1)


def shares(number_of, total, limit, slope, full):
    loads = [(1 << 20) // math.isqrt(standing ** slope) + 1 for standing in range(1, number_of + 1)]
    largest = limit if full else min(limit, max(-(-total // number_of), total * loads[0] // sum(loads)))
    least = 1 if total - largest >= number_of - 1 else 0
    holding, surplus = [largest] + [least] * (number_of - 1), total - largest - least * (number_of - 1)
    while surplus > 0:
        candidates = [i for i in range(1, number_of) if holding[i] < largest] or [i for i in range(1, number_of) if holding[i] < limit]
        pool, left = sum([loads[i] for i in candidates]), surplus
        for i in candidates:
            more = min(limit - holding[i], max(1, left * loads[i] // pool), surplus)
            holding[i] = holding[i] + more
            surplus = surplus - more
    return np.array(holding)


def noise(key, extent, deviation, limit, pieces=(), kind=jnp.bfloat16):
    values = jax.random.normal(key, extent, jnp.float32) * deviation
    if len(pieces) > 0:
        values = steps_of(key, extent, pieces, -0.22, 0.18) * values
    return jnp.clip(values, min=-limit, max=limit).astype(kind)


def setup_inputs(seed: int = 0) -> dict:
    keys = jax.random.split(jax.random.key(seed), 16)
    layer_input = noise(keys[0], (TOKENS, D), 1.0, 6.0, ((0, 32),))
    cotangent = noise(keys[1], (TOKENS, D), 1.0, 6.0, ((0, 32),))
    expert_index_keys = jax.random.split(jax.random.fold_in(keys[2], 1), TOKENS // TOK_DEV)
    expert_index_turns = jax.random.permutation(jax.random.fold_in(keys[2], 3), TOKENS // TOK_DEV)
    expert_index = jax.vmap(lambda own, number: deal_out(jax.random.fold_in(keys[2], 2), own, number, TOK_DEV, EXPERTS, TOP, CAP, 1))(expert_index_keys, expert_index_turns).reshape((TOKENS, TOP))
    attention_gain = jnp.clip(1.0 + 0.1 * jax.random.normal(keys[3], (D,), jnp.float32), 0.5, 1.5).astype(jnp.bfloat16)
    query_gain = draw_query_gain(jax.random.fold_in(keys[15], 71), 0)
    key_gain = draw_key_gain(jax.random.fold_in(keys[15], 71), 0)
    query_weight = draw_query_weight(jax.random.fold_in(keys[15], 71), 0)
    key_weight = draw_key_weight(jax.random.fold_in(keys[15], 71), 0)
    value_weight = noise(keys[8], (D, D), D ** -0.5, 0.125, ((0, 8), (1, 4)))
    output_weight = noise(keys[9], (D, D), (D // 64) ** -0.5, 1.0, ((0, 4), (1, 8)))
    feed_gain = jnp.clip(1.0 + 0.1 * jax.random.normal(keys[10], (D,), jnp.float32), 0.5, 1.5).astype(jnp.bfloat16)
    router_weight = draw_router_weight(jax.random.fold_in(keys[15], 71), 0)
    gate_weight = noise(keys[12], (EXPERTS, D, FF), D ** -0.5, 0.125, ((0, 8), (2, 4)))
    up_weight = noise(keys[13], (EXPERTS, D, FF), D ** -0.5, 0.125, ((0, 8), (2, 4)))
    down_weight = noise(keys[14], (EXPERTS, FF, D), (FF // 64) ** -0.5, 1.5, ((0, 8), (1, 4)))
    return {"layer_input": layer_input, "cotangent": cotangent, "expert_index": expert_index, "attention_gain": attention_gain, "query_gain": query_gain, "key_gain": key_gain, "query_weight": query_weight, "key_weight": key_weight, "value_weight": value_weight, "output_weight": output_weight, "feed_gain": feed_gain, "router_weight": router_weight, "gate_weight": gate_weight, "up_weight": up_weight, "down_weight": down_weight}


EPS = 1e-05
THETA = 10000.0
MASKED = -1e+30

@jax.custom_vjp
def low(v):
    return lax.optimization_barrier(v.astype(jnp.bfloat16)).astype(jnp.float32)

@jax.custom_vjp
def low_back(v):
    return v

def low_keep(v):
    return (low(v), None)

def low_pass(kept, grad):
    return (grad,)

def back_keep(v):
    return (v, None)

def back_low(kept, grad):
    return (low(grad),)
low.defvjp(low_keep, low_pass)
low_back.defvjp(back_keep, back_low)

def product(left, right):
    return jnp.dot(left, right, precision=lax.Precision.HIGHEST)

def rms_scale(field):
    return lax.rsqrt(lax.optimization_barrier(jnp.mean(field * field, axis=-1, keepdims=True)) + EPS)

def rope_tables(length):
    half_size = HD // 2
    freqs = THETA ** (-(jnp.arange(half_size, dtype=jnp.float32) * 2.0) / HD)
    angles = jnp.arange(length, dtype=jnp.float32)[:, None] * freqs[None, :]
    cosine = jnp.concatenate([jnp.cos(angles), jnp.cos(angles)], axis=-1)[:, None, :]
    sine_table = jnp.concatenate([jnp.sin(angles), jnp.sin(angles)], axis=-1)[:, None, :]
    return (cosine, sine_table)

def rotate(field, cosine, sine_table):
    half_size = field.shape[-1] // 2
    turned = jnp.concatenate([-field[..., half_size:], field[..., :half_size]], axis=-1)
    return field * cosine + turned * sine_table

def attend(queries, keys_rotated, value_heads):
    length = queries.shape[0]
    block_rows = min(512, length)
    score_scale = HD ** (-0.5)
    key_position = jnp.arange(length, dtype=jnp.int32)

    def one_block(offset):
        query_rows = lax.dynamic_slice_in_dim(queries, offset, block_rows, 0)
        scores = low_back(jnp.einsum('qhd,khd->hqk', query_rows, keys_rotated, precision=lax.Precision.HIGHEST) * score_scale)
        query_position = offset + jnp.arange(block_rows, dtype=jnp.int32)
        allowed = query_position[:, None] >= key_position[None, :]
        scores = jnp.where(allowed[None, :, :], scores, MASKED)
        row_top = lax.optimization_barrier(jnp.max(scores, axis=-1, keepdims=True))
        exponent = jnp.exp(scores - row_top)
        weights = low(exponent / lax.optimization_barrier(jnp.sum(exponent, axis=-1, keepdims=True)))
        return jnp.einsum('hqk,khd->qhd', weights, value_heads, precision=lax.Precision.HIGHEST)
    starts = jnp.arange(length // block_rows, dtype=jnp.int32) * block_rows
    blocks = lax.map(jax.checkpoint(one_block), starts)
    return blocks.reshape(length, queries.shape[1], queries.shape[2])

def attention_branch(sequence, params):
    attention_gain, query_gain, key_gain, query_weight, key_weight, value_weight, output_weight = params
    length = sequence.shape[0]
    normed = low(sequence * rms_scale(sequence) * attention_gain)
    query_raw = low_back(product(normed, query_weight))
    key_raw = low_back(product(normed, key_weight))
    value_rows = low(low_back(product(normed, value_weight)))
    query_normed = query_raw * rms_scale(query_raw) * query_gain
    key_normed = key_raw * rms_scale(key_raw) * key_gain
    cosine, sine_table = rope_tables(length)
    queries = low(rotate(query_normed.reshape(length, HEADS, HD), cosine, sine_table))
    keys_rotated = low(rotate(key_normed.reshape(length, HEADS, HD), cosine, sine_table))
    mixed_heads = attend(queries, keys_rotated, value_rows.reshape(length, HEADS, HD)).reshape(length, D)
    mixed_heads = low(low_back(mixed_heads))
    return low_back(product(mixed_heads, output_weight))

def slot_tables(expert_index):
    devices = N_ROW * N_COL
    flat_index = expert_index.reshape(devices, TOK_DEV * TOP)
    onehot = (flat_index[:, :, None] == jnp.arange(EXPERTS, dtype=jnp.int32)[None, None, :]).astype(jnp.int32)
    running = jnp.cumsum(onehot, axis=1, dtype=jnp.int32) - 1
    slot_rank = lax.optimization_barrier(jnp.sum(running * onehot, axis=-1, dtype=jnp.int32)).astype(jnp.int32)
    owners = jnp.arange(devices, dtype=jnp.int32)[:, None]
    slot_index = (flat_index * (devices * CAP) + owners * CAP + slot_rank).reshape(-1).astype(jnp.int32)
    entries = (jnp.arange(devices * TOK_DEV * TOP, dtype=jnp.int32) // TOP).astype(jnp.int32)
    slot_source = jnp.full((EXPERTS * devices * CAP,), devices * TOK_DEV, dtype=jnp.int32).at[slot_index].set(entries)
    return (slot_index.reshape(-1, TOP), slot_source.reshape(EXPERTS, devices * CAP))

def forward(layer_input, attention_gain, query_gain, key_gain, query_weight, key_weight, value_weight, output_weight, feed_gain, router_weight, gate_weight, up_weight, down_weight, expert_index):
    length = TOK_DEV * N_ROW
    params = (attention_gain, query_gain, key_gain, query_weight, key_weight, value_weight, output_weight)

    def one_sequence(sequence):
        return attention_branch(sequence, params)
    branch = lax.map(jax.checkpoint(one_sequence), layer_input.reshape(N_COL, length, D)).reshape(-1, D)
    hidden = layer_input + branch
    feed_normed = low(hidden * rms_scale(hidden) * feed_gain)
    logits = low_back(product(feed_normed, router_weight))
    logit_top = lax.optimization_barrier(jnp.max(logits, axis=-1, keepdims=True))
    logit_exp = jnp.exp(logits - logit_top)
    router_probs = logit_exp / lax.optimization_barrier(jnp.sum(logit_exp, axis=-1, keepdims=True))
    chosen = expert_index[:, :, None] == jnp.arange(EXPERTS, dtype=jnp.int32)[None, None, :]
    gate_probs = lax.optimization_barrier(jnp.sum(jnp.where(chosen, router_probs[:, None, :], 0.0), axis=-1))
    slot_index, slot_source = slot_tables(expert_index)
    padded = jnp.concatenate([feed_normed, jnp.zeros((1, D), feed_normed.dtype)], axis=0)
    expert_rows = low_back(padded[slot_source])

    def expert(operands):
        rows_in, gate_mat, up_mat, down_mat = operands
        gate_val = low_back(product(rows_in, gate_mat))
        up_val = low_back(product(rows_in, up_mat))
        activated = low(jax.nn.silu(gate_val) * up_val)
        return low(low_back(product(activated, down_mat)))
    expert_out = lax.map(jax.checkpoint(expert), (expert_rows, gate_weight, up_weight, down_weight)).reshape(-1, D)
    mixture = jnp.zeros_like(hidden)
    for column in range(TOP):
        mixture = mixture + gate_probs[:, column:column + 1] * expert_out[slot_index[:, column]]
    return hidden + mixture

def reference(layer_input, cotangent, expert_index, attention_gain, query_gain, key_gain, query_weight, key_weight, value_weight, output_weight, feed_gain, router_weight, gate_weight, up_weight, down_weight):
    floats = [item.astype(jnp.float32) for item in (layer_input, attention_gain, query_gain, key_gain, query_weight, key_weight, value_weight, output_weight, feed_gain, router_weight, gate_weight, up_weight, down_weight)]

    def wrapped(*values):
        return forward(*values, expert_index)
    layer_output, pullback = jax.vjp(wrapped, *floats)
    grads = pullback(cotangent.astype(jnp.float32))
    return (layer_output, grads[0], grads[1], grads[2], grads[3], grads[4], grads[5], grads[6], grads[7], grads[8], grads[9], grads[10], grads[11], grads[12])
```

```python
import jax
import jax.numpy as jnp
from jax import lax
from jax.experimental import pallas as pl
from jax.experimental.pallas import tpu as pltpu
from jax.sharding import PartitionSpec as P

HD = 128
SLOTS = 40
BLOCK = 512


EPS = 1e-05
THETA = 10000.0
MASKED = -1e30


def wide_dot(left, right):
    return jnp.dot(left, right, preferred_element_type=jnp.float32)


def inner_rows(left, right):
    return lax.dot_general(
        left, right, (((0,), (0,)), ((), ())), preferred_element_type=jnp.float32
    )


def outer_cols(left, right):
    return lax.dot_general(
        left, right, (((1,), (1,)), ((), ())), preferred_element_type=jnp.float32
    )


def rms_scale(field):
    return lax.rsqrt(jnp.mean(field * field, axis=-1, keepdims=True) + EPS)


def rope_tables(length):
    half_size = HD // 2
    freqs = THETA ** (-(jnp.arange(half_size, dtype=jnp.float32) * 2.0) / HD)
    angles = jnp.arange(length, dtype=jnp.float32)[:, None] * freqs[None, :]
    cosine = jnp.concatenate([jnp.cos(angles), jnp.cos(angles)], axis=-1)[:, None, :]
    sine_table = jnp.concatenate([jnp.sin(angles), jnp.sin(angles)], axis=-1)[:, None, :]
    return (cosine, sine_table)


def rotate(field, cosine, sine_table):
    half_size = field.shape[-1] // 2
    turned = jnp.concatenate([-field[..., half_size:], field[..., :half_size]], axis=-1)
    return field * cosine + turned * sine_table


def unrotate(gradient, cosine, sine_table):
    half_size = gradient.shape[-1] // 2
    moved = gradient * sine_table
    back_turned = jnp.concatenate([moved[..., half_size:], -moved[..., :half_size]], axis=-1)
    return gradient * cosine + back_turned


def dispatch_body(pick_ref, field_ref, rows_ref):
    groups = rows_ref.shape[0]
    first = wide_dot(pick_ref[0], field_ref[0]).reshape(groups, SLOTS, -1)
    second = wide_dot(pick_ref[1], field_ref[1]).reshape(groups, SLOTS, -1)
    rows_ref[...] = jnp.concatenate([first, second], axis=1).astype(jnp.bfloat16)


def dispatch(pick, field):
    ranks, width, tokens = pick.shape
    groups, depth = width // SLOTS, field.shape[1]
    return pl.pallas_call(
        dispatch_body,
        grid=(ranks // 2, depth // BLOCK),
        in_specs=[
            pl.BlockSpec((2, width, tokens), lambda i, k: (i, 0, 0)),
            pl.BlockSpec((2, tokens, BLOCK), lambda i, k: (i, 0, k)),
        ],
        out_specs=pl.BlockSpec((groups, 2 * SLOTS, BLOCK), lambda i, k: (0, i, k)),
        out_shape=jax.ShapeDtypeStruct((groups, ranks * SLOTS, depth), jnp.bfloat16),
    )(pick, field.reshape(ranks, tokens, depth))


def combine_body(spread_ref, rows_ref, field_ref):
    rows = rows_ref[...].astype(jnp.float32)
    width = rows.shape[0] * SLOTS
    for side in range(2):
        part = rows[:, side * SLOTS : (side + 1) * SLOTS].reshape(width, -1).astype(jnp.bfloat16)
        field_ref[side] = wide_dot(spread_ref[side], part).astype(jnp.bfloat16)


def combine(spread, rows):
    ranks, tokens, width = spread.shape
    groups, depth = width // SLOTS, rows.shape[2]
    field = pl.pallas_call(
        combine_body,
        grid=(ranks // 2, depth // BLOCK),
        in_specs=[
            pl.BlockSpec((2, tokens, width), lambda i, k: (i, 0, 0)),
            pl.BlockSpec((groups, 2 * SLOTS, BLOCK), lambda i, k: (0, i, k)),
        ],
        out_specs=pl.BlockSpec((2, tokens, BLOCK), lambda i, k: (i, 0, k)),
        out_shape=jax.ShapeDtypeStruct((ranks, tokens, depth), jnp.bfloat16),
    )(spread, rows)
    return field.reshape(ranks * tokens, depth)


def scatter_all(field):
    part = lax.psum_scatter(field, "col", scatter_dimension=0, tiled=True)
    return lax.psum_scatter(part, "row", scatter_dimension=0, tiled=True)


def pieces_of(ranks, depth):
    count = max(1, ranks // 32)
    step = depth // count
    return [(at, at + step) for at in range(0, depth, step)]


def gather_rows(pick, field):
    rows = []
    for start, stop in pieces_of(pick.shape[0], field.shape[1]):
        part = field[:, start:stop]
        if rows:
            part = lax.optimization_barrier((part, rows[-1]))[0]
        whole = lax.all_gather(part, ("col", "row"), axis=0, tiled=True)
        rows.append(dispatch(pick, whole))
    return rows[0] if len(rows) == 1 else jnp.concatenate(rows, axis=2)


def return_rows(spread, rows):
    sums = []
    for start, stop in pieces_of(spread.shape[0], rows.shape[2]):
        part = rows[:, :, start:stop]
        if sums:
            part = lax.optimization_barrier((part, sums[-1]))[0]
        sums.append(scatter_all(combine(spread, part)))
    return sums[0] if len(sums) == 1 else jnp.concatenate(sums, axis=1)


def local(
    layer_input,
    cotangent,
    expert_index,
    attention_gain,
    query_gain,
    key_gain,
    query_weight,
    key_weight,
    value_weight,
    output_weight,
    feed_gain,
    router_weight,
    gate_weight,
    up_weight,
    down_weight,
):
    tokens = layer_input.shape[0]
    rows_count = lax.axis_size("row")
    (
        attention_full,
        query_scale_w,
        key_scale_w,
        query_full,
        key_full,
        value_full,
        output_full,
        feed_full,
        router_full,
    ) = (
        lax.all_gather(attention_gain, "col", axis=0, tiled=True),
        lax.all_gather(query_gain, "col", axis=0, tiled=True),
        lax.all_gather(key_gain, "col", axis=0, tiled=True),
        lax.all_gather(query_weight, "col", axis=0, tiled=True),
        lax.all_gather(key_weight, "col", axis=0, tiled=True),
        lax.all_gather(value_weight, "col", axis=0, tiled=True),
        lax.all_gather(output_weight, "col", axis=1, tiled=True),
        lax.all_gather(feed_gain, "col", axis=0, tiled=True),
        lax.all_gather(router_weight, "col", axis=0, tiled=True),
    )
    sequence = lax.all_gather(layer_input, "row", axis=0, tiled=True)
    length = sequence.shape[0]
    model_width = sequence.shape[1]
    local_width = query_full.shape[1]
    local_heads = local_width // HD
    seq_float = sequence.astype(jnp.float32)
    seq_scale = rms_scale(seq_float)
    attention_float = attention_full.astype(jnp.float32)
    normed = (seq_float * seq_scale * attention_float).astype(jnp.bfloat16)
    query_raw = wide_dot(normed, query_full)
    key_raw = wide_dot(normed, key_full)
    value_heads = wide_dot(normed, value_full).astype(jnp.bfloat16).reshape(length, local_heads, HD)
    query_total, key_total = lax.psum(
        (jnp.sum(query_raw * query_raw, axis=-1), jnp.sum(key_raw * key_raw, axis=-1)), "row"
    )
    query_rs = lax.rsqrt(query_total / model_width + EPS)[:, None]
    key_rs = lax.rsqrt(key_total / model_width + EPS)[:, None]
    query_gain_f = query_scale_w.astype(jnp.float32)
    key_gain_f = key_scale_w.astype(jnp.float32)
    cosine, sine_table = rope_tables(length)
    queries = rotate(
        (query_raw * query_rs * query_gain_f).reshape(length, local_heads, HD), cosine, sine_table
    ).astype(jnp.bfloat16)
    keys_rotated = rotate(
        (key_raw * key_rs * key_gain_f).reshape(length, local_heads, HD), cosine, sine_table
    ).astype(jnp.bfloat16)
    block_rows = min(512, length)
    starts = jnp.arange(length // block_rows, dtype=jnp.int32) * block_rows
    key_position = jnp.arange(length, dtype=jnp.int32)
    score_scale = HD ** (-0.5)

    def block_scores(offset):
        query_rows = lax.dynamic_slice_in_dim(queries, offset, block_rows, 0)
        scores = (
            jnp.einsum("qhd,khd->hqk", query_rows, keys_rotated, preferred_element_type=jnp.float32)
            * score_scale
        )
        query_position = offset + jnp.arange(block_rows, dtype=jnp.int32)
        allowed = query_position[:, None] >= key_position[None, :]
        return (query_rows, jnp.where(allowed[None, :, :], scores, MASKED))

    def forward_block(offset):
        query_rows, scores = block_scores(offset)
        row_top = jnp.max(scores, axis=-1, keepdims=True)
        exponent = jnp.exp(scores - row_top)
        row_total = jnp.sum(exponent, axis=-1, keepdims=True)
        weights = (exponent / row_total).astype(jnp.bfloat16)
        mixed_block = jnp.einsum(
            "hqk,khd->qhd", weights, value_heads, preferred_element_type=jnp.float32
        )
        return (mixed_block, (row_top + jnp.log(row_total))[..., 0])

    mixed_blocks, lse_blocks = lax.map(forward_block, starts)
    mixed_heads = mixed_blocks.reshape(length, local_width).astype(jnp.bfloat16)
    lse_all = jnp.moveaxis(lse_blocks, 0, 1).reshape(local_heads, length)
    branch = lax.psum_scatter(
        wide_dot(mixed_heads, output_full).astype(jnp.bfloat16), "row", scatter_dimension=0, tiled=True
    ).astype(jnp.float32)
    hidden = layer_input.astype(jnp.float32) + branch
    feed_scale = rms_scale(hidden)
    feed_float = feed_full.astype(jnp.float32)
    feed_normed = (hidden * feed_scale * feed_float).astype(jnp.bfloat16)
    logits = wide_dot(feed_normed, router_full)
    logit_top = jnp.max(logits, axis=-1, keepdims=True)
    logit_exp = jnp.exp(logits - logit_top)
    router_probs = logit_exp / jnp.sum(logit_exp, axis=-1, keepdims=True)
    experts = router_full.shape[1]
    experts_local = gate_weight.shape[0]
    ranks = lax.axis_size("col") * rows_count
    gate_hits = expert_index[:, :, None] == jnp.arange(experts, dtype=jnp.int32)
    gate_probs = jnp.sum(jnp.where(gate_hits, router_probs[:, None, :], 0.0), axis=-1)

    index_all = lax.all_gather(expert_index, ("col", "row"), axis=0, tiled=True)
    probs_all = lax.all_gather(gate_probs, ("col", "row"), axis=0, tiled=True)
    own = (index_all - lax.axis_index("col") * experts_local).reshape(ranks, tokens, -1)
    matches = own[..., None] == jnp.arange(experts_local, dtype=jnp.int32)
    hit = jnp.sum(matches.astype(jnp.float32), axis=2)
    earlier = jnp.tril(jnp.ones((tokens, tokens), jnp.bfloat16), -1)
    rank = jnp.einsum(
        "tu,sue->ste", earlier, hit.astype(jnp.bfloat16), preferred_element_type=jnp.float32
    )
    slot = jnp.where(hit > 0, rank, -1.0)
    places = jnp.arange(SLOTS, dtype=jnp.float32)
    slot_t = jnp.swapaxes(slot, 1, 2)
    width = experts_local * SLOTS
    pick = (slot_t[:, :, None, :] == places[None, None, :, None]).astype(jnp.bfloat16)
    pick = pick.reshape(ranks, width, tokens)
    spread = slot[:, :, :, None] == places
    probs_own = jnp.sum(
        jnp.where(matches, probs_all.reshape(ranks, tokens, -1, 1), 0.0), axis=2
    )
    spread_plain = spread.astype(jnp.bfloat16).reshape(ranks, tokens, width)
    spread_probs = (
        jnp.where(spread, probs_own[..., None], 0.0).astype(jnp.bfloat16).reshape(ranks, tokens, width)
    )
    row_probs = jnp.sum(jnp.where(spread, probs_own[..., None], 0.0), axis=1)
    row_probs = jnp.swapaxes(row_probs, 0, 1).reshape(experts_local, ranks * SLOTS, 1)

    expert_grads = gather_rows(pick, cotangent)
    expert_rows = gather_rows(pick, feed_normed)
    gate_val = jnp.einsum("erd,edf->erf", expert_rows, gate_weight, preferred_element_type=jnp.float32)
    up_val = jnp.einsum("erd,edf->erf", expert_rows, up_weight, preferred_element_type=jnp.float32)
    plain_act = jnp.einsum("erd,efd->erf", expert_grads, down_weight, preferred_element_type=jnp.float32)
    sigmoid_val = jax.nn.sigmoid(gate_val)
    silu_val = gate_val * sigmoid_val
    activated = silu_val * up_val
    grad_act = plain_act * row_probs
    grad_up = (grad_act * silu_val).astype(jnp.bfloat16)
    grad_gate = (
        grad_act * up_val * sigmoid_val * (1.0 + gate_val * (1.0 - sigmoid_val))
    ).astype(jnp.bfloat16)
    row_gates = jnp.sum(activated * plain_act, axis=-1).reshape(experts_local, ranks, 1, SLOTS)
    weighted_act = (activated * row_probs).astype(jnp.bfloat16)
    activated = activated.astype(jnp.bfloat16)
    own_gates = jnp.sum(jnp.where(spread, jnp.transpose(row_gates, (1, 2, 0, 3)), 0.0), axis=-1)
    own_gates = lax.psum_scatter(
        own_gates.reshape(-1, rows_count, tokens, experts_local), "row", scatter_dimension=1
    )
    grad_probs = lax.all_to_all(own_gates, "col", split_axis=0, concat_axis=2, tiled=True)[0]

    back_rows = (
        jnp.einsum("erf,edf->erd", grad_gate, gate_weight, preferred_element_type=jnp.float32)
        + jnp.einsum("erf,edf->erd", grad_up, up_weight, preferred_element_type=jnp.float32)
    ).astype(jnp.bfloat16)
    grad_feed = return_rows(spread_plain, back_rows).astype(jnp.float32)
    out_rows = jnp.einsum(
        "erf,efd->erd", activated, down_weight, preferred_element_type=jnp.float32
    ).astype(jnp.bfloat16)
    mixture = return_rows(spread_probs, out_rows).astype(jnp.float32)
    layer_output = hidden + mixture
    grad_gate_weight = jnp.einsum("erd,erf->edf", expert_rows, grad_gate, preferred_element_type=jnp.float32)
    grad_up_weight = jnp.einsum("erd,erf->edf", expert_rows, grad_up, preferred_element_type=jnp.float32)
    grad_down_weight = jnp.einsum("erf,erd->efd", weighted_act, expert_grads, preferred_element_type=jnp.float32)
    grad_out = cotangent.astype(jnp.float32)
    grad_logits = (
        router_probs * (grad_probs - jnp.sum(router_probs * grad_probs, axis=-1, keepdims=True))
    ).astype(jnp.bfloat16)
    router_grad = inner_rows(feed_normed, grad_logits)
    grad_feed = grad_feed + outer_cols(grad_logits, router_full)
    feed_gain_term = jnp.sum(grad_feed * hidden * feed_scale, axis=0)
    feed_weighted = grad_feed * feed_float
    grad_hidden = (
        grad_out
        + feed_scale * feed_weighted
        - hidden * feed_scale**3 * jnp.mean(feed_weighted * hidden, axis=-1, keepdims=True)
    )
    grad_branch = lax.all_gather(grad_hidden.astype(jnp.bfloat16), "row", axis=0, tiled=True)
    output_grad = inner_rows(mixed_heads, grad_branch)
    grad_mixed = (
        outer_cols(grad_branch, output_full).astype(jnp.bfloat16).reshape(length, local_heads, HD)
    )

    def backward_block(carry, offset):
        grad_keys, grad_values = carry
        query_rows, scores = block_scores(offset)
        lse_rows = lax.dynamic_slice_in_dim(lse_all, offset, block_rows, 1)
        probs_block = jnp.exp(scores - lse_rows[:, :, None])
        weights_low = probs_block.astype(jnp.bfloat16)
        grad_rows_out = lax.dynamic_slice_in_dim(grad_mixed, offset, block_rows, 0)
        grad_weights = jnp.einsum(
            "qhd,khd->hqk", grad_rows_out, value_heads, preferred_element_type=jnp.float32
        )
        grad_values = grad_values + jnp.einsum(
            "hqk,qhd->khd", weights_low, grad_rows_out, preferred_element_type=jnp.float32
        )
        delta_rows = jnp.sum(probs_block * grad_weights, axis=-1, keepdims=True)
        grad_scores = (probs_block * (grad_weights - delta_rows)).astype(jnp.bfloat16)
        grad_query_block = (
            jnp.einsum(
                "hqk,khd->qhd", grad_scores, keys_rotated, preferred_element_type=jnp.float32
            )
            * score_scale
        )
        grad_keys = (
            grad_keys
            + jnp.einsum(
                "hqk,qhd->khd", grad_scores, query_rows, preferred_element_type=jnp.float32
            )
            * score_scale
        )
        return ((grad_keys, grad_values), grad_query_block)

    zero_heads = jnp.zeros((length, local_heads, HD), jnp.float32)
    (grad_keys, grad_values), grad_query_blocks = lax.scan(
        backward_block, (zero_heads, zero_heads), starts
    )
    grad_queries = grad_query_blocks.reshape(length, local_heads, HD)
    grad_query_normed = unrotate(grad_queries, cosine, sine_table).reshape(length, local_width)
    grad_key_normed = unrotate(grad_keys, cosine, sine_table).reshape(length, local_width)
    grad_value_low = grad_values.reshape(length, local_width).astype(jnp.bfloat16)
    query_weighted = grad_query_normed * query_gain_f
    key_weighted = grad_key_normed * key_gain_f
    query_gain_term = jnp.sum(grad_query_normed * query_raw * query_rs, axis=0)
    key_gain_term = jnp.sum(grad_key_normed * key_raw * key_rs, axis=0)
    query_inner, key_inner, feed_gain_total, router_total = (
        lax.psum(jnp.sum(query_weighted * query_raw, axis=-1).astype(jnp.bfloat16), "row").astype(
            jnp.float32
        ),
        lax.psum(jnp.sum(key_weighted * key_raw, axis=-1).astype(jnp.bfloat16), "row").astype(
            jnp.float32
        ),
        lax.psum(feed_gain_term.astype(jnp.bfloat16), "row").astype(jnp.float32),
        lax.psum(router_grad.astype(jnp.bfloat16), "row").astype(jnp.float32),
    )
    grad_query_raw = (
        query_rs * query_weighted - query_raw * query_rs**3 * (query_inner / model_width)[:, None]
    ).astype(jnp.bfloat16)
    grad_key_raw = (
        key_rs * key_weighted - key_raw * key_rs**3 * (key_inner / model_width)[:, None]
    ).astype(jnp.bfloat16)
    query_grad = inner_rows(normed, grad_query_raw)
    key_grad = inner_rows(normed, grad_key_raw)
    value_grad = inner_rows(normed, grad_value_low)
    grad_normed = (
        outer_cols(grad_query_raw, query_full)
        + outer_cols(grad_key_raw, key_full)
        + outer_cols(grad_value_low, value_full)
    )
    attention_weighted = grad_normed * attention_float
    grad_seq_part = seq_scale * attention_weighted - seq_float * seq_scale**3 * jnp.mean(
        attention_weighted * seq_float, axis=-1, keepdims=True
    )
    attention_gain_term = jnp.sum(grad_normed * seq_float * seq_scale, axis=0)
    stacked = jnp.concatenate(
        [
            grad_seq_part.reshape(rows_count, tokens, model_width),
            jnp.broadcast_to(attention_gain_term[None, None, :], (rows_count, 1, model_width)),
        ],
        axis=1,
    ).reshape(rows_count * (tokens + 1), model_width)
    summed = lax.psum_scatter(
        stacked.astype(jnp.bfloat16), "row", scatter_dimension=0, tiled=True
    ).astype(jnp.float32)
    input_grad = grad_hidden + summed[:tokens]
    attention_gain_total = summed[tokens]
    (
        grad_attention_gain,
        grad_query_gain,
        grad_key_gain,
        grad_query_weight,
        grad_key_weight,
        grad_value_weight,
        grad_output_weight,
        grad_feed_gain,
        grad_router_weight,
    ) = (
        lax.psum_scatter(
            attention_gain_total.astype(jnp.bfloat16), "col", scatter_dimension=0, tiled=True
        ).astype(jnp.float32),
        lax.psum_scatter(
            query_gain_term.astype(jnp.bfloat16), "col", scatter_dimension=0, tiled=True
        ).astype(jnp.float32),
        lax.psum_scatter(
            key_gain_term.astype(jnp.bfloat16), "col", scatter_dimension=0, tiled=True
        ).astype(jnp.float32),
        lax.psum_scatter(
            query_grad.astype(jnp.bfloat16), "col", scatter_dimension=0, tiled=True
        ).astype(jnp.float32),
        lax.psum_scatter(
            key_grad.astype(jnp.bfloat16), "col", scatter_dimension=0, tiled=True
        ).astype(jnp.float32),
        lax.psum_scatter(
            value_grad.astype(jnp.bfloat16), "col", scatter_dimension=0, tiled=True
        ).astype(jnp.float32),
        lax.psum_scatter(
            output_grad.astype(jnp.bfloat16), "col", scatter_dimension=1, tiled=True
        ).astype(jnp.float32),
        lax.psum_scatter(
            feed_gain_total.astype(jnp.bfloat16), "col", scatter_dimension=0, tiled=True
        ).astype(jnp.float32),
        lax.psum_scatter(
            router_total.astype(jnp.bfloat16), "col", scatter_dimension=0, tiled=True
        ).astype(jnp.float32),
    )
    return (
        layer_output,
        input_grad,
        grad_attention_gain,
        grad_query_gain,
        grad_key_gain,
        grad_query_weight,
        grad_key_weight,
        grad_value_weight,
        grad_output_weight,
        grad_feed_gain,
        grad_router_weight,
        grad_gate_weight,
        grad_up_weight,
        grad_down_weight,
    )


def solution(mesh):
    placed = (
        P(("col", "row"), None),
        P(("col", "row"), None),
        P(("col", "row"), None),
        P("col"),
        P(("row", "col")),
        P(("row", "col")),
        P("col", "row"),
        P("col", "row"),
        P("col", "row"),
        P("row", "col"),
        P("col"),
        P("col", None),
        P("col", None, "row"),
        P("col", None, "row"),
        P("col", "row", None),
    )
    return jax.shard_map(
        local,
        mesh=mesh,
        in_specs=placed,
        out_specs=(
            P(("col", "row"), None),
            P(("col", "row"), None),
            P("col"),
            P(("row", "col")),
            P(("row", "col")),
            P("col", "row"),
            P("col", "row"),
            P("col", "row"),
            P("row", "col"),
            P("col"),
            P("col", None),
            P("col", None, "row"),
            P("col", None, "row"),
            P("col", "row", None),
        ),
        check_vma=False,
    )
```

```python
import functools

import jax
import jax.numpy as jnp
from jax import lax
from jax.experimental import pallas as pl
from jax.experimental.pallas import tpu as pltpu
from jax.sharding import PartitionSpec as P

HD = 128
SLOTS = 40
BLOCK = 512
CHUNK = 256
UNROLL = 4


EPS = 1e-05
THETA = 10000.0
MASKED = -1e30


def wide_dot(left, right):
    return jnp.dot(left, right, preferred_element_type=jnp.float32)


def inner_rows(left, right):
    return lax.dot_general(
        left, right, (((0,), (0,)), ((), ())), preferred_element_type=jnp.float32
    )


def outer_cols(left, right):
    return lax.dot_general(
        left, right, (((1,), (1,)), ((), ())), preferred_element_type=jnp.float32
    )


def rms_scale(field):
    return lax.rsqrt(jnp.mean(field * field, axis=-1, keepdims=True) + EPS)


def rope_tables(length):
    half_size = HD // 2
    freqs = THETA ** (-(jnp.arange(half_size, dtype=jnp.float32) * 2.0) / HD)
    angles = jnp.arange(length, dtype=jnp.float32)[:, None] * freqs[None, :]
    cosine = jnp.concatenate([jnp.cos(angles), jnp.cos(angles)], axis=-1)[:, None, :]
    sine_table = jnp.concatenate([jnp.sin(angles), jnp.sin(angles)], axis=-1)[:, None, :]
    return (cosine, sine_table)


def rotate(field, cosine, sine_table):
    half_size = field.shape[-1] // 2
    turned = jnp.concatenate([-field[..., half_size:], field[..., :half_size]], axis=-1)
    return field * cosine + turned * sine_table


def unrotate(gradient, cosine, sine_table):
    half_size = gradient.shape[-1] // 2
    moved = gradient * sine_table
    back_turned = jnp.concatenate([moved[..., half_size:], -moved[..., :half_size]], axis=-1)
    return gradient * cosine + back_turned


def dispatch_body(pick_ref, field_ref, rows_ref):
    groups = rows_ref.shape[0]
    first = wide_dot(pick_ref[0], field_ref[0]).reshape(groups, SLOTS, -1)
    second = wide_dot(pick_ref[1], field_ref[1]).reshape(groups, SLOTS, -1)
    rows_ref[...] = jnp.concatenate([first, second], axis=1).astype(jnp.bfloat16)


def dispatch(pick, field):
    ranks, width, tokens = pick.shape
    groups, depth = width // SLOTS, field.shape[1]
    return pl.pallas_call(
        dispatch_body,
        grid=(ranks // 2, depth // BLOCK),
        in_specs=[
            pl.BlockSpec((2, width, tokens), lambda i, k: (i, 0, 0)),
            pl.BlockSpec((2, tokens, BLOCK), lambda i, k: (i, 0, k)),
        ],
        out_specs=pl.BlockSpec((groups, 2 * SLOTS, BLOCK), lambda i, k: (0, i, k)),
        out_shape=jax.ShapeDtypeStruct((groups, ranks * SLOTS, depth), jnp.bfloat16),
    )(pick, field.reshape(ranks, tokens, depth))


def combine_body(spread_ref, rows_ref, field_ref):
    rows = rows_ref[...].astype(jnp.float32)
    width = rows.shape[0] * SLOTS
    for side in range(2):
        part = rows[:, side * SLOTS : (side + 1) * SLOTS].reshape(width, -1).astype(jnp.bfloat16)
        field_ref[side] = wide_dot(spread_ref[side], part).astype(jnp.bfloat16)


def combine(spread, rows):
    ranks, tokens, width = spread.shape
    groups, depth = width // SLOTS, rows.shape[2]
    field = pl.pallas_call(
        combine_body,
        grid=(ranks // 2, depth // BLOCK),
        in_specs=[
            pl.BlockSpec((2, tokens, width), lambda i, k: (i, 0, 0)),
            pl.BlockSpec((groups, 2 * SLOTS, BLOCK), lambda i, k: (0, i, k)),
        ],
        out_specs=pl.BlockSpec((2, tokens, BLOCK), lambda i, k: (i, 0, k)),
        out_shape=jax.ShapeDtypeStruct((ranks, tokens, depth), jnp.bfloat16),
    )(spread, rows)
    return field.reshape(ranks * tokens, depth)


def scatter_all(field):
    part = lax.psum_scatter(field, "col", scatter_dimension=0, tiled=True)
    return lax.psum_scatter(part, "row", scatter_dimension=0, tiled=True)


def pieces_of(ranks, depth):
    count = max(1, ranks // 32)
    step = depth // count
    return [(at, at + step) for at in range(0, depth, step)]


def gather_rows(pick, field):
    rows = []
    for start, stop in pieces_of(pick.shape[0], field.shape[1]):
        part = field[:, start:stop]
        if rows:
            part = lax.optimization_barrier((part, rows[-1]))[0]
        whole = lax.all_gather(part, ("col", "row"), axis=0, tiled=True)
        rows.append(dispatch(pick, whole))
    return rows[0] if len(rows) == 1 else jnp.concatenate(rows, axis=2)


def return_rows(spread, rows):
    sums = []
    for start, stop in pieces_of(spread.shape[0], rows.shape[2]):
        part = rows[:, :, start:stop]
        if sums:
            part = lax.optimization_barrier((part, sums[-1]))[0]
        sums.append(scatter_all(combine(spread, part)))
    return sums[0] if len(sums) == 1 else jnp.concatenate(sums, axis=1)


MESH = pl.DeviceIdType.MESH


def seat():
    r, c = lax.axis_index("row"), lax.axis_index("col")
    y, x = r // 2, r % 2
    z, core = c // 2, c % 2
    first = y * (1 - core) + x * core
    second = x * (1 - core) + y * core
    return r, c, y, x, z, core, first, second


def partners():
    r, c, y, x, z, core, first, second = seat()
    pair = (r, z * 2 + (1 - core))
    flip_y = (1 - y) * 2 + x
    flip_x = y * 2 + (1 - x)
    along_first = (flip_y * (1 - core) + flip_x * core, c)
    along_second = (flip_x * (1 - core) + flip_y * core, c)
    up = [(r, ((z + k) % 4) * 2 + core) for k in range(1, 4)]
    return pair, along_first, along_second, up


RANKS = 32


def nth(offset):
    spot = (lax.axis_index("col") * 4 + lax.axis_index("row") + offset) % RANKS
    return spot, (spot % 4, spot // 4)


def meet():
    barrier = pltpu.get_barrier_semaphore()

    @pl.loop(1, RANKS)
    def _(offset):
        pl.semaphore_signal(barrier, inc=1, device_id=nth(offset)[1], device_id_type=MESH)

    pl.semaphore_wait(barrier, RANKS - 1)


def small_copy(src_of, small_all, small_send, small_recv, offset):
    spot, device = nth(offset)
    return send(
        src_of(spot), small_all.at[nth(0)[0]], small_send.at[offset], small_recv.at[offset], device
    )


def row_of(core, first, second):
    y = first * (1 - core) + second * core
    x = second * (1 - core) + first * core
    return y, x


def send(src, dst, send_sem, recv_sem, device):
    return pltpu.make_async_remote_copy(
        src_ref=src, dst_ref=dst, send_sem=send_sem, recv_sem=recv_sem, device_id=device, device_id_type=MESH
    )


GSTEPS = 4


def gather_body(own_ref, small_ref, all_ref, small_all, here_sem, small_here, small_send, small_recv, z_send, z_recv, g_send, g_recv, f_send, f_recv, p_send, p_recv):
    r, c, y, x, z, core, first, second = seat()
    pair, along_first, along_second, up = partners()
    tokens = own_ref.shape[0]
    step = tokens // GSTEPS

    def rows(q):
        return pl.ds(pl.multiple_of(q * step, step), step)

    def place(zz, f, s, q):
        yy, xx = row_of(core, f, s)
        return all_ref.at[zz, core, yy, xx, rows(q)]

    meet()
    here = pltpu.make_async_copy(own_ref, all_ref.at[z, core, y, x], here_sem)
    here.start()
    small_local = pltpu.make_async_copy(small_ref, small_all.at[nth(0)[0]], small_here)
    small_local.start()

    def small(offset):
        return small_copy(lambda spot: small_ref, small_all, small_send, small_recv, offset)

    @pl.loop(1, RANKS)
    def _(offset):
        small(offset).start()

    def z_copy(k, q):
        return send(own_ref.at[rows(q)], place(z, first, second, q), z_send.at[k - 1, q], z_recv.at[k - 1, q], up[k - 1])

    def g_copy(k, q, src):
        zz = (z + 4 - k) % 4
        return send(src, place(zz, first, second, q), g_send.at[k, q], g_recv.at[k, q], along_second)

    def f_copy(k, s, q, src):
        zz = (z + 4 - k) % 4
        sec = second * (1 - s) + (1 - second) * s
        return send(src, place(zz, first, sec, q), f_send.at[s, k, q], f_recv.at[s, k, q], along_first)

    def p_copy(k, s, f, q, src):
        zz = (z + 4 - k) % 4
        sec = second * (1 - s) + (1 - second) * s
        fir = first * (1 - f) + (1 - first) * f
        return send(src, place(zz, fir, sec, q), p_send.at[f, s, k, q], p_recv.at[f, s, k, q], pair)

    def out_of(k, s, f, q):
        zz = (z + 4 - k) % 4
        sec = second * (1 - s) + (1 - second) * s
        fir = first * (1 - f) + (1 - first) * f
        return place(zz, fir, sec, q)

    @pl.loop(0, GSTEPS)
    def _(q):
        src = own_ref.at[rows(q)]
        for k in (2, 1, 3):
            z_copy(k, q).start()
        g_copy(0, q, src).start()
        f_copy(0, 0, q, src).start()
        p_copy(0, 0, 0, q, src).start()

    @pl.loop(0, GSTEPS)
    def _(q):
        for k in (1, 3, 2):
            z_copy(k, q).wait_recv()
            src = out_of(k, 0, 0, q)
            g_copy(k, q, src).start()
            f_copy(k, 0, q, src).start()
            p_copy(k, 0, 0, q, src).start()
        for k in (0, 1, 3, 2):
            src = out_of(k, 1, 0, q)
            g_copy(k, q, src).wait_recv()
            f_copy(k, 1, q, src).start()
            p_copy(k, 1, 0, q, src).start()
        for k in (0, 1, 3, 2):
            src = out_of(k, 0, 1, q)
            f_copy(k, 0, q, src).wait_recv()
            p_copy(k, 0, 1, q, src).start()

    @pl.loop(0, GSTEPS)
    def _(q):
        for k in (0, 1, 3, 2):
            src = out_of(k, 1, 1, q)
            f_copy(k, 1, q, src).wait_recv()
            p_copy(k, 1, 1, q, src).start()

    here.wait()
    small_local.wait()

    @pl.loop(1, RANKS)
    def _(offset):
        small(offset).wait()

    @pl.loop(0, GSTEPS)
    def _(q):
        for k in range(4):
            src = own_ref.at[rows(q)]
            if k:
                z_copy(k, q).wait_send()
            g_copy(k, q, src).wait_send()
            for s in range(2):
                f_copy(k, s, q, src).wait_send()
                for f in range(2):
                    p_copy(k, s, f, q, src).wait()


def gather_near(own, small, collective_id):
    tokens, depth = own.shape
    dma = pltpu.SemaphoreType.DMA
    out, small_out = pl.pallas_call(
        gather_body,
        out_shape=(
            jax.ShapeDtypeStruct((4, 2, 2, 2, tokens, depth), own.dtype),
            jax.ShapeDtypeStruct((RANKS, *small.shape), small.dtype),
        ),
        in_specs=[pl.BlockSpec(memory_space=pl.ANY)] * 2,
        out_specs=[pl.BlockSpec(memory_space=pl.ANY)] * 2,
        scratch_shapes=[
            dma(()), dma(()), dma((RANKS,)), dma((RANKS,)),
            dma((3, GSTEPS)), dma((3, GSTEPS)),
            dma((4, GSTEPS)), dma((4, GSTEPS)),
            dma((2, 4, GSTEPS)), dma((2, 4, GSTEPS)),
            dma((2, 2, 4, GSTEPS)), dma((2, 2, 4, GSTEPS)),
        ],
        compiler_params=pltpu.CompilerParams(collective_id=collective_id, has_side_effects=True),
    )(own, small)
    return out.reshape(RANKS, tokens, depth), small_out


RSTEPS = 8
TILE = 16


def reduce_body(part_ref, small_ref, out_ref, small_all, mine, pair_in, first_in, second_in, z_in, total,
                load_sem, p_send, p_recv, f_send, f_recv, g_send, g_recv, z_send, z_recv, out_sem,
                small_here, small_send, small_recv):
    r, c, y, x, z, core, first, second = seat()
    pair, along_first, along_second, up = partners()
    tokens, depth = out_ref.shape
    step = tokens // RSTEPS
    other = 1 - core

    def rows(q):
        return pl.ds(pl.multiple_of(q * step, step), step)

    meet()

    small_local = pltpu.make_async_copy(small_ref.at[nth(0)[0]], small_all.at[nth(0)[0]], small_here)
    small_local.start()

    def small(offset):
        return small_copy(lambda spot: small_ref.at[spot], small_all, small_send, small_recv, offset)

    @pl.loop(1, RANKS)
    def _(offset):
        small(offset).start()

    def load(f, s, q):
        yy, xx = row_of(core, f, s)
        return pltpu.make_async_copy(part_ref.at[:, core, yy, xx, rows(q)], mine.at[f, s, :, rows(q)], load_sem.at[f, s, q])

    def give(f, s, q):
        yy, xx = row_of(other, f, s)
        return send(part_ref.at[:, other, yy, xx, rows(q)], pair_in.at[f, s, :, rows(q)],
                    p_send.at[f, s, q], p_recv.at[f, s, q], pair)

    def f_copy(s, q):
        return send(mine.at[1 - first, s, :, rows(q)], first_in.at[s, :, rows(q)], f_send.at[s, q], f_recv.at[s, q], along_first)

    def g_copy(q):
        return send(mine.at[first, 1 - second, :, rows(q)], second_in.at[:, rows(q)], g_send.at[q], g_recv.at[q], along_second)

    def z_copy(k, q):
        return send(mine.at[first, second, (z + k) % 4, rows(q)], z_in.at[k - 1, rows(q)],
                    z_send.at[k - 1, q], z_recv.at[k - 1, q], up[k - 1])

    def order(me_first, me_second):
        return [(1 - me_first, 1 - me_second), (1 - me_first, me_second), (me_first, 1 - me_second), (me_first, me_second)]

    @pl.loop(0, RSTEPS)
    def _(q):
        for f, s in order(second, first):
            give(f, s, q).start()
        for f, s in order(first, second):
            load(f, s, q).start()

    def add_into(f, s, q, extra):
        @pl.loop(0, 4 * (step // TILE))
        def _(t):
            zz, at = t // (step // TILE), t % (step // TILE)
            here = pl.ds(pl.multiple_of(q * step + at * TILE, TILE), TILE)
            value = mine[f, s, zz, here].astype(jnp.float32) + pair_in[f, s, zz, here].astype(jnp.float32)
            for ref in extra:
                value = value + ref[zz, here].astype(jnp.float32)
            mine[f, s, zz, here] = value.astype(jnp.bfloat16)

    def stage_first(q):
        for s in (1 - second, second):
            load(1 - first, s, q).wait()
            give(1 - first, s, q).wait_recv()
            add_into(1 - first, s, q, [])
            f_copy(s, q).start()

    def stage_second(q):
        load(first, 1 - second, q).wait()
        give(first, 1 - second, q).wait_recv()
        f_copy(1 - second, q).wait_recv()
        add_into(first, 1 - second, q, [first_in.at[1 - second]])
        g_copy(q).start()

    def stage_z(q):
        load(first, second, q).wait()
        give(first, second, q).wait_recv()
        f_copy(second, q).wait_recv()
        g_copy(q).wait_recv()
        add_into(first, second, q, [first_in.at[second], second_in])
        for k in (2, 1, 3):
            z_copy(k, q).start()

    def stage_out(q):
        for k in (1, 3, 2):
            z_copy(k, q).wait_recv()

        @pl.loop(0, step // TILE)
        def _(t):
            here = pl.ds(pl.multiple_of(q * step + t * TILE, TILE), TILE)
            value = mine[first, second, z, here].astype(jnp.float32)
            for k in range(3):
                value = value + z_in[k, here].astype(jnp.float32)
            total[here] = value

    LAG1, LAG2, LAG3 = 1, 2, 4

    @pl.loop(0, RSTEPS + LAG3)
    def _(q):
        @pl.when(q < RSTEPS)
        def _():
            stage_first(q)

        @pl.when((q >= LAG1) & (q < RSTEPS + LAG1))
        def _():
            stage_second(q - LAG1)

        @pl.when((q >= LAG2) & (q < RSTEPS + LAG2))
        def _():
            stage_z(q - LAG2)

        @pl.when(q >= LAG3)
        def _():
            stage_out(q - LAG3)

    done = pltpu.make_async_copy(total, out_ref, out_sem)
    done.start()

    @pl.loop(0, RSTEPS)
    def _(q):
        for f in range(2):
            for s in range(2):
                give(f, s, q).wait_send()
        for s in range(2):
            f_copy(s, q).wait_send()
        g_copy(q).wait_send()
        for k in (1, 2, 3):
            z_copy(k, q).wait_send()

    small_local.wait()

    @pl.loop(1, RANKS)
    def _(offset):
        small(offset).wait()

    done.wait()


def reduce_near(part, small, collective_id):
    tokens, depth = part.shape[0] // RANKS, part.shape[1]
    dma = pltpu.SemaphoreType.DMA
    return pl.pallas_call(
        reduce_body,
        out_shape=(
            jax.ShapeDtypeStruct((tokens, depth), jnp.float32),
            jax.ShapeDtypeStruct(small.shape, small.dtype),
        ),
        in_specs=[pl.BlockSpec(memory_space=pl.ANY)] * 2,
        out_specs=[pl.BlockSpec(memory_space=pl.ANY)] * 2,
        scratch_shapes=[
            pltpu.VMEM((2, 2, 4, tokens, depth), jnp.bfloat16),
            pltpu.VMEM((2, 2, 4, tokens, depth), jnp.bfloat16),
            pltpu.VMEM((2, 4, tokens, depth), jnp.bfloat16),
            pltpu.VMEM((4, tokens, depth), jnp.bfloat16),
            pltpu.VMEM((3, tokens, depth), jnp.bfloat16),
            pltpu.VMEM((tokens, depth), jnp.float32),
            dma((2, 2, RSTEPS)),
            dma((2, 2, RSTEPS)), dma((2, 2, RSTEPS)),
            dma((2, RSTEPS)), dma((2, RSTEPS)),
            dma((RSTEPS,)), dma((RSTEPS,)),
            dma((3, RSTEPS)), dma((3, RSTEPS)),
            dma(()),
            dma(()), dma((RANKS,)), dma((RANKS,)),
        ],
        compiler_params=pltpu.CompilerParams(
            collective_id=collective_id, has_side_effects=True, vmem_limit_bytes=60 * 1024 * 1024
        ),
    )(part.reshape(4, 2, 2, 2, tokens, depth), small)


def project_body(flipped, pick_ref, field_ref, *refs):
    count = len(flipped)
    weights, (rows_ref, *outs), sums = refs[:count], refs[count:2*count+1], refs[2*count+1:]
    k = pl.program_id(0)
    ranks = pick_ref.shape[0]
    groups = rows_ref.shape[0]

    @pl.loop(0, ranks // 2, unroll=UNROLL)
    def _(i):
        parts = [
            wide_dot(pick_ref[2 * i + side], field_ref[2 * i + side]).reshape(groups, SLOTS, CHUNK)
            for side in range(2)
        ]
        rows_ref[:, pl.ds(pl.multiple_of(i * 2 * SLOTS, 2 * SLOTS), 2 * SLOTS)] = jnp.concatenate(parts, axis=1).astype(jnp.bfloat16)

    def project(e, first):
        rows = rows_ref[e]
        for weight, flip, total in zip(weights, flipped, sums):
            term = outer_cols(rows, weight[e]) if flip else wide_dot(rows, weight[e])
            if first: total[e] = term
            else: total[e] += term

    @pl.when(k == 0)
    def _():
        @pl.loop(0, groups)
        def _(e):
            project(e, True)

    @pl.when(k > 0)
    def _():
        @pl.loop(0, groups)
        def _(e):
            project(e, False)

    @pl.when(k == pl.num_programs(0) - 1)
    def _():
        for out, total in zip(outs, sums):
            pltpu.sync_copy(total, out)

def project(pick, field, weights, flipped):
    ranks, width, tokens = pick.shape
    groups, depth = width // SLOTS, field.shape[-1]
    length = ranks * SLOTS
    inner = weights[0].shape[1] if flipped[0] else weights[0].shape[2]
    wspecs = [pl.BlockSpec((groups, inner, CHUNK), lambda k: (0, 0, k)) if f else pl.BlockSpec((groups, CHUNK, inner), lambda k: (0, k, 0)) for f in flipped]
    flops = 2 * groups * length * depth * (tokens + inner * len(weights))
    return pl.pallas_call(
        functools.partial(project_body, flipped),
        grid=(depth // CHUNK,),
        in_specs=[
            pl.BlockSpec((ranks, width, tokens), lambda k: (0, 0, 0), pipeline_mode=pl.Buffered(1)),
            pl.BlockSpec((ranks, tokens, CHUNK), lambda k: (0, 0, k)),
            *wspecs,
        ],
        out_specs=[pl.BlockSpec((groups, length, CHUNK), lambda k: (0, 0, k))] + [pl.BlockSpec(memory_space=pl.ANY)] * len(weights),
        out_shape=[jax.ShapeDtypeStruct((groups, length, depth), jnp.bfloat16)]
        + [jax.ShapeDtypeStruct((groups, length, inner), jnp.float32)] * len(weights),
        scratch_shapes=[pltpu.VMEM((groups, length, inner), jnp.float32)] * len(weights),
        compiler_params=pltpu.CompilerParams(vmem_limit_bytes=63 * 1024 * 1024),
        cost_estimate=pl.CostEstimate(flops=flops, bytes_accessed=120 << 20, transcendentals=0),
    )(pick, field.reshape(ranks, tokens, depth), *weights)


def restore_body(flipped, spread_ref, *refs):
    count = len(flipped)
    lefts, weights, field_ref, rows = refs[:count], refs[count:2*count], refs[2*count], refs[2*count+1]
    groups = rows.shape[0]
    ranks = spread_ref.shape[0]

    @pl.loop(0, groups)
    def _(e):
        total = None
        for left, weight, flip in zip(lefts, weights, flipped):
            term = outer_cols(left[e], weight[e]) if flip else wide_dot(left[e], weight[e])
            total = term if total is None else total + term
        rows[e] = total

    @pl.loop(0, ranks, unroll=2*UNROLL)
    def _(s):
        part = rows[:, pl.ds(pl.multiple_of(s * SLOTS, SLOTS), SLOTS)].reshape(groups * SLOTS, CHUNK).astype(jnp.bfloat16)
        field_ref[s] = wide_dot(spread_ref[s], part).astype(jnp.bfloat16)

def restore(spread, lefts, weights, flipped):
    ranks, tokens, width = spread.shape
    groups = width // SLOTS
    length = ranks * SLOTS
    inner = lefts[0].shape[2]
    depth = weights[0].shape[1] if flipped[0] else weights[0].shape[2]
    wspecs = [pl.BlockSpec((groups, CHUNK, inner), lambda k: (0, k, 0)) if f else pl.BlockSpec((groups, inner, CHUNK), lambda k: (0, 0, k)) for f in flipped]
    flops = 2 * groups * length * depth * (tokens + inner * len(weights))
    field = pl.pallas_call(
        functools.partial(restore_body, flipped),
        grid=(depth // CHUNK,),
        in_specs=[pl.BlockSpec((ranks, tokens, width), lambda k: (0, 0, 0), pipeline_mode=pl.Buffered(1))]
        + [pl.BlockSpec((groups, length, inner), lambda k: (0, 0, 0), pipeline_mode=pl.Buffered(1))] * len(lefts) + wspecs,
        out_specs=pl.BlockSpec((ranks, tokens, CHUNK), lambda k: (0, 0, k)),
        out_shape=jax.ShapeDtypeStruct((ranks, tokens, depth), jnp.bfloat16),
        scratch_shapes=[pltpu.VMEM((groups, length, CHUNK), jnp.float32)],
        compiler_params=pltpu.CompilerParams(vmem_limit_bytes=63 * 1024 * 1024),
        cost_estimate=pl.CostEstimate(flops=flops, bytes_accessed=60 << 20, transcendentals=0),
    )(spread, *lefts, *weights)
    return field.reshape(ranks * tokens, depth)


def local(
    layer_input,
    cotangent,
    expert_index,
    attention_gain,
    query_gain,
    key_gain,
    query_weight,
    key_weight,
    value_weight,
    output_weight,
    feed_gain,
    router_weight,
    gate_weight,
    up_weight,
    down_weight,
):
    tokens = layer_input.shape[0]
    rows_count = lax.axis_size("row")
    (
        attention_full,
        query_scale_w,
        key_scale_w,
        query_full,
        key_full,
        value_full,
        output_full,
        feed_full,
        router_full,
    ) = (
        lax.all_gather(attention_gain, "col", axis=0, tiled=True),
        lax.all_gather(query_gain, "col", axis=0, tiled=True),
        lax.all_gather(key_gain, "col", axis=0, tiled=True),
        lax.all_gather(query_weight, "col", axis=0, tiled=True),
        lax.all_gather(key_weight, "col", axis=0, tiled=True),
        lax.all_gather(value_weight, "col", axis=0, tiled=True),
        lax.all_gather(output_weight, "col", axis=1, tiled=True),
        lax.all_gather(feed_gain, "col", axis=0, tiled=True),
        lax.all_gather(router_weight, "col", axis=0, tiled=True),
    )
    sequence = lax.all_gather(layer_input, "row", axis=0, tiled=True)
    length = sequence.shape[0]
    model_width = sequence.shape[1]
    local_width = query_full.shape[1]
    local_heads = local_width // HD
    seq_float = sequence.astype(jnp.float32)
    seq_scale = rms_scale(seq_float)
    attention_float = attention_full.astype(jnp.float32)
    normed = (seq_float * seq_scale * attention_float).astype(jnp.bfloat16)
    query_raw = wide_dot(normed, query_full)
    key_raw = wide_dot(normed, key_full)
    value_heads = wide_dot(normed, value_full).astype(jnp.bfloat16).reshape(length, local_heads, HD)
    query_total, key_total = lax.psum(
        (jnp.sum(query_raw * query_raw, axis=-1), jnp.sum(key_raw * key_raw, axis=-1)), "row"
    )
    query_rs = lax.rsqrt(query_total / model_width + EPS)[:, None]
    key_rs = lax.rsqrt(key_total / model_width + EPS)[:, None]
    query_gain_f = query_scale_w.astype(jnp.float32)
    key_gain_f = key_scale_w.astype(jnp.float32)
    cosine, sine_table = rope_tables(length)
    queries = rotate(
        (query_raw * query_rs * query_gain_f).reshape(length, local_heads, HD), cosine, sine_table
    ).astype(jnp.bfloat16)
    keys_rotated = rotate(
        (key_raw * key_rs * key_gain_f).reshape(length, local_heads, HD), cosine, sine_table
    ).astype(jnp.bfloat16)
    block_rows = min(512, length)
    starts = jnp.arange(length // block_rows, dtype=jnp.int32) * block_rows
    key_position = jnp.arange(length, dtype=jnp.int32)
    score_scale = HD ** (-0.5)

    def block_scores(offset):
        query_rows = lax.dynamic_slice_in_dim(queries, offset, block_rows, 0)
        scores = (
            jnp.einsum("qhd,khd->hqk", query_rows, keys_rotated, preferred_element_type=jnp.float32)
            * score_scale
        )
        query_position = offset + jnp.arange(block_rows, dtype=jnp.int32)
        allowed = query_position[:, None] >= key_position[None, :]
        return (query_rows, jnp.where(allowed[None, :, :], scores, MASKED))

    def forward_block(offset):
        query_rows, scores = block_scores(offset)
        row_top = jnp.max(scores, axis=-1, keepdims=True)
        exponent = jnp.exp(scores - row_top)
        row_total = jnp.sum(exponent, axis=-1, keepdims=True)
        weights = (exponent / row_total).astype(jnp.bfloat16)
        mixed_block = jnp.einsum(
            "hqk,khd->qhd", weights, value_heads, preferred_element_type=jnp.float32
        )
        return (mixed_block, (row_top + jnp.log(row_total))[..., 0])

    mixed_blocks, lse_blocks = lax.map(forward_block, starts)
    mixed_heads = mixed_blocks.reshape(length, local_width).astype(jnp.bfloat16)
    lse_all = jnp.moveaxis(lse_blocks, 0, 1).reshape(local_heads, length)
    branch = lax.psum_scatter(
        wide_dot(mixed_heads, output_full).astype(jnp.bfloat16), "row", scatter_dimension=0, tiled=True
    ).astype(jnp.float32)
    hidden = layer_input.astype(jnp.float32) + branch
    feed_scale = rms_scale(hidden)
    feed_float = feed_full.astype(jnp.float32)
    feed_normed = (hidden * feed_scale * feed_float).astype(jnp.bfloat16)
    logits = wide_dot(feed_normed, router_full)
    logit_top = jnp.max(logits, axis=-1, keepdims=True)
    logit_exp = jnp.exp(logits - logit_top)
    router_probs = logit_exp / jnp.sum(logit_exp, axis=-1, keepdims=True)
    experts = router_full.shape[1]
    experts_local = gate_weight.shape[0]
    ranks = lax.axis_size("col") * rows_count
    gate_hits = expert_index[:, :, None] == jnp.arange(experts, dtype=jnp.int32)
    gate_probs = jnp.sum(jnp.where(gate_hits, router_probs[:, None, :], 0.0), axis=-1)

    near = rows_count == 4 and lax.axis_size("col") == 8
    if near:
        cotangent_all, index_all = gather_near(cotangent, expert_index.T, 1)
        index_all = jnp.swapaxes(index_all, 1, 2)
    else:
        index_all = lax.all_gather(expert_index, ("col", "row"), axis=0, tiled=True)
    own = (index_all - lax.axis_index("col") * experts_local).reshape(ranks, tokens, -1)
    matches = own[..., None] == jnp.arange(experts_local, dtype=jnp.int32)
    hit = jnp.sum(matches.astype(jnp.float32), axis=2)
    earlier = jnp.tril(jnp.ones((tokens, tokens), jnp.bfloat16), -1)
    rank = jnp.einsum(
        "tu,sue->ste", earlier, hit.astype(jnp.bfloat16), preferred_element_type=jnp.float32
    )
    slot = jnp.where(hit > 0, rank, -1.0)
    places = jnp.arange(SLOTS, dtype=jnp.float32)
    slot_t = jnp.swapaxes(slot, 1, 2)
    width = experts_local * SLOTS
    pick = (slot_t[:, :, None, :] == places[None, None, :, None]).astype(jnp.bfloat16)
    pick = pick.reshape(ranks, width, tokens)
    spread = slot[:, :, :, None] == places
    spread_plain = spread.astype(jnp.bfloat16).reshape(ranks, tokens, width)
    if near:
        expert_grads, plain_act = project(pick, cotangent_all, [down_weight], (True,))
        feed_all, probs_all = gather_near(feed_normed, gate_probs.T, 2)
        probs_all = jnp.swapaxes(probs_all, 1, 2)
        expert_rows, gate_val, up_val = project(
            pick, feed_all, [gate_weight, up_weight], (False, False)
        )
    else:
        probs_all = lax.all_gather(gate_probs, ("col", "row"), axis=0, tiled=True)
        expert_grads = gather_rows(pick, cotangent)
        expert_rows = gather_rows(pick, feed_normed)
        gate_val = jnp.einsum(
            "erd,edf->erf", expert_rows, gate_weight, preferred_element_type=jnp.float32
        )
        up_val = jnp.einsum(
            "erd,edf->erf", expert_rows, up_weight, preferred_element_type=jnp.float32
        )
        plain_act = jnp.einsum(
            "erd,efd->erf", expert_grads, down_weight, preferred_element_type=jnp.float32
        )
    probs_own = jnp.sum(
        jnp.where(matches, probs_all.reshape(ranks, tokens, -1, 1), 0.0), axis=2
    )
    weighted = jnp.where(spread, probs_own[..., None], 0.0)
    spread_probs = weighted.astype(jnp.bfloat16).reshape(ranks, tokens, width)
    row_probs = jnp.sum(weighted, axis=1)
    row_probs = jnp.swapaxes(row_probs, 0, 1).reshape(experts_local, ranks * SLOTS, 1)
    sigmoid_val = jax.nn.sigmoid(gate_val)
    silu_val = gate_val * sigmoid_val
    activated = silu_val * up_val
    grad_act = plain_act * row_probs
    grad_up = (grad_act * silu_val).astype(jnp.bfloat16)
    grad_gate = (
        grad_act * up_val * sigmoid_val * (1.0 + gate_val * (1.0 - sigmoid_val))
    ).astype(jnp.bfloat16)
    row_gates = jnp.sum(activated * plain_act, axis=-1).reshape(experts_local, ranks, 1, SLOTS)
    weighted_act = (activated * row_probs).astype(jnp.bfloat16)
    activated = activated.astype(jnp.bfloat16)
    own_gates = jnp.sum(jnp.where(spread, jnp.transpose(row_gates, (1, 2, 0, 3)), 0.0), axis=-1)
    if near:
        own_gates = jnp.swapaxes(own_gates, 1, 2)
        grad_feed_part = restore(
            spread_plain, [grad_gate, grad_up], [gate_weight, up_weight], (True, True)
        )
        grad_feed, gates_in = reduce_near(grad_feed_part, own_gates, 3)
        gates_in = jnp.sum(gates_in.reshape(-1, rows_count, experts_local, tokens), axis=1)
        grad_probs = gates_in.reshape(experts, tokens).T
        mixture_part = restore(spread_probs, [activated], [down_weight], (False,))
        mixture = reduce_near(mixture_part, own_gates, 3)[0]
    else:
        own_gates = lax.psum_scatter(
            own_gates.reshape(-1, rows_count, tokens, experts_local), "row", scatter_dimension=1
        )
        grad_probs = lax.all_to_all(own_gates, "col", split_axis=0, concat_axis=2, tiled=True)[0]
        back_rows = (
            jnp.einsum("erf,edf->erd", grad_gate, gate_weight, preferred_element_type=jnp.float32)
            + jnp.einsum("erf,edf->erd", grad_up, up_weight, preferred_element_type=jnp.float32)
        ).astype(jnp.bfloat16)
        grad_feed = return_rows(spread_plain, back_rows).astype(jnp.float32)
        out_rows = jnp.einsum(
            "erf,efd->erd", activated, down_weight, preferred_element_type=jnp.float32
        ).astype(jnp.bfloat16)
        mixture = return_rows(spread_probs, out_rows).astype(jnp.float32)
    layer_output = hidden + mixture
    grad_gate_weight = jnp.einsum(
        "erd,erf->edf", expert_rows, grad_gate, preferred_element_type=jnp.float32
    )
    grad_up_weight = jnp.einsum(
        "erd,erf->edf", expert_rows, grad_up, preferred_element_type=jnp.float32
    )
    grad_down_weight = jnp.einsum(
        "erf,erd->efd", weighted_act, expert_grads, preferred_element_type=jnp.float32
    )
    grad_out = cotangent.astype(jnp.float32)
    grad_logits = (
        router_probs * (grad_probs - jnp.sum(router_probs * grad_probs, axis=-1, keepdims=True))
    ).astype(jnp.bfloat16)
    router_grad = inner_rows(feed_normed, grad_logits)
    grad_feed = grad_feed + outer_cols(grad_logits, router_full)
    feed_gain_term = jnp.sum(grad_feed * hidden * feed_scale, axis=0)
    feed_weighted = grad_feed * feed_float
    grad_hidden = (
        grad_out
        + feed_scale * feed_weighted
        - hidden * feed_scale**3 * jnp.mean(feed_weighted * hidden, axis=-1, keepdims=True)
    )
    grad_branch = lax.all_gather(grad_hidden.astype(jnp.bfloat16), "row", axis=0, tiled=True)
    output_grad = inner_rows(mixed_heads, grad_branch)
    grad_mixed = (
        outer_cols(grad_branch, output_full).astype(jnp.bfloat16).reshape(length, local_heads, HD)
    )

    def backward_block(carry, offset):
        grad_keys, grad_values = carry
        query_rows, scores = block_scores(offset)
        lse_rows = lax.dynamic_slice_in_dim(lse_all, offset, block_rows, 1)
        probs_block = jnp.exp(scores - lse_rows[:, :, None])
        weights_low = probs_block.astype(jnp.bfloat16)
        grad_rows_out = lax.dynamic_slice_in_dim(grad_mixed, offset, block_rows, 0)
        grad_weights = jnp.einsum(
            "qhd,khd->hqk", grad_rows_out, value_heads, preferred_element_type=jnp.float32
        )
        grad_values = grad_values + jnp.einsum(
            "hqk,qhd->khd", weights_low, grad_rows_out, preferred_element_type=jnp.float32
        )
        delta_rows = jnp.sum(probs_block * grad_weights, axis=-1, keepdims=True)
        grad_scores = (probs_block * (grad_weights - delta_rows)).astype(jnp.bfloat16)
        grad_query_block = (
            jnp.einsum(
                "hqk,khd->qhd", grad_scores, keys_rotated, preferred_element_type=jnp.float32
            )
            * score_scale
        )
        grad_keys = (
            grad_keys
            + jnp.einsum(
                "hqk,qhd->khd", grad_scores, query_rows, preferred_element_type=jnp.float32
            )
            * score_scale
        )
        return ((grad_keys, grad_values), grad_query_block)

    zero_heads = jnp.zeros((length, local_heads, HD), jnp.float32)
    (grad_keys, grad_values), grad_query_blocks = lax.scan(
        backward_block, (zero_heads, zero_heads), starts
    )
    grad_queries = grad_query_blocks.reshape(length, local_heads, HD)
    grad_query_normed = unrotate(grad_queries, cosine, sine_table).reshape(length, local_width)
    grad_key_normed = unrotate(grad_keys, cosine, sine_table).reshape(length, local_width)
    grad_value_low = grad_values.reshape(length, local_width).astype(jnp.bfloat16)
    query_weighted = grad_query_normed * query_gain_f
    key_weighted = grad_key_normed * key_gain_f
    query_gain_term = jnp.sum(grad_query_normed * query_raw * query_rs, axis=0)
    key_gain_term = jnp.sum(grad_key_normed * key_raw * key_rs, axis=0)
    query_inner, key_inner, feed_gain_total, router_total = (
        lax.psum(jnp.sum(query_weighted * query_raw, axis=-1).astype(jnp.bfloat16), "row").astype(
            jnp.float32
        ),
        lax.psum(jnp.sum(key_weighted * key_raw, axis=-1).astype(jnp.bfloat16), "row").astype(
            jnp.float32
        ),
        lax.psum(feed_gain_term.astype(jnp.bfloat16), "row").astype(jnp.float32),
        lax.psum(router_grad.astype(jnp.bfloat16), "row").astype(jnp.float32),
    )
    grad_query_raw = (
        query_rs * query_weighted - query_raw * query_rs**3 * (query_inner / model_width)[:, None]
    ).astype(jnp.bfloat16)
    grad_key_raw = (
        key_rs * key_weighted - key_raw * key_rs**3 * (key_inner / model_width)[:, None]
    ).astype(jnp.bfloat16)
    query_grad = inner_rows(normed, grad_query_raw)
    key_grad = inner_rows(normed, grad_key_raw)
    value_grad = inner_rows(normed, grad_value_low)
    grad_normed = (
        outer_cols(grad_query_raw, query_full)
        + outer_cols(grad_key_raw, key_full)
        + outer_cols(grad_value_low, value_full)
    )
    attention_weighted = grad_normed * attention_float
    grad_seq_part = seq_scale * attention_weighted - seq_float * seq_scale**3 * jnp.mean(
        attention_weighted * seq_float, axis=-1, keepdims=True
    )
    attention_gain_term = jnp.sum(grad_normed * seq_float * seq_scale, axis=0)
    stacked = jnp.concatenate(
        [
            grad_seq_part.reshape(rows_count, tokens, model_width),
            jnp.broadcast_to(attention_gain_term[None, None, :], (rows_count, 1, model_width)),
        ],
        axis=1,
    ).reshape(rows_count * (tokens + 1), model_width)
    summed = lax.psum_scatter(
        stacked.astype(jnp.bfloat16), "row", scatter_dimension=0, tiled=True
    ).astype(jnp.float32)
    input_grad = grad_hidden + summed[:tokens]
    attention_gain_total = summed[tokens]
    (
        grad_attention_gain,
        grad_query_gain,
        grad_key_gain,
        grad_query_weight,
        grad_key_weight,
        grad_value_weight,
        grad_output_weight,
        grad_feed_gain,
        grad_router_weight,
    ) = (
        lax.psum_scatter(
            attention_gain_total.astype(jnp.bfloat16), "col", scatter_dimension=0, tiled=True
        ).astype(jnp.float32),
        lax.psum_scatter(
            query_gain_term.astype(jnp.bfloat16), "col", scatter_dimension=0, tiled=True
        ).astype(jnp.float32),
        lax.psum_scatter(
            key_gain_term.astype(jnp.bfloat16), "col", scatter_dimension=0, tiled=True
        ).astype(jnp.float32),
        lax.psum_scatter(
            query_grad.astype(jnp.bfloat16), "col", scatter_dimension=0, tiled=True
        ).astype(jnp.float32),
        lax.psum_scatter(
            key_grad.astype(jnp.bfloat16), "col", scatter_dimension=0, tiled=True
        ).astype(jnp.float32),
        lax.psum_scatter(
            value_grad.astype(jnp.bfloat16), "col", scatter_dimension=0, tiled=True
        ).astype(jnp.float32),
        lax.psum_scatter(
            output_grad.astype(jnp.bfloat16), "col", scatter_dimension=1, tiled=True
        ).astype(jnp.float32),
        lax.psum_scatter(
            feed_gain_total.astype(jnp.bfloat16), "col", scatter_dimension=0, tiled=True
        ).astype(jnp.float32),
        lax.psum_scatter(
            router_total.astype(jnp.bfloat16), "col", scatter_dimension=0, tiled=True
        ).astype(jnp.float32),
    )
    return (
        layer_output,
        input_grad,
        grad_attention_gain,
        grad_query_gain,
        grad_key_gain,
        grad_query_weight,
        grad_key_weight,
        grad_value_weight,
        grad_output_weight,
        grad_feed_gain,
        grad_router_weight,
        grad_gate_weight,
        grad_up_weight,
        grad_down_weight,
    )


def solution(mesh):
    placed = (
        P(("col", "row"), None),
        P(("col", "row"), None),
        P(("col", "row"), None),
        P("col"),
        P(("row", "col")),
        P(("row", "col")),
        P("col", "row"),
        P("col", "row"),
        P("col", "row"),
        P("row", "col"),
        P("col"),
        P("col", None),
        P("col", None, "row"),
        P("col", None, "row"),
        P("col", "row", None),
    )
    return jax.shard_map(
        local,
        mesh=mesh,
        in_specs=placed,
        out_specs=(
            P(("col", "row"), None),
            P(("col", "row"), None),
            P("col"),
            P(("row", "col")),
            P(("row", "col")),
            P("col", "row"),
            P("col", "row"),
            P("col", "row"),
            P("row", "col"),
            P("col"),
            P("col", None),
            P("col", None, "row"),
            P("col", None, "row"),
            P("col", "row", None),
        ),
        check_vma=False,
    )
```

```python
import functools

import jax
import jax.numpy as jnp
from jax import lax
from jax.experimental import pallas as pl
from jax.experimental.pallas import tpu as pltpu
from jax.sharding import PartitionSpec as P

HD = 128
SLOTS = 40
BLOCK = 512
CHUNK = 256
UNROLL = 4
PACK_ROWS = 144


EPS = 1e-05
THETA = 10000.0
MASKED = -1e30


def wide_dot(left, right):
    return jnp.dot(left, right, preferred_element_type=jnp.float32)


def inner_rows(left, right):
    return lax.dot_general(
        left, right, (((0,), (0,)), ((), ())), preferred_element_type=jnp.float32
    )


def outer_cols(left, right):
    return lax.dot_general(
        left, right, (((1,), (1,)), ((), ())), preferred_element_type=jnp.float32
    )


def rms_scale(field):
    return lax.rsqrt(jnp.mean(field * field, axis=-1, keepdims=True) + EPS)


def rope_tables(length):
    half_size = HD // 2
    freqs = THETA ** (-(jnp.arange(half_size, dtype=jnp.float32) * 2.0) / HD)
    angles = jnp.arange(length, dtype=jnp.float32)[:, None] * freqs[None, :]
    cosine = jnp.concatenate([jnp.cos(angles), jnp.cos(angles)], axis=-1)[:, None, :]
    sine_table = jnp.concatenate([jnp.sin(angles), jnp.sin(angles)], axis=-1)[:, None, :]
    return (cosine, sine_table)


def rotate(field, cosine, sine_table):
    half_size = field.shape[-1] // 2
    turned = jnp.concatenate([-field[..., half_size:], field[..., :half_size]], axis=-1)
    return field * cosine + turned * sine_table


def unrotate(gradient, cosine, sine_table):
    half_size = gradient.shape[-1] // 2
    moved = gradient * sine_table
    back_turned = jnp.concatenate([moved[..., half_size:], -moved[..., :half_size]], axis=-1)
    return gradient * cosine + back_turned


def dispatch_body(pick_ref, field_ref, rows_ref):
    groups = rows_ref.shape[0]
    first = wide_dot(pick_ref[0], field_ref[0]).reshape(groups, SLOTS, -1)
    second = wide_dot(pick_ref[1], field_ref[1]).reshape(groups, SLOTS, -1)
    rows_ref[...] = jnp.concatenate([first, second], axis=1).astype(jnp.bfloat16)


def dispatch(pick, field):
    ranks, width, tokens = pick.shape
    groups, depth = width // SLOTS, field.shape[1]
    return pl.pallas_call(
        dispatch_body,
        grid=(ranks // 2, depth // BLOCK),
        in_specs=[
            pl.BlockSpec((2, width, tokens), lambda i, k: (i, 0, 0)),
            pl.BlockSpec((2, tokens, BLOCK), lambda i, k: (i, 0, k)),
        ],
        out_specs=pl.BlockSpec((groups, 2 * SLOTS, BLOCK), lambda i, k: (0, i, k)),
        out_shape=jax.ShapeDtypeStruct((groups, ranks * SLOTS, depth), jnp.bfloat16),
    )(pick, field.reshape(ranks, tokens, depth))


def combine_body(spread_ref, rows_ref, field_ref):
    rows = rows_ref[...].astype(jnp.float32)
    width = rows.shape[0] * SLOTS
    for side in range(2):
        part = rows[:, side * SLOTS : (side + 1) * SLOTS].reshape(width, -1).astype(jnp.bfloat16)
        field_ref[side] = wide_dot(spread_ref[side], part).astype(jnp.bfloat16)


def combine(spread, rows):
    ranks, tokens, width = spread.shape
    groups, depth = width // SLOTS, rows.shape[2]
    field = pl.pallas_call(
        combine_body,
        grid=(ranks // 2, depth // BLOCK),
        in_specs=[
            pl.BlockSpec((2, tokens, width), lambda i, k: (i, 0, 0)),
            pl.BlockSpec((groups, 2 * SLOTS, BLOCK), lambda i, k: (0, i, k)),
        ],
        out_specs=pl.BlockSpec((2, tokens, BLOCK), lambda i, k: (i, 0, k)),
        out_shape=jax.ShapeDtypeStruct((ranks, tokens, depth), jnp.bfloat16),
    )(spread, rows)
    return field.reshape(ranks * tokens, depth)


def scatter_all(field):
    part = lax.psum_scatter(field, "col", scatter_dimension=0, tiled=True)
    return lax.psum_scatter(part, "row", scatter_dimension=0, tiled=True)


def pieces_of(ranks, depth):
    count = max(1, ranks // 32)
    step = depth // count
    return [(at, at + step) for at in range(0, depth, step)]


def gather_rows(pick, field):
    rows = []
    for start, stop in pieces_of(pick.shape[0], field.shape[1]):
        part = field[:, start:stop]
        if rows:
            part = lax.optimization_barrier((part, rows[-1]))[0]
        whole = lax.all_gather(part, ("col", "row"), axis=0, tiled=True)
        rows.append(dispatch(pick, whole))
    return rows[0] if len(rows) == 1 else jnp.concatenate(rows, axis=2)


def return_rows(spread, rows):
    sums = []
    for start, stop in pieces_of(spread.shape[0], rows.shape[2]):
        part = rows[:, :, start:stop]
        if sums:
            part = lax.optimization_barrier((part, sums[-1]))[0]
        sums.append(scatter_all(combine(spread, part)))
    return sums[0] if len(sums) == 1 else jnp.concatenate(sums, axis=1)


MESH = pl.DeviceIdType.MESH


def seat():
    r, c = lax.axis_index("row"), lax.axis_index("col")
    y, x = r // 2, r % 2
    z, core = c // 2, c % 2
    first = y * (1 - core) + x * core
    second = x * (1 - core) + y * core
    return r, c, y, x, z, core, first, second


def partners():
    r, c, y, x, z, core, first, second = seat()
    pair = (r, z * 2 + (1 - core))
    flip_y = (1 - y) * 2 + x
    flip_x = y * 2 + (1 - x)
    along_first = (flip_y * (1 - core) + flip_x * core, c)
    along_second = (flip_x * (1 - core) + flip_y * core, c)
    up = [(r, ((z + k) % 4) * 2 + core) for k in range(1, 4)]
    return pair, along_first, along_second, up


RANKS = 32


def nth(offset):
    spot = (lax.axis_index("col") * 4 + lax.axis_index("row") + offset) % RANKS
    return spot, (spot % 4, spot // 4)


def meet():
    barrier = pltpu.get_barrier_semaphore()

    @pl.loop(1, RANKS)
    def _(offset):
        pl.semaphore_signal(barrier, inc=1, device_id=nth(offset)[1], device_id_type=MESH)

    pl.semaphore_wait(barrier, RANKS - 1)


def small_copy(src_of, small_all, small_send, small_recv, offset):
    spot, device = nth(offset)
    return send(
        src_of(spot), small_all.at[nth(0)[0]], small_send.at[offset], small_recv.at[offset], device
    )


def row_of(core, first, second):
    y = first * (1 - core) + second * core
    x = second * (1 - core) + first * core
    return y, x


def send(src, dst, send_sem, recv_sem, device):
    return pltpu.make_async_remote_copy(
        src_ref=src, dst_ref=dst, send_sem=send_sem, recv_sem=recv_sem, device_id=device, device_id_type=MESH
    )


GSTEPS = 4
QUEUE = (2, 1, 3)
ARRIVE = (1, 3, 2)


def spread_out(own_ref, all_ref, sems):
    r, c, y, x, z, core, first, second = seat()
    pair, along_first, along_second, up = partners()
    here_sem, z_send, z_recv, g_send, g_recv, f_send, f_recv, p_send, p_recv = sems
    step = own_ref.shape[0] // GSTEPS

    def rows(q):
        return pl.ds(pl.multiple_of(q * step, step), step)

    def place(k, s, f, q):
        sec = second * (1 - s) + (1 - second) * s
        fir = first * (1 - f) + (1 - first) * f
        yy, xx = row_of(core, fir, sec)
        return all_ref.at[(z + 4 - k) % 4, core, yy, xx, rows(q)]

    def z_copy(k, q):
        return send(
            own_ref.at[rows(q)], place(0, 0, 0, q), z_send.at[k - 1, q], z_recv.at[k - 1, q], up[k - 1]
        )

    def g_copy(k, q, src):
        return send(src, place(k, 0, 0, q), g_send.at[k, q], g_recv.at[k, q], along_second)

    def f_copy(k, s, q, src):
        return send(src, place(k, s, 0, q), f_send.at[s, k, q], f_recv.at[s, k, q], along_first)

    def p_copy(k, s, f, q, src):
        return send(src, place(k, s, f, q), p_send.at[f, s, k, q], p_recv.at[f, s, k, q], pair)

    here = pltpu.make_async_copy(own_ref, all_ref.at[z, core, y, x], here_sem)

    def begin():
        here.start()

        @pl.loop(0, GSTEPS)
        def _(q):
            src = own_ref.at[rows(q)]
            for k in QUEUE:
                z_copy(k, q).start()
            g_copy(0, q, src).start()
            f_copy(0, 0, q, src).start()
            p_copy(0, 0, 0, q, src).start()

    def forward(q):
        for k in ARRIVE:
            z_copy(k, q).wait_recv()
            src = place(k, 0, 0, q)
            g_copy(k, q, src).start()
            f_copy(k, 0, q, src).start()
            p_copy(k, 0, 0, q, src).start()
        for k in (0, *ARRIVE):
            src = place(k, 1, 0, q)
            g_copy(k, q, src).wait_recv()
            f_copy(k, 1, q, src).start()
            p_copy(k, 1, 0, q, src).start()
        for k in (0, *ARRIVE):
            src = place(k, 0, 1, q)
            f_copy(k, 0, q, src).wait_recv()
            p_copy(k, 0, 1, q, src).start()

    def finish():
        @pl.loop(0, GSTEPS)
        def _(q):
            for k in (0, *ARRIVE):
                src = place(k, 1, 1, q)
                f_copy(k, 1, q, src).wait_recv()
                p_copy(k, 1, 1, q, src).start()

        here.wait()

        @pl.loop(0, GSTEPS)
        def _(q):
            for k in range(4):
                src = own_ref.at[rows(q)]
                if k:
                    z_copy(k, q).wait_send()
                g_copy(k, q, src).wait_send()
                for s in range(2):
                    f_copy(k, s, q, src).wait_send()
                    for f in range(2):
                        p_copy(k, s, f, q, src).wait()

    return begin, forward, finish


def spread_sems():
    dma = pltpu.SemaphoreType.DMA
    shapes = [(3, GSTEPS), (4, GSTEPS), (2, 4, GSTEPS), (2, 2, 4, GSTEPS)]
    return [dma(())] + [dma(shape) for shape in shapes for _ in range(2)]


def small_out(small_ref, small_all, sems):
    here_sem, small_send, small_recv = sems
    local = pltpu.make_async_copy(small_ref, small_all.at[nth(0)[0]], here_sem)

    def copy(offset):
        return small_copy(lambda spot: small_ref, small_all, small_send, small_recv, offset)

    def begin():
        local.start()

        @pl.loop(1, RANKS)
        def _(offset):
            copy(offset).start()

    def finish():
        local.wait()

        @pl.loop(1, RANKS)
        def _(offset):
            copy(offset).wait()

    return begin, finish


def small_sems():
    dma = pltpu.SemaphoreType.DMA
    return [dma(()), dma((RANKS,)), dma((RANKS,))]


def gather_body(own_ref, small_ref, all_ref, small_all, *sems):
    begin, forward, finish = spread_out(own_ref, all_ref, sems[:9])
    small_begin, small_finish = small_out(small_ref, small_all, sems[9:])
    meet()
    small_begin()
    begin()

    @pl.loop(0, GSTEPS)
    def _(q):
        forward(q)

    finish()
    small_finish()


ANYWHERE = pl.BlockSpec(memory_space=pl.ANY)


def gather_near(own, small, collective_id):
    tokens, depth = own.shape
    out, small_all = pl.pallas_call(
        gather_body,
        out_shape=(
            jax.ShapeDtypeStruct((4, 2, 2, 2, tokens, depth), own.dtype),
            jax.ShapeDtypeStruct((RANKS, *small.shape), small.dtype),
        ),
        in_specs=[ANYWHERE] * 2,
        out_specs=[ANYWHERE] * 2,
        scratch_shapes=spread_sems() + small_sems(),
        compiler_params=pltpu.CompilerParams(collective_id=collective_id, has_side_effects=True),
    )(own, small)
    return out.reshape(RANKS, tokens, depth), small_all


def start_body(x_ref, q_ref, k_ref, v_ref, o_ref, pack_ref, own_ref, small_ref,
               x_all, q_all, k_all, v_all, o_all, pack_all, all_ref, small_all, *sems):
    r, c, y, x, z, core, first, second = seat()
    pair, along_first, along_second, up = partners()
    begin, forward, finish = spread_out(own_ref, all_ref, sems[:9])
    small_begin, small_finish = small_out(small_ref, small_all, sems[9:12])
    here_sem, x_send, x_recv, w_send, w_recv, v_send, v_recv = sems[12:]
    weights = [(q_ref, q_all), (k_ref, k_all), (v_ref, v_all), (o_ref, o_all), (pack_ref, pack_all)]

    def block(index, col):
        ref, whole = weights[index]
        if index == 4:
            return whole.at[col]
        if index == 3:
            width = ref.shape[1]
            return whole.at[:, pl.ds(pl.multiple_of(col * width, width), width)]
        height = ref.shape[0]
        return whole.at[pl.ds(pl.multiple_of(col * height, height), height)]

    def w_copy(index, k):
        return send(
            weights[index][0], block(index, c), w_send.at[index, k - 1], w_recv.at[index, k - 1], up[k - 1]
        )

    def pair_copy(index, k):
        col = ((z + 4 - k) % 4) * 2 + core
        src = weights[index][0] if k == 0 else block(index, col)
        return send(src, block(index, col), v_send.at[index, k], v_recv.at[index, k], pair)

    locals_ = [pltpu.make_async_copy(x_ref, x_all.at[r], here_sem.at[5])] + [
        pltpu.make_async_copy(weights[i][0], block(i, c), here_sem.at[i]) for i in range(5)
    ]
    y1, x1 = row_of(core, first, 1 - second)
    near_row = y1 * 2 + x1
    x_first = send(x_ref, x_all.at[r], x_send.at[0], x_recv.at[0], along_first)
    x_second = send(x_ref, x_all.at[r], x_send.at[1], x_recv.at[1], along_second)
    x_relay = send(x_all.at[near_row], x_all.at[near_row], x_send.at[2], x_recv.at[2], along_first)

    meet()
    small_begin()
    x_second.start()
    x_first.start()
    for index in (4, 0, 1, 2, 3):
        for k in QUEUE:
            w_copy(index, k).start()
        pair_copy(index, 0).start()
    begin()
    for item in locals_:
        item.start()
    x_second.wait_recv()
    x_relay.start()
    for index in (4, 0, 1, 2, 3):
        for k in ARRIVE:
            w_copy(index, k).wait_recv()
            pair_copy(index, k).start()

    @pl.loop(0, GSTEPS)
    def _(q):
        forward(q)

    finish()
    small_finish()
    for item in locals_:
        item.wait()
    x_first.wait()
    x_second.wait_send()
    x_relay.wait()
    for index in range(5):
        for k in range(4):
            if k:
                w_copy(index, k).wait_send()
            pair_copy(index, k).wait()


def start_near(x, weights, pack, own, small, collective_id):
    tokens, depth = own.shape
    dma = pltpu.SemaphoreType.DMA
    height, width = weights[0].shape
    shaped = lambda shape, like: jax.ShapeDtypeStruct(shape, like.dtype)
    outs = pl.pallas_call(
        start_body,
        out_shape=(
            shaped((4, *x.shape), x),
            *[shaped((8 * height, width), w) for w in weights[:3]],
            shaped((weights[3].shape[0], 8 * weights[3].shape[1]), weights[3]),
            shaped((8, *pack.shape), pack),
            shaped((4, 2, 2, 2, tokens, depth), own),
            shaped((RANKS, *small.shape), small),
        ),
        in_specs=[ANYWHERE] * 8,
        out_specs=[ANYWHERE] * 8,
        scratch_shapes=spread_sems()
        + small_sems()
        + [dma((6,)), dma((3,)), dma((3,)), dma((5, 3)), dma((5, 3)), dma((5, 4)), dma((5, 4))],
        compiler_params=pltpu.CompilerParams(collective_id=collective_id, has_side_effects=True),
    )(x, *weights, pack, own, small)
    x_all, q, k, v, o, pack_all, whole, small_all = outs
    return x_all.reshape(-1, x.shape[1]), q, k, v, o, pack_all, whole.reshape(RANKS, tokens, depth), small_all


def finish_body(field_ref, q_ref, k_ref, v_ref, o_ref, pack_ref,
                out_ref, q_out, k_out, v_out, o_out, pack_all,
                mine, first_in, second_in, total,
                q_mine, k_mine, v_mine, o_mine, q_pair, k_pair, v_pair, o_pair, q_z, k_z, v_z, o_z,
                q_sum, k_sum, v_sum, o_sum,
                load_sem, f_send, f_recv, g_send, g_recv, w_load, p_send, p_recv, z_send, z_recv, out_sem,
                *small):
    r, c, y, x, z, core, first, second = seat()
    pair, along_first, along_second, up = partners()
    here_sem, small_send, small_recv = small
    tokens, depth = out_ref.shape
    other = 1 - core
    grads = [q_ref, k_ref, v_ref, o_ref]
    kept, pairs, zs = [q_mine, k_mine, v_mine, o_mine], [q_pair, k_pair, v_pair, o_pair], [q_z, k_z, v_z, o_z]
    sums, outs = [q_sum, k_sum, v_sum, o_sum], [q_out, k_out, v_out, o_out]

    def block(index, col):
        ref = grads[index]
        if index == 3:
            width = ref.shape[1] // 8
            return ref.at[:, pl.ds(pl.multiple_of(col * width, width), width)]
        height = ref.shape[0] // 8
        return ref.at[pl.ds(pl.multiple_of(col * height, height), height)]

    def row(fir, sec):
        yy, xx = row_of(core, fir, sec)
        return yy * 2 + xx

    local = pltpu.make_async_copy(pack_ref.at[c], pack_all.at[nth(0)[0]], here_sem)

    def small_of(offset):
        return small_copy(lambda spot: pack_ref.at[spot // 4], pack_all, small_send, small_recv, offset)

    def load(fir, sec):
        return pltpu.make_async_copy(field_ref.at[row(fir, sec)], mine.at[fir, sec], load_sem.at[fir, sec])

    def f_copy(sec):
        return send(field_ref.at[row(1 - first, sec)], first_in.at[sec], f_send.at[sec], f_recv.at[sec], along_first)

    g_copy = send(mine.at[first, 1 - second], second_in, g_send, g_recv, along_second)

    def w_load_copy(index, zz):
        return pltpu.make_async_copy(block(index, zz * 2 + core), kept[index].at[zz], w_load.at[index, zz])

    def w_give(index, zz):
        return send(
            block(index, zz * 2 + other), pairs[index].at[zz], p_send.at[index, zz], p_recv.at[index, zz], pair
        )

    def w_z(index, k):
        return send(
            kept[index].at[(z + k) % 4], zs[index].at[k - 1], z_send.at[index, k - 1], z_recv.at[index, k - 1], up[k - 1]
        )

    def add(ref, extras):
        @pl.loop(0, ref.shape[0] // TILE)
        def _(t):
            here = pl.ds(pl.multiple_of(t * TILE, TILE), TILE)
            value = ref[here].astype(jnp.float32)
            for extra in extras:
                value = value + extra[here].astype(jnp.float32)
            ref[here] = value.astype(jnp.bfloat16)

    def add_out(ref, extras, result):
        @pl.loop(0, ref.shape[0] // TILE)
        def _(t):
            here = pl.ds(pl.multiple_of(t * TILE, TILE), TILE)
            value = ref[here].astype(jnp.float32)
            for extra in extras:
                value = value + extra[here].astype(jnp.float32)
            result[here] = value

    meet()
    f_copy(1 - second).start()
    f_copy(second).start()
    for index in range(4):
        for k in (2, 1, 3, 0):
            w_give(index, (z + k) % 4).start()
            w_load_copy(index, (z + k) % 4).start()
    load(first, 1 - second).start()
    load(first, second).start()
    local.start()

    @pl.loop(1, RANKS)
    def _(offset):
        small_of(offset).start()

    for index in range(4):
        for k in (2, 1, 3):
            zz = (z + k) % 4
            w_load_copy(index, zz).wait()
            w_give(index, zz).wait_recv()
            add(kept[index].at[zz], [pairs[index].at[zz]])
            w_z(index, k).start()
    load(first, 1 - second).wait()
    f_copy(1 - second).wait_recv()
    add(mine.at[first, 1 - second], [first_in.at[1 - second]])
    g_copy.start()
    load(first, second).wait()
    f_copy(second).wait_recv()
    for index in range(4):
        w_load_copy(index, z).wait()
        w_give(index, z).wait_recv()
    g_copy.wait_recv()
    add_out(mine.at[first, second], [first_in.at[second], second_in], total)
    pltpu.make_async_copy(total, out_ref, out_sem.at[4]).start()
    for index in range(4):
        for k in ARRIVE:
            w_z(index, k).wait_recv()
        add_out(
            kept[index].at[z], [pairs[index].at[z]] + [zs[index].at[k] for k in range(3)], sums[index]
        )
        pltpu.make_async_copy(sums[index], outs[index], out_sem.at[index]).start()
    for sec in range(2):
        f_copy(sec).wait_send()
    g_copy.wait_send()
    for index in range(4):
        for k in range(4):
            w_give(index, (z + k) % 4).wait_send()
            if k:
                w_z(index, k).wait_send()
        pltpu.make_async_copy(sums[index], outs[index], out_sem.at[index]).wait()
    local.wait()

    @pl.loop(1, RANKS)
    def _(offset):
        small_of(offset).wait()

    pltpu.make_async_copy(total, out_ref, out_sem.at[4]).wait()


def finish_near(field, grads, pack, collective_id):
    rows_count, tokens, depth = field.shape
    dma = pltpu.SemaphoreType.DMA
    blocks = [(g.shape[0] // 8, g.shape[1]) for g in grads[:3]] + [(grads[3].shape[0], grads[3].shape[1] // 8)]
    half = lambda *shape: pltpu.VMEM(shape, jnp.bfloat16)
    return pl.pallas_call(
        finish_body,
        out_shape=(
            jax.ShapeDtypeStruct((tokens, depth), jnp.float32),
            *[jax.ShapeDtypeStruct(b, jnp.float32) for b in blocks],
            jax.ShapeDtypeStruct((RANKS, *pack.shape[1:]), pack.dtype),
        ),
        in_specs=[ANYWHERE] * 6,
        out_specs=[ANYWHERE] * 6,
        scratch_shapes=[
            half(2, 2, tokens, depth), half(2, tokens, depth), half(tokens, depth),
            pltpu.VMEM((tokens, depth), jnp.float32),
            *[half(4, *b) for b in blocks], *[half(4, *b) for b in blocks], *[half(3, *b) for b in blocks],
            *[pltpu.VMEM(b, jnp.float32) for b in blocks],
            dma((2, 2)), dma((2,)), dma((2,)), dma(()), dma(()),
            dma((4, 4)), dma((4, 4)), dma((4, 4)), dma((4, 3)), dma((4, 3)), dma((5,)),
        ]
        + small_sems(),
        compiler_params=pltpu.CompilerParams(
            collective_id=collective_id, has_side_effects=True, vmem_limit_bytes=60 * 1024 * 1024
        ),
    )(field, *grads, pack)


RSTEPS = 8
TILE = 16


def reduce_body(part_ref, small_ref, out_ref, small_all, mine, pair_in, first_in, second_in, z_in, total,
                load_sem, p_send, p_recv, f_send, f_recv, g_send, g_recv, z_send, z_recv, out_sem,
                small_here, small_send, small_recv):
    r, c, y, x, z, core, first, second = seat()
    pair, along_first, along_second, up = partners()
    tokens, depth = out_ref.shape
    step = tokens // RSTEPS
    other = 1 - core

    def rows(q):
        return pl.ds(pl.multiple_of(q * step, step), step)

    meet()

    small_local = pltpu.make_async_copy(small_ref.at[nth(0)[0]], small_all.at[nth(0)[0]], small_here)
    small_local.start()

    def small(offset):
        return small_copy(lambda spot: small_ref.at[spot], small_all, small_send, small_recv, offset)

    @pl.loop(1, RANKS)
    def _(offset):
        small(offset).start()

    def load(f, s, q):
        yy, xx = row_of(core, f, s)
        return pltpu.make_async_copy(part_ref.at[:, core, yy, xx, rows(q)], mine.at[f, s, :, rows(q)], load_sem.at[f, s, q])

    def give(f, s, q):
        yy, xx = row_of(other, f, s)
        return send(part_ref.at[:, other, yy, xx, rows(q)], pair_in.at[f, s, :, rows(q)],
                    p_send.at[f, s, q], p_recv.at[f, s, q], pair)

    def f_copy(s, q):
        return send(mine.at[1 - first, s, :, rows(q)], first_in.at[s, :, rows(q)], f_send.at[s, q], f_recv.at[s, q], along_first)

    def g_copy(q):
        return send(mine.at[first, 1 - second, :, rows(q)], second_in.at[:, rows(q)], g_send.at[q], g_recv.at[q], along_second)

    def z_copy(k, q):
        return send(mine.at[first, second, (z + k) % 4, rows(q)], z_in.at[k - 1, rows(q)],
                    z_send.at[k - 1, q], z_recv.at[k - 1, q], up[k - 1])

    def order(me_first, me_second):
        return [(1 - me_first, 1 - me_second), (1 - me_first, me_second), (me_first, 1 - me_second), (me_first, me_second)]

    @pl.loop(0, RSTEPS)
    def _(q):
        for f, s in order(second, first):
            give(f, s, q).start()
        for f, s in order(first, second):
            load(f, s, q).start()

    def add_into(f, s, q, extra):
        @pl.loop(0, 4 * (step // TILE))
        def _(t):
            zz, at = t // (step // TILE), t % (step // TILE)
            here = pl.ds(pl.multiple_of(q * step + at * TILE, TILE), TILE)
            value = mine[f, s, zz, here].astype(jnp.float32) + pair_in[f, s, zz, here].astype(jnp.float32)
            for ref in extra:
                value = value + ref[zz, here].astype(jnp.float32)
            mine[f, s, zz, here] = value.astype(jnp.bfloat16)

    def stage_first(q):
        for s in (1 - second, second):
            load(1 - first, s, q).wait()
            give(1 - first, s, q).wait_recv()
            add_into(1 - first, s, q, [])
            f_copy(s, q).start()

    def stage_second(q):
        load(first, 1 - second, q).wait()
        give(first, 1 - second, q).wait_recv()
        f_copy(1 - second, q).wait_recv()
        add_into(first, 1 - second, q, [first_in.at[1 - second]])
        g_copy(q).start()

    def stage_z(q):
        load(first, second, q).wait()
        give(first, second, q).wait_recv()
        f_copy(second, q).wait_recv()
        g_copy(q).wait_recv()
        add_into(first, second, q, [first_in.at[second], second_in])
        for k in (2, 1, 3):
            z_copy(k, q).start()

    def stage_out(q):
        for k in (1, 3, 2):
            z_copy(k, q).wait_recv()

        @pl.loop(0, step // TILE)
        def _(t):
            here = pl.ds(pl.multiple_of(q * step + t * TILE, TILE), TILE)
            value = mine[first, second, z, here].astype(jnp.float32)
            for k in range(3):
                value = value + z_in[k, here].astype(jnp.float32)
            total[here] = value

    LAG1, LAG2, LAG3 = 1, 2, 4

    @pl.loop(0, RSTEPS + LAG3)
    def _(q):
        @pl.when(q < RSTEPS)
        def _():
            stage_first(q)

        @pl.when((q >= LAG1) & (q < RSTEPS + LAG1))
        def _():
            stage_second(q - LAG1)

        @pl.when((q >= LAG2) & (q < RSTEPS + LAG2))
        def _():
            stage_z(q - LAG2)

        @pl.when(q >= LAG3)
        def _():
            stage_out(q - LAG3)

    done = pltpu.make_async_copy(total, out_ref, out_sem)
    done.start()

    @pl.loop(0, RSTEPS)
    def _(q):
        for f in range(2):
            for s in range(2):
                give(f, s, q).wait_send()
        for s in range(2):
            f_copy(s, q).wait_send()
        g_copy(q).wait_send()
        for k in (1, 2, 3):
            z_copy(k, q).wait_send()

    small_local.wait()

    @pl.loop(1, RANKS)
    def _(offset):
        small(offset).wait()

    done.wait()


def reduce_near(part, small, collective_id):
    tokens, depth = part.shape[0] // RANKS, part.shape[1]
    dma = pltpu.SemaphoreType.DMA
    return pl.pallas_call(
        reduce_body,
        out_shape=(
            jax.ShapeDtypeStruct((tokens, depth), jnp.float32),
            jax.ShapeDtypeStruct(small.shape, small.dtype),
        ),
        in_specs=[pl.BlockSpec(memory_space=pl.ANY)] * 2,
        out_specs=[pl.BlockSpec(memory_space=pl.ANY)] * 2,
        scratch_shapes=[
            pltpu.VMEM((2, 2, 4, tokens, depth), jnp.bfloat16),
            pltpu.VMEM((2, 2, 4, tokens, depth), jnp.bfloat16),
            pltpu.VMEM((2, 4, tokens, depth), jnp.bfloat16),
            pltpu.VMEM((4, tokens, depth), jnp.bfloat16),
            pltpu.VMEM((3, tokens, depth), jnp.bfloat16),
            pltpu.VMEM((tokens, depth), jnp.float32),
            dma((2, 2, RSTEPS)),
            dma((2, 2, RSTEPS)), dma((2, 2, RSTEPS)),
            dma((2, RSTEPS)), dma((2, RSTEPS)),
            dma((RSTEPS,)), dma((RSTEPS,)),
            dma((3, RSTEPS)), dma((3, RSTEPS)),
            dma(()),
            dma(()), dma((RANKS,)), dma((RANKS,)),
        ],
        compiler_params=pltpu.CompilerParams(
            collective_id=collective_id, has_side_effects=True, vmem_limit_bytes=60 * 1024 * 1024
        ),
    )(part.reshape(4, 2, 2, 2, tokens, depth), small)


def project_body(flipped, pick_ref, field_ref, *refs):
    count = len(flipped)
    weights, (rows_ref, *outs), sums = refs[:count], refs[count:2*count+1], refs[2*count+1:]
    k = pl.program_id(0)
    ranks = pick_ref.shape[0]
    groups = rows_ref.shape[0]

    @pl.loop(0, ranks // 2, unroll=UNROLL)
    def _(i):
        parts = [
            wide_dot(pick_ref[2 * i + side], field_ref[2 * i + side]).reshape(groups, SLOTS, CHUNK)
            for side in range(2)
        ]
        rows_ref[:, pl.ds(pl.multiple_of(i * 2 * SLOTS, 2 * SLOTS), 2 * SLOTS)] = jnp.concatenate(parts, axis=1).astype(jnp.bfloat16)

    def project(e, first):
        rows = rows_ref[e]
        for weight, flip, total in zip(weights, flipped, sums):
            term = outer_cols(rows, weight[e]) if flip else wide_dot(rows, weight[e])
            if first: total[e] = term
            else: total[e] += term

    @pl.when(k == 0)
    def _():
        @pl.loop(0, groups)
        def _(e):
            project(e, True)

    @pl.when(k > 0)
    def _():
        @pl.loop(0, groups)
        def _(e):
            project(e, False)

    @pl.when(k == pl.num_programs(0) - 1)
    def _():
        for out, total in zip(outs, sums):
            pltpu.sync_copy(total, out)

def project(pick, field, weights, flipped):
    ranks, width, tokens = pick.shape
    groups, depth = width // SLOTS, field.shape[-1]
    length = ranks * SLOTS
    inner = weights[0].shape[1] if flipped[0] else weights[0].shape[2]
    wspecs = [pl.BlockSpec((groups, inner, CHUNK), lambda k: (0, 0, k)) if f else pl.BlockSpec((groups, CHUNK, inner), lambda k: (0, k, 0)) for f in flipped]
    flops = 2 * groups * length * depth * (tokens + inner * len(weights))
    return pl.pallas_call(
        functools.partial(project_body, flipped),
        grid=(depth // CHUNK,),
        in_specs=[
            pl.BlockSpec((ranks, width, tokens), lambda k: (0, 0, 0), pipeline_mode=pl.Buffered(1)),
            pl.BlockSpec((ranks, tokens, CHUNK), lambda k: (0, 0, k)),
            *wspecs,
        ],
        out_specs=[pl.BlockSpec((groups, length, CHUNK), lambda k: (0, 0, k))] + [pl.BlockSpec(memory_space=pl.ANY)] * len(weights),
        out_shape=[jax.ShapeDtypeStruct((groups, length, depth), jnp.bfloat16)]
        + [jax.ShapeDtypeStruct((groups, length, inner), jnp.float32)] * len(weights),
        scratch_shapes=[pltpu.VMEM((groups, length, inner), jnp.float32)] * len(weights),
        compiler_params=pltpu.CompilerParams(vmem_limit_bytes=63 * 1024 * 1024),
        cost_estimate=pl.CostEstimate(flops=flops, bytes_accessed=120 << 20, transcendentals=0),
    )(pick, field.reshape(ranks, tokens, depth), *weights)


def restore_body(flipped, spread_ref, *refs):
    count = len(flipped)
    lefts, weights, field_ref, rows = refs[:count], refs[count:2*count], refs[2*count], refs[2*count+1]
    groups = rows.shape[0]
    ranks = spread_ref.shape[0]

    @pl.loop(0, groups)
    def _(e):
        total = None
        for left, weight, flip in zip(lefts, weights, flipped):
            term = outer_cols(left[e], weight[e]) if flip else wide_dot(left[e], weight[e])
            total = term if total is None else total + term
        rows[e] = total

    @pl.loop(0, ranks, unroll=2*UNROLL)
    def _(s):
        part = rows[:, pl.ds(pl.multiple_of(s * SLOTS, SLOTS), SLOTS)].reshape(groups * SLOTS, CHUNK).astype(jnp.bfloat16)
        field_ref[s] = wide_dot(spread_ref[s], part).astype(jnp.bfloat16)

def restore(spread, lefts, weights, flipped):
    ranks, tokens, width = spread.shape
    groups = width // SLOTS
    length = ranks * SLOTS
    inner = lefts[0].shape[2]
    depth = weights[0].shape[1] if flipped[0] else weights[0].shape[2]
    wspecs = [pl.BlockSpec((groups, CHUNK, inner), lambda k: (0, k, 0)) if f else pl.BlockSpec((groups, inner, CHUNK), lambda k: (0, 0, k)) for f in flipped]
    flops = 2 * groups * length * depth * (tokens + inner * len(weights))
    field = pl.pallas_call(
        functools.partial(restore_body, flipped),
        grid=(depth // CHUNK,),
        in_specs=[pl.BlockSpec((ranks, tokens, width), lambda k: (0, 0, 0), pipeline_mode=pl.Buffered(1))]
        + [pl.BlockSpec((groups, length, inner), lambda k: (0, 0, 0), pipeline_mode=pl.Buffered(1))] * len(lefts) + wspecs,
        out_specs=pl.BlockSpec((ranks, tokens, CHUNK), lambda k: (0, 0, k)),
        out_shape=jax.ShapeDtypeStruct((ranks, tokens, depth), jnp.bfloat16),
        scratch_shapes=[pltpu.VMEM((groups, length, CHUNK), jnp.float32)],
        compiler_params=pltpu.CompilerParams(vmem_limit_bytes=63 * 1024 * 1024),
        cost_estimate=pl.CostEstimate(flops=flops, bytes_accessed=60 << 20, transcendentals=0),
    )(spread, *lefts, *weights)
    return field.reshape(ranks * tokens, depth)


def local(
    layer_input,
    cotangent,
    expert_index,
    attention_gain,
    query_gain,
    key_gain,
    query_weight,
    key_weight,
    value_weight,
    output_weight,
    feed_gain,
    router_weight,
    gate_weight,
    up_weight,
    down_weight,
):
    tokens = layer_input.shape[0]
    rows_count = lax.axis_size("row")
    near = rows_count == 4 and lax.axis_size("col") == 8
    if near:
        head_part = query_gain.shape[0]
        slice_width = attention_gain.shape[0]
        pack = jnp.concatenate(
            [attention_gain, feed_gain, query_gain, key_gain, router_weight.reshape(-1)]
        )
        pack = jnp.pad(pack, (0, PACK_ROWS * 128 - pack.shape[0])).reshape(PACK_ROWS, 128)
        (
            sequence, query_full, key_full, value_full, output_full, pack_all, cotangent_all, index_all
        ) = start_near(
            layer_input,
            [query_weight, key_weight, value_weight, output_weight],
            pack,
            cotangent,
            expert_index.T,
            1,
        )
        index_all = jnp.swapaxes(index_all, 1, 2)
        pack_all = pack_all.reshape(8, -1)
        ends = [slice_width, 2 * slice_width, 2 * slice_width + head_part, 2 * slice_width + 2 * head_part]
        attention_full = pack_all[:, : ends[0]].reshape(-1)
        feed_full = pack_all[:, ends[0] : ends[1]].reshape(-1)
        query_scale_w = pack_all[:, ends[1] : ends[2]].reshape(-1)
        key_scale_w = pack_all[:, ends[2] : ends[3]].reshape(-1)
        router_full = pack_all[:, ends[3] : ends[3] + router_weight.size].reshape(
            -1, router_weight.shape[1]
        )
    else:
        (
            attention_full,
            query_scale_w,
            key_scale_w,
            query_full,
            key_full,
            value_full,
            output_full,
            feed_full,
            router_full,
        ) = (
            lax.all_gather(attention_gain, "col", axis=0, tiled=True),
            lax.all_gather(query_gain, "col", axis=0, tiled=True),
            lax.all_gather(key_gain, "col", axis=0, tiled=True),
            lax.all_gather(query_weight, "col", axis=0, tiled=True),
            lax.all_gather(key_weight, "col", axis=0, tiled=True),
            lax.all_gather(value_weight, "col", axis=0, tiled=True),
            lax.all_gather(output_weight, "col", axis=1, tiled=True),
            lax.all_gather(feed_gain, "col", axis=0, tiled=True),
            lax.all_gather(router_weight, "col", axis=0, tiled=True),
        )
        sequence = lax.all_gather(layer_input, "row", axis=0, tiled=True)
    length = sequence.shape[0]
    model_width = sequence.shape[1]
    local_width = query_full.shape[1]
    local_heads = local_width // HD
    seq_float = sequence.astype(jnp.float32)
    seq_scale = rms_scale(seq_float)
    attention_float = attention_full.astype(jnp.float32)
    normed = (seq_float * seq_scale * attention_float).astype(jnp.bfloat16)
    query_raw = wide_dot(normed, query_full)
    key_raw = wide_dot(normed, key_full)
    value_heads = wide_dot(normed, value_full).astype(jnp.bfloat16).reshape(length, local_heads, HD)
    query_total, key_total = lax.psum(
        (jnp.sum(query_raw * query_raw, axis=-1), jnp.sum(key_raw * key_raw, axis=-1)), "row"
    )
    query_rs = lax.rsqrt(query_total / model_width + EPS)[:, None]
    key_rs = lax.rsqrt(key_total / model_width + EPS)[:, None]
    query_gain_f = query_scale_w.astype(jnp.float32)
    key_gain_f = key_scale_w.astype(jnp.float32)
    cosine, sine_table = rope_tables(length)
    queries = rotate(
        (query_raw * query_rs * query_gain_f).reshape(length, local_heads, HD), cosine, sine_table
    ).astype(jnp.bfloat16)
    keys_rotated = rotate(
        (key_raw * key_rs * key_gain_f).reshape(length, local_heads, HD), cosine, sine_table
    ).astype(jnp.bfloat16)
    block_rows = min(512, length)
    starts = jnp.arange(length // block_rows, dtype=jnp.int32) * block_rows
    key_position = jnp.arange(length, dtype=jnp.int32)
    score_scale = HD ** (-0.5)

    def block_scores(offset):
        query_rows = lax.dynamic_slice_in_dim(queries, offset, block_rows, 0)
        scores = (
            jnp.einsum("qhd,khd->hqk", query_rows, keys_rotated, preferred_element_type=jnp.float32)
            * score_scale
        )
        query_position = offset + jnp.arange(block_rows, dtype=jnp.int32)
        allowed = query_position[:, None] >= key_position[None, :]
        return (query_rows, jnp.where(allowed[None, :, :], scores, MASKED))

    def forward_block(offset):
        query_rows, scores = block_scores(offset)
        row_top = jnp.max(scores, axis=-1, keepdims=True)
        exponent = jnp.exp(scores - row_top)
        row_total = jnp.sum(exponent, axis=-1, keepdims=True)
        weights = (exponent / row_total).astype(jnp.bfloat16)
        mixed_block = jnp.einsum(
            "hqk,khd->qhd", weights, value_heads, preferred_element_type=jnp.float32
        )
        return (mixed_block, (row_top + jnp.log(row_total))[..., 0])

    mixed_blocks, lse_blocks = lax.map(forward_block, starts)
    mixed_heads = mixed_blocks.reshape(length, local_width).astype(jnp.bfloat16)
    lse_all = jnp.moveaxis(lse_blocks, 0, 1).reshape(local_heads, length)
    branch = lax.psum_scatter(
        wide_dot(mixed_heads, output_full).astype(jnp.bfloat16), "row", scatter_dimension=0, tiled=True
    ).astype(jnp.float32)
    hidden = layer_input.astype(jnp.float32) + branch
    feed_scale = rms_scale(hidden)
    feed_float = feed_full.astype(jnp.float32)
    feed_normed = (hidden * feed_scale * feed_float).astype(jnp.bfloat16)
    logits = wide_dot(feed_normed, router_full)
    logit_top = jnp.max(logits, axis=-1, keepdims=True)
    logit_exp = jnp.exp(logits - logit_top)
    router_probs = logit_exp / jnp.sum(logit_exp, axis=-1, keepdims=True)
    experts = router_full.shape[1]
    experts_local = gate_weight.shape[0]
    ranks = lax.axis_size("col") * rows_count
    gate_hits = expert_index[:, :, None] == jnp.arange(experts, dtype=jnp.int32)
    gate_probs = jnp.sum(jnp.where(gate_hits, router_probs[:, None, :], 0.0), axis=-1)

    if not near:
        index_all = lax.all_gather(expert_index, ("col", "row"), axis=0, tiled=True)
    own = (index_all - lax.axis_index("col") * experts_local).reshape(ranks, tokens, -1)
    matches = own[..., None] == jnp.arange(experts_local, dtype=jnp.int32)
    hit = jnp.sum(matches.astype(jnp.float32), axis=2)
    earlier = jnp.tril(jnp.ones((tokens, tokens), jnp.bfloat16), -1)
    rank = jnp.einsum(
        "tu,sue->ste", earlier, hit.astype(jnp.bfloat16), preferred_element_type=jnp.float32
    )
    slot = jnp.where(hit > 0, rank, -1.0)
    places = jnp.arange(SLOTS, dtype=jnp.float32)
    slot_t = jnp.swapaxes(slot, 1, 2)
    width = experts_local * SLOTS
    pick = (slot_t[:, :, None, :] == places[None, None, :, None]).astype(jnp.bfloat16)
    pick = pick.reshape(ranks, width, tokens)
    spread = slot[:, :, :, None] == places
    spread_plain = spread.astype(jnp.bfloat16).reshape(ranks, tokens, width)
    if near:
        expert_grads, plain_act = project(pick, cotangent_all, [down_weight], (True,))
        feed_all, probs_all = gather_near(feed_normed, gate_probs.T, 2)
        probs_all = jnp.swapaxes(probs_all, 1, 2)
        expert_rows, gate_val, up_val = project(
            pick, feed_all, [gate_weight, up_weight], (False, False)
        )
    else:
        probs_all = lax.all_gather(gate_probs, ("col", "row"), axis=0, tiled=True)
        expert_grads = gather_rows(pick, cotangent)
        expert_rows = gather_rows(pick, feed_normed)
        gate_val = jnp.einsum(
            "erd,edf->erf", expert_rows, gate_weight, preferred_element_type=jnp.float32
        )
        up_val = jnp.einsum(
            "erd,edf->erf", expert_rows, up_weight, preferred_element_type=jnp.float32
        )
        plain_act = jnp.einsum(
            "erd,efd->erf", expert_grads, down_weight, preferred_element_type=jnp.float32
        )
    probs_own = jnp.sum(
        jnp.where(matches, probs_all.reshape(ranks, tokens, -1, 1), 0.0), axis=2
    )
    weighted = jnp.where(spread, probs_own[..., None], 0.0)
    spread_probs = weighted.astype(jnp.bfloat16).reshape(ranks, tokens, width)
    row_probs = jnp.sum(weighted, axis=1)
    row_probs = jnp.swapaxes(row_probs, 0, 1).reshape(experts_local, ranks * SLOTS, 1)
    sigmoid_val = jax.nn.sigmoid(gate_val)
    silu_val = gate_val * sigmoid_val
    activated = silu_val * up_val
    grad_act = plain_act * row_probs
    grad_up = (grad_act * silu_val).astype(jnp.bfloat16)
    grad_gate = (
        grad_act * up_val * sigmoid_val * (1.0 + gate_val * (1.0 - sigmoid_val))
    ).astype(jnp.bfloat16)
    row_gates = jnp.sum(activated * plain_act, axis=-1).reshape(experts_local, ranks, 1, SLOTS)
    weighted_act = (activated * row_probs).astype(jnp.bfloat16)
    activated = activated.astype(jnp.bfloat16)
    own_gates = jnp.sum(jnp.where(spread, jnp.transpose(row_gates, (1, 2, 0, 3)), 0.0), axis=-1)
    if near:
        own_gates = jnp.swapaxes(own_gates, 1, 2)
        grad_feed_part = restore(
            spread_plain, [grad_gate, grad_up], [gate_weight, up_weight], (True, True)
        )
        grad_feed, gates_in = reduce_near(grad_feed_part, own_gates, 3)
        gates_in = jnp.sum(gates_in.reshape(-1, rows_count, experts_local, tokens), axis=1)
        grad_probs = gates_in.reshape(experts, tokens).T
        mixture_part = restore(spread_probs, [activated], [down_weight], (False,))
        mixture = reduce_near(mixture_part, own_gates, 3)[0]
    else:
        own_gates = lax.psum_scatter(
            own_gates.reshape(-1, rows_count, tokens, experts_local), "row", scatter_dimension=1
        )
        grad_probs = lax.all_to_all(own_gates, "col", split_axis=0, concat_axis=2, tiled=True)[0]
        back_rows = (
            jnp.einsum("erf,edf->erd", grad_gate, gate_weight, preferred_element_type=jnp.float32)
            + jnp.einsum("erf,edf->erd", grad_up, up_weight, preferred_element_type=jnp.float32)
        ).astype(jnp.bfloat16)
        grad_feed = return_rows(spread_plain, back_rows).astype(jnp.float32)
        out_rows = jnp.einsum(
            "erf,efd->erd", activated, down_weight, preferred_element_type=jnp.float32
        ).astype(jnp.bfloat16)
        mixture = return_rows(spread_probs, out_rows).astype(jnp.float32)
    layer_output = hidden + mixture
    grad_gate_weight = jnp.einsum(
        "erd,erf->edf", expert_rows, grad_gate, preferred_element_type=jnp.float32
    )
    grad_up_weight = jnp.einsum(
        "erd,erf->edf", expert_rows, grad_up, preferred_element_type=jnp.float32
    )
    grad_down_weight = jnp.einsum(
        "erf,erd->efd", weighted_act, expert_grads, preferred_element_type=jnp.float32
    )
    grad_out = cotangent.astype(jnp.float32)
    grad_logits = (
        router_probs * (grad_probs - jnp.sum(router_probs * grad_probs, axis=-1, keepdims=True))
    ).astype(jnp.bfloat16)
    router_grad = inner_rows(feed_normed, grad_logits)
    grad_feed = grad_feed + outer_cols(grad_logits, router_full)
    feed_gain_term = jnp.sum(grad_feed * hidden * feed_scale, axis=0)
    feed_weighted = grad_feed * feed_float
    grad_hidden = (
        grad_out
        + feed_scale * feed_weighted
        - hidden * feed_scale**3 * jnp.mean(feed_weighted * hidden, axis=-1, keepdims=True)
    )
    grad_branch = lax.all_gather(grad_hidden.astype(jnp.bfloat16), "row", axis=0, tiled=True)
    output_grad = inner_rows(mixed_heads, grad_branch)
    grad_mixed = (
        outer_cols(grad_branch, output_full).astype(jnp.bfloat16).reshape(length, local_heads, HD)
    )

    def backward_block(carry, offset):
        grad_keys, grad_values = carry
        query_rows, scores = block_scores(offset)
        lse_rows = lax.dynamic_slice_in_dim(lse_all, offset, block_rows, 1)
        probs_block = jnp.exp(scores - lse_rows[:, :, None])
        weights_low = probs_block.astype(jnp.bfloat16)
        grad_rows_out = lax.dynamic_slice_in_dim(grad_mixed, offset, block_rows, 0)
        grad_weights = jnp.einsum(
            "qhd,khd->hqk", grad_rows_out, value_heads, preferred_element_type=jnp.float32
        )
        grad_values = grad_values + jnp.einsum(
            "hqk,qhd->khd", weights_low, grad_rows_out, preferred_element_type=jnp.float32
        )
        delta_rows = jnp.sum(probs_block * grad_weights, axis=-1, keepdims=True)
        grad_scores = (probs_block * (grad_weights - delta_rows)).astype(jnp.bfloat16)
        grad_query_block = (
            jnp.einsum(
                "hqk,khd->qhd", grad_scores, keys_rotated, preferred_element_type=jnp.float32
            )
            * score_scale
        )
        grad_keys = (
            grad_keys
            + jnp.einsum(
                "hqk,qhd->khd", grad_scores, query_rows, preferred_element_type=jnp.float32
            )
            * score_scale
        )
        return ((grad_keys, grad_values), grad_query_block)

    zero_heads = jnp.zeros((length, local_heads, HD), jnp.float32)
    (grad_keys, grad_values), grad_query_blocks = lax.scan(
        backward_block, (zero_heads, zero_heads), starts
    )
    grad_queries = grad_query_blocks.reshape(length, local_heads, HD)
    grad_query_normed = unrotate(grad_queries, cosine, sine_table).reshape(length, local_width)
    grad_key_normed = unrotate(grad_keys, cosine, sine_table).reshape(length, local_width)
    grad_value_low = grad_values.reshape(length, local_width).astype(jnp.bfloat16)
    query_weighted = grad_query_normed * query_gain_f
    key_weighted = grad_key_normed * key_gain_f
    query_gain_term = jnp.sum(grad_query_normed * query_raw * query_rs, axis=0)
    key_gain_term = jnp.sum(grad_key_normed * key_raw * key_rs, axis=0)
    query_inner, key_inner = (
        lax.psum(jnp.sum(query_weighted * query_raw, axis=-1).astype(jnp.bfloat16), "row").astype(
            jnp.float32
        ),
        lax.psum(jnp.sum(key_weighted * key_raw, axis=-1).astype(jnp.bfloat16), "row").astype(
            jnp.float32
        ),
    )
    grad_query_raw = (
        query_rs * query_weighted - query_raw * query_rs**3 * (query_inner / model_width)[:, None]
    ).astype(jnp.bfloat16)
    grad_key_raw = (
        key_rs * key_weighted - key_raw * key_rs**3 * (key_inner / model_width)[:, None]
    ).astype(jnp.bfloat16)
    query_grad = inner_rows(normed, grad_query_raw)
    key_grad = inner_rows(normed, grad_key_raw)
    value_grad = inner_rows(normed, grad_value_low)
    grad_normed = (
        outer_cols(grad_query_raw, query_full)
        + outer_cols(grad_key_raw, key_full)
        + outer_cols(grad_value_low, value_full)
    )
    attention_weighted = grad_normed * attention_float
    grad_seq_part = seq_scale * attention_weighted - seq_float * seq_scale**3 * jnp.mean(
        attention_weighted * seq_float, axis=-1, keepdims=True
    )
    attention_gain_term = jnp.sum(grad_normed * seq_float * seq_scale, axis=0)
    if near:
        cols = lax.axis_size("col")
        pack = jnp.concatenate(
            [
                attention_gain_term.reshape(cols, -1),
                feed_gain_term.reshape(cols, -1),
                query_gain_term.reshape(cols, -1),
                key_gain_term.reshape(cols, -1),
                router_grad.reshape(cols, -1),
            ],
            axis=1,
        )
        pack = jnp.pad(pack, ((0, 0), (0, PACK_ROWS * 128 - pack.shape[1])))
        pack = pack.astype(jnp.bfloat16).reshape(cols, PACK_ROWS, 128)
        (
            summed, grad_query_weight, grad_key_weight, grad_value_weight, grad_output_weight, packs
        ) = finish_near(
            grad_seq_part.astype(jnp.bfloat16).reshape(rows_count, tokens, model_width),
            [grad.astype(jnp.bfloat16) for grad in (query_grad, key_grad, value_grad, output_grad)],
            pack,
            4,
        )
        input_grad = grad_hidden + summed
        packs = packs.reshape(cols, rows_count, -1).astype(jnp.float32)
        whole = jnp.sum(packs, axis=(0, 1))
        heads_sum = jnp.sum(
            lax.dynamic_index_in_dim(packs, lax.axis_index("row"), 1, keepdims=False), axis=0
        )
        grad_attention_gain = whole[: ends[0]]
        grad_feed_gain = whole[ends[0] : ends[1]]
        grad_query_gain = heads_sum[ends[1] : ends[2]]
        grad_key_gain = heads_sum[ends[2] : ends[3]]
        grad_router_weight = whole[ends[3] : ends[3] + router_weight.size].reshape(router_weight.shape)
    else:
        stacked = jnp.concatenate(
            [
                grad_seq_part.reshape(rows_count, tokens, model_width),
                jnp.broadcast_to(attention_gain_term[None, None, :], (rows_count, 1, model_width)),
            ],
            axis=1,
        ).reshape(rows_count * (tokens + 1), model_width)
        summed = lax.psum_scatter(
            stacked.astype(jnp.bfloat16), "row", scatter_dimension=0, tiled=True
        ).astype(jnp.float32)
        input_grad = grad_hidden + summed[:tokens]
        attention_gain_total = summed[tokens]
        feed_gain_total, router_total = (
            lax.psum(feed_gain_term.astype(jnp.bfloat16), "row").astype(jnp.float32),
            lax.psum(router_grad.astype(jnp.bfloat16), "row").astype(jnp.float32),
        )
        (
            grad_attention_gain,
            grad_query_gain,
            grad_key_gain,
            grad_query_weight,
            grad_key_weight,
            grad_value_weight,
            grad_output_weight,
            grad_feed_gain,
            grad_router_weight,
        ) = (
            lax.psum_scatter(
                attention_gain_total.astype(jnp.bfloat16), "col", scatter_dimension=0, tiled=True
            ).astype(jnp.float32),
            lax.psum_scatter(
                query_gain_term.astype(jnp.bfloat16), "col", scatter_dimension=0, tiled=True
            ).astype(jnp.float32),
            lax.psum_scatter(
                key_gain_term.astype(jnp.bfloat16), "col", scatter_dimension=0, tiled=True
            ).astype(jnp.float32),
            lax.psum_scatter(
                query_grad.astype(jnp.bfloat16), "col", scatter_dimension=0, tiled=True
            ).astype(jnp.float32),
            lax.psum_scatter(
                key_grad.astype(jnp.bfloat16), "col", scatter_dimension=0, tiled=True
            ).astype(jnp.float32),
            lax.psum_scatter(
                value_grad.astype(jnp.bfloat16), "col", scatter_dimension=0, tiled=True
            ).astype(jnp.float32),
            lax.psum_scatter(
                output_grad.astype(jnp.bfloat16), "col", scatter_dimension=1, tiled=True
            ).astype(jnp.float32),
            lax.psum_scatter(
                feed_gain_total.astype(jnp.bfloat16), "col", scatter_dimension=0, tiled=True
            ).astype(jnp.float32),
            lax.psum_scatter(
                router_total.astype(jnp.bfloat16), "col", scatter_dimension=0, tiled=True
            ).astype(jnp.float32),
        )
    return (
        layer_output,
        input_grad,
        grad_attention_gain,
        grad_query_gain,
        grad_key_gain,
        grad_query_weight,
        grad_key_weight,
        grad_value_weight,
        grad_output_weight,
        grad_feed_gain,
        grad_router_weight,
        grad_gate_weight,
        grad_up_weight,
        grad_down_weight,
    )


def solution(mesh):
    placed = (
        P(("col", "row"), None),
        P(("col", "row"), None),
        P(("col", "row"), None),
        P("col"),
        P(("row", "col")),
        P(("row", "col")),
        P("col", "row"),
        P("col", "row"),
        P("col", "row"),
        P("row", "col"),
        P("col"),
        P("col", None),
        P("col", None, "row"),
        P("col", None, "row"),
        P("col", "row", None),
    )
    return jax.shard_map(
        local,
        mesh=mesh,
        in_specs=placed,
        out_specs=(
            P(("col", "row"), None),
            P(("col", "row"), None),
            P("col"),
            P(("row", "col")),
            P(("row", "col")),
            P("col", "row"),
            P("col", "row"),
            P("col", "row"),
            P("row", "col"),
            P("col"),
            P("col", None),
            P("col", None, "row"),
            P("col", None, "row"),
            P("col", "row", None),
        ),
        check_vma=False,
    )
```

```python
import functools

import jax
import jax.numpy as jnp
from jax import lax
from jax.experimental import pallas as pl
from jax.experimental.pallas import tpu as pltpu
from jax.sharding import PartitionSpec as P

HD = 128
SLOTS = 40
BLOCK = 512
CHUNK = 256
UNROLL = 4
PACK_ROWS = 144


EPS = 1e-05
THETA = 10000.0
MASKED = -1e30


def wide_dot(left, right):
    return jnp.dot(left, right, preferred_element_type=jnp.float32)


def inner_rows(left, right):
    return lax.dot_general(
        left, right, (((0,), (0,)), ((), ())), preferred_element_type=jnp.float32
    )


def outer_cols(left, right):
    return lax.dot_general(
        left, right, (((1,), (1,)), ((), ())), preferred_element_type=jnp.float32
    )


def rms_scale(field):
    return lax.rsqrt(jnp.mean(field * field, axis=-1, keepdims=True) + EPS)


def rope_tables(length):
    half_size = HD // 2
    freqs = THETA ** (-(jnp.arange(half_size, dtype=jnp.float32) * 2.0) / HD)
    angles = jnp.arange(length, dtype=jnp.float32)[:, None] * freqs[None, :]
    cosine = jnp.concatenate([jnp.cos(angles), jnp.cos(angles)], axis=-1)[:, None, :]
    sine_table = jnp.concatenate([jnp.sin(angles), jnp.sin(angles)], axis=-1)[:, None, :]
    return (cosine, sine_table)


def rotate(field, cosine, sine_table):
    half_size = field.shape[-1] // 2
    turned = jnp.concatenate([-field[..., half_size:], field[..., :half_size]], axis=-1)
    return field * cosine + turned * sine_table


def unrotate(gradient, cosine, sine_table):
    half_size = gradient.shape[-1] // 2
    moved = gradient * sine_table
    back_turned = jnp.concatenate([moved[..., half_size:], -moved[..., :half_size]], axis=-1)
    return gradient * cosine + back_turned


def dispatch_body(pick_ref, field_ref, rows_ref):
    groups = rows_ref.shape[0]
    first = wide_dot(pick_ref[0], field_ref[0]).reshape(groups, SLOTS, -1)
    second = wide_dot(pick_ref[1], field_ref[1]).reshape(groups, SLOTS, -1)
    rows_ref[...] = jnp.concatenate([first, second], axis=1).astype(jnp.bfloat16)


def dispatch(pick, field):
    ranks, width, tokens = pick.shape
    groups, depth = width // SLOTS, field.shape[1]
    return pl.pallas_call(
        dispatch_body,
        grid=(ranks // 2, depth // BLOCK),
        in_specs=[
            pl.BlockSpec((2, width, tokens), lambda i, k: (i, 0, 0)),
            pl.BlockSpec((2, tokens, BLOCK), lambda i, k: (i, 0, k)),
        ],
        out_specs=pl.BlockSpec((groups, 2 * SLOTS, BLOCK), lambda i, k: (0, i, k)),
        out_shape=jax.ShapeDtypeStruct((groups, ranks * SLOTS, depth), jnp.bfloat16),
    )(pick, field.reshape(ranks, tokens, depth))


def combine_body(spread_ref, rows_ref, field_ref):
    rows = rows_ref[...].astype(jnp.float32)
    width = rows.shape[0] * SLOTS
    for side in range(2):
        part = rows[:, side * SLOTS : (side + 1) * SLOTS].reshape(width, -1).astype(jnp.bfloat16)
        field_ref[side] = wide_dot(spread_ref[side], part).astype(jnp.bfloat16)


def combine(spread, rows):
    ranks, tokens, width = spread.shape
    groups, depth = width // SLOTS, rows.shape[2]
    field = pl.pallas_call(
        combine_body,
        grid=(ranks // 2, depth // BLOCK),
        in_specs=[
            pl.BlockSpec((2, tokens, width), lambda i, k: (i, 0, 0)),
            pl.BlockSpec((groups, 2 * SLOTS, BLOCK), lambda i, k: (0, i, k)),
        ],
        out_specs=pl.BlockSpec((2, tokens, BLOCK), lambda i, k: (i, 0, k)),
        out_shape=jax.ShapeDtypeStruct((ranks, tokens, depth), jnp.bfloat16),
    )(spread, rows)
    return field.reshape(ranks * tokens, depth)


def scatter_all(field):
    part = lax.psum_scatter(field, "col", scatter_dimension=0, tiled=True)
    return lax.psum_scatter(part, "row", scatter_dimension=0, tiled=True)


def pieces_of(ranks, depth):
    count = max(1, ranks // 32)
    step = depth // count
    return [(at, at + step) for at in range(0, depth, step)]


def gather_rows(pick, field):
    rows = []
    for start, stop in pieces_of(pick.shape[0], field.shape[1]):
        part = field[:, start:stop]
        if rows:
            part = lax.optimization_barrier((part, rows[-1]))[0]
        whole = lax.all_gather(part, ("col", "row"), axis=0, tiled=True)
        rows.append(dispatch(pick, whole))
    return rows[0] if len(rows) == 1 else jnp.concatenate(rows, axis=2)


def return_rows(spread, rows):
    sums = []
    for start, stop in pieces_of(spread.shape[0], rows.shape[2]):
        part = rows[:, :, start:stop]
        if sums:
            part = lax.optimization_barrier((part, sums[-1]))[0]
        sums.append(scatter_all(combine(spread, part)))
    return sums[0] if len(sums) == 1 else jnp.concatenate(sums, axis=1)


MESH = pl.DeviceIdType.MESH


def seat():
    r, c = lax.axis_index("row"), lax.axis_index("col")
    y, x = r // 2, r % 2
    z, core = c // 2, c % 2
    first = y * (1 - core) + x * core
    second = x * (1 - core) + y * core
    return r, c, y, x, z, core, first, second


def partners():
    r, c, y, x, z, core, first, second = seat()
    pair = (r, z * 2 + (1 - core))
    flip_y = (1 - y) * 2 + x
    flip_x = y * 2 + (1 - x)
    along_first = (flip_y * (1 - core) + flip_x * core, c)
    along_second = (flip_x * (1 - core) + flip_y * core, c)
    up = [(r, ((z + k) % 4) * 2 + core) for k in range(1, 4)]
    return pair, along_first, along_second, up


RANKS = 32


def nth(offset):
    spot = (lax.axis_index("col") * 4 + lax.axis_index("row") + offset) % RANKS
    return spot, (spot % 4, spot // 4)


def meet():
    barrier = pltpu.get_barrier_semaphore()

    @pl.loop(1, RANKS)
    def _(offset):
        pl.semaphore_signal(barrier, inc=1, device_id=nth(offset)[1], device_id_type=MESH)

    pl.semaphore_wait(barrier, RANKS - 1)


def small_copy(src_of, small_all, small_send, small_recv, offset):
    spot, device = nth(offset)
    return send(
        src_of(spot), small_all.at[nth(0)[0]], small_send.at[offset], small_recv.at[offset], device
    )


def row_of(core, first, second):
    y = first * (1 - core) + second * core
    x = second * (1 - core) + first * core
    return y, x


def send(src, dst, send_sem, recv_sem, device):
    return pltpu.make_async_remote_copy(
        src_ref=src, dst_ref=dst, send_sem=send_sem, recv_sem=recv_sem, device_id=device, device_id_type=MESH
    )


GSTEPS = 4
QUEUE = (2, 1, 3)
ARRIVE = (1, 3, 2)


def spread_out(own_ref, all_ref, sems):
    r, c, y, x, z, core, first, second = seat()
    pair, along_first, along_second, up = partners()
    here_sem, z_send, z_recv, g_send, g_recv, f_send, f_recv, p_send, p_recv = sems
    step = own_ref.shape[0] // GSTEPS

    def rows(q):
        return pl.ds(pl.multiple_of(q * step, step), step)

    def place(k, s, f, q):
        sec = second * (1 - s) + (1 - second) * s
        fir = first * (1 - f) + (1 - first) * f
        yy, xx = row_of(core, fir, sec)
        return all_ref.at[(z + 4 - k) % 4, core, yy, xx, rows(q)]

    def z_copy(k, q):
        return send(
            own_ref.at[rows(q)], place(0, 0, 0, q), z_send.at[k - 1, q], z_recv.at[k - 1, q], up[k - 1]
        )

    def g_copy(k, q, src):
        return send(src, place(k, 0, 0, q), g_send.at[k, q], g_recv.at[k, q], along_second)

    def f_copy(k, s, q, src):
        return send(src, place(k, s, 0, q), f_send.at[s, k, q], f_recv.at[s, k, q], along_first)

    def p_copy(k, s, f, q, src):
        return send(src, place(k, s, f, q), p_send.at[f, s, k, q], p_recv.at[f, s, k, q], pair)

    here = pltpu.make_async_copy(own_ref, all_ref.at[z, core, y, x], here_sem)

    def begin():
        here.start()

        @pl.loop(0, GSTEPS)
        def _(q):
            src = own_ref.at[rows(q)]
            for k in QUEUE:
                z_copy(k, q).start()
            g_copy(0, q, src).start()
            f_copy(0, 0, q, src).start()
            p_copy(0, 0, 0, q, src).start()

    def forward(q):
        for k in ARRIVE:
            z_copy(k, q).wait_recv()
            src = place(k, 0, 0, q)
            g_copy(k, q, src).start()
            f_copy(k, 0, q, src).start()
            p_copy(k, 0, 0, q, src).start()
        for k in (0, *ARRIVE):
            src = place(k, 1, 0, q)
            g_copy(k, q, src).wait_recv()
            f_copy(k, 1, q, src).start()
            p_copy(k, 1, 0, q, src).start()
        for k in (0, *ARRIVE):
            src = place(k, 0, 1, q)
            f_copy(k, 0, q, src).wait_recv()
            p_copy(k, 0, 1, q, src).start()

    def finish():
        @pl.loop(0, GSTEPS)
        def _(q):
            for k in (0, *ARRIVE):
                src = place(k, 1, 1, q)
                f_copy(k, 1, q, src).wait_recv()
                p_copy(k, 1, 1, q, src).start()

        here.wait()

        @pl.loop(0, GSTEPS)
        def _(q):
            for k in range(4):
                src = own_ref.at[rows(q)]
                if k:
                    z_copy(k, q).wait_send()
                g_copy(k, q, src).wait_send()
                for s in range(2):
                    f_copy(k, s, q, src).wait_send()
                    for f in range(2):
                        p_copy(k, s, f, q, src).wait()

    return begin, forward, finish


def spread_sems():
    dma = pltpu.SemaphoreType.DMA
    shapes = [(3, GSTEPS), (4, GSTEPS), (2, 4, GSTEPS), (2, 2, 4, GSTEPS)]
    return [dma(())] + [dma(shape) for shape in shapes for _ in range(2)]


def small_out(small_ref, small_all, sems):
    here_sem, small_send, small_recv = sems
    local = pltpu.make_async_copy(small_ref, small_all.at[nth(0)[0]], here_sem)

    def copy(offset):
        return small_copy(lambda spot: small_ref, small_all, small_send, small_recv, offset)

    def begin():
        local.start()

        @pl.loop(1, RANKS)
        def _(offset):
            copy(offset).start()

    def finish():
        local.wait()

        @pl.loop(1, RANKS)
        def _(offset):
            copy(offset).wait()

    return begin, finish


def small_sems():
    dma = pltpu.SemaphoreType.DMA
    return [dma(()), dma((RANKS,)), dma((RANKS,))]


ANYWHERE = pl.BlockSpec(memory_space=pl.ANY)


def start_body(x_ref, q_ref, k_ref, v_ref, o_ref, pack_ref, own_ref, small_ref,
               x_all, q_all, k_all, v_all, o_all, pack_all, all_ref, small_all, *sems):
    r, c, y, x, z, core, first, second = seat()
    pair, along_first, along_second, up = partners()
    begin, forward, finish = spread_out(own_ref, all_ref, sems[:9])
    small_begin, small_finish = small_out(small_ref, small_all, sems[9:12])
    here_sem, x_send, x_recv, w_send, w_recv, v_send, v_recv = sems[12:]
    weights = [(q_ref, q_all), (k_ref, k_all), (v_ref, v_all), (o_ref, o_all), (pack_ref, pack_all)]

    def block(index, col):
        ref, whole = weights[index]
        if index == 4:
            return whole.at[col]
        if index == 3:
            width = ref.shape[1]
            return whole.at[:, pl.ds(pl.multiple_of(col * width, width), width)]
        height = ref.shape[0]
        return whole.at[pl.ds(pl.multiple_of(col * height, height), height)]

    def w_copy(index, k):
        return send(
            weights[index][0], block(index, c), w_send.at[index, k - 1], w_recv.at[index, k - 1], up[k - 1]
        )

    def pair_copy(index, k):
        col = ((z + 4 - k) % 4) * 2 + core
        src = weights[index][0] if k == 0 else block(index, col)
        return send(src, block(index, col), v_send.at[index, k], v_recv.at[index, k], pair)

    locals_ = [pltpu.make_async_copy(x_ref, x_all.at[r], here_sem.at[5])] + [
        pltpu.make_async_copy(weights[i][0], block(i, c), here_sem.at[i]) for i in range(5)
    ]
    y1, x1 = row_of(core, first, 1 - second)
    near_row = y1 * 2 + x1
    x_first = send(x_ref, x_all.at[r], x_send.at[0], x_recv.at[0], along_first)
    x_second = send(x_ref, x_all.at[r], x_send.at[1], x_recv.at[1], along_second)
    x_relay = send(x_all.at[near_row], x_all.at[near_row], x_send.at[2], x_recv.at[2], along_first)

    meet()
    small_begin()
    x_second.start()
    x_first.start()
    begin()
    for index in (4, 0, 1, 2, 3):
        for k in QUEUE:
            w_copy(index, k).start()
        pair_copy(index, 0).start()
    for item in locals_:
        item.start()
    x_second.wait_recv()
    x_relay.start()

    @pl.loop(0, GSTEPS)
    def _(q):
        forward(q)

    for index in (4, 0, 1, 2, 3):
        for k in ARRIVE:
            w_copy(index, k).wait_recv()
            pair_copy(index, k).start()
    finish()
    small_finish()
    for item in locals_:
        item.wait()
    x_first.wait()
    x_second.wait_send()
    x_relay.wait()
    for index in range(5):
        for k in range(4):
            if k:
                w_copy(index, k).wait_send()
            pair_copy(index, k).wait()


def start_near(x, weights, pack, own, small, collective_id):
    tokens, depth = own.shape
    dma = pltpu.SemaphoreType.DMA
    height, width = weights[0].shape
    shaped = lambda shape, like: jax.ShapeDtypeStruct(shape, like.dtype)
    outs = pl.pallas_call(
        start_body,
        out_shape=(
            shaped((4, *x.shape), x),
            *[shaped((8 * height, width), w) for w in weights[:3]],
            shaped((weights[3].shape[0], 8 * weights[3].shape[1]), weights[3]),
            shaped((8, *pack.shape), pack),
            shaped((4, 2, 2, 2, tokens, depth), own),
            shaped((RANKS, *small.shape), small),
        ),
        in_specs=[ANYWHERE] * 8,
        out_specs=[ANYWHERE] * 8,
        scratch_shapes=spread_sems()
        + small_sems()
        + [dma((6,)), dma((3,)), dma((3,)), dma((5, 3)), dma((5, 3)), dma((5, 4)), dma((5, 4))],
        compiler_params=pltpu.CompilerParams(collective_id=collective_id, has_side_effects=True),
    )(x, *weights, pack, own, small)
    x_all, q, k, v, o, pack_all, whole, small_all = outs
    return x_all.reshape(-1, x.shape[1]), q, k, v, o, pack_all, whole.reshape(RANKS, tokens, depth), small_all


def finish_body(field_ref, q_ref, k_ref, v_ref, o_ref, pack_ref,
                out_ref, q_out, k_out, v_out, o_out, pack_all,
                mine, first_in, second_in, total,
                q_mine, k_mine, v_mine, o_mine, q_pair, k_pair, v_pair, o_pair, q_z, k_z, v_z, o_z,
                q_sum, k_sum, v_sum, o_sum,
                load_sem, f_send, f_recv, g_send, g_recv, w_load, p_send, p_recv, z_send, z_recv, out_sem,
                *small):
    r, c, y, x, z, core, first, second = seat()
    pair, along_first, along_second, up = partners()
    here_sem, small_send, small_recv = small
    tokens, depth = out_ref.shape
    other = 1 - core
    grads = [q_ref, k_ref, v_ref, o_ref]
    kept, pairs, zs = [q_mine, k_mine, v_mine, o_mine], [q_pair, k_pair, v_pair, o_pair], [q_z, k_z, v_z, o_z]
    sums, outs = [q_sum, k_sum, v_sum, o_sum], [q_out, k_out, v_out, o_out]

    def block(index, col):
        ref = grads[index]
        if index == 3:
            width = ref.shape[1] // 8
            return ref.at[:, pl.ds(pl.multiple_of(col * width, width), width)]
        height = ref.shape[0] // 8
        return ref.at[pl.ds(pl.multiple_of(col * height, height), height)]

    def row(fir, sec):
        yy, xx = row_of(core, fir, sec)
        return yy * 2 + xx

    local = pltpu.make_async_copy(pack_ref.at[c], pack_all.at[nth(0)[0]], here_sem)

    def small_of(offset):
        return small_copy(lambda spot: pack_ref.at[spot // 4], pack_all, small_send, small_recv, offset)

    def load(fir, sec):
        return pltpu.make_async_copy(field_ref.at[row(fir, sec)], mine.at[fir, sec], load_sem.at[fir, sec])

    def f_copy(sec):
        return send(field_ref.at[row(1 - first, sec)], first_in.at[sec], f_send.at[sec], f_recv.at[sec], along_first)

    g_copy = send(mine.at[first, 1 - second], second_in, g_send, g_recv, along_second)

    def w_load_copy(index, zz):
        return pltpu.make_async_copy(block(index, zz * 2 + core), kept[index].at[zz], w_load.at[index, zz])

    def w_give(index, zz):
        return send(
            block(index, zz * 2 + other), pairs[index].at[zz], p_send.at[index, zz], p_recv.at[index, zz], pair
        )

    def w_z(index, k):
        return send(
            kept[index].at[(z + k) % 4], zs[index].at[k - 1], z_send.at[index, k - 1], z_recv.at[index, k - 1], up[k - 1]
        )

    def add(ref, extras):
        @pl.loop(0, ref.shape[0] // TILE)
        def _(t):
            here = pl.ds(pl.multiple_of(t * TILE, TILE), TILE)
            value = ref[here].astype(jnp.float32)
            for extra in extras:
                value = value + extra[here].astype(jnp.float32)
            ref[here] = value.astype(jnp.bfloat16)

    def add_out(ref, extras, result):
        @pl.loop(0, ref.shape[0] // TILE)
        def _(t):
            here = pl.ds(pl.multiple_of(t * TILE, TILE), TILE)
            value = ref[here].astype(jnp.float32)
            for extra in extras:
                value = value + extra[here].astype(jnp.float32)
            result[here] = value

    meet()
    f_copy(1 - second).start()
    f_copy(second).start()
    for index in range(4):
        for k in (2, 1, 3, 0):
            w_give(index, (z + k) % 4).start()
            w_load_copy(index, (z + k) % 4).start()
    load(first, 1 - second).start()
    load(first, second).start()
    local.start()

    @pl.loop(1, RANKS)
    def _(offset):
        small_of(offset).start()

    for index in range(4):
        for k in (2, 1, 3):
            zz = (z + k) % 4
            w_load_copy(index, zz).wait()
            w_give(index, zz).wait_recv()
            add(kept[index].at[zz], [pairs[index].at[zz]])
            w_z(index, k).start()
    load(first, 1 - second).wait()
    f_copy(1 - second).wait_recv()
    add(mine.at[first, 1 - second], [first_in.at[1 - second]])
    g_copy.start()
    load(first, second).wait()
    f_copy(second).wait_recv()
    for index in range(4):
        w_load_copy(index, z).wait()
        w_give(index, z).wait_recv()
    g_copy.wait_recv()
    add_out(mine.at[first, second], [first_in.at[second], second_in], total)
    pltpu.make_async_copy(total, out_ref, out_sem.at[4]).start()
    for index in range(4):
        for k in ARRIVE:
            w_z(index, k).wait_recv()
        add_out(
            kept[index].at[z], [pairs[index].at[z]] + [zs[index].at[k] for k in range(3)], sums[index]
        )
        pltpu.make_async_copy(sums[index], outs[index], out_sem.at[index]).start()
    for sec in range(2):
        f_copy(sec).wait_send()
    g_copy.wait_send()
    for index in range(4):
        for k in range(4):
            w_give(index, (z + k) % 4).wait_send()
            if k:
                w_z(index, k).wait_send()
        pltpu.make_async_copy(sums[index], outs[index], out_sem.at[index]).wait()
    local.wait()

    @pl.loop(1, RANKS)
    def _(offset):
        small_of(offset).wait()

    pltpu.make_async_copy(total, out_ref, out_sem.at[4]).wait()


def finish_near(field, grads, pack, collective_id):
    rows_count, tokens, depth = field.shape
    dma = pltpu.SemaphoreType.DMA
    blocks = [(g.shape[0] // 8, g.shape[1]) for g in grads[:3]] + [(grads[3].shape[0], grads[3].shape[1] // 8)]
    half = lambda *shape: pltpu.VMEM(shape, jnp.bfloat16)
    return pl.pallas_call(
        finish_body,
        out_shape=(
            jax.ShapeDtypeStruct((tokens, depth), jnp.float32),
            *[jax.ShapeDtypeStruct(b, jnp.float32) for b in blocks],
            jax.ShapeDtypeStruct((RANKS, *pack.shape[1:]), pack.dtype),
        ),
        in_specs=[ANYWHERE] * 6,
        out_specs=[ANYWHERE] * 6,
        scratch_shapes=[
            half(2, 2, tokens, depth), half(2, tokens, depth), half(tokens, depth),
            pltpu.VMEM((tokens, depth), jnp.float32),
            *[half(4, *b) for b in blocks], *[half(4, *b) for b in blocks], *[half(3, *b) for b in blocks],
            *[pltpu.VMEM(b, jnp.float32) for b in blocks],
            dma((2, 2)), dma((2,)), dma((2,)), dma(()), dma(()),
            dma((4, 4)), dma((4, 4)), dma((4, 4)), dma((4, 3)), dma((4, 3)), dma((5,)),
        ]
        + small_sems(),
        compiler_params=pltpu.CompilerParams(
            collective_id=collective_id, has_side_effects=True, vmem_limit_bytes=60 * 1024 * 1024
        ),
    )(field, *grads, pack)


RSTEPS = 8
TILE = 16


def reduce_body(part_ref, small_ref, out_ref, small_all, mine, pair_in, first_in, second_in, z_in, total,
                load_sem, p_send, p_recv, f_send, f_recv, g_send, g_recv, z_send, z_recv, out_sem,
                small_here, small_send, small_recv):
    r, c, y, x, z, core, first, second = seat()
    pair, along_first, along_second, up = partners()
    tokens, depth = out_ref.shape
    step = tokens // RSTEPS
    other = 1 - core

    def rows(q):
        return pl.ds(pl.multiple_of(q * step, step), step)

    meet()

    small_local = pltpu.make_async_copy(small_ref.at[nth(0)[0]], small_all.at[nth(0)[0]], small_here)
    small_local.start()

    def small(offset):
        return small_copy(lambda spot: small_ref.at[spot], small_all, small_send, small_recv, offset)

    @pl.loop(1, RANKS)
    def _(offset):
        small(offset).start()

    def load(f, s, q):
        yy, xx = row_of(core, f, s)
        return pltpu.make_async_copy(part_ref.at[:, core, yy, xx, rows(q)], mine.at[f, s, :, rows(q)], load_sem.at[f, s, q])

    def give(f, s, q):
        yy, xx = row_of(other, f, s)
        return send(part_ref.at[:, other, yy, xx, rows(q)], pair_in.at[f, s, :, rows(q)],
                    p_send.at[f, s, q], p_recv.at[f, s, q], pair)

    def f_copy(s, q):
        return send(mine.at[1 - first, s, :, rows(q)], first_in.at[s, :, rows(q)], f_send.at[s, q], f_recv.at[s, q], along_first)

    def g_copy(q):
        return send(mine.at[first, 1 - second, :, rows(q)], second_in.at[:, rows(q)], g_send.at[q], g_recv.at[q], along_second)

    def z_copy(k, q):
        return send(mine.at[first, second, (z + k) % 4, rows(q)], z_in.at[k - 1, rows(q)],
                    z_send.at[k - 1, q], z_recv.at[k - 1, q], up[k - 1])

    def order(me_first, me_second):
        return [(1 - me_first, 1 - me_second), (1 - me_first, me_second), (me_first, 1 - me_second), (me_first, me_second)]

    @pl.loop(0, RSTEPS)
    def _(q):
        for f, s in order(second, first):
            give(f, s, q).start()
        for f, s in order(first, second):
            load(f, s, q).start()

    def add_into(f, s, q, extra):
        @pl.loop(0, 4 * (step // TILE))
        def _(t):
            zz, at = t // (step // TILE), t % (step // TILE)
            here = pl.ds(pl.multiple_of(q * step + at * TILE, TILE), TILE)
            value = mine[f, s, zz, here].astype(jnp.float32) + pair_in[f, s, zz, here].astype(jnp.float32)
            for ref in extra:
                value = value + ref[zz, here].astype(jnp.float32)
            mine[f, s, zz, here] = value.astype(jnp.bfloat16)

    def stage_first(q):
        for s in (1 - second, second):
            load(1 - first, s, q).wait()
            give(1 - first, s, q).wait_recv()
            add_into(1 - first, s, q, [])
            f_copy(s, q).start()

    def stage_second(q):
        load(first, 1 - second, q).wait()
        give(first, 1 - second, q).wait_recv()
        f_copy(1 - second, q).wait_recv()
        add_into(first, 1 - second, q, [first_in.at[1 - second]])
        g_copy(q).start()

    def stage_z(q):
        load(first, second, q).wait()
        give(first, second, q).wait_recv()
        f_copy(second, q).wait_recv()
        g_copy(q).wait_recv()
        add_into(first, second, q, [first_in.at[second], second_in])
        for k in (2, 1, 3):
            z_copy(k, q).start()

    def stage_out(q):
        for k in (1, 3, 2):
            z_copy(k, q).wait_recv()

        @pl.loop(0, step // TILE)
        def _(t):
            here = pl.ds(pl.multiple_of(q * step + t * TILE, TILE), TILE)
            value = mine[first, second, z, here].astype(jnp.float32)
            for k in range(3):
                value = value + z_in[k, here].astype(jnp.float32)
            total[here] = value

    LAG1, LAG2, LAG3 = 1, 2, 4

    @pl.loop(0, RSTEPS + LAG3)
    def _(q):
        @pl.when(q < RSTEPS)
        def _():
            stage_first(q)

        @pl.when((q >= LAG1) & (q < RSTEPS + LAG1))
        def _():
            stage_second(q - LAG1)

        @pl.when((q >= LAG2) & (q < RSTEPS + LAG2))
        def _():
            stage_z(q - LAG2)

        @pl.when(q >= LAG3)
        def _():
            stage_out(q - LAG3)

    done = pltpu.make_async_copy(total, out_ref, out_sem)
    done.start()

    @pl.loop(0, RSTEPS)
    def _(q):
        for f in range(2):
            for s in range(2):
                give(f, s, q).wait_send()
        for s in range(2):
            f_copy(s, q).wait_send()
        g_copy(q).wait_send()
        for k in (1, 2, 3):
            z_copy(k, q).wait_send()

    small_local.wait()

    @pl.loop(1, RANKS)
    def _(offset):
        small(offset).wait()

    done.wait()


def reduce_near(part, small, collective_id):
    tokens, depth = part.shape[0] // RANKS, part.shape[1]
    dma = pltpu.SemaphoreType.DMA
    return pl.pallas_call(
        reduce_body,
        out_shape=(
            jax.ShapeDtypeStruct((tokens, depth), jnp.float32),
            jax.ShapeDtypeStruct(small.shape, small.dtype),
        ),
        in_specs=[pl.BlockSpec(memory_space=pl.ANY)] * 2,
        out_specs=[pl.BlockSpec(memory_space=pl.ANY)] * 2,
        scratch_shapes=[
            pltpu.VMEM((2, 2, 4, tokens, depth), jnp.bfloat16),
            pltpu.VMEM((2, 2, 4, tokens, depth), jnp.bfloat16),
            pltpu.VMEM((2, 4, tokens, depth), jnp.bfloat16),
            pltpu.VMEM((4, tokens, depth), jnp.bfloat16),
            pltpu.VMEM((3, tokens, depth), jnp.bfloat16),
            pltpu.VMEM((tokens, depth), jnp.float32),
            dma((2, 2, RSTEPS)),
            dma((2, 2, RSTEPS)), dma((2, 2, RSTEPS)),
            dma((2, RSTEPS)), dma((2, RSTEPS)),
            dma((RSTEPS,)), dma((RSTEPS,)),
            dma((3, RSTEPS)), dma((3, RSTEPS)),
            dma(()),
            dma(()), dma((RANKS,)), dma((RANKS,)),
        ],
        compiler_params=pltpu.CompilerParams(
            collective_id=collective_id, has_side_effects=True, vmem_limit_bytes=60 * 1024 * 1024
        ),
    )(part.reshape(4, 2, 2, 2, tokens, depth), small)


def fill_rows(pick_ref, field_ref, rows_ref):
    ranks, groups = pick_ref.shape[0], rows_ref.shape[0]

    @pl.loop(0, ranks // 2, unroll=UNROLL)
    def _(i):
        parts = [
            wide_dot(pick_ref[2 * i + side], field_ref[2 * i + side]).reshape(groups, SLOTS, CHUNK)
            for side in range(2)
        ]
        here = pl.ds(pl.multiple_of(i * 2 * SLOTS, 2 * SLOTS), 2 * SLOTS)
        rows_ref[:, here] = jnp.concatenate(parts, axis=1).astype(jnp.bfloat16)


def add_products(k, rows_ref, pairs):
    groups = rows_ref.shape[0]

    def products(e, first):
        for product, total in pairs:
            term = product(rows_ref[e], e)
            if first:
                total[e] = term
            else:
                total[e] += term

    @pl.when(k == 0)
    def _():
        @pl.loop(0, groups)
        def _(e):
            products(e, True)

    @pl.when(k > 0)
    def _():
        @pl.loop(0, groups)
        def _(e):
            products(e, False)


def grads_in_body(pick_ref, field_ref, down_ref, own_ref, small_ref,
                  rows_ref, plain_ref, all_ref, small_all, total, *sems):
    begin, forward, finish = spread_out(own_ref, all_ref, sems[:9])
    small_begin, small_finish = small_out(small_ref, small_all, sems[9:])
    k, last = pl.program_id(0), pl.num_programs(0) - 1

    @pl.when(k == 0)
    def _():
        meet()
        small_begin()
        begin()

    fill_rows(pick_ref, field_ref, rows_ref)
    add_products(k, rows_ref, [(lambda rows, e: outer_cols(rows, down_ref[e]), total)])

    @pl.when(k % 2 == 1)
    def _():
        forward(k // 2)

    @pl.when(k == last)
    def _():
        pltpu.sync_copy(total, plain_ref)
        finish()
        small_finish()


def grads_in(pick, field, down, own, small, collective_id):
    ranks, width, tokens = pick.shape
    groups, depth = width // SLOTS, field.shape[-1]
    length, inner = ranks * SLOTS, down.shape[1]
    steps = depth // CHUNK
    rows, plain, whole, small_all = pl.pallas_call(
        grads_in_body,
        grid=(steps,),
        in_specs=[
            pl.BlockSpec((ranks, width, tokens), lambda k: (0, 0, 0), pipeline_mode=pl.Buffered(1)),
            pl.BlockSpec((ranks, tokens, CHUNK), lambda k: (0, 0, k)),
            pl.BlockSpec((groups, inner, CHUNK), lambda k: (0, 0, k)),
            ANYWHERE,
            ANYWHERE,
        ],
        out_specs=[pl.BlockSpec((groups, length, CHUNK), lambda k: (0, 0, k))] + [ANYWHERE] * 3,
        out_shape=[
            jax.ShapeDtypeStruct((groups, length, depth), jnp.bfloat16),
            jax.ShapeDtypeStruct((groups, length, inner), jnp.float32),
            jax.ShapeDtypeStruct((4, 2, 2, 2, *own.shape), own.dtype),
            jax.ShapeDtypeStruct((RANKS, *small.shape), small.dtype),
        ],
        scratch_shapes=[pltpu.VMEM((groups, length, inner), jnp.float32)] + spread_sems() + small_sems(),
        compiler_params=pltpu.CompilerParams(
            collective_id=collective_id, has_side_effects=True, vmem_limit_bytes=62 * 1024 * 1024
        ),
    )(pick, field, down, own, small)
    return rows, plain, whole.reshape(RANKS, *own.shape), small_all


def feed_in_body(steps, pick_ref, field_ref, gate_ref, up_ref, plain_ref, probs_ref,
                 rows_ref, act_ref, weighted_ref, grad_gate_ref, grad_up_ref, gates_ref, gate_sum, up_sum):
    k = pl.program_id(0)

    @pl.when(k < steps)
    def _():
        fill_rows(pick_ref, field_ref, rows_ref)
        add_products(
            k,
            rows_ref,
            [
                (lambda rows, e: wide_dot(rows, gate_ref[e]), gate_sum),
                (lambda rows, e: wide_dot(rows, up_ref[e]), up_sum),
            ],
        )

    @pl.when(k >= steps)
    def _():
        e = k - steps
        length = act_ref.shape[1]

        @pl.loop(0, length // 128)
        def _(t):
            here = pl.ds(pl.multiple_of(t * 128, 128), 128)
            gate_val, up_val = gate_sum[e, here], up_sum[e, here]
            plain, probs = plain_ref[0, here], probs_ref[0, here]
            sigmoid_val = jax.nn.sigmoid(gate_val)
            silu_val = gate_val * sigmoid_val
            activated = silu_val * up_val
            grad_act = plain * probs
            grad_up_ref[0, here] = (grad_act * silu_val).astype(jnp.bfloat16)
            grad_gate_ref[0, here] = (
                grad_act * up_val * (sigmoid_val * (1.0 + gate_val * (1.0 - sigmoid_val)))
            ).astype(jnp.bfloat16)
            gates_ref[0, here] = jnp.sum(activated * plain, axis=-1, keepdims=True)
            weighted_ref[0, here] = (activated * probs).astype(jnp.bfloat16)
            act_ref[0, here] = activated.astype(jnp.bfloat16)


def feed_in(pick, field, gate, up, plain, probs):
    ranks, width, tokens = pick.shape
    groups, depth = width // SLOTS, field.shape[-1]
    length, inner = ranks * SLOTS, gate.shape[2]
    steps = depth // CHUNK
    held = lambda k: jnp.minimum(k, steps - 1)
    late = lambda k: (jnp.maximum(k - steps, 0), 0, 0)
    wide = pl.BlockSpec((1, length, inner), late)
    thin = pl.BlockSpec((1, length, 1), late)
    low = jax.ShapeDtypeStruct((groups, length, inner), jnp.bfloat16)
    return pl.pallas_call(
        functools.partial(feed_in_body, steps),
        grid=(steps + groups,),
        in_specs=[
            pl.BlockSpec((ranks, width, tokens), lambda k: (0, 0, 0), pipeline_mode=pl.Buffered(1)),
            pl.BlockSpec((ranks, tokens, CHUNK), lambda k: (0, 0, held(k))),
            pl.BlockSpec((groups, CHUNK, inner), lambda k: (0, held(k), 0)),
            pl.BlockSpec((groups, CHUNK, inner), lambda k: (0, held(k), 0)),
            wide,
            thin,
        ],
        out_specs=[pl.BlockSpec((groups, length, CHUNK), lambda k: (0, 0, held(k))), wide, wide, wide, wide, thin],
        out_shape=[
            jax.ShapeDtypeStruct((groups, length, depth), jnp.bfloat16),
            low, low, low, low,
            jax.ShapeDtypeStruct((groups, length, 1), jnp.float32),
        ],
        scratch_shapes=[pltpu.VMEM((groups, length, inner), jnp.float32)] * 2,
        compiler_params=pltpu.CompilerParams(vmem_limit_bytes=63 * 1024 * 1024),
        cost_estimate=pl.CostEstimate(
            flops=2 * groups * length * depth * (tokens + 2 * inner), bytes_accessed=120 << 20, transcendentals=0
        ),
    )(pick, field, gate, up, plain, probs)


def restore_body(flipped, spread_ref, *refs):
    count = len(flipped)
    lefts, weights, field_ref, rows = refs[:count], refs[count:2*count], refs[2*count], refs[2*count+1]
    groups = rows.shape[0]
    ranks = spread_ref.shape[0]

    @pl.loop(0, groups)
    def _(e):
        total = None
        for left, weight, flip in zip(lefts, weights, flipped):
            term = outer_cols(left[e], weight[e]) if flip else wide_dot(left[e], weight[e])
            total = term if total is None else total + term
        rows[e] = total

    @pl.loop(0, ranks, unroll=2*UNROLL)
    def _(s):
        part = rows[:, pl.ds(pl.multiple_of(s * SLOTS, SLOTS), SLOTS)].reshape(groups * SLOTS, CHUNK).astype(jnp.bfloat16)
        field_ref[s] = wide_dot(spread_ref[s], part).astype(jnp.bfloat16)

def restore(spread, lefts, weights, flipped):
    ranks, tokens, width = spread.shape
    groups = width // SLOTS
    length = ranks * SLOTS
    inner = lefts[0].shape[2]
    depth = weights[0].shape[1] if flipped[0] else weights[0].shape[2]
    wspecs = [pl.BlockSpec((groups, CHUNK, inner), lambda k: (0, k, 0)) if f else pl.BlockSpec((groups, inner, CHUNK), lambda k: (0, 0, k)) for f in flipped]
    flops = 2 * groups * length * depth * (tokens + inner * len(weights))
    field = pl.pallas_call(
        functools.partial(restore_body, flipped),
        grid=(depth // CHUNK,),
        in_specs=[pl.BlockSpec((ranks, tokens, width), lambda k: (0, 0, 0), pipeline_mode=pl.Buffered(1))]
        + [pl.BlockSpec((groups, length, inner), lambda k: (0, 0, 0), pipeline_mode=pl.Buffered(1))] * len(lefts) + wspecs,
        out_specs=pl.BlockSpec((ranks, tokens, CHUNK), lambda k: (0, 0, k)),
        out_shape=jax.ShapeDtypeStruct((ranks, tokens, depth), jnp.bfloat16),
        scratch_shapes=[pltpu.VMEM((groups, length, CHUNK), jnp.float32)],
        compiler_params=pltpu.CompilerParams(vmem_limit_bytes=63 * 1024 * 1024),
        cost_estimate=pl.CostEstimate(flops=flops, bytes_accessed=60 << 20, transcendentals=0),
    )(spread, *lefts, *weights)
    return field.reshape(ranks * tokens, depth)


def local(
    layer_input,
    cotangent,
    expert_index,
    attention_gain,
    query_gain,
    key_gain,
    query_weight,
    key_weight,
    value_weight,
    output_weight,
    feed_gain,
    router_weight,
    gate_weight,
    up_weight,
    down_weight,
):
    tokens = layer_input.shape[0]
    rows_count = lax.axis_size("row")
    near = rows_count == 4 and lax.axis_size("col") == 8
    if near:
        head_part = query_gain.shape[0]
        slice_width = attention_gain.shape[0]
        pack = jnp.concatenate(
            [attention_gain, feed_gain, query_gain, key_gain, router_weight.reshape(-1)]
        )
        pack = jnp.pad(pack, (0, PACK_ROWS * 128 - pack.shape[0])).reshape(PACK_ROWS, 128)
        (
            sequence, query_full, key_full, value_full, output_full, pack_all, cotangent_all, index_all
        ) = start_near(
            layer_input,
            [query_weight, key_weight, value_weight, output_weight],
            pack,
            cotangent,
            expert_index.T,
            1,
        )
        index_all = jnp.swapaxes(index_all, 1, 2)
        pack_all = pack_all.reshape(8, -1)
        ends = [slice_width, 2 * slice_width, 2 * slice_width + head_part, 2 * slice_width + 2 * head_part]
        attention_full = pack_all[:, : ends[0]].reshape(-1)
        feed_full = pack_all[:, ends[0] : ends[1]].reshape(-1)
        query_scale_w = pack_all[:, ends[1] : ends[2]].reshape(-1)
        key_scale_w = pack_all[:, ends[2] : ends[3]].reshape(-1)
        router_full = pack_all[:, ends[3] : ends[3] + router_weight.size].reshape(
            -1, router_weight.shape[1]
        )
    else:
        (
            attention_full,
            query_scale_w,
            key_scale_w,
            query_full,
            key_full,
            value_full,
            output_full,
            feed_full,
            router_full,
        ) = (
            lax.all_gather(attention_gain, "col", axis=0, tiled=True),
            lax.all_gather(query_gain, "col", axis=0, tiled=True),
            lax.all_gather(key_gain, "col", axis=0, tiled=True),
            lax.all_gather(query_weight, "col", axis=0, tiled=True),
            lax.all_gather(key_weight, "col", axis=0, tiled=True),
            lax.all_gather(value_weight, "col", axis=0, tiled=True),
            lax.all_gather(output_weight, "col", axis=1, tiled=True),
            lax.all_gather(feed_gain, "col", axis=0, tiled=True),
            lax.all_gather(router_weight, "col", axis=0, tiled=True),
        )
        sequence = lax.all_gather(layer_input, "row", axis=0, tiled=True)
    length = sequence.shape[0]
    model_width = sequence.shape[1]
    local_width = query_full.shape[1]
    local_heads = local_width // HD
    seq_float = sequence.astype(jnp.float32)
    seq_scale = rms_scale(seq_float)
    attention_float = attention_full.astype(jnp.float32)
    normed = (seq_float * seq_scale * attention_float).astype(jnp.bfloat16)
    query_raw = wide_dot(normed, query_full)
    key_raw = wide_dot(normed, key_full)
    value_heads = wide_dot(normed, value_full).astype(jnp.bfloat16).reshape(length, local_heads, HD)
    query_total, key_total = lax.psum(
        (jnp.sum(query_raw * query_raw, axis=-1), jnp.sum(key_raw * key_raw, axis=-1)), "row"
    )
    query_rs = lax.rsqrt(query_total / model_width + EPS)[:, None]
    key_rs = lax.rsqrt(key_total / model_width + EPS)[:, None]
    query_gain_f = query_scale_w.astype(jnp.float32)
    key_gain_f = key_scale_w.astype(jnp.float32)
    cosine, sine_table = rope_tables(length)
    queries = rotate(
        (query_raw * query_rs * query_gain_f).reshape(length, local_heads, HD), cosine, sine_table
    ).astype(jnp.bfloat16)
    keys_rotated = rotate(
        (key_raw * key_rs * key_gain_f).reshape(length, local_heads, HD), cosine, sine_table
    ).astype(jnp.bfloat16)
    block_rows = min(512, length)
    starts = jnp.arange(length // block_rows, dtype=jnp.int32) * block_rows
    key_position = jnp.arange(length, dtype=jnp.int32)
    score_scale = HD ** (-0.5)

    def block_scores(offset):
        query_rows = lax.dynamic_slice_in_dim(queries, offset, block_rows, 0)
        scores = (
            jnp.einsum("qhd,khd->hqk", query_rows, keys_rotated, preferred_element_type=jnp.float32)
            * score_scale
        )
        query_position = offset + jnp.arange(block_rows, dtype=jnp.int32)
        allowed = query_position[:, None] >= key_position[None, :]
        return (query_rows, jnp.where(allowed[None, :, :], scores, MASKED))

    def forward_block(offset):
        query_rows, scores = block_scores(offset)
        row_top = jnp.max(scores, axis=-1, keepdims=True)
        exponent = jnp.exp(scores - row_top)
        row_total = jnp.sum(exponent, axis=-1, keepdims=True)
        weights = (exponent / row_total).astype(jnp.bfloat16)
        mixed_block = jnp.einsum(
            "hqk,khd->qhd", weights, value_heads, preferred_element_type=jnp.float32
        )
        return (mixed_block, (row_top + jnp.log(row_total))[..., 0])

    mixed_blocks, lse_blocks = lax.map(forward_block, starts)
    mixed_heads = mixed_blocks.reshape(length, local_width).astype(jnp.bfloat16)
    lse_all = jnp.moveaxis(lse_blocks, 0, 1).reshape(local_heads, length)
    branch = lax.psum_scatter(
        wide_dot(mixed_heads, output_full).astype(jnp.bfloat16), "row", scatter_dimension=0, tiled=True
    ).astype(jnp.float32)
    hidden = layer_input.astype(jnp.float32) + branch
    feed_scale = rms_scale(hidden)
    feed_float = feed_full.astype(jnp.float32)
    feed_normed = (hidden * feed_scale * feed_float).astype(jnp.bfloat16)
    logits = wide_dot(feed_normed, router_full)
    logit_top = jnp.max(logits, axis=-1, keepdims=True)
    logit_exp = jnp.exp(logits - logit_top)
    router_probs = logit_exp / jnp.sum(logit_exp, axis=-1, keepdims=True)
    experts = router_full.shape[1]
    experts_local = gate_weight.shape[0]
    ranks = lax.axis_size("col") * rows_count
    gate_hits = expert_index[:, :, None] == jnp.arange(experts, dtype=jnp.int32)
    gate_probs = jnp.sum(jnp.where(gate_hits, router_probs[:, None, :], 0.0), axis=-1)

    if not near:
        index_all = lax.all_gather(expert_index, ("col", "row"), axis=0, tiled=True)
    own = (index_all - lax.axis_index("col") * experts_local).reshape(ranks, tokens, -1)
    matches = own[..., None] == jnp.arange(experts_local, dtype=jnp.int32)
    hit = jnp.sum(matches.astype(jnp.float32), axis=2)
    earlier = jnp.tril(jnp.ones((tokens, tokens), jnp.bfloat16), -1)
    rank = jnp.einsum(
        "tu,sue->ste", earlier, hit.astype(jnp.bfloat16), preferred_element_type=jnp.float32
    )
    slot = jnp.where(hit > 0, rank, -1.0)
    places = jnp.arange(SLOTS, dtype=jnp.float32)
    slot_t = jnp.swapaxes(slot, 1, 2)
    width = experts_local * SLOTS
    picked = slot_t[:, :, None, :] == places[None, None, :, None]
    pick = picked.astype(jnp.bfloat16).reshape(ranks, width, tokens)
    lanes = jnp.arange(width, dtype=jnp.int32)
    widen = (lanes[None, :] // SLOTS == jnp.arange(experts_local)[:, None]).astype(jnp.bfloat16)
    spread = jnp.einsum(
        "ste,ew->stw", slot.astype(jnp.bfloat16), widen, preferred_element_type=jnp.float32
    ) == (lanes % SLOTS).astype(jnp.float32)
    spread_plain = spread.astype(jnp.bfloat16)

    def weigh(probs_all):
        probs_own = jnp.sum(
            jnp.where(matches, probs_all.reshape(ranks, tokens, -1, 1), 0.0), axis=2
        )
        probs_wide = jnp.einsum(
            "ste,ew->stw", probs_own.astype(jnp.bfloat16), widen, preferred_element_type=jnp.float32
        )
        spread_probs = jnp.where(spread, probs_wide, 0.0).astype(jnp.bfloat16)
        probs_t = jnp.swapaxes(probs_own, 1, 2)
        row_probs = jnp.sum(jnp.where(picked, probs_t[:, :, None, :], 0.0), axis=-1)
        row_probs = jnp.swapaxes(row_probs, 0, 1).reshape(experts_local, ranks * SLOTS, 1)
        return spread_probs, row_probs

    if near:
        expert_grads, plain_act, feed_all, probs_all = grads_in(
            pick, cotangent_all, down_weight, feed_normed, gate_probs.T, 2
        )
        spread_probs, row_probs = weigh(jnp.swapaxes(probs_all, 1, 2))
        expert_rows, activated, weighted_act, grad_gate, grad_up, row_gates = feed_in(
            pick, feed_all, gate_weight, up_weight, plain_act, row_probs
        )
    else:
        probs_all = lax.all_gather(gate_probs, ("col", "row"), axis=0, tiled=True)
        spread_probs, row_probs = weigh(probs_all)
        expert_grads = gather_rows(pick, cotangent)
        expert_rows = gather_rows(pick, feed_normed)
        gate_val = jnp.einsum(
            "erd,edf->erf", expert_rows, gate_weight, preferred_element_type=jnp.float32
        )
        up_val = jnp.einsum(
            "erd,edf->erf", expert_rows, up_weight, preferred_element_type=jnp.float32
        )
        plain_act = jnp.einsum(
            "erd,efd->erf", expert_grads, down_weight, preferred_element_type=jnp.float32
        )
        sigmoid_val = jax.nn.sigmoid(gate_val)
        silu_val = gate_val * sigmoid_val
        activated = silu_val * up_val
        grad_act = plain_act * row_probs
        grad_up = (grad_act * silu_val).astype(jnp.bfloat16)
        grad_gate = (
            grad_act * up_val * sigmoid_val * (1.0 + gate_val * (1.0 - sigmoid_val))
        ).astype(jnp.bfloat16)
        row_gates = jnp.sum(activated * plain_act, axis=-1)
        weighted_act = (activated * row_probs).astype(jnp.bfloat16)
        activated = activated.astype(jnp.bfloat16)
    row_gates = jnp.swapaxes(row_gates.reshape(experts_local, ranks, SLOTS), 0, 1)
    own_gates = jnp.sum(jnp.where(picked, row_gates[..., None], 0.0), axis=2)
    if near:
        grad_feed_part = restore(
            spread_plain, [grad_gate, grad_up], [gate_weight, up_weight], (True, True)
        )
        grad_feed, gates_in = reduce_near(grad_feed_part, own_gates, 3)
        gates_in = jnp.sum(gates_in.reshape(-1, rows_count, experts_local, tokens), axis=1)
        grad_probs = gates_in.reshape(experts, tokens).T
        mixture_part = restore(spread_probs, [activated], [down_weight], (False,))
        mixture = reduce_near(mixture_part, own_gates, 3)[0]
    else:
        own_gates = lax.psum_scatter(
            jnp.swapaxes(own_gates, 1, 2).reshape(-1, rows_count, tokens, experts_local),
            "row",
            scatter_dimension=1,
        )
        grad_probs = lax.all_to_all(own_gates, "col", split_axis=0, concat_axis=2, tiled=True)[0]
        back_rows = (
            jnp.einsum("erf,edf->erd", grad_gate, gate_weight, preferred_element_type=jnp.float32)
            + jnp.einsum("erf,edf->erd", grad_up, up_weight, preferred_element_type=jnp.float32)
        ).astype(jnp.bfloat16)
        grad_feed = return_rows(spread_plain, back_rows).astype(jnp.float32)
        out_rows = jnp.einsum(
            "erf,efd->erd", activated, down_weight, preferred_element_type=jnp.float32
        ).astype(jnp.bfloat16)
        mixture = return_rows(spread_probs, out_rows).astype(jnp.float32)
    layer_output = hidden + mixture
    grad_gate_weight = jnp.einsum(
        "erd,erf->edf", expert_rows, grad_gate, preferred_element_type=jnp.float32
    )
    grad_up_weight = jnp.einsum(
        "erd,erf->edf", expert_rows, grad_up, preferred_element_type=jnp.float32
    )
    grad_down_weight = jnp.einsum(
        "erf,erd->efd", weighted_act, expert_grads, preferred_element_type=jnp.float32
    )
    grad_out = cotangent.astype(jnp.float32)
    grad_logits = (
        router_probs * (grad_probs - jnp.sum(router_probs * grad_probs, axis=-1, keepdims=True))
    ).astype(jnp.bfloat16)
    router_grad = inner_rows(feed_normed, grad_logits)
    grad_feed = grad_feed + outer_cols(grad_logits, router_full)
    feed_gain_term = jnp.sum(grad_feed * hidden * feed_scale, axis=0)
    feed_weighted = grad_feed * feed_float
    grad_hidden = (
        grad_out
        + feed_scale * feed_weighted
        - hidden * feed_scale**3 * jnp.mean(feed_weighted * hidden, axis=-1, keepdims=True)
    )
    grad_branch = lax.all_gather(grad_hidden.astype(jnp.bfloat16), "row", axis=0, tiled=True)
    output_grad = inner_rows(mixed_heads, grad_branch)
    grad_mixed = (
        outer_cols(grad_branch, output_full).astype(jnp.bfloat16).reshape(length, local_heads, HD)
    )

    def backward_block(carry, offset):
        grad_keys, grad_values = carry
        query_rows, scores = block_scores(offset)
        lse_rows = lax.dynamic_slice_in_dim(lse_all, offset, block_rows, 1)
        probs_block = jnp.exp(scores - lse_rows[:, :, None])
        weights_low = probs_block.astype(jnp.bfloat16)
        grad_rows_out = lax.dynamic_slice_in_dim(grad_mixed, offset, block_rows, 0)
        grad_weights = jnp.einsum(
            "qhd,khd->hqk", grad_rows_out, value_heads, preferred_element_type=jnp.float32
        )
        grad_values = grad_values + jnp.einsum(
            "hqk,qhd->khd", weights_low, grad_rows_out, preferred_element_type=jnp.float32
        )
        delta_rows = jnp.sum(probs_block * grad_weights, axis=-1, keepdims=True)
        grad_scores = (probs_block * (grad_weights - delta_rows)).astype(jnp.bfloat16)
        grad_query_block = (
            jnp.einsum(
                "hqk,khd->qhd", grad_scores, keys_rotated, preferred_element_type=jnp.float32
            )
            * score_scale
        )
        grad_keys = (
            grad_keys
            + jnp.einsum(
                "hqk,qhd->khd", grad_scores, query_rows, preferred_element_type=jnp.float32
            )
            * score_scale
        )
        return ((grad_keys, grad_values), grad_query_block)

    zero_heads = jnp.zeros((length, local_heads, HD), jnp.float32)
    (grad_keys, grad_values), grad_query_blocks = lax.scan(
        backward_block, (zero_heads, zero_heads), starts
    )
    grad_queries = grad_query_blocks.reshape(length, local_heads, HD)
    grad_query_normed = unrotate(grad_queries, cosine, sine_table).reshape(length, local_width)
    grad_key_normed = unrotate(grad_keys, cosine, sine_table).reshape(length, local_width)
    grad_value_low = grad_values.reshape(length, local_width).astype(jnp.bfloat16)
    query_weighted = grad_query_normed * query_gain_f
    key_weighted = grad_key_normed * key_gain_f
    query_gain_term = jnp.sum(grad_query_normed * query_raw * query_rs, axis=0)
    key_gain_term = jnp.sum(grad_key_normed * key_raw * key_rs, axis=0)
    query_inner, key_inner = (
        lax.psum(jnp.sum(query_weighted * query_raw, axis=-1).astype(jnp.bfloat16), "row").astype(
            jnp.float32
        ),
        lax.psum(jnp.sum(key_weighted * key_raw, axis=-1).astype(jnp.bfloat16), "row").astype(
            jnp.float32
        ),
    )
    grad_query_raw = (
        query_rs * query_weighted - query_raw * query_rs**3 * (query_inner / model_width)[:, None]
    ).astype(jnp.bfloat16)
    grad_key_raw = (
        key_rs * key_weighted - key_raw * key_rs**3 * (key_inner / model_width)[:, None]
    ).astype(jnp.bfloat16)
    query_grad = inner_rows(normed, grad_query_raw)
    key_grad = inner_rows(normed, grad_key_raw)
    value_grad = inner_rows(normed, grad_value_low)
    grad_normed = (
        outer_cols(grad_query_raw, query_full)
        + outer_cols(grad_key_raw, key_full)
        + outer_cols(grad_value_low, value_full)
    )
    attention_weighted = grad_normed * attention_float
    grad_seq_part = seq_scale * attention_weighted - seq_float * seq_scale**3 * jnp.mean(
        attention_weighted * seq_float, axis=-1, keepdims=True
    )
    attention_gain_term = jnp.sum(grad_normed * seq_float * seq_scale, axis=0)
    if near:
        cols = lax.axis_size("col")
        pack = jnp.concatenate(
            [
                attention_gain_term.reshape(cols, -1),
                feed_gain_term.reshape(cols, -1),
                query_gain_term.reshape(cols, -1),
                key_gain_term.reshape(cols, -1),
                router_grad.reshape(cols, -1),
            ],
            axis=1,
        )
        pack = jnp.pad(pack, ((0, 0), (0, PACK_ROWS * 128 - pack.shape[1])))
        pack = pack.astype(jnp.bfloat16).reshape(cols, PACK_ROWS, 128)
        (
            summed, grad_query_weight, grad_key_weight, grad_value_weight, grad_output_weight, packs
        ) = finish_near(
            grad_seq_part.astype(jnp.bfloat16).reshape(rows_count, tokens, model_width),
            [grad.astype(jnp.bfloat16) for grad in (query_grad, key_grad, value_grad, output_grad)],
            pack,
            4,
        )
        input_grad = grad_hidden + summed
        packs = packs.reshape(cols, rows_count, -1).astype(jnp.float32)
        whole = jnp.sum(packs, axis=(0, 1))
        heads_sum = jnp.sum(
            lax.dynamic_index_in_dim(packs, lax.axis_index("row"), 1, keepdims=False), axis=0
        )
        grad_attention_gain = whole[: ends[0]]
        grad_feed_gain = whole[ends[0] : ends[1]]
        grad_query_gain = heads_sum[ends[1] : ends[2]]
        grad_key_gain = heads_sum[ends[2] : ends[3]]
        grad_router_weight = whole[ends[3] : ends[3] + router_weight.size].reshape(router_weight.shape)
    else:
        stacked = jnp.concatenate(
            [
                grad_seq_part.reshape(rows_count, tokens, model_width),
                jnp.broadcast_to(attention_gain_term[None, None, :], (rows_count, 1, model_width)),
            ],
            axis=1,
        ).reshape(rows_count * (tokens + 1), model_width)
        summed = lax.psum_scatter(
            stacked.astype(jnp.bfloat16), "row", scatter_dimension=0, tiled=True
        ).astype(jnp.float32)
        input_grad = grad_hidden + summed[:tokens]
        attention_gain_total = summed[tokens]
        feed_gain_total, router_total = (
            lax.psum(feed_gain_term.astype(jnp.bfloat16), "row").astype(jnp.float32),
            lax.psum(router_grad.astype(jnp.bfloat16), "row").astype(jnp.float32),
        )
        (
            grad_attention_gain,
            grad_query_gain,
            grad_key_gain,
            grad_query_weight,
            grad_key_weight,
            grad_value_weight,
            grad_output_weight,
            grad_feed_gain,
            grad_router_weight,
        ) = (
            lax.psum_scatter(
                attention_gain_total.astype(jnp.bfloat16), "col", scatter_dimension=0, tiled=True
            ).astype(jnp.float32),
            lax.psum_scatter(
                query_gain_term.astype(jnp.bfloat16), "col", scatter_dimension=0, tiled=True
            ).astype(jnp.float32),
            lax.psum_scatter(
                key_gain_term.astype(jnp.bfloat16), "col", scatter_dimension=0, tiled=True
            ).astype(jnp.float32),
            lax.psum_scatter(
                query_grad.astype(jnp.bfloat16), "col", scatter_dimension=0, tiled=True
            ).astype(jnp.float32),
            lax.psum_scatter(
                key_grad.astype(jnp.bfloat16), "col", scatter_dimension=0, tiled=True
            ).astype(jnp.float32),
            lax.psum_scatter(
                value_grad.astype(jnp.bfloat16), "col", scatter_dimension=0, tiled=True
            ).astype(jnp.float32),
            lax.psum_scatter(
                output_grad.astype(jnp.bfloat16), "col", scatter_dimension=1, tiled=True
            ).astype(jnp.float32),
            lax.psum_scatter(
                feed_gain_total.astype(jnp.bfloat16), "col", scatter_dimension=0, tiled=True
            ).astype(jnp.float32),
            lax.psum_scatter(
                router_total.astype(jnp.bfloat16), "col", scatter_dimension=0, tiled=True
            ).astype(jnp.float32),
        )
    return (
        layer_output,
        input_grad,
        grad_attention_gain,
        grad_query_gain,
        grad_key_gain,
        grad_query_weight,
        grad_key_weight,
        grad_value_weight,
        grad_output_weight,
        grad_feed_gain,
        grad_router_weight,
        grad_gate_weight,
        grad_up_weight,
        grad_down_weight,
    )


def solution(mesh):
    placed = (
        P(("col", "row"), None),
        P(("col", "row"), None),
        P(("col", "row"), None),
        P("col"),
        P(("row", "col")),
        P(("row", "col")),
        P("col", "row"),
        P("col", "row"),
        P("col", "row"),
        P("row", "col"),
        P("col"),
        P("col", None),
        P("col", None, "row"),
        P("col", None, "row"),
        P("col", "row", None),
    )
    return jax.shard_map(
        local,
        mesh=mesh,
        in_specs=placed,
        out_specs=(
            P(("col", "row"), None),
            P(("col", "row"), None),
            P("col"),
            P(("row", "col")),
            P(("row", "col")),
            P("col", "row"),
            P("col", "row"),
            P("col", "row"),
            P("row", "col"),
            P("col"),
            P("col", None),
            P("col", None, "row"),
            P("col", None, "row"),
            P("col", "row", None),
        ),
        check_vma=False,
    )
```

```python
import functools

import jax
import jax.numpy as jnp
from jax import lax
from jax.experimental import pallas as pl
from jax.experimental.pallas import tpu as pltpu
from jax.sharding import PartitionSpec as P

HD = 128
SLOTS = 40
BLOCK = 512
CHUNK = 256
UNROLL = 4
PACK_ROWS = 144


EPS = 1e-05
THETA = 10000.0
MASKED = -1e30


def wide_dot(left, right):
    return jnp.dot(left, right, preferred_element_type=jnp.float32)


def inner_rows(left, right):
    return lax.dot_general(
        left, right, (((0,), (0,)), ((), ())), preferred_element_type=jnp.float32
    )


def outer_cols(left, right):
    return lax.dot_general(
        left, right, (((1,), (1,)), ((), ())), preferred_element_type=jnp.float32
    )


def rms_scale(field):
    return lax.rsqrt(jnp.mean(field * field, axis=-1, keepdims=True) + EPS)


def rope_tables(length):
    half_size = HD // 2
    freqs = THETA ** (-(jnp.arange(half_size, dtype=jnp.float32) * 2.0) / HD)
    angles = jnp.arange(length, dtype=jnp.float32)[:, None] * freqs[None, :]
    cosine = jnp.concatenate([jnp.cos(angles), jnp.cos(angles)], axis=-1)[:, None, :]
    sine_table = jnp.concatenate([jnp.sin(angles), jnp.sin(angles)], axis=-1)[:, None, :]
    return (cosine, sine_table)


def rotate(field, cosine, sine_table):
    half_size = field.shape[-1] // 2
    turned = jnp.concatenate([-field[..., half_size:], field[..., :half_size]], axis=-1)
    return field * cosine + turned * sine_table


def unrotate(gradient, cosine, sine_table):
    half_size = gradient.shape[-1] // 2
    moved = gradient * sine_table
    back_turned = jnp.concatenate([moved[..., half_size:], -moved[..., :half_size]], axis=-1)
    return gradient * cosine + back_turned


def dispatch_body(pick_ref, field_ref, rows_ref):
    groups = rows_ref.shape[0]
    first = wide_dot(pick_ref[0], field_ref[0]).reshape(groups, SLOTS, -1)
    second = wide_dot(pick_ref[1], field_ref[1]).reshape(groups, SLOTS, -1)
    rows_ref[...] = jnp.concatenate([first, second], axis=1).astype(jnp.bfloat16)


def dispatch(pick, field):
    ranks, width, tokens = pick.shape
    groups, depth = width // SLOTS, field.shape[1]
    return pl.pallas_call(
        dispatch_body,
        grid=(ranks // 2, depth // BLOCK),
        in_specs=[
            pl.BlockSpec((2, width, tokens), lambda i, k: (i, 0, 0)),
            pl.BlockSpec((2, tokens, BLOCK), lambda i, k: (i, 0, k)),
        ],
        out_specs=pl.BlockSpec((groups, 2 * SLOTS, BLOCK), lambda i, k: (0, i, k)),
        out_shape=jax.ShapeDtypeStruct((groups, ranks * SLOTS, depth), jnp.bfloat16),
    )(pick, field.reshape(ranks, tokens, depth))


def combine_body(spread_ref, rows_ref, field_ref):
    rows = rows_ref[...].astype(jnp.float32)
    width = rows.shape[0] * SLOTS
    for side in range(2):
        part = rows[:, side * SLOTS : (side + 1) * SLOTS].reshape(width, -1).astype(jnp.bfloat16)
        field_ref[side] = wide_dot(spread_ref[side], part).astype(jnp.bfloat16)


def combine(spread, rows):
    ranks, tokens, width = spread.shape
    groups, depth = width // SLOTS, rows.shape[2]
    field = pl.pallas_call(
        combine_body,
        grid=(ranks // 2, depth // BLOCK),
        in_specs=[
            pl.BlockSpec((2, tokens, width), lambda i, k: (i, 0, 0)),
            pl.BlockSpec((groups, 2 * SLOTS, BLOCK), lambda i, k: (0, i, k)),
        ],
        out_specs=pl.BlockSpec((2, tokens, BLOCK), lambda i, k: (i, 0, k)),
        out_shape=jax.ShapeDtypeStruct((ranks, tokens, depth), jnp.bfloat16),
    )(spread, rows)
    return field.reshape(ranks * tokens, depth)


def scatter_all(field):
    part = lax.psum_scatter(field, "col", scatter_dimension=0, tiled=True)
    return lax.psum_scatter(part, "row", scatter_dimension=0, tiled=True)


def pieces_of(ranks, depth):
    count = max(1, ranks // 32)
    step = depth // count
    return [(at, at + step) for at in range(0, depth, step)]


def gather_rows(pick, field):
    rows = []
    for start, stop in pieces_of(pick.shape[0], field.shape[1]):
        part = field[:, start:stop]
        if rows:
            part = lax.optimization_barrier((part, rows[-1]))[0]
        whole = lax.all_gather(part, ("col", "row"), axis=0, tiled=True)
        rows.append(dispatch(pick, whole))
    return rows[0] if len(rows) == 1 else jnp.concatenate(rows, axis=2)


def return_rows(spread, rows):
    sums = []
    for start, stop in pieces_of(spread.shape[0], rows.shape[2]):
        part = rows[:, :, start:stop]
        if sums:
            part = lax.optimization_barrier((part, sums[-1]))[0]
        sums.append(scatter_all(combine(spread, part)))
    return sums[0] if len(sums) == 1 else jnp.concatenate(sums, axis=1)


MESH = pl.DeviceIdType.MESH


def seat():
    r, c = lax.axis_index("row"), lax.axis_index("col")
    y, x = r // 2, r % 2
    z, core = c // 2, c % 2
    first = y * (1 - core) + x * core
    second = x * (1 - core) + y * core
    return r, c, y, x, z, core, first, second


def partners():
    r, c, y, x, z, core, first, second = seat()
    pair = (r, z * 2 + (1 - core))
    flip_y = (1 - y) * 2 + x
    flip_x = y * 2 + (1 - x)
    along_first = (flip_y * (1 - core) + flip_x * core, c)
    along_second = (flip_x * (1 - core) + flip_y * core, c)
    up = [(r, ((z + k) % 4) * 2 + core) for k in range(1, 4)]
    return pair, along_first, along_second, up


RANKS = 32


def nth(offset):
    spot = (lax.axis_index("col") * 4 + lax.axis_index("row") + offset) % RANKS
    return spot, (spot % 4, spot // 4)


def meet():
    barrier = pltpu.get_barrier_semaphore()

    @pl.loop(1, RANKS)
    def _(offset):
        pl.semaphore_signal(barrier, inc=1, device_id=nth(offset)[1], device_id_type=MESH)

    pl.semaphore_wait(barrier, RANKS - 1)


def small_copy(src_of, small_all, small_send, small_recv, offset):
    spot, device = nth(offset)
    return send(
        src_of(spot), small_all.at[nth(0)[0]], small_send.at[offset], small_recv.at[offset], device
    )


def row_of(core, first, second):
    y = first * (1 - core) + second * core
    x = second * (1 - core) + first * core
    return y, x


def send(src, dst, send_sem, recv_sem, device):
    return pltpu.make_async_remote_copy(
        src_ref=src, dst_ref=dst, send_sem=send_sem, recv_sem=recv_sem, device_id=device, device_id_type=MESH
    )


GSTEPS = 4
QUEUE = (2, 1, 3)
ARRIVE = (1, 3, 2)


def spread_out(own_ref, all_ref, sems):
    r, c, y, x, z, core, first, second = seat()
    pair, along_first, along_second, up = partners()
    here_sem, z_send, z_recv, g_send, g_recv, f_send, f_recv, p_send, p_recv = sems
    step = own_ref.shape[0] // GSTEPS

    def rows(q):
        return pl.ds(pl.multiple_of(q * step, step), step)

    def place(k, s, f, q):
        sec = second * (1 - s) + (1 - second) * s
        fir = first * (1 - f) + (1 - first) * f
        yy, xx = row_of(core, fir, sec)
        return all_ref.at[(z + 4 - k) % 4, core, yy, xx, rows(q)]

    def z_copy(k, q):
        return send(
            own_ref.at[rows(q)], place(0, 0, 0, q), z_send.at[k - 1, q], z_recv.at[k - 1, q], up[k - 1]
        )

    def g_copy(k, q, src):
        return send(src, place(k, 0, 0, q), g_send.at[k, q], g_recv.at[k, q], along_second)

    def f_copy(k, s, q, src):
        return send(src, place(k, s, 0, q), f_send.at[s, k, q], f_recv.at[s, k, q], along_first)

    def p_copy(k, s, f, q, src):
        return send(src, place(k, s, f, q), p_send.at[f, s, k, q], p_recv.at[f, s, k, q], pair)

    here = pltpu.make_async_copy(own_ref, all_ref.at[z, core, y, x], here_sem)

    def begin():
        here.start()

        @pl.loop(0, GSTEPS)
        def _(q):
            src = own_ref.at[rows(q)]
            for k in QUEUE:
                z_copy(k, q).start()
            g_copy(0, q, src).start()
            f_copy(0, 0, q, src).start()
            p_copy(0, 0, 0, q, src).start()

    def forward(q):
        for k in ARRIVE:
            z_copy(k, q).wait_recv()
            src = place(k, 0, 0, q)
            g_copy(k, q, src).start()
            f_copy(k, 0, q, src).start()
            p_copy(k, 0, 0, q, src).start()
        for k in (0, *ARRIVE):
            src = place(k, 1, 0, q)
            g_copy(k, q, src).wait_recv()
            f_copy(k, 1, q, src).start()
            p_copy(k, 1, 0, q, src).start()
        for k in (0, *ARRIVE):
            src = place(k, 0, 1, q)
            f_copy(k, 0, q, src).wait_recv()
            p_copy(k, 0, 1, q, src).start()

    def finish():
        @pl.loop(0, GSTEPS)
        def _(q):
            for k in (0, *ARRIVE):
                src = place(k, 1, 1, q)
                f_copy(k, 1, q, src).wait_recv()
                p_copy(k, 1, 1, q, src).start()

        here.wait()

        @pl.loop(0, GSTEPS)
        def _(q):
            for k in range(4):
                src = own_ref.at[rows(q)]
                if k:
                    z_copy(k, q).wait_send()
                g_copy(k, q, src).wait_send()
                for s in range(2):
                    f_copy(k, s, q, src).wait_send()
                    for f in range(2):
                        p_copy(k, s, f, q, src).wait()

    return begin, forward, finish


def spread_sems():
    dma = pltpu.SemaphoreType.DMA
    shapes = [(3, GSTEPS), (4, GSTEPS), (2, 4, GSTEPS), (2, 2, 4, GSTEPS)]
    return [dma(())] + [dma(shape) for shape in shapes for _ in range(2)]


def small_out(small_ref, small_all, sems):
    here_sem, small_send, small_recv = sems
    local = pltpu.make_async_copy(small_ref, small_all.at[nth(0)[0]], here_sem)

    def copy(offset):
        return small_copy(lambda spot: small_ref, small_all, small_send, small_recv, offset)

    def begin():
        local.start()

        @pl.loop(1, RANKS)
        def _(offset):
            copy(offset).start()

    def finish():
        local.wait()

        @pl.loop(1, RANKS)
        def _(offset):
            copy(offset).wait()

    return begin, finish


def small_sems():
    dma = pltpu.SemaphoreType.DMA
    return [dma(()), dma((RANKS,)), dma((RANKS,))]


ANYWHERE = pl.BlockSpec(memory_space=pl.ANY)


def start_body(x_ref, q_ref, k_ref, v_ref, o_ref, pack_ref, own_ref, small_ref,
               x_all, q_all, k_all, v_all, o_all, pack_all, all_ref, small_all, *sems):
    r, c, y, x, z, core, first, second = seat()
    pair, along_first, along_second, up = partners()
    begin, forward, finish = spread_out(own_ref, all_ref, sems[:9])
    small_begin, small_finish = small_out(small_ref, small_all, sems[9:12])
    here_sem, x_send, x_recv, w_send, w_recv, v_send, v_recv = sems[12:]
    weights = [(q_ref, q_all), (k_ref, k_all), (v_ref, v_all), (o_ref, o_all), (pack_ref, pack_all)]

    def block(index, col):
        ref, whole = weights[index]
        if index == 4:
            return whole.at[col]
        if index == 3:
            width = ref.shape[1]
            return whole.at[:, pl.ds(pl.multiple_of(col * width, width), width)]
        height = ref.shape[0]
        return whole.at[pl.ds(pl.multiple_of(col * height, height), height)]

    def w_copy(index, k):
        return send(
            weights[index][0], block(index, c), w_send.at[index, k - 1], w_recv.at[index, k - 1], up[k - 1]
        )

    def pair_copy(index, k):
        col = ((z + 4 - k) % 4) * 2 + core
        src = weights[index][0] if k == 0 else block(index, col)
        return send(src, block(index, col), v_send.at[index, k], v_recv.at[index, k], pair)

    locals_ = [pltpu.make_async_copy(x_ref, x_all.at[r], here_sem.at[5])] + [
        pltpu.make_async_copy(weights[i][0], block(i, c), here_sem.at[i]) for i in range(5)
    ]
    y1, x1 = row_of(core, first, 1 - second)
    near_row = y1 * 2 + x1
    x_first = send(x_ref, x_all.at[r], x_send.at[0], x_recv.at[0], along_first)
    x_second = send(x_ref, x_all.at[r], x_send.at[1], x_recv.at[1], along_second)
    x_relay = send(x_all.at[near_row], x_all.at[near_row], x_send.at[2], x_recv.at[2], along_first)

    meet()
    small_begin()
    x_second.start()
    x_first.start()
    begin()
    for index in (4, 0, 1, 2, 3):
        for k in QUEUE:
            w_copy(index, k).start()
        pair_copy(index, 0).start()
    for item in locals_:
        item.start()
    x_second.wait_recv()
    x_relay.start()

    @pl.loop(0, GSTEPS)
    def _(q):
        forward(q)

    for index in (4, 0, 1, 2, 3):
        for k in ARRIVE:
            w_copy(index, k).wait_recv()
            pair_copy(index, k).start()
    finish()
    small_finish()
    for item in locals_:
        item.wait()
    x_first.wait()
    x_second.wait_send()
    x_relay.wait()
    for index in range(5):
        for k in range(4):
            if k:
                w_copy(index, k).wait_send()
            pair_copy(index, k).wait()


def start_near(x, weights, pack, own, small, collective_id):
    tokens, depth = own.shape
    dma = pltpu.SemaphoreType.DMA
    height, width = weights[0].shape
    shaped = lambda shape, like: jax.ShapeDtypeStruct(shape, like.dtype)
    outs = pl.pallas_call(
        start_body,
        out_shape=(
            shaped((4, *x.shape), x),
            *[shaped((8 * height, width), w) for w in weights[:3]],
            shaped((weights[3].shape[0], 8 * weights[3].shape[1]), weights[3]),
            shaped((8, *pack.shape), pack),
            shaped((4, 2, 2, 2, tokens, depth), own),
            shaped((RANKS, *small.shape), small),
        ),
        in_specs=[ANYWHERE] * 8,
        out_specs=[ANYWHERE] * 8,
        scratch_shapes=spread_sems()
        + small_sems()
        + [dma((6,)), dma((3,)), dma((3,)), dma((5, 3)), dma((5, 3)), dma((5, 4)), dma((5, 4))],
        compiler_params=pltpu.CompilerParams(collective_id=collective_id, has_side_effects=True),
    )(x, *weights, pack, own, small)
    x_all, q, k, v, o, pack_all, whole, small_all = outs
    return x_all.reshape(-1, x.shape[1]), q, k, v, o, pack_all, whole.reshape(RANKS, tokens, depth), small_all


def finish_body(part_ref, field_ref, q_ref, k_ref, v_ref, o_ref, pack_ref,
                mixture_ref, out_ref, q_out, k_out, v_out, o_out, pack_all,
                mine, first_in, second_in, total,
                q_mine, k_mine, v_mine, o_mine, q_pair, k_pair, v_pair, o_pair, q_z, k_z, v_z, o_z,
                q_sum, k_sum, v_sum, o_sum,
                load_sem, f_send, f_recv, g_send, g_recv, w_load, p_send, p_recv, z_send, z_recv, out_sem,
                *rest):
    r, c, y, x, z, core, first, second = seat()
    pair, along_first, along_second, up = partners()
    small_begin, small_finish = small_each(pack_ref, pack_all, rest[:3], lambda spot: spot // 4)
    begin, tick, finish = shrink(part_ref, *rest[3:9], rest[9:18])
    mixture = rest[8]
    tokens, depth = out_ref.shape
    other = 1 - core
    grads = [q_ref, k_ref, v_ref, o_ref]
    kept, pairs, zs = [q_mine, k_mine, v_mine, o_mine], [q_pair, k_pair, v_pair, o_pair], [q_z, k_z, v_z, o_z]
    sums, outs = [q_sum, k_sum, v_sum, o_sum], [q_out, k_out, v_out, o_out]

    def block(index, col):
        ref = grads[index]
        if index == 3:
            width = ref.shape[1] // 8
            return ref.at[:, pl.ds(pl.multiple_of(col * width, width), width)]
        height = ref.shape[0] // 8
        return ref.at[pl.ds(pl.multiple_of(col * height, height), height)]

    def row(fir, sec):
        yy, xx = row_of(core, fir, sec)
        return yy * 2 + xx

    def load(fir, sec):
        return pltpu.make_async_copy(field_ref.at[row(fir, sec)], mine.at[fir, sec], load_sem.at[fir, sec])

    def f_copy(sec):
        return send(field_ref.at[row(1 - first, sec)], first_in.at[sec], f_send.at[sec], f_recv.at[sec], along_first)

    g_copy = send(mine.at[first, 1 - second], second_in, g_send, g_recv, along_second)

    def w_load_copy(index, zz):
        return pltpu.make_async_copy(block(index, zz * 2 + core), kept[index].at[zz], w_load.at[index, zz])

    def w_give(index, zz):
        return send(
            block(index, zz * 2 + other), pairs[index].at[zz], p_send.at[index, zz], p_recv.at[index, zz], pair
        )

    def w_z(index, k):
        return send(
            kept[index].at[(z + k) % 4], zs[index].at[k - 1], z_send.at[index, k - 1], z_recv.at[index, k - 1], up[k - 1]
        )

    def add(ref, extras):
        @pl.loop(0, ref.shape[0] // TILE)
        def _(t):
            here = pl.ds(pl.multiple_of(t * TILE, TILE), TILE)
            value = ref[here].astype(jnp.float32)
            for extra in extras:
                value = value + extra[here].astype(jnp.float32)
            ref[here] = value.astype(jnp.bfloat16)

    def add_out(ref, extras, result):
        @pl.loop(0, ref.shape[0] // TILE)
        def _(t):
            here = pl.ds(pl.multiple_of(t * TILE, TILE), TILE)
            value = ref[here].astype(jnp.float32)
            for extra in extras:
                value = value + extra[here].astype(jnp.float32)
            result[here] = value

    meet()
    for index in range(4):
        for k in (2, 1, 3, 0):
            w_give(index, (z + k) % 4).start()
            w_load_copy(index, (z + k) % 4).start()
    begin()
    f_copy(1 - second).start()
    f_copy(second).start()
    load(first, 1 - second).start()
    load(first, second).start()
    small_begin()
    for index in range(4):
        for k in QUEUE:
            zz = (z + k) % 4
            w_load_copy(index, zz).wait()
            w_give(index, zz).wait_recv()
            add(kept[index].at[zz], [pairs[index].at[zz]])
            w_z(index, k).start()

    @pl.loop(0, RSTEPS)
    def _(i):
        tick(i)

        @pl.when(i == 2)
        def _():
            load(first, 1 - second).wait()
            f_copy(1 - second).wait_recv()
            add(mine.at[first, 1 - second], [first_in.at[1 - second]])
            g_copy.start()

    for index in range(4):
        w_load_copy(index, z).wait()
        w_give(index, z).wait_recv()
        for k in ARRIVE:
            w_z(index, k).wait_recv()
        add_out(
            kept[index].at[z], [pairs[index].at[z]] + [zs[index].at[k] for k in range(3)], sums[index]
        )
        pltpu.make_async_copy(sums[index], outs[index], out_sem.at[index]).start()
    load(first, second).wait()
    f_copy(second).wait_recv()
    g_copy.wait_recv()
    add_out(mine.at[first, second], [first_in.at[second], second_in], total)
    pltpu.make_async_copy(total, out_ref, out_sem.at[4]).start()

    @pl.loop(RSTEPS, TICKS)
    def _(i):
        tick(i)

    pltpu.make_async_copy(mixture, mixture_ref, out_sem.at[5]).start()
    finish()
    for sec in range(2):
        f_copy(sec).wait_send()
    g_copy.wait_send()
    for index in range(4):
        for k in range(4):
            w_give(index, (z + k) % 4).wait_send()
            if k:
                w_z(index, k).wait_send()
        pltpu.make_async_copy(sums[index], outs[index], out_sem.at[index]).wait()
    small_finish()
    pltpu.make_async_copy(total, out_ref, out_sem.at[4]).wait()
    pltpu.make_async_copy(mixture, mixture_ref, out_sem.at[5]).wait()


def finish_near(part, field, grads, pack, collective_id):
    rows_count, tokens, depth = field.shape
    dma = pltpu.SemaphoreType.DMA
    blocks = [(g.shape[0] // 8, g.shape[1]) for g in grads[:3]] + [(grads[3].shape[0], grads[3].shape[1] // 8)]
    half = lambda *shape: pltpu.VMEM(shape, jnp.bfloat16)
    return pl.pallas_call(
        finish_body,
        out_shape=(
            jax.ShapeDtypeStruct((tokens, depth), jnp.float32),
            jax.ShapeDtypeStruct((tokens, depth), jnp.float32),
            *[jax.ShapeDtypeStruct(b, jnp.float32) for b in blocks],
            jax.ShapeDtypeStruct((RANKS, *pack.shape[1:]), pack.dtype),
        ),
        in_specs=[ANYWHERE] * 7,
        out_specs=[ANYWHERE] * 7,
        scratch_shapes=[
            half(2, 2, tokens, depth), half(2, tokens, depth), half(tokens, depth),
            pltpu.VMEM((tokens, depth), jnp.float32),
            *[half(4, *b) for b in blocks], *[half(4, *b) for b in blocks], *[half(3, *b) for b in blocks],
            *[pltpu.VMEM(b, jnp.float32) for b in blocks],
            dma((2, 2)), dma((2,)), dma((2,)), dma(()), dma(()),
            dma((4, 4)), dma((4, 4)), dma((4, 4)), dma((4, 3)), dma((4, 3)), dma((6,)),
        ]
        + small_sems()
        + shrink_scratch(tokens, depth),
        compiler_params=pltpu.CompilerParams(
            collective_id=collective_id, has_side_effects=True, vmem_limit_bytes=63 * 1024 * 1024
        ),
    )(part.reshape(4, 2, 2, 2, tokens, depth), field, *grads, pack)


RSTEPS = 8
TILE = 16
LAGS = (0, 1, 2, 4)
TICKS = RSTEPS + LAGS[3]


def shrink(part_ref, sums, near_own, first_in, second_in, z_in, total, sems):
    r, c, y, x, z, core, first, second = seat()
    pair, along_first, along_second, up = partners()
    load_sem, p_send, p_recv, f_send, f_recv, g_send, g_recv, z_send, z_recv = sems
    tokens = total.shape[0]
    step = tokens // RSTEPS
    other = 1 - core

    def rows(q):
        return pl.ds(pl.multiple_of(q * step, step), step)

    def spot(kind):
        fir = (1 - first) if kind < 2 else first
        sec = (1 - second) if kind in (0, 2) else second
        return fir, sec

    def load(kind, q):
        yy, xx = row_of(core, *spot(kind))
        return pltpu.make_async_copy(
            part_ref.at[:, core, yy, xx, rows(q)], near_own.at[q % 2, kind], load_sem.at[kind, q % 2]
        )

    def give(fir, sec, q):
        yy, xx = row_of(other, fir, sec)
        return send(
            part_ref.at[:, other, yy, xx, rows(q)],
            sums.at[fir, sec, :, rows(q)],
            p_send.at[fir, sec, q],
            p_recv.at[fir, sec, q],
            pair,
        )

    def f_copy(sec, q):
        return send(
            sums.at[1 - first, sec, :, rows(q)],
            first_in.at[sec, :, rows(q)],
            f_send.at[sec, q],
            f_recv.at[sec, q],
            along_first,
        )

    def g_copy(q):
        return send(
            sums.at[first, 1 - second, :, rows(q)], second_in.at[:, rows(q)], g_send.at[q], g_recv.at[q], along_second
        )

    def z_copy(k, q):
        return send(
            sums.at[first, second, (z + k) % 4, rows(q)],
            z_in.at[k - 1, rows(q)],
            z_send.at[k - 1, q],
            z_recv.at[k - 1, q],
            up[k - 1],
        )

    def begin():
        @pl.loop(0, RSTEPS)
        def _(q):
            for fir, sec in ((1 - second, 1 - first), (1 - second, first), (second, 1 - first), (second, first)):
                give(fir, sec, q).start()

        for kind in range(4):
            load(kind, 0).start()

    def add(kind, q, extra):
        fir, sec = spot(kind)

        @pl.when(q + 1 < RSTEPS)
        def _():
            load(kind, q + 1).start()

        load(kind, q).wait()
        give(fir, sec, q).wait_recv()

        @pl.loop(0, 4 * (step // TILE))
        def _(t):
            zz, at = t // (step // TILE), t % (step // TILE)
            here = pl.ds(pl.multiple_of(q * step + at * TILE, TILE), TILE)
            near = pl.ds(pl.multiple_of(at * TILE, TILE), TILE)
            value = sums[fir, sec, zz, here].astype(jnp.float32)
            value = value + near_own[q % 2, kind, zz, near].astype(jnp.float32)
            for ref in extra:
                value = value + ref[zz, here].astype(jnp.float32)
            sums[fir, sec, zz, here] = value.astype(jnp.bfloat16)

    def stage_first(q):
        for kind, sec in ((0, 1 - second), (1, second)):
            add(kind, q, [])
            f_copy(sec, q).start()

    def stage_second(q):
        f_copy(1 - second, q).wait_recv()
        add(2, q, [first_in.at[1 - second]])
        g_copy(q).start()

    def stage_z(q):
        f_copy(second, q).wait_recv()
        g_copy(q).wait_recv()
        add(3, q, [first_in.at[second], second_in])
        for k in QUEUE:
            z_copy(k, q).start()

    def stage_out(q):
        for k in ARRIVE:
            z_copy(k, q).wait_recv()

        @pl.loop(0, step // TILE)
        def _(t):
            here = pl.ds(pl.multiple_of(q * step + t * TILE, TILE), TILE)
            value = sums[first, second, z, here].astype(jnp.float32)
            for k in range(3):
                value = value + z_in[k, here].astype(jnp.float32)
            total[here] = value

    def tick(i):
        for stage, lag in zip((stage_first, stage_second, stage_z, stage_out), LAGS):

            @pl.when((i >= lag) & (i < RSTEPS + lag))
            def _(stage=stage, lag=lag):
                stage(i - lag)

    def finish():
        @pl.loop(0, RSTEPS)
        def _(q):
            for fir in range(2):
                for sec in range(2):
                    give(fir, sec, q).wait_send()
            for sec in range(2):
                f_copy(sec, q).wait_send()
            g_copy(q).wait_send()
            for k in QUEUE:
                z_copy(k, q).wait_send()

    return begin, tick, finish


def shrink_scratch(tokens, depth):
    dma = pltpu.SemaphoreType.DMA
    low = lambda *shape: pltpu.VMEM((*shape, depth), jnp.bfloat16)
    buffers = [
        low(2, 2, 4, tokens), low(2, 4, 4, tokens // RSTEPS), low(2, 4, tokens), low(4, tokens), low(3, tokens),
        pltpu.VMEM((tokens, depth), jnp.float32),
    ]
    shapes = [(2, 2, RSTEPS), (2, RSTEPS), (RSTEPS,), (3, RSTEPS)]
    return buffers + [dma((4, 2))] + [dma(shape) for shape in shapes for _ in range(2)]


def small_each(small_ref, small_all, sems, pick):
    here_sem, small_send, small_recv = sems
    local = pltpu.make_async_copy(small_ref.at[pick(nth(0)[0])], small_all.at[nth(0)[0]], here_sem)

    def copy(offset):
        return small_copy(lambda spot: small_ref.at[pick(spot)], small_all, small_send, small_recv, offset)

    def begin():
        local.start()

        @pl.loop(1, RANKS)
        def _(offset):
            copy(offset).start()

    def finish():
        local.wait()

        @pl.loop(1, RANKS)
        def _(offset):
            copy(offset).wait()

    return begin, finish


SPACING = 5


def feed_back_body(part_ref, small_ref, rows_ref, gate_ref, up_ref, act_ref, grads_ref,
                   out_ref, small_all, gate_out, up_out, down_out, *scratch):
    begin, tick, finish = shrink(part_ref, *scratch[:6], scratch[6:15])
    total, out_sem = scratch[5], scratch[15]
    small_begin, small_finish = small_each(small_ref, small_all, scratch[16:], lambda spot: spot)
    e, k = pl.program_id(0), pl.program_id(1)
    step = e * pl.num_programs(1) + k
    last = pl.num_programs(0) * pl.num_programs(1) - 1

    @pl.when(step == 0)
    def _():
        meet()
        small_begin()
        begin()

    rows = rows_ref[0]
    gate_out[0] = inner_rows(rows, gate_ref[0])
    up_out[0] = inner_rows(rows, up_ref[0])
    down_out[0] = inner_rows(act_ref[0], grads_ref[0])

    @pl.when((step % SPACING == 0) & (step // SPACING < TICKS))
    def _():
        tick(step // SPACING)

    @pl.when(step == last)
    def _():
        done = pltpu.make_async_copy(total, out_ref, out_sem)
        done.start()
        finish()
        small_finish()
        done.wait()


def feed_back(part, small, rows, grad_gate, grad_up, act, grads, collective_id):
    tokens, depth = part.shape[0] // RANKS, part.shape[1]
    groups, length, inner = grad_gate.shape
    dma = pltpu.SemaphoreType.DMA
    slab = pl.BlockSpec((1, length, CHUNK), lambda e, k: (e, 0, k))
    held = pl.BlockSpec((1, length, inner), lambda e, k: (e, 0, 0))
    return pl.pallas_call(
        feed_back_body,
        grid=(groups, depth // CHUNK),
        in_specs=[ANYWHERE, ANYWHERE, slab, held, held, held, slab],
        out_specs=[
            ANYWHERE,
            ANYWHERE,
            pl.BlockSpec((1, CHUNK, inner), lambda e, k: (e, k, 0)),
            pl.BlockSpec((1, CHUNK, inner), lambda e, k: (e, k, 0)),
            pl.BlockSpec((1, inner, CHUNK), lambda e, k: (e, 0, k)),
        ],
        out_shape=(
            jax.ShapeDtypeStruct((tokens, depth), jnp.float32),
            jax.ShapeDtypeStruct(small.shape, small.dtype),
            jax.ShapeDtypeStruct((groups, depth, inner), jnp.float32),
            jax.ShapeDtypeStruct((groups, depth, inner), jnp.float32),
            jax.ShapeDtypeStruct((groups, inner, depth), jnp.float32),
        ),
        scratch_shapes=shrink_scratch(tokens, depth) + [dma(())] + small_sems(),
        compiler_params=pltpu.CompilerParams(
            collective_id=collective_id, has_side_effects=True, vmem_limit_bytes=63 * 1024 * 1024
        ),
    )(part.reshape(4, 2, 2, 2, tokens, depth), small, rows, grad_gate, grad_up, act, grads)


def fill_rows(pick_ref, field_ref, rows_ref):
    ranks, groups = pick_ref.shape[0], rows_ref.shape[0]

    @pl.loop(0, ranks // 2, unroll=UNROLL)
    def _(i):
        parts = [
            wide_dot(pick_ref[2 * i + side], field_ref[2 * i + side]).reshape(groups, SLOTS, CHUNK)
            for side in range(2)
        ]
        here = pl.ds(pl.multiple_of(i * 2 * SLOTS, 2 * SLOTS), 2 * SLOTS)
        rows_ref[:, here] = jnp.concatenate(parts, axis=1).astype(jnp.bfloat16)


def add_products(k, rows_ref, pairs):
    groups = rows_ref.shape[0]

    def products(e, first):
        for product, total in pairs:
            term = product(rows_ref[e], e)
            if first:
                total[e] = term
            else:
                total[e] += term

    @pl.when(k == 0)
    def _():
        @pl.loop(0, groups)
        def _(e):
            products(e, True)

    @pl.when(k > 0)
    def _():
        @pl.loop(0, groups)
        def _(e):
            products(e, False)


def grads_in_body(pick_ref, field_ref, down_ref, own_ref, small_ref,
                  rows_ref, plain_ref, all_ref, small_all, total, *sems):
    begin, forward, finish = spread_out(own_ref, all_ref, sems[:9])
    small_begin, small_finish = small_out(small_ref, small_all, sems[9:])
    k, last = pl.program_id(0), pl.num_programs(0) - 1

    @pl.when(k == 0)
    def _():
        meet()
        small_begin()
        begin()

    fill_rows(pick_ref, field_ref, rows_ref)
    add_products(k, rows_ref, [(lambda rows, e: outer_cols(rows, down_ref[e]), total)])

    @pl.when(k % 2 == 1)
    def _():
        forward(k // 2)

    @pl.when(k == last)
    def _():
        pltpu.sync_copy(total, plain_ref)
        finish()
        small_finish()


def grads_in(pick, field, down, own, small, collective_id):
    ranks, width, tokens = pick.shape
    groups, depth = width // SLOTS, field.shape[-1]
    length, inner = ranks * SLOTS, down.shape[1]
    steps = depth // CHUNK
    rows, plain, whole, small_all = pl.pallas_call(
        grads_in_body,
        grid=(steps,),
        in_specs=[
            pl.BlockSpec((ranks, width, tokens), lambda k: (0, 0, 0), pipeline_mode=pl.Buffered(1)),
            pl.BlockSpec((ranks, tokens, CHUNK), lambda k: (0, 0, k)),
            pl.BlockSpec((groups, inner, CHUNK), lambda k: (0, 0, k)),
            ANYWHERE,
            ANYWHERE,
        ],
        out_specs=[pl.BlockSpec((groups, length, CHUNK), lambda k: (0, 0, k))] + [ANYWHERE] * 3,
        out_shape=[
            jax.ShapeDtypeStruct((groups, length, depth), jnp.bfloat16),
            jax.ShapeDtypeStruct((groups, length, inner), jnp.float32),
            jax.ShapeDtypeStruct((4, 2, 2, 2, *own.shape), own.dtype),
            jax.ShapeDtypeStruct((RANKS, *small.shape), small.dtype),
        ],
        scratch_shapes=[pltpu.VMEM((groups, length, inner), jnp.float32)] + spread_sems() + small_sems(),
        compiler_params=pltpu.CompilerParams(
            collective_id=collective_id, has_side_effects=True, vmem_limit_bytes=62 * 1024 * 1024
        ),
    )(pick, field, down, own, small)
    return rows, plain, whole.reshape(RANKS, *own.shape), small_all


def feed_in_body(steps, pick_ref, field_ref, gate_ref, up_ref, plain_ref, probs_ref,
                 rows_ref, act_ref, weighted_ref, grad_gate_ref, grad_up_ref, gates_ref, gate_sum, up_sum):
    k = pl.program_id(0)

    @pl.when(k < steps)
    def _():
        fill_rows(pick_ref, field_ref, rows_ref)
        add_products(
            k,
            rows_ref,
            [
                (lambda rows, e: wide_dot(rows, gate_ref[e]), gate_sum),
                (lambda rows, e: wide_dot(rows, up_ref[e]), up_sum),
            ],
        )

    @pl.when(k >= steps)
    def _():
        e = k - steps
        length = act_ref.shape[1]

        @pl.loop(0, length // 128)
        def _(t):
            here = pl.ds(pl.multiple_of(t * 128, 128), 128)
            gate_val, up_val = gate_sum[e, here], up_sum[e, here]
            plain, probs = plain_ref[0, here], probs_ref[0, here]
            sigmoid_val = jax.nn.sigmoid(gate_val)
            silu_val = gate_val * sigmoid_val
            activated = silu_val * up_val
            grad_act = plain * probs
            grad_up_ref[0, here] = (grad_act * silu_val).astype(jnp.bfloat16)
            grad_gate_ref[0, here] = (
                grad_act * up_val * (sigmoid_val * (1.0 + gate_val * (1.0 - sigmoid_val)))
            ).astype(jnp.bfloat16)
            gates_ref[0, here] = jnp.sum(activated * plain, axis=-1, keepdims=True)
            weighted_ref[0, here] = (activated * probs).astype(jnp.bfloat16)
            act_ref[0, here] = activated.astype(jnp.bfloat16)


def feed_in(pick, field, gate, up, plain, probs):
    ranks, width, tokens = pick.shape
    groups, depth = width // SLOTS, field.shape[-1]
    length, inner = ranks * SLOTS, gate.shape[2]
    steps = depth // CHUNK
    held = lambda k: jnp.minimum(k, steps - 1)
    late = lambda k: (jnp.maximum(k - steps, 0), 0, 0)
    wide = pl.BlockSpec((1, length, inner), late)
    thin = pl.BlockSpec((1, length, 1), late)
    low = jax.ShapeDtypeStruct((groups, length, inner), jnp.bfloat16)
    return pl.pallas_call(
        functools.partial(feed_in_body, steps),
        grid=(steps + groups,),
        in_specs=[
            pl.BlockSpec((ranks, width, tokens), lambda k: (0, 0, 0), pipeline_mode=pl.Buffered(1)),
            pl.BlockSpec((ranks, tokens, CHUNK), lambda k: (0, 0, held(k))),
            pl.BlockSpec((groups, CHUNK, inner), lambda k: (0, held(k), 0)),
            pl.BlockSpec((groups, CHUNK, inner), lambda k: (0, held(k), 0)),
            wide,
            thin,
        ],
        out_specs=[pl.BlockSpec((groups, length, CHUNK), lambda k: (0, 0, held(k))), wide, wide, wide, wide, thin],
        out_shape=[
            jax.ShapeDtypeStruct((groups, length, depth), jnp.bfloat16),
            low, low, low, low,
            jax.ShapeDtypeStruct((groups, length, 1), jnp.float32),
        ],
        scratch_shapes=[pltpu.VMEM((groups, length, inner), jnp.float32)] * 2,
        compiler_params=pltpu.CompilerParams(vmem_limit_bytes=63 * 1024 * 1024),
        cost_estimate=pl.CostEstimate(
            flops=2 * groups * length * depth * (tokens + 2 * inner), bytes_accessed=120 << 20, transcendentals=0
        ),
    )(pick, field, gate, up, plain, probs)


def restore_body(flipped, spread_ref, *refs):
    count = len(flipped)
    lefts, weights, field_ref, rows = refs[:count], refs[count:2*count], refs[2*count], refs[2*count+1]
    groups = rows.shape[0]
    ranks = spread_ref.shape[0]

    @pl.loop(0, groups)
    def _(e):
        total = None
        for left, weight, flip in zip(lefts, weights, flipped):
            term = outer_cols(left[e], weight[e]) if flip else wide_dot(left[e], weight[e])
            total = term if total is None else total + term
        rows[e] = total

    @pl.loop(0, ranks, unroll=2*UNROLL)
    def _(s):
        part = rows[:, pl.ds(pl.multiple_of(s * SLOTS, SLOTS), SLOTS)].reshape(groups * SLOTS, CHUNK).astype(jnp.bfloat16)
        field_ref[s] = wide_dot(spread_ref[s], part).astype(jnp.bfloat16)

def restore(spread, lefts, weights, flipped):
    ranks, tokens, width = spread.shape
    groups = width // SLOTS
    length = ranks * SLOTS
    inner = lefts[0].shape[2]
    depth = weights[0].shape[1] if flipped[0] else weights[0].shape[2]
    wspecs = [pl.BlockSpec((groups, CHUNK, inner), lambda k: (0, k, 0)) if f else pl.BlockSpec((groups, inner, CHUNK), lambda k: (0, 0, k)) for f in flipped]
    flops = 2 * groups * length * depth * (tokens + inner * len(weights))
    field = pl.pallas_call(
        functools.partial(restore_body, flipped),
        grid=(depth // CHUNK,),
        in_specs=[pl.BlockSpec((ranks, tokens, width), lambda k: (0, 0, 0), pipeline_mode=pl.Buffered(1))]
        + [pl.BlockSpec((groups, length, inner), lambda k: (0, 0, 0), pipeline_mode=pl.Buffered(1))] * len(lefts) + wspecs,
        out_specs=pl.BlockSpec((ranks, tokens, CHUNK), lambda k: (0, 0, k)),
        out_shape=jax.ShapeDtypeStruct((ranks, tokens, depth), jnp.bfloat16),
        scratch_shapes=[pltpu.VMEM((groups, length, CHUNK), jnp.float32)],
        compiler_params=pltpu.CompilerParams(vmem_limit_bytes=63 * 1024 * 1024),
        cost_estimate=pl.CostEstimate(flops=flops, bytes_accessed=60 << 20, transcendentals=0),
    )(spread, *lefts, *weights)
    return field.reshape(ranks * tokens, depth)


def local(
    layer_input,
    cotangent,
    expert_index,
    attention_gain,
    query_gain,
    key_gain,
    query_weight,
    key_weight,
    value_weight,
    output_weight,
    feed_gain,
    router_weight,
    gate_weight,
    up_weight,
    down_weight,
):
    tokens = layer_input.shape[0]
    rows_count = lax.axis_size("row")
    near = rows_count == 4 and lax.axis_size("col") == 8
    if near:
        head_part = query_gain.shape[0]
        slice_width = attention_gain.shape[0]
        pack = jnp.concatenate(
            [attention_gain, feed_gain, query_gain, key_gain, router_weight.reshape(-1)]
        )
        pack = jnp.pad(pack, (0, PACK_ROWS * 128 - pack.shape[0])).reshape(PACK_ROWS, 128)
        (
            sequence, query_full, key_full, value_full, output_full, pack_all, cotangent_all, index_all
        ) = start_near(
            layer_input,
            [query_weight, key_weight, value_weight, output_weight],
            pack,
            cotangent,
            expert_index.T,
            1,
        )
        index_all = jnp.swapaxes(index_all, 1, 2)
        pack_all = pack_all.reshape(8, -1)
        ends = [slice_width, 2 * slice_width, 2 * slice_width + head_part, 2 * slice_width + 2 * head_part]
        attention_full = pack_all[:, : ends[0]].reshape(-1)
        feed_full = pack_all[:, ends[0] : ends[1]].reshape(-1)
        query_scale_w = pack_all[:, ends[1] : ends[2]].reshape(-1)
        key_scale_w = pack_all[:, ends[2] : ends[3]].reshape(-1)
        router_full = pack_all[:, ends[3] : ends[3] + router_weight.size].reshape(
            -1, router_weight.shape[1]
        )
    else:
        (
            attention_full,
            query_scale_w,
            key_scale_w,
            query_full,
            key_full,
            value_full,
            output_full,
            feed_full,
            router_full,
        ) = (
            lax.all_gather(attention_gain, "col", axis=0, tiled=True),
            lax.all_gather(query_gain, "col", axis=0, tiled=True),
            lax.all_gather(key_gain, "col", axis=0, tiled=True),
            lax.all_gather(query_weight, "col", axis=0, tiled=True),
            lax.all_gather(key_weight, "col", axis=0, tiled=True),
            lax.all_gather(value_weight, "col", axis=0, tiled=True),
            lax.all_gather(output_weight, "col", axis=1, tiled=True),
            lax.all_gather(feed_gain, "col", axis=0, tiled=True),
            lax.all_gather(router_weight, "col", axis=0, tiled=True),
        )
        sequence = lax.all_gather(layer_input, "row", axis=0, tiled=True)
    length = sequence.shape[0]
    model_width = sequence.shape[1]
    local_width = query_full.shape[1]
    local_heads = local_width // HD
    seq_float = sequence.astype(jnp.float32)
    seq_scale = rms_scale(seq_float)
    attention_float = attention_full.astype(jnp.float32)
    normed = (seq_float * seq_scale * attention_float).astype(jnp.bfloat16)
    query_raw = wide_dot(normed, query_full)
    key_raw = wide_dot(normed, key_full)
    value_heads = wide_dot(normed, value_full).astype(jnp.bfloat16).reshape(length, local_heads, HD)
    query_total, key_total = lax.psum(
        (jnp.sum(query_raw * query_raw, axis=-1), jnp.sum(key_raw * key_raw, axis=-1)), "row"
    )
    query_rs = lax.rsqrt(query_total / model_width + EPS)[:, None]
    key_rs = lax.rsqrt(key_total / model_width + EPS)[:, None]
    query_gain_f = query_scale_w.astype(jnp.float32)
    key_gain_f = key_scale_w.astype(jnp.float32)
    cosine, sine_table = rope_tables(length)
    queries = rotate(
        (query_raw * query_rs * query_gain_f).reshape(length, local_heads, HD), cosine, sine_table
    ).astype(jnp.bfloat16)
    keys_rotated = rotate(
        (key_raw * key_rs * key_gain_f).reshape(length, local_heads, HD), cosine, sine_table
    ).astype(jnp.bfloat16)
    block_rows = min(512, length)
    starts = jnp.arange(length // block_rows, dtype=jnp.int32) * block_rows
    key_position = jnp.arange(length, dtype=jnp.int32)
    score_scale = HD ** (-0.5)

    def block_scores(offset):
        query_rows = lax.dynamic_slice_in_dim(queries, offset, block_rows, 0)
        scores = (
            jnp.einsum("qhd,khd->hqk", query_rows, keys_rotated, preferred_element_type=jnp.float32)
            * score_scale
        )
        query_position = offset + jnp.arange(block_rows, dtype=jnp.int32)
        allowed = query_position[:, None] >= key_position[None, :]
        return (query_rows, jnp.where(allowed[None, :, :], scores, MASKED))

    def forward_block(offset):
        query_rows, scores = block_scores(offset)
        row_top = jnp.max(scores, axis=-1, keepdims=True)
        exponent = jnp.exp(scores - row_top)
        row_total = jnp.sum(exponent, axis=-1, keepdims=True)
        weights = (exponent / row_total).astype(jnp.bfloat16)
        mixed_block = jnp.einsum(
            "hqk,khd->qhd", weights, value_heads, preferred_element_type=jnp.float32
        )
        return (mixed_block, (row_top + jnp.log(row_total))[..., 0])

    mixed_blocks, lse_blocks = lax.map(forward_block, starts)
    mixed_heads = mixed_blocks.reshape(length, local_width).astype(jnp.bfloat16)
    lse_all = jnp.moveaxis(lse_blocks, 0, 1).reshape(local_heads, length)
    branch = lax.psum_scatter(
        wide_dot(mixed_heads, output_full).astype(jnp.bfloat16), "row", scatter_dimension=0, tiled=True
    ).astype(jnp.float32)
    hidden = layer_input.astype(jnp.float32) + branch
    feed_scale = rms_scale(hidden)
    feed_float = feed_full.astype(jnp.float32)
    feed_normed = (hidden * feed_scale * feed_float).astype(jnp.bfloat16)
    logits = wide_dot(feed_normed, router_full)
    logit_top = jnp.max(logits, axis=-1, keepdims=True)
    logit_exp = jnp.exp(logits - logit_top)
    router_probs = logit_exp / jnp.sum(logit_exp, axis=-1, keepdims=True)
    experts = router_full.shape[1]
    experts_local = gate_weight.shape[0]
    ranks = lax.axis_size("col") * rows_count
    gate_hits = expert_index[:, :, None] == jnp.arange(experts, dtype=jnp.int32)
    gate_probs = jnp.sum(jnp.where(gate_hits, router_probs[:, None, :], 0.0), axis=-1)

    if not near:
        index_all = lax.all_gather(expert_index, ("col", "row"), axis=0, tiled=True)
    own = (index_all - lax.axis_index("col") * experts_local).reshape(ranks, tokens, -1)
    matches = own[..., None] == jnp.arange(experts_local, dtype=jnp.int32)
    hit = jnp.sum(matches.astype(jnp.float32), axis=2)
    earlier = jnp.tril(jnp.ones((tokens, tokens), jnp.bfloat16), -1)
    rank = jnp.einsum(
        "tu,sue->ste", earlier, hit.astype(jnp.bfloat16), preferred_element_type=jnp.float32
    )
    slot = jnp.where(hit > 0, rank, -1.0)
    places = jnp.arange(SLOTS, dtype=jnp.float32)
    slot_t = jnp.swapaxes(slot, 1, 2)
    width = experts_local * SLOTS
    picked = slot_t[:, :, None, :] == places[None, None, :, None]
    pick = picked.astype(jnp.bfloat16).reshape(ranks, width, tokens)
    lanes = jnp.arange(width, dtype=jnp.int32)
    widen = (lanes[None, :] // SLOTS == jnp.arange(experts_local)[:, None]).astype(jnp.bfloat16)
    spread = jnp.einsum(
        "ste,ew->stw", slot.astype(jnp.bfloat16), widen, preferred_element_type=jnp.float32
    ) == (lanes % SLOTS).astype(jnp.float32)
    spread_plain = spread.astype(jnp.bfloat16)

    def weigh(probs_all):
        probs_own = jnp.sum(
            jnp.where(matches, probs_all.reshape(ranks, tokens, -1, 1), 0.0), axis=2
        )
        probs_wide = jnp.einsum(
            "ste,ew->stw", probs_own.astype(jnp.bfloat16), widen, preferred_element_type=jnp.float32
        )
        spread_probs = jnp.where(spread, probs_wide, 0.0).astype(jnp.bfloat16)
        probs_t = jnp.swapaxes(probs_own, 1, 2)
        row_probs = jnp.sum(jnp.where(picked, probs_t[:, :, None, :], 0.0), axis=-1)
        row_probs = jnp.swapaxes(row_probs, 0, 1).reshape(experts_local, ranks * SLOTS, 1)
        return spread_probs, row_probs

    if near:
        expert_grads, plain_act, feed_all, probs_all = grads_in(
            pick, cotangent_all, down_weight, feed_normed, gate_probs.T, 2
        )
        spread_probs, row_probs = weigh(jnp.swapaxes(probs_all, 1, 2))
        expert_rows, activated, weighted_act, grad_gate, grad_up, row_gates = feed_in(
            pick, feed_all, gate_weight, up_weight, plain_act, row_probs
        )
    else:
        probs_all = lax.all_gather(gate_probs, ("col", "row"), axis=0, tiled=True)
        spread_probs, row_probs = weigh(probs_all)
        expert_grads = gather_rows(pick, cotangent)
        expert_rows = gather_rows(pick, feed_normed)
        gate_val = jnp.einsum(
            "erd,edf->erf", expert_rows, gate_weight, preferred_element_type=jnp.float32
        )
        up_val = jnp.einsum(
            "erd,edf->erf", expert_rows, up_weight, preferred_element_type=jnp.float32
        )
        plain_act = jnp.einsum(
            "erd,efd->erf", expert_grads, down_weight, preferred_element_type=jnp.float32
        )
        sigmoid_val = jax.nn.sigmoid(gate_val)
        silu_val = gate_val * sigmoid_val
        activated = silu_val * up_val
        grad_act = plain_act * row_probs
        grad_up = (grad_act * silu_val).astype(jnp.bfloat16)
        grad_gate = (
            grad_act * up_val * sigmoid_val * (1.0 + gate_val * (1.0 - sigmoid_val))
        ).astype(jnp.bfloat16)
        row_gates = jnp.sum(activated * plain_act, axis=-1)
        weighted_act = (activated * row_probs).astype(jnp.bfloat16)
        activated = activated.astype(jnp.bfloat16)
    row_gates = jnp.swapaxes(row_gates.reshape(experts_local, ranks, SLOTS), 0, 1)
    own_gates = jnp.sum(jnp.where(picked, row_gates[..., None], 0.0), axis=2)
    if near:
        grad_feed_part = restore(
            spread_plain, [grad_gate, grad_up], [gate_weight, up_weight], (True, True)
        )
        grad_feed, gates_in, grad_gate_weight, grad_up_weight, grad_down_weight = feed_back(
            grad_feed_part, own_gates, expert_rows, grad_gate, grad_up, weighted_act, expert_grads, 3
        )
        activated = lax.optimization_barrier((activated, grad_feed))[0]
        gates_in = jnp.sum(gates_in.reshape(-1, rows_count, experts_local, tokens), axis=1)
        grad_probs = gates_in.reshape(experts, tokens).T
        mixture_part = restore(spread_probs, [activated], [down_weight], (False,))
    else:
        own_gates = lax.psum_scatter(
            jnp.swapaxes(own_gates, 1, 2).reshape(-1, rows_count, tokens, experts_local),
            "row",
            scatter_dimension=1,
        )
        grad_probs = lax.all_to_all(own_gates, "col", split_axis=0, concat_axis=2, tiled=True)[0]
        back_rows = (
            jnp.einsum("erf,edf->erd", grad_gate, gate_weight, preferred_element_type=jnp.float32)
            + jnp.einsum("erf,edf->erd", grad_up, up_weight, preferred_element_type=jnp.float32)
        ).astype(jnp.bfloat16)
        grad_feed = return_rows(spread_plain, back_rows).astype(jnp.float32)
        out_rows = jnp.einsum(
            "erf,efd->erd", activated, down_weight, preferred_element_type=jnp.float32
        ).astype(jnp.bfloat16)
        mixture = return_rows(spread_probs, out_rows).astype(jnp.float32)
        grad_gate_weight = jnp.einsum(
            "erd,erf->edf", expert_rows, grad_gate, preferred_element_type=jnp.float32
        )
        grad_up_weight = jnp.einsum(
            "erd,erf->edf", expert_rows, grad_up, preferred_element_type=jnp.float32
        )
        grad_down_weight = jnp.einsum(
            "erf,erd->efd", weighted_act, expert_grads, preferred_element_type=jnp.float32
        )
    grad_out = cotangent.astype(jnp.float32)
    grad_logits = (
        router_probs * (grad_probs - jnp.sum(router_probs * grad_probs, axis=-1, keepdims=True))
    ).astype(jnp.bfloat16)
    router_grad = inner_rows(feed_normed, grad_logits)
    grad_feed = grad_feed + outer_cols(grad_logits, router_full)
    feed_gain_term = jnp.sum(grad_feed * hidden * feed_scale, axis=0)
    feed_weighted = grad_feed * feed_float
    grad_hidden = (
        grad_out
        + feed_scale * feed_weighted
        - hidden * feed_scale**3 * jnp.mean(feed_weighted * hidden, axis=-1, keepdims=True)
    )
    grad_branch = lax.all_gather(grad_hidden.astype(jnp.bfloat16), "row", axis=0, tiled=True)
    output_grad = inner_rows(mixed_heads, grad_branch)
    grad_mixed = (
        outer_cols(grad_branch, output_full).astype(jnp.bfloat16).reshape(length, local_heads, HD)
    )

    def backward_block(carry, offset):
        grad_keys, grad_values = carry
        query_rows, scores = block_scores(offset)
        lse_rows = lax.dynamic_slice_in_dim(lse_all, offset, block_rows, 1)
        probs_block = jnp.exp(scores - lse_rows[:, :, None])
        weights_low = probs_block.astype(jnp.bfloat16)
        grad_rows_out = lax.dynamic_slice_in_dim(grad_mixed, offset, block_rows, 0)
        grad_weights = jnp.einsum(
            "qhd,khd->hqk", grad_rows_out, value_heads, preferred_element_type=jnp.float32
        )
        grad_values = grad_values + jnp.einsum(
            "hqk,qhd->khd", weights_low, grad_rows_out, preferred_element_type=jnp.float32
        )
        delta_rows = jnp.sum(probs_block * grad_weights, axis=-1, keepdims=True)
        grad_scores = (probs_block * (grad_weights - delta_rows)).astype(jnp.bfloat16)
        grad_query_block = (
            jnp.einsum(
                "hqk,khd->qhd", grad_scores, keys_rotated, preferred_element_type=jnp.float32
            )
            * score_scale
        )
        grad_keys = (
            grad_keys
            + jnp.einsum(
                "hqk,qhd->khd", grad_scores, query_rows, preferred_element_type=jnp.float32
            )
            * score_scale
        )
        return ((grad_keys, grad_values), grad_query_block)

    zero_heads = jnp.zeros((length, local_heads, HD), jnp.float32)
    (grad_keys, grad_values), grad_query_blocks = lax.scan(
        backward_block, (zero_heads, zero_heads), starts
    )
    grad_queries = grad_query_blocks.reshape(length, local_heads, HD)
    grad_query_normed = unrotate(grad_queries, cosine, sine_table).reshape(length, local_width)
    grad_key_normed = unrotate(grad_keys, cosine, sine_table).reshape(length, local_width)
    grad_value_low = grad_values.reshape(length, local_width).astype(jnp.bfloat16)
    query_weighted = grad_query_normed * query_gain_f
    key_weighted = grad_key_normed * key_gain_f
    query_gain_term = jnp.sum(grad_query_normed * query_raw * query_rs, axis=0)
    key_gain_term = jnp.sum(grad_key_normed * key_raw * key_rs, axis=0)
    query_inner, key_inner = (
        lax.psum(jnp.sum(query_weighted * query_raw, axis=-1).astype(jnp.bfloat16), "row").astype(
            jnp.float32
        ),
        lax.psum(jnp.sum(key_weighted * key_raw, axis=-1).astype(jnp.bfloat16), "row").astype(
            jnp.float32
        ),
    )
    grad_query_raw = (
        query_rs * query_weighted - query_raw * query_rs**3 * (query_inner / model_width)[:, None]
    ).astype(jnp.bfloat16)
    grad_key_raw = (
        key_rs * key_weighted - key_raw * key_rs**3 * (key_inner / model_width)[:, None]
    ).astype(jnp.bfloat16)
    query_grad = inner_rows(normed, grad_query_raw)
    key_grad = inner_rows(normed, grad_key_raw)
    value_grad = inner_rows(normed, grad_value_low)
    grad_normed = (
        outer_cols(grad_query_raw, query_full)
        + outer_cols(grad_key_raw, key_full)
        + outer_cols(grad_value_low, value_full)
    )
    attention_weighted = grad_normed * attention_float
    grad_seq_part = seq_scale * attention_weighted - seq_float * seq_scale**3 * jnp.mean(
        attention_weighted * seq_float, axis=-1, keepdims=True
    )
    attention_gain_term = jnp.sum(grad_normed * seq_float * seq_scale, axis=0)
    if near:
        cols = lax.axis_size("col")
        pack = jnp.concatenate(
            [
                attention_gain_term.reshape(cols, -1),
                feed_gain_term.reshape(cols, -1),
                query_gain_term.reshape(cols, -1),
                key_gain_term.reshape(cols, -1),
                router_grad.reshape(cols, -1),
            ],
            axis=1,
        )
        pack = jnp.pad(pack, ((0, 0), (0, PACK_ROWS * 128 - pack.shape[1])))
        pack = pack.astype(jnp.bfloat16).reshape(cols, PACK_ROWS, 128)
        (
            mixture, summed, grad_query_weight, grad_key_weight, grad_value_weight, grad_output_weight, packs
        ) = finish_near(
            mixture_part,
            grad_seq_part.astype(jnp.bfloat16).reshape(rows_count, tokens, model_width),
            [grad.astype(jnp.bfloat16) for grad in (query_grad, key_grad, value_grad, output_grad)],
            pack,
            4,
        )
        input_grad = grad_hidden + summed
        packs = packs.reshape(cols, rows_count, -1).astype(jnp.float32)
        whole = jnp.sum(packs, axis=(0, 1))
        heads_sum = jnp.sum(
            lax.dynamic_index_in_dim(packs, lax.axis_index("row"), 1, keepdims=False), axis=0
        )
        grad_attention_gain = whole[: ends[0]]
        grad_feed_gain = whole[ends[0] : ends[1]]
        grad_query_gain = heads_sum[ends[1] : ends[2]]
        grad_key_gain = heads_sum[ends[2] : ends[3]]
        grad_router_weight = whole[ends[3] : ends[3] + router_weight.size].reshape(router_weight.shape)
    else:
        stacked = jnp.concatenate(
            [
                grad_seq_part.reshape(rows_count, tokens, model_width),
                jnp.broadcast_to(attention_gain_term[None, None, :], (rows_count, 1, model_width)),
            ],
            axis=1,
        ).reshape(rows_count * (tokens + 1), model_width)
        summed = lax.psum_scatter(
            stacked.astype(jnp.bfloat16), "row", scatter_dimension=0, tiled=True
        ).astype(jnp.float32)
        input_grad = grad_hidden + summed[:tokens]
        attention_gain_total = summed[tokens]
        feed_gain_total, router_total = (
            lax.psum(feed_gain_term.astype(jnp.bfloat16), "row").astype(jnp.float32),
            lax.psum(router_grad.astype(jnp.bfloat16), "row").astype(jnp.float32),
        )
        (
            grad_attention_gain,
            grad_query_gain,
            grad_key_gain,
            grad_query_weight,
            grad_key_weight,
            grad_value_weight,
            grad_output_weight,
            grad_feed_gain,
            grad_router_weight,
        ) = (
            lax.psum_scatter(
                attention_gain_total.astype(jnp.bfloat16), "col", scatter_dimension=0, tiled=True
            ).astype(jnp.float32),
            lax.psum_scatter(
                query_gain_term.astype(jnp.bfloat16), "col", scatter_dimension=0, tiled=True
            ).astype(jnp.float32),
            lax.psum_scatter(
                key_gain_term.astype(jnp.bfloat16), "col", scatter_dimension=0, tiled=True
            ).astype(jnp.float32),
            lax.psum_scatter(
                query_grad.astype(jnp.bfloat16), "col", scatter_dimension=0, tiled=True
            ).astype(jnp.float32),
            lax.psum_scatter(
                key_grad.astype(jnp.bfloat16), "col", scatter_dimension=0, tiled=True
            ).astype(jnp.float32),
            lax.psum_scatter(
                value_grad.astype(jnp.bfloat16), "col", scatter_dimension=0, tiled=True
            ).astype(jnp.float32),
            lax.psum_scatter(
                output_grad.astype(jnp.bfloat16), "col", scatter_dimension=1, tiled=True
            ).astype(jnp.float32),
            lax.psum_scatter(
                feed_gain_total.astype(jnp.bfloat16), "col", scatter_dimension=0, tiled=True
            ).astype(jnp.float32),
            lax.psum_scatter(
                router_total.astype(jnp.bfloat16), "col", scatter_dimension=0, tiled=True
            ).astype(jnp.float32),
        )
    layer_output = hidden + mixture
    return (
        layer_output,
        input_grad,
        grad_attention_gain,
        grad_query_gain,
        grad_key_gain,
        grad_query_weight,
        grad_key_weight,
        grad_value_weight,
        grad_output_weight,
        grad_feed_gain,
        grad_router_weight,
        grad_gate_weight,
        grad_up_weight,
        grad_down_weight,
    )


def solution(mesh):
    placed = (
        P(("col", "row"), None),
        P(("col", "row"), None),
        P(("col", "row"), None),
        P("col"),
        P(("row", "col")),
        P(("row", "col")),
        P("col", "row"),
        P("col", "row"),
        P("col", "row"),
        P("row", "col"),
        P("col"),
        P("col", None),
        P("col", None, "row"),
        P("col", None, "row"),
        P("col", "row", None),
    )
    return jax.shard_map(
        local,
        mesh=mesh,
        in_specs=placed,
        out_specs=(
            P(("col", "row"), None),
            P(("col", "row"), None),
            P("col"),
            P(("row", "col")),
            P(("row", "col")),
            P("col", "row"),
            P("col", "row"),
            P("col", "row"),
            P("row", "col"),
            P("col"),
            P("col", None),
            P("col", None, "row"),
            P("col", None, "row"),
            P("col", "row", None),
        ),
        check_vma=False,
    )
```

```python
import functools

import jax
import jax.numpy as jnp
from jax import lax
from jax.experimental import pallas as pl
from jax.experimental.pallas import tpu as pltpu
from jax.sharding import PartitionSpec as P

HD = 128
SLOTS = 40
BLOCK = 512
CHUNK = 256
UNROLL = 4
PACK_ROWS = 144


EPS = 1e-05
THETA = 10000.0
MASKED = -1e30


def wide_dot(left, right):
    return jnp.dot(left, right, preferred_element_type=jnp.float32)


def inner_rows(left, right):
    return lax.dot_general(
        left, right, (((0,), (0,)), ((), ())), preferred_element_type=jnp.float32
    )


def outer_cols(left, right):
    return lax.dot_general(
        left, right, (((1,), (1,)), ((), ())), preferred_element_type=jnp.float32
    )


def rms_scale(field):
    return lax.rsqrt(jnp.mean(field * field, axis=-1, keepdims=True) + EPS)


def rope_tables(length):
    half_size = HD // 2
    freqs = THETA ** (-(jnp.arange(half_size, dtype=jnp.float32) * 2.0) / HD)
    angles = jnp.arange(length, dtype=jnp.float32)[:, None] * freqs[None, :]
    cosine = jnp.concatenate([jnp.cos(angles), jnp.cos(angles)], axis=-1)
    sine_table = jnp.concatenate([-jnp.sin(angles), jnp.sin(angles)], axis=-1)
    return (cosine, sine_table)


def dispatch_body(pick_ref, field_ref, rows_ref):
    groups = rows_ref.shape[0]
    first = wide_dot(pick_ref[0], field_ref[0]).reshape(groups, SLOTS, -1)
    second = wide_dot(pick_ref[1], field_ref[1]).reshape(groups, SLOTS, -1)
    rows_ref[...] = jnp.concatenate([first, second], axis=1).astype(jnp.bfloat16)


def dispatch(pick, field):
    ranks, width, tokens = pick.shape
    groups, depth = width // SLOTS, field.shape[1]
    return pl.pallas_call(
        dispatch_body,
        grid=(ranks // 2, depth // BLOCK),
        in_specs=[
            pl.BlockSpec((2, width, tokens), lambda i, k: (i, 0, 0)),
            pl.BlockSpec((2, tokens, BLOCK), lambda i, k: (i, 0, k)),
        ],
        out_specs=pl.BlockSpec((groups, 2 * SLOTS, BLOCK), lambda i, k: (0, i, k)),
        out_shape=jax.ShapeDtypeStruct((groups, ranks * SLOTS, depth), jnp.bfloat16),
    )(pick, field.reshape(ranks, tokens, depth))


def combine_body(spread_ref, rows_ref, field_ref):
    rows = rows_ref[...].astype(jnp.float32)
    width = rows.shape[0] * SLOTS
    for side in range(2):
        part = rows[:, side * SLOTS : (side + 1) * SLOTS].reshape(width, -1).astype(jnp.bfloat16)
        field_ref[side] = wide_dot(spread_ref[side], part).astype(jnp.bfloat16)


def combine(spread, rows):
    ranks, tokens, width = spread.shape
    groups, depth = width // SLOTS, rows.shape[2]
    field = pl.pallas_call(
        combine_body,
        grid=(ranks // 2, depth // BLOCK),
        in_specs=[
            pl.BlockSpec((2, tokens, width), lambda i, k: (i, 0, 0)),
            pl.BlockSpec((groups, 2 * SLOTS, BLOCK), lambda i, k: (0, i, k)),
        ],
        out_specs=pl.BlockSpec((2, tokens, BLOCK), lambda i, k: (i, 0, k)),
        out_shape=jax.ShapeDtypeStruct((ranks, tokens, depth), jnp.bfloat16),
    )(spread, rows)
    return field.reshape(ranks * tokens, depth)


def scatter_all(field):
    part = lax.psum_scatter(field, "col", scatter_dimension=0, tiled=True)
    return lax.psum_scatter(part, "row", scatter_dimension=0, tiled=True)


def pieces_of(ranks, depth):
    count = max(1, ranks // 32)
    step = depth // count
    return [(at, at + step) for at in range(0, depth, step)]


def gather_rows(pick, field):
    rows = []
    for start, stop in pieces_of(pick.shape[0], field.shape[1]):
        part = field[:, start:stop]
        if rows:
            part = lax.optimization_barrier((part, rows[-1]))[0]
        whole = lax.all_gather(part, ("col", "row"), axis=0, tiled=True)
        rows.append(dispatch(pick, whole))
    return rows[0] if len(rows) == 1 else jnp.concatenate(rows, axis=2)


def return_rows(spread, rows):
    sums = []
    for start, stop in pieces_of(spread.shape[0], rows.shape[2]):
        part = rows[:, :, start:stop]
        if sums:
            part = lax.optimization_barrier((part, sums[-1]))[0]
        sums.append(scatter_all(combine(spread, part)))
    return sums[0] if len(sums) == 1 else jnp.concatenate(sums, axis=1)


MESH = pl.DeviceIdType.MESH


def seat():
    r, c = lax.axis_index("row"), lax.axis_index("col")
    y, x = r // 2, r % 2
    z, core = c // 2, c % 2
    first = y * (1 - core) + x * core
    second = x * (1 - core) + y * core
    return r, c, y, x, z, core, first, second


def partners():
    r, c, y, x, z, core, first, second = seat()
    pair = (r, z * 2 + (1 - core))
    flip_y = (1 - y) * 2 + x
    flip_x = y * 2 + (1 - x)
    along_first = (flip_y * (1 - core) + flip_x * core, c)
    along_second = (flip_x * (1 - core) + flip_y * core, c)
    up = [(r, ((z + k) % 4) * 2 + core) for k in range(1, 4)]
    return pair, along_first, along_second, up


RANKS = 32


def nth(offset):
    spot = (lax.axis_index("col") * 4 + lax.axis_index("row") + offset) % RANKS
    return spot, (spot % 4, spot // 4)


def meet():
    barrier = pltpu.get_barrier_semaphore()

    @pl.loop(1, RANKS)
    def _(offset):
        pl.semaphore_signal(barrier, inc=1, device_id=nth(offset)[1], device_id_type=MESH)

    pl.semaphore_wait(barrier, RANKS - 1)


def small_copy(src_of, small_all, small_send, small_recv, offset):
    spot, device = nth(offset)
    return send(
        src_of(spot), small_all.at[nth(0)[0]], small_send.at[offset], small_recv.at[offset], device
    )


def row_of(core, first, second):
    y = first * (1 - core) + second * core
    x = second * (1 - core) + first * core
    return y, x


def send(src, dst, send_sem, recv_sem, device):
    return pltpu.make_async_remote_copy(
        src_ref=src, dst_ref=dst, send_sem=send_sem, recv_sem=recv_sem, device_id=device, device_id_type=MESH
    )


GSTEPS = 4
QUEUE = (2, 1, 3)
ARRIVE = (1, 3, 2)


def spread_out(own_ref, all_ref, sems):
    r, c, y, x, z, core, first, second = seat()
    pair, along_first, along_second, up = partners()
    here_sem, z_send, z_recv, g_send, g_recv, f_send, f_recv, p_send, p_recv = sems
    step = own_ref.shape[0] // GSTEPS

    def rows(q):
        return pl.ds(pl.multiple_of(q * step, step), step)

    def place(k, s, f, q):
        sec = second * (1 - s) + (1 - second) * s
        fir = first * (1 - f) + (1 - first) * f
        yy, xx = row_of(core, fir, sec)
        return all_ref.at[(z + 4 - k) % 4, core, yy, xx, rows(q)]

    def z_copy(k, q):
        return send(
            own_ref.at[rows(q)], place(0, 0, 0, q), z_send.at[k - 1, q], z_recv.at[k - 1, q], up[k - 1]
        )

    def g_copy(k, q, src):
        return send(src, place(k, 0, 0, q), g_send.at[k, q], g_recv.at[k, q], along_second)

    def f_copy(k, s, q, src):
        return send(src, place(k, s, 0, q), f_send.at[s, k, q], f_recv.at[s, k, q], along_first)

    def p_copy(k, s, f, q, src):
        return send(src, place(k, s, f, q), p_send.at[f, s, k, q], p_recv.at[f, s, k, q], pair)

    here = pltpu.make_async_copy(own_ref, all_ref.at[z, core, y, x], here_sem)

    def begin():
        here.start()

        @pl.loop(0, GSTEPS)
        def _(q):
            src = own_ref.at[rows(q)]
            for k in QUEUE:
                z_copy(k, q).start()
            g_copy(0, q, src).start()
            f_copy(0, 0, q, src).start()
            p_copy(0, 0, 0, q, src).start()

    def forward(q):
        for k in ARRIVE:
            z_copy(k, q).wait_recv()
            src = place(k, 0, 0, q)
            g_copy(k, q, src).start()
            f_copy(k, 0, q, src).start()
            p_copy(k, 0, 0, q, src).start()
        for k in (0, *ARRIVE):
            src = place(k, 1, 0, q)
            g_copy(k, q, src).wait_recv()
            f_copy(k, 1, q, src).start()
            p_copy(k, 1, 0, q, src).start()
        for k in (0, *ARRIVE):
            src = place(k, 0, 1, q)
            f_copy(k, 0, q, src).wait_recv()
            p_copy(k, 0, 1, q, src).start()

    def finish():
        @pl.loop(0, GSTEPS)
        def _(q):
            for k in (0, *ARRIVE):
                src = place(k, 1, 1, q)
                f_copy(k, 1, q, src).wait_recv()
                p_copy(k, 1, 1, q, src).start()

        here.wait()

        @pl.loop(0, GSTEPS)
        def _(q):
            for k in range(4):
                src = own_ref.at[rows(q)]
                if k:
                    z_copy(k, q).wait_send()
                g_copy(k, q, src).wait_send()
                for s in range(2):
                    f_copy(k, s, q, src).wait_send()
                    for f in range(2):
                        p_copy(k, s, f, q, src).wait()

    return begin, forward, finish


def spread_sems():
    dma = pltpu.SemaphoreType.DMA
    shapes = [(3, GSTEPS), (4, GSTEPS), (2, 4, GSTEPS), (2, 2, 4, GSTEPS)]
    return [dma(())] + [dma(shape) for shape in shapes for _ in range(2)]


def small_out(small_ref, small_all, sems):
    here_sem, small_send, small_recv = sems
    local = pltpu.make_async_copy(small_ref, small_all.at[nth(0)[0]], here_sem)

    def copy(offset):
        return small_copy(lambda spot: small_ref, small_all, small_send, small_recv, offset)

    def begin():
        local.start()

        @pl.loop(1, RANKS)
        def _(offset):
            copy(offset).start()

    def finish():
        local.wait()

        @pl.loop(1, RANKS)
        def _(offset):
            copy(offset).wait()

    return begin, finish


def small_sems():
    dma = pltpu.SemaphoreType.DMA
    return [dma(()), dma((RANKS,)), dma((RANKS,))]


ANYWHERE = pl.BlockSpec(memory_space=pl.ANY)


def start_body(x_ref, q_ref, k_ref, v_ref, o_ref, pack_ref, own_ref, small_ref,
               x_all, q_all, k_all, v_all, o_all, pack_all, all_ref, small_all, *sems):
    r, c, y, x, z, core, first, second = seat()
    pair, along_first, along_second, up = partners()
    begin, forward, finish = spread_out(own_ref, all_ref, sems[:9])
    small_begin, small_finish = small_out(small_ref, small_all, sems[9:12])
    here_sem, x_send, x_recv, w_send, w_recv, v_send, v_recv = sems[12:]
    weights = [(q_ref, q_all), (k_ref, k_all), (v_ref, v_all), (o_ref, o_all), (pack_ref, pack_all)]

    def block(index, col):
        ref, whole = weights[index]
        if index == 4:
            return whole.at[col]
        if index == 3:
            width = ref.shape[1]
            return whole.at[:, pl.ds(pl.multiple_of(col * width, width), width)]
        height = ref.shape[0]
        return whole.at[pl.ds(pl.multiple_of(col * height, height), height)]

    def w_copy(index, k):
        return send(
            weights[index][0], block(index, c), w_send.at[index, k - 1], w_recv.at[index, k - 1], up[k - 1]
        )

    def pair_copy(index, k):
        col = ((z + 4 - k) % 4) * 2 + core
        src = weights[index][0] if k == 0 else block(index, col)
        return send(src, block(index, col), v_send.at[index, k], v_recv.at[index, k], pair)

    locals_ = [pltpu.make_async_copy(x_ref, x_all.at[r], here_sem.at[5])] + [
        pltpu.make_async_copy(weights[i][0], block(i, c), here_sem.at[i]) for i in range(5)
    ]
    y1, x1 = row_of(core, first, 1 - second)
    near_row = y1 * 2 + x1
    x_first = send(x_ref, x_all.at[r], x_send.at[0], x_recv.at[0], along_first)
    x_second = send(x_ref, x_all.at[r], x_send.at[1], x_recv.at[1], along_second)
    x_relay = send(x_all.at[near_row], x_all.at[near_row], x_send.at[2], x_recv.at[2], along_first)

    meet()
    small_begin()
    x_second.start()
    x_first.start()
    begin()
    for index in (4, 0, 1, 2, 3):
        for k in QUEUE:
            w_copy(index, k).start()
        pair_copy(index, 0).start()
    for item in locals_:
        item.start()
    x_second.wait_recv()
    x_relay.start()

    @pl.loop(0, GSTEPS)
    def _(q):
        forward(q)

    for index in (4, 0, 1, 2, 3):
        for k in ARRIVE:
            w_copy(index, k).wait_recv()
            pair_copy(index, k).start()
    finish()
    small_finish()
    for item in locals_:
        item.wait()
    x_first.wait()
    x_second.wait_send()
    x_relay.wait()
    for index in range(5):
        for k in range(4):
            if k:
                w_copy(index, k).wait_send()
            pair_copy(index, k).wait()


def start_near(x, weights, pack, own, small, collective_id):
    tokens, depth = own.shape
    dma = pltpu.SemaphoreType.DMA
    height, width = weights[0].shape
    shaped = lambda shape, like: jax.ShapeDtypeStruct(shape, like.dtype)
    outs = pl.pallas_call(
        start_body,
        out_shape=(
            shaped((4, *x.shape), x),
            *[shaped((8 * height, width), w) for w in weights[:3]],
            shaped((weights[3].shape[0], 8 * weights[3].shape[1]), weights[3]),
            shaped((8, *pack.shape), pack),
            shaped((4, 2, 2, 2, tokens, depth), own),
            shaped((RANKS, *small.shape), small),
        ),
        in_specs=[ANYWHERE] * 8,
        out_specs=[ANYWHERE] * 8,
        scratch_shapes=spread_sems()
        + small_sems()
        + [dma((6,)), dma((3,)), dma((3,)), dma((5, 3)), dma((5, 3)), dma((5, 4)), dma((5, 4))],
        compiler_params=pltpu.CompilerParams(collective_id=collective_id, has_side_effects=True),
    )(x, *weights, pack, own, small)
    x_all, q, k, v, o, pack_all, whole, small_all = outs
    return x_all.reshape(-1, x.shape[1]), q, k, v, o, pack_all, whole.reshape(RANKS, tokens, depth), small_all


def finish_body(part_ref, field_ref, q_ref, k_ref, v_ref, o_ref, pack_ref,
                mixture_ref, out_ref, q_out, k_out, v_out, o_out, pack_all,
                mine, first_in, second_in, total,
                q_mine, k_mine, v_mine, o_mine, q_pair, k_pair, v_pair, o_pair, q_z, k_z, v_z, o_z,
                q_sum, k_sum, v_sum, o_sum,
                load_sem, f_send, f_recv, g_send, g_recv, w_load, p_send, p_recv, z_send, z_recv, out_sem,
                *rest):
    r, c, y, x, z, core, first, second = seat()
    pair, along_first, along_second, up = partners()
    small_begin, small_finish = small_each(pack_ref, pack_all, rest[:3], lambda spot: spot // 4)
    begin, tick, finish = shrink(part_ref, *rest[3:9], rest[9:18])
    mixture = rest[8]
    tokens, depth = out_ref.shape
    other = 1 - core
    grads = [q_ref, k_ref, v_ref, o_ref]
    kept, pairs, zs = [q_mine, k_mine, v_mine, o_mine], [q_pair, k_pair, v_pair, o_pair], [q_z, k_z, v_z, o_z]
    sums, outs = [q_sum, k_sum, v_sum, o_sum], [q_out, k_out, v_out, o_out]

    def block(index, col):
        ref = grads[index]
        if index == 3:
            width = ref.shape[1] // 8
            return ref.at[:, pl.ds(pl.multiple_of(col * width, width), width)]
        height = ref.shape[0] // 8
        return ref.at[pl.ds(pl.multiple_of(col * height, height), height)]

    def row(fir, sec):
        yy, xx = row_of(core, fir, sec)
        return yy * 2 + xx

    def load(fir, sec):
        return pltpu.make_async_copy(field_ref.at[row(fir, sec)], mine.at[fir, sec], load_sem.at[fir, sec])

    def f_copy(sec):
        return send(field_ref.at[row(1 - first, sec)], first_in.at[sec], f_send.at[sec], f_recv.at[sec], along_first)

    g_copy = send(mine.at[first, 1 - second], second_in, g_send, g_recv, along_second)

    def w_load_copy(index, zz):
        return pltpu.make_async_copy(block(index, zz * 2 + core), kept[index].at[zz], w_load.at[index, zz])

    def w_give(index, zz):
        return send(
            block(index, zz * 2 + other), pairs[index].at[zz], p_send.at[index, zz], p_recv.at[index, zz], pair
        )

    def w_z(index, k):
        return send(
            kept[index].at[(z + k) % 4], zs[index].at[k - 1], z_send.at[index, k - 1], z_recv.at[index, k - 1], up[k - 1]
        )

    def add(ref, extras):
        @pl.loop(0, ref.shape[0] // TILE)
        def _(t):
            here = pl.ds(pl.multiple_of(t * TILE, TILE), TILE)
            value = ref[here].astype(jnp.float32)
            for extra in extras:
                value = value + extra[here].astype(jnp.float32)
            ref[here] = value.astype(jnp.bfloat16)

    def add_out(ref, extras, result):
        @pl.loop(0, ref.shape[0] // TILE)
        def _(t):
            here = pl.ds(pl.multiple_of(t * TILE, TILE), TILE)
            value = ref[here].astype(jnp.float32)
            for extra in extras:
                value = value + extra[here].astype(jnp.float32)
            result[here] = value

    meet()
    for index in range(4):
        for k in (2, 1, 3, 0):
            w_give(index, (z + k) % 4).start()
            w_load_copy(index, (z + k) % 4).start()
    begin()
    f_copy(1 - second).start()
    f_copy(second).start()
    load(first, 1 - second).start()
    load(first, second).start()
    small_begin()
    for index in range(4):
        for k in QUEUE:
            zz = (z + k) % 4
            w_load_copy(index, zz).wait()
            w_give(index, zz).wait_recv()
            add(kept[index].at[zz], [pairs[index].at[zz]])
            w_z(index, k).start()

    @pl.loop(0, RSTEPS)
    def _(i):
        tick(i)

        @pl.when(i == 2)
        def _():
            load(first, 1 - second).wait()
            f_copy(1 - second).wait_recv()
            add(mine.at[first, 1 - second], [first_in.at[1 - second]])
            g_copy.start()

    for index in range(4):
        w_load_copy(index, z).wait()
        w_give(index, z).wait_recv()
        for k in ARRIVE:
            w_z(index, k).wait_recv()
        add_out(
            kept[index].at[z], [pairs[index].at[z]] + [zs[index].at[k] for k in range(3)], sums[index]
        )
        pltpu.make_async_copy(sums[index], outs[index], out_sem.at[index]).start()
    load(first, second).wait()
    f_copy(second).wait_recv()
    g_copy.wait_recv()
    add_out(mine.at[first, second], [first_in.at[second], second_in], total)
    pltpu.make_async_copy(total, out_ref, out_sem.at[4]).start()

    @pl.loop(RSTEPS, TICKS)
    def _(i):
        tick(i)

    pltpu.make_async_copy(mixture, mixture_ref, out_sem.at[5]).start()
    finish()
    for sec in range(2):
        f_copy(sec).wait_send()
    g_copy.wait_send()
    for index in range(4):
        for k in range(4):
            w_give(index, (z + k) % 4).wait_send()
            if k:
                w_z(index, k).wait_send()
        pltpu.make_async_copy(sums[index], outs[index], out_sem.at[index]).wait()
    small_finish()
    pltpu.make_async_copy(total, out_ref, out_sem.at[4]).wait()
    pltpu.make_async_copy(mixture, mixture_ref, out_sem.at[5]).wait()


def finish_near(part, field, grads, pack, collective_id):
    rows_count, tokens, depth = field.shape
    dma = pltpu.SemaphoreType.DMA
    blocks = [(g.shape[0] // 8, g.shape[1]) for g in grads[:3]] + [(grads[3].shape[0], grads[3].shape[1] // 8)]
    half = lambda *shape: pltpu.VMEM(shape, jnp.bfloat16)
    return pl.pallas_call(
        finish_body,
        out_shape=(
            jax.ShapeDtypeStruct((tokens, depth), jnp.float32),
            jax.ShapeDtypeStruct((tokens, depth), jnp.float32),
            *[jax.ShapeDtypeStruct(b, jnp.float32) for b in blocks],
            jax.ShapeDtypeStruct((RANKS, *pack.shape[1:]), pack.dtype),
        ),
        in_specs=[ANYWHERE] * 7,
        out_specs=[ANYWHERE] * 7,
        scratch_shapes=[
            half(2, 2, tokens, depth), half(2, tokens, depth), half(tokens, depth),
            pltpu.VMEM((tokens, depth), jnp.float32),
            *[half(4, *b) for b in blocks], *[half(4, *b) for b in blocks], *[half(3, *b) for b in blocks],
            *[pltpu.VMEM(b, jnp.float32) for b in blocks],
            dma((2, 2)), dma((2,)), dma((2,)), dma(()), dma(()),
            dma((4, 4)), dma((4, 4)), dma((4, 4)), dma((4, 3)), dma((4, 3)), dma((6,)),
        ]
        + small_sems()
        + shrink_scratch(tokens, depth),
        compiler_params=pltpu.CompilerParams(
            collective_id=collective_id, has_side_effects=True, vmem_limit_bytes=63 * 1024 * 1024
        ),
    )(part.reshape(4, 2, 2, 2, tokens, depth), field, *grads, pack)


RSTEPS = 8
TILE = 16
LAGS = (0, 1, 2, 4)
TICKS = RSTEPS + LAGS[3]


def shrink(part_ref, sums, near_own, first_in, second_in, z_in, total, sems):
    r, c, y, x, z, core, first, second = seat()
    pair, along_first, along_second, up = partners()
    load_sem, p_send, p_recv, f_send, f_recv, g_send, g_recv, z_send, z_recv = sems
    tokens = total.shape[0]
    step = tokens // RSTEPS
    other = 1 - core

    def rows(q):
        return pl.ds(pl.multiple_of(q * step, step), step)

    def spot(kind):
        fir = (1 - first) if kind < 2 else first
        sec = (1 - second) if kind in (0, 2) else second
        return fir, sec

    def load(kind, q):
        yy, xx = row_of(core, *spot(kind))
        return pltpu.make_async_copy(
            part_ref.at[:, core, yy, xx, rows(q)], near_own.at[q % 2, kind], load_sem.at[kind, q % 2]
        )

    def give(fir, sec, q):
        yy, xx = row_of(other, fir, sec)
        return send(
            part_ref.at[:, other, yy, xx, rows(q)],
            sums.at[fir, sec, :, rows(q)],
            p_send.at[fir, sec, q],
            p_recv.at[fir, sec, q],
            pair,
        )

    def f_copy(sec, q):
        return send(
            sums.at[1 - first, sec, :, rows(q)],
            first_in.at[sec, :, rows(q)],
            f_send.at[sec, q],
            f_recv.at[sec, q],
            along_first,
        )

    def g_copy(q):
        return send(
            sums.at[first, 1 - second, :, rows(q)], second_in.at[:, rows(q)], g_send.at[q], g_recv.at[q], along_second
        )

    def z_copy(k, q):
        return send(
            sums.at[first, second, (z + k) % 4, rows(q)],
            z_in.at[k - 1, rows(q)],
            z_send.at[k - 1, q],
            z_recv.at[k - 1, q],
            up[k - 1],
        )

    def begin():
        @pl.loop(0, RSTEPS)
        def _(q):
            for fir, sec in ((1 - second, 1 - first), (1 - second, first), (second, 1 - first), (second, first)):
                give(fir, sec, q).start()

        for kind in range(4):
            load(kind, 0).start()

    def add(kind, q, extra):
        fir, sec = spot(kind)

        @pl.when(q + 1 < RSTEPS)
        def _():
            load(kind, q + 1).start()

        load(kind, q).wait()
        give(fir, sec, q).wait_recv()

        @pl.loop(0, 4 * (step // TILE))
        def _(t):
            zz, at = t // (step // TILE), t % (step // TILE)
            here = pl.ds(pl.multiple_of(q * step + at * TILE, TILE), TILE)
            near = pl.ds(pl.multiple_of(at * TILE, TILE), TILE)
            value = sums[fir, sec, zz, here].astype(jnp.float32)
            value = value + near_own[q % 2, kind, zz, near].astype(jnp.float32)
            for ref in extra:
                value = value + ref[zz, here].astype(jnp.float32)
            sums[fir, sec, zz, here] = value.astype(jnp.bfloat16)

    def stage_first(q):
        for kind, sec in ((0, 1 - second), (1, second)):
            add(kind, q, [])
            f_copy(sec, q).start()

    def stage_second(q):
        f_copy(1 - second, q).wait_recv()
        add(2, q, [first_in.at[1 - second]])
        g_copy(q).start()

    def stage_z(q):
        f_copy(second, q).wait_recv()
        g_copy(q).wait_recv()
        add(3, q, [first_in.at[second], second_in])
        for k in QUEUE:
            z_copy(k, q).start()

    def stage_out(q):
        for k in ARRIVE:
            z_copy(k, q).wait_recv()

        @pl.loop(0, step // TILE)
        def _(t):
            here = pl.ds(pl.multiple_of(q * step + t * TILE, TILE), TILE)
            value = sums[first, second, z, here].astype(jnp.float32)
            for k in range(3):
                value = value + z_in[k, here].astype(jnp.float32)
            total[here] = value

    def tick(i):
        for stage, lag in zip((stage_first, stage_second, stage_z, stage_out), LAGS):

            @pl.when((i >= lag) & (i < RSTEPS + lag))
            def _(stage=stage, lag=lag):
                stage(i - lag)

    def finish():
        @pl.loop(0, RSTEPS)
        def _(q):
            for fir in range(2):
                for sec in range(2):
                    give(fir, sec, q).wait_send()
            for sec in range(2):
                f_copy(sec, q).wait_send()
            g_copy(q).wait_send()
            for k in QUEUE:
                z_copy(k, q).wait_send()

    return begin, tick, finish


def shrink_scratch(tokens, depth):
    dma = pltpu.SemaphoreType.DMA
    low = lambda *shape: pltpu.VMEM((*shape, depth), jnp.bfloat16)
    buffers = [
        low(2, 2, 4, tokens), low(2, 4, 4, tokens // RSTEPS), low(2, 4, tokens), low(4, tokens), low(3, tokens),
        pltpu.VMEM((tokens, depth), jnp.float32),
    ]
    shapes = [(2, 2, RSTEPS), (2, RSTEPS), (RSTEPS,), (3, RSTEPS)]
    return buffers + [dma((4, 2))] + [dma(shape) for shape in shapes for _ in range(2)]


def small_each(small_ref, small_all, sems, pick):
    here_sem, small_send, small_recv = sems
    local = pltpu.make_async_copy(small_ref.at[pick(nth(0)[0])], small_all.at[nth(0)[0]], here_sem)

    def copy(offset):
        return small_copy(lambda spot: small_ref.at[pick(spot)], small_all, small_send, small_recv, offset)

    def begin():
        local.start()

        @pl.loop(1, RANKS)
        def _(offset):
            copy(offset).start()

    def finish():
        local.wait()

        @pl.loop(1, RANKS)
        def _(offset):
            copy(offset).wait()

    return begin, finish


SPACING = 5


def feed_back_body(part_ref, small_ref, rows_ref, gate_ref, up_ref, act_ref, grads_ref,
                   out_ref, small_all, gate_out, up_out, down_out, *scratch):
    begin, tick, finish = shrink(part_ref, *scratch[:6], scratch[6:15])
    total, out_sem = scratch[5], scratch[15]
    small_begin, small_finish = small_each(small_ref, small_all, scratch[16:], lambda spot: spot)
    e, k = pl.program_id(0), pl.program_id(1)
    step = e * pl.num_programs(1) + k
    last = pl.num_programs(0) * pl.num_programs(1) - 1

    @pl.when(step == 0)
    def _():
        meet()
        small_begin()
        begin()

    rows = rows_ref[0]
    gate_out[0] = inner_rows(rows, gate_ref[0]).astype(jnp.bfloat16)
    up_out[0] = inner_rows(rows, up_ref[0]).astype(jnp.bfloat16)
    down_out[0] = inner_rows(act_ref[0], grads_ref[0]).astype(jnp.bfloat16)

    @pl.when((step % SPACING == 0) & (step // SPACING < TICKS))
    def _():
        tick(step // SPACING)

    @pl.when(step == last)
    def _():
        done = pltpu.make_async_copy(total, out_ref, out_sem)
        done.start()
        finish()
        small_finish()
        done.wait()


def feed_back(part, small, rows, grad_gate, grad_up, act, grads, collective_id):
    tokens, depth = part.shape[0] // RANKS, part.shape[1]
    groups, length, inner = grad_gate.shape
    dma = pltpu.SemaphoreType.DMA
    slab = pl.BlockSpec((1, length, CHUNK), lambda e, k: (e, 0, k))
    held = pl.BlockSpec((1, length, inner), lambda e, k: (e, 0, 0))
    return pl.pallas_call(
        feed_back_body,
        grid=(groups, depth // CHUNK),
        in_specs=[ANYWHERE, ANYWHERE, slab, held, held, held, slab],
        out_specs=[
            ANYWHERE,
            ANYWHERE,
            pl.BlockSpec((1, CHUNK, inner), lambda e, k: (e, k, 0)),
            pl.BlockSpec((1, CHUNK, inner), lambda e, k: (e, k, 0)),
            pl.BlockSpec((1, inner, CHUNK), lambda e, k: (e, 0, k)),
        ],
        out_shape=(
            jax.ShapeDtypeStruct((tokens, depth), jnp.float32),
            jax.ShapeDtypeStruct(small.shape, small.dtype),
            jax.ShapeDtypeStruct((groups, depth, inner), jnp.bfloat16),
            jax.ShapeDtypeStruct((groups, depth, inner), jnp.bfloat16),
            jax.ShapeDtypeStruct((groups, inner, depth), jnp.bfloat16),
        ),
        scratch_shapes=shrink_scratch(tokens, depth) + [dma(())] + small_sems(),
        compiler_params=pltpu.CompilerParams(
            collective_id=collective_id, has_side_effects=True, vmem_limit_bytes=63 * 1024 * 1024
        ),
    )(part.reshape(4, 2, 2, 2, tokens, depth), small, rows, grad_gate, grad_up, act, grads)


def fill_rows(pick_ref, field_ref, rows_ref):
    ranks, groups = pick_ref.shape[0], rows_ref.shape[0]

    @pl.loop(0, ranks // 2, unroll=UNROLL)
    def _(i):
        parts = [
            wide_dot(pick_ref[2 * i + side], field_ref[2 * i + side]).reshape(groups, SLOTS, CHUNK)
            for side in range(2)
        ]
        here = pl.ds(pl.multiple_of(i * 2 * SLOTS, 2 * SLOTS), 2 * SLOTS)
        rows_ref[:, here] = jnp.concatenate(parts, axis=1).astype(jnp.bfloat16)


def add_products(k, rows_ref, pairs):
    groups = rows_ref.shape[0]

    def products(e, first):
        for product, total in pairs:
            term = product(rows_ref[e], e)
            if first:
                total[e] = term
            else:
                total[e] += term

    @pl.when(k == 0)
    def _():
        @pl.loop(0, groups)
        def _(e):
            products(e, True)

    @pl.when(k > 0)
    def _():
        @pl.loop(0, groups)
        def _(e):
            products(e, False)


def grads_in_body(pick_ref, field_ref, down_ref, own_ref, small_ref,
                  rows_ref, plain_ref, all_ref, small_all, total, *sems):
    begin, forward, finish = spread_out(own_ref, all_ref, sems[:9])
    small_begin, small_finish = small_out(small_ref, small_all, sems[9:])
    k, last = pl.program_id(0), pl.num_programs(0) - 1

    @pl.when(k == 0)
    def _():
        meet()
        small_begin()
        begin()

    fill_rows(pick_ref, field_ref, rows_ref)
    add_products(k, rows_ref, [(lambda rows, e: outer_cols(rows, down_ref[e]), total)])

    @pl.when(k % 2 == 1)
    def _():
        forward(k // 2)

    @pl.when(k == last)
    def _():
        pltpu.sync_copy(total, plain_ref)
        finish()
        small_finish()


def grads_in(pick, field, down, own, small, collective_id):
    ranks, width, tokens = pick.shape
    groups, depth = width // SLOTS, field.shape[-1]
    length, inner = ranks * SLOTS, down.shape[1]
    steps = depth // CHUNK
    rows, plain, whole, small_all = pl.pallas_call(
        grads_in_body,
        grid=(steps,),
        in_specs=[
            pl.BlockSpec((ranks, width, tokens), lambda k: (0, 0, 0), pipeline_mode=pl.Buffered(1)),
            pl.BlockSpec((ranks, tokens, CHUNK), lambda k: (0, 0, k)),
            pl.BlockSpec((groups, inner, CHUNK), lambda k: (0, 0, k)),
            ANYWHERE,
            ANYWHERE,
        ],
        out_specs=[pl.BlockSpec((groups, length, CHUNK), lambda k: (0, 0, k))] + [ANYWHERE] * 3,
        out_shape=[
            jax.ShapeDtypeStruct((groups, length, depth), jnp.bfloat16),
            jax.ShapeDtypeStruct((groups, length, inner), jnp.float32),
            jax.ShapeDtypeStruct((4, 2, 2, 2, *own.shape), own.dtype),
            jax.ShapeDtypeStruct((RANKS, *small.shape), small.dtype),
        ],
        scratch_shapes=[pltpu.VMEM((groups, length, inner), jnp.float32)] + spread_sems() + small_sems(),
        compiler_params=pltpu.CompilerParams(
            collective_id=collective_id, has_side_effects=True, vmem_limit_bytes=62 * 1024 * 1024
        ),
    )(pick, field, down, own, small)
    return rows, plain, whole.reshape(RANKS, *own.shape), small_all


def feed_in_body(steps, pick_ref, field_ref, gate_ref, up_ref, plain_ref, probs_ref,
                 rows_ref, act_ref, weighted_ref, grad_gate_ref, grad_up_ref, gates_ref, gate_sum, up_sum):
    k = pl.program_id(0)

    @pl.when(k < steps)
    def _():
        fill_rows(pick_ref, field_ref, rows_ref)
        add_products(
            k,
            rows_ref,
            [
                (lambda rows, e: wide_dot(rows, gate_ref[e]), gate_sum),
                (lambda rows, e: wide_dot(rows, up_ref[e]), up_sum),
            ],
        )

    @pl.when(k >= steps)
    def _():
        e = k - steps
        length = act_ref.shape[1]

        @pl.loop(0, length // 128)
        def _(t):
            here = pl.ds(pl.multiple_of(t * 128, 128), 128)
            gate_val, up_val = gate_sum[e, here], up_sum[e, here]
            plain, probs = plain_ref[0, here], probs_ref[0, here]
            sigmoid_val = jax.nn.sigmoid(gate_val)
            silu_val = gate_val * sigmoid_val
            activated = silu_val * up_val
            grad_act = plain * probs
            grad_up_ref[0, here] = (grad_act * silu_val).astype(jnp.bfloat16)
            grad_gate_ref[0, here] = (
                grad_act * up_val * (sigmoid_val * (1.0 + gate_val * (1.0 - sigmoid_val)))
            ).astype(jnp.bfloat16)
            gates_ref[0, here] = jnp.sum(activated * plain, axis=-1, keepdims=True)
            weighted_ref[0, here] = (activated * probs).astype(jnp.bfloat16)
            act_ref[0, here] = activated.astype(jnp.bfloat16)


def feed_in(pick, field, gate, up, plain, probs):
    ranks, width, tokens = pick.shape
    groups, depth = width // SLOTS, field.shape[-1]
    length, inner = ranks * SLOTS, gate.shape[2]
    steps = depth // CHUNK
    held = lambda k: jnp.minimum(k, steps - 1)
    late = lambda k: (jnp.maximum(k - steps, 0), 0, 0)
    wide = pl.BlockSpec((1, length, inner), late)
    thin = pl.BlockSpec((1, length, 1), late)
    low = jax.ShapeDtypeStruct((groups, length, inner), jnp.bfloat16)
    return pl.pallas_call(
        functools.partial(feed_in_body, steps),
        grid=(steps + groups,),
        in_specs=[
            pl.BlockSpec((ranks, width, tokens), lambda k: (0, 0, 0), pipeline_mode=pl.Buffered(1)),
            pl.BlockSpec((ranks, tokens, CHUNK), lambda k: (0, 0, held(k))),
            pl.BlockSpec((groups, CHUNK, inner), lambda k: (0, held(k), 0)),
            pl.BlockSpec((groups, CHUNK, inner), lambda k: (0, held(k), 0)),
            wide,
            thin,
        ],
        out_specs=[pl.BlockSpec((groups, length, CHUNK), lambda k: (0, 0, held(k))), wide, wide, wide, wide, thin],
        out_shape=[
            jax.ShapeDtypeStruct((groups, length, depth), jnp.bfloat16),
            low, low, low, low,
            jax.ShapeDtypeStruct((groups, length, 1), jnp.float32),
        ],
        scratch_shapes=[pltpu.VMEM((groups, length, inner), jnp.float32)] * 2,
        compiler_params=pltpu.CompilerParams(vmem_limit_bytes=63 * 1024 * 1024),
        cost_estimate=pl.CostEstimate(
            flops=2 * groups * length * depth * (tokens + 2 * inner), bytes_accessed=120 << 20, transcendentals=0
        ),
    )(pick, field, gate, up, plain, probs)


def fill_field(flipped, spread_ref, lefts, weights, field_ref, rows):
    groups = rows.shape[0]
    ranks = spread_ref.shape[0]

    @pl.loop(0, groups)
    def _(e):
        total = None
        for left, weight, flip in zip(lefts, weights, flipped):
            term = outer_cols(left[e], weight[e]) if flip else wide_dot(left[e], weight[e])
            total = term if total is None else total + term
        rows[e] = total

    @pl.loop(0, ranks, unroll=2 * UNROLL)
    def _(s):
        part = rows[:, pl.ds(pl.multiple_of(s * SLOTS, SLOTS), SLOTS)]
        part = part.reshape(groups * SLOTS, CHUNK).astype(jnp.bfloat16)
        field_ref[s] = wide_dot(spread_ref[s], part).astype(jnp.bfloat16)


def restore_body(flipped, spread_ref, *refs):
    count = len(flipped)
    fill_field(flipped, spread_ref, refs[:count], refs[count : 2 * count], *refs[2 * count :])


def restore_specs(spread, lefts, weights, flipped):
    ranks, tokens, width = spread.shape
    groups = width // SLOTS
    length, inner = ranks * SLOTS, lefts[0].shape[2]
    depth = weights[0].shape[1] if flipped[0] else weights[0].shape[2]
    once = pl.Buffered(1)
    in_specs = (
        [pl.BlockSpec((ranks, tokens, width), lambda k: (0, 0, 0), pipeline_mode=once)]
        + [pl.BlockSpec((groups, length, inner), lambda k: (0, 0, 0), pipeline_mode=once)] * len(lefts)
        + [
            pl.BlockSpec((groups, CHUNK, inner), lambda k: (0, k, 0))
            if flip
            else pl.BlockSpec((groups, inner, CHUNK), lambda k: (0, 0, k))
            for flip in flipped
        ]
    )
    out_spec = pl.BlockSpec((ranks, tokens, CHUNK), lambda k: (0, 0, k))
    out_shape = jax.ShapeDtypeStruct((ranks, tokens, depth), jnp.bfloat16)
    return depth // CHUNK, in_specs, out_spec, out_shape, pltpu.VMEM((groups, length, CHUNK), jnp.float32)


def restore(spread, lefts, weights, flipped):
    steps, in_specs, out_spec, out_shape, rows = restore_specs(spread, lefts, weights, flipped)
    field = pl.pallas_call(
        functools.partial(restore_body, flipped),
        grid=(steps,),
        in_specs=in_specs,
        out_specs=out_spec,
        out_shape=out_shape,
        scratch_shapes=[rows],
        compiler_params=pltpu.CompilerParams(vmem_limit_bytes=63 * 1024 * 1024),
    )(spread, *lefts, *weights)
    return field.reshape(-1, field.shape[2])


PARTS = 4


def restore_out_body(spread_ref, left_ref, weight_ref, own_ref, field_ref, all_ref, rows,
                     here_sem, f_send, f_recv, g_send, g_recv, h_send, h_recv):
    r, c, y, x, z, core, first, second = seat()
    pair, along_first, along_second, up = partners()
    y1, x1 = row_of(core, first, 1 - second)
    near_row = y1 * 2 + x1
    step = own_ref.shape[0] // PARTS
    k = pl.program_id(0)
    here = pltpu.make_async_copy(own_ref, all_ref.at[r], here_sem)

    def part(ref, q):
        return ref.at[pl.ds(q * step, step)]

    def f_copy(q):
        return send(part(own_ref, q), part(all_ref.at[r], q), f_send.at[q], f_recv.at[q], along_first)

    def g_copy(q):
        return send(part(own_ref, q), part(all_ref.at[r], q), g_send.at[q], g_recv.at[q], along_second)

    def h_copy(q):
        there = part(all_ref.at[near_row], q)
        return send(there, there, h_send.at[q], h_recv.at[q], along_first)

    @pl.when(k == 0)
    def _():
        meet()
        here.start()
        for q in range(PARTS):
            g_copy(q).start()
            f_copy(q).start()

    fill_field((False,), spread_ref, [left_ref], [weight_ref], field_ref, rows)

    @pl.when(k == 1)
    def _():
        for q in range(PARTS):
            g_copy(q).wait_recv()
            h_copy(q).start()

    @pl.when(k == pl.num_programs(0) - 1)
    def _():
        here.wait()
        for q in range(PARTS):
            g_copy(q).wait_send()
            f_copy(q).wait()
            h_copy(q).wait()


def restore_out(spread, left, weight, own, collective_id):
    steps, in_specs, out_spec, out_shape, rows = restore_specs(spread, [left], [weight], (False,))
    dma = pltpu.SemaphoreType.DMA
    field, whole = pl.pallas_call(
        restore_out_body,
        grid=(steps,),
        in_specs=in_specs + [ANYWHERE],
        out_specs=[out_spec, ANYWHERE],
        out_shape=[out_shape, jax.ShapeDtypeStruct((4, *own.shape), own.dtype)],
        scratch_shapes=[rows, dma(())] + [dma((PARTS,))] * 6,
        compiler_params=pltpu.CompilerParams(
            collective_id=collective_id, has_side_effects=True, vmem_limit_bytes=63 * 1024 * 1024
        ),
    )(spread, left, weight, own)
    return field.reshape(-1, field.shape[2]), whole.reshape(-1, own.shape[1])


def branch_body(mixed_ref, weight_ref, out_ref, away, near, first_in, second_in,
                f_send, f_recv, g_send, g_recv):
    r, c, y, x, z, core, first, second = seat()
    pair, along_first, along_second, up = partners()
    tokens, depth = out_ref.shape
    width = depth // PARTS

    def columns(j):
        return pl.ds(j * width, width)

    def product(fir, sec, j):
        yy, xx = row_of(core, fir, sec)
        rows = pl.ds(pl.multiple_of((yy * 2 + xx) * tokens, tokens), tokens)
        return wide_dot(mixed_ref[rows], weight_ref[:, columns(j)])

    def f_copy(sec, j):
        return send(
            away.at[sec, :, columns(j)], first_in.at[sec, :, columns(j)], f_send.at[sec, j], f_recv.at[sec, j], along_first
        )

    def g_copy(j):
        return send(near.at[:, columns(j)], second_in.at[:, columns(j)], g_send.at[j], g_recv.at[j], along_second)

    meet()
    for j in range(PARTS):
        away[1 - second, :, columns(j)] = product(1 - first, 1 - second, j).astype(jnp.bfloat16)
        f_copy(1 - second, j).start()
    for j in range(PARTS):
        away[second, :, columns(j)] = product(1 - first, second, j).astype(jnp.bfloat16)
        f_copy(second, j).start()
    for j in range(PARTS):
        value = product(first, 1 - second, j)
        f_copy(1 - second, j).wait_recv()
        value = value + first_in[1 - second, :, columns(j)].astype(jnp.float32)
        near[:, columns(j)] = value.astype(jnp.bfloat16)
        g_copy(j).start()
    for j in range(PARTS):
        out_ref[:, columns(j)] = product(first, second, j)
    for j in range(PARTS):
        f_copy(second, j).wait_recv()
        g_copy(j).wait_recv()
        out_ref[:, columns(j)] += first_in[second, :, columns(j)].astype(jnp.float32) + second_in[
            :, columns(j)
        ].astype(jnp.float32)
    for j in range(PARTS):
        g_copy(j).wait_send()
        for sec in range(2):
            f_copy(sec, j).wait_send()


def branch_near(mixed, weight, collective_id):
    tokens, depth = mixed.shape[0] // 4, weight.shape[1]
    dma = pltpu.SemaphoreType.DMA
    inside = pl.BlockSpec(memory_space=pltpu.VMEM)
    low = lambda *shape: pltpu.VMEM((*shape, tokens, depth), jnp.bfloat16)
    return pl.pallas_call(
        branch_body,
        in_specs=[inside] * 2,
        out_specs=inside,
        out_shape=jax.ShapeDtypeStruct((tokens, depth), jnp.float32),
        scratch_shapes=[
            low(2), low(), low(2), low(), dma((2, PARTS)), dma((2, PARTS)), dma((PARTS,)), dma((PARTS,))
        ],
        compiler_params=pltpu.CompilerParams(
            collective_id=collective_id, has_side_effects=True, vmem_limit_bytes=40 * 1024 * 1024
        ),
    )(mixed, weight)


def causal_scores(query_rows, key_rows):
    scores = outer_cols(query_rows, key_rows) * HD ** (-0.5)
    count, length = scores.shape
    position = lax.broadcasted_iota(jnp.int32, scores.shape, 0) + (length - count)
    return jnp.where(position >= lax.broadcasted_iota(jnp.int32, scores.shape, 1), scores, MASKED)


def attend_body(q_raw, k_raw, v_ref, q_rs, k_rs, q_gain, k_gain, cos_ref, sin_ref,
                mixed_ref, q_out, k_out, lse_ref):
    length = v_ref.shape[0]
    block = min(256, length)
    for raw, scale, gain, out in ((q_raw, q_rs, q_gain, q_out), (k_raw, k_rs, k_gain, k_out)):
        normed = raw[...] * scale[...] * gain[...]
        turned = normed * cos_ref[...] + pltpu.roll(normed, HD // 2, 1) * sin_ref[...]
        out[...] = turned.astype(jnp.bfloat16)
    for start in range(0, length, block):
        here, seen = pl.ds(start, block), pl.ds(0, start + block)
        scores = causal_scores(q_out[here], k_out[seen])
        row_top = jnp.max(scores, axis=-1, keepdims=True)
        exponent = jnp.exp(scores - row_top)
        row_total = jnp.sum(exponent, axis=-1, keepdims=True)
        weights = (exponent / row_total).astype(jnp.bfloat16)
        mixed_ref[here] = wide_dot(weights, v_ref[seen]).astype(jnp.bfloat16)
        lse_ref[0, here] = row_top + jnp.log(row_total)


def attend(q_raw, k_raw, values, q_rs, k_rs, q_gain, k_gain, cosine, sine):
    length, width = q_raw.shape
    heads = width // HD
    slab = pl.BlockSpec((length, HD), lambda h: (0, h))
    thin = pl.BlockSpec((length, 1), lambda h: (0, 0))
    line = pl.BlockSpec((1, HD), lambda h: (0, h))
    table = pl.BlockSpec((length, HD), lambda h: (0, 0))
    low = jax.ShapeDtypeStruct((length, width), jnp.bfloat16)
    return pl.pallas_call(
        attend_body,
        grid=(heads,),
        in_specs=[slab, slab, slab, thin, thin, line, line, table, table],
        out_specs=[slab, slab, slab, pl.BlockSpec((1, length, 1), lambda h: (h, 0, 0))],
        out_shape=[low, low, low, jax.ShapeDtypeStruct((heads, length, 1), jnp.float32)],
        cost_estimate=pl.CostEstimate(
            flops=4 * heads * length * length * HD, bytes_accessed=8 << 20, transcendentals=heads * length * length
        ),
    )(q_raw, k_raw, values, q_rs, k_rs, q_gain[None], k_gain[None], cosine, sine)


def attend_back_body(q_ref, k_ref, v_ref, grad_ref, lse_ref, q_raw, k_raw, q_rs, k_rs, q_gain, k_gain, cos_ref, sin_ref,
                     v_grad, q_grad, k_grad, q_term, k_term, q_inner, k_inner, dq, dk, dv):
    length = v_ref.shape[0]
    block = min(256, length)
    dk[...] = jnp.zeros_like(dk)
    dv[...] = jnp.zeros_like(dv)
    for start in range(0, length, block):
        here, seen = pl.ds(start, block), pl.ds(0, start + block)
        query_rows, key_rows, grads = q_ref[here], k_ref[seen], grad_ref[here]
        probs = jnp.exp(causal_scores(query_rows, key_rows) - lse_ref[0, here])
        dv[seen] += inner_rows(probs.astype(jnp.bfloat16), grads)
        weights = outer_cols(grads, v_ref[seen])
        delta = jnp.sum(probs * weights, axis=-1, keepdims=True)
        scores = (probs * (weights - delta)).astype(jnp.bfloat16)
        dq[here] = wide_dot(scores, key_rows) * HD ** (-0.5)
        dk[seen] += inner_rows(scores, query_rows) * HD ** (-0.5)
    v_grad[...] = dv[...].astype(jnp.bfloat16)
    for raw, scale, gain, grad, out, term, inner in (
        (q_raw, q_rs, q_gain, dq, q_grad, q_term, q_inner),
        (k_raw, k_rs, k_gain, dk, k_grad, k_term, k_inner),
    ):
        field, value = raw[...], grad[...]
        normed = value * cos_ref[...] + pltpu.roll(value * sin_ref[...], HD // 2, 1)
        weighted = normed * gain[...]
        out[...] = weighted
        term[...] = jnp.sum(normed * field * scale[...], axis=0, keepdims=True)
        inner[0] = jnp.sum(weighted * field, axis=-1, keepdims=True)


def attend_back(queries, keys, values, grads, lse, q_raw, k_raw, q_rs, k_rs, q_gain, k_gain, cosine, sine):
    length, width = q_raw.shape
    heads = width // HD
    slab = pl.BlockSpec((length, HD), lambda h: (0, h))
    thin = pl.BlockSpec((length, 1), lambda h: (0, 0))
    line = pl.BlockSpec((1, HD), lambda h: (0, h))
    table = pl.BlockSpec((length, HD), lambda h: (0, 0))
    column = pl.BlockSpec((1, length, 1), lambda h: (h, 0, 0))
    wide = jax.ShapeDtypeStruct((length, width), jnp.float32)
    return pl.pallas_call(
        attend_back_body,
        grid=(heads,),
        in_specs=[slab] * 4 + [column, slab, slab, thin, thin, line, line, table, table],
        out_specs=[slab, slab, slab, line, line, column, column],
        out_shape=[
            jax.ShapeDtypeStruct((length, width), jnp.bfloat16),
            wide,
            wide,
            jax.ShapeDtypeStruct((1, width), jnp.float32),
            jax.ShapeDtypeStruct((1, width), jnp.float32),
            jax.ShapeDtypeStruct((heads, length, 1), jnp.float32),
            jax.ShapeDtypeStruct((heads, length, 1), jnp.float32),
        ],
        scratch_shapes=[pltpu.VMEM((length, HD), jnp.float32)] * 3,
        cost_estimate=pl.CostEstimate(
            flops=10 * heads * length * length * HD, bytes_accessed=16 << 20, transcendentals=heads * length * length
        ),
    )(queries, keys, values, grads, lse, q_raw, k_raw, q_rs, k_rs, q_gain[None], k_gain[None], cosine, sine)


def local(
    layer_input,
    cotangent,
    expert_index,
    attention_gain,
    query_gain,
    key_gain,
    query_weight,
    key_weight,
    value_weight,
    output_weight,
    feed_gain,
    router_weight,
    gate_weight,
    up_weight,
    down_weight,
):
    tokens = layer_input.shape[0]
    rows_count = lax.axis_size("row")
    near = rows_count == 4 and lax.axis_size("col") == 8
    if near:
        head_part = query_gain.shape[0]
        slice_width = attention_gain.shape[0]
        pack = jnp.concatenate(
            [attention_gain, feed_gain, query_gain, key_gain, router_weight.reshape(-1)]
        )
        pack = jnp.pad(pack, (0, PACK_ROWS * 128 - pack.shape[0])).reshape(PACK_ROWS, 128)
        (
            sequence, query_full, key_full, value_full, output_full, pack_all, cotangent_all, index_all
        ) = start_near(
            layer_input,
            [query_weight, key_weight, value_weight, output_weight],
            pack,
            cotangent,
            expert_index.T,
            1,
        )
        index_all = jnp.swapaxes(index_all, 1, 2)
        pack_all = pack_all.reshape(8, -1)
        ends = [slice_width, 2 * slice_width, 2 * slice_width + head_part, 2 * slice_width + 2 * head_part]
        attention_full = pack_all[:, : ends[0]].reshape(-1)
        feed_full = pack_all[:, ends[0] : ends[1]].reshape(-1)
        query_scale_w = pack_all[:, ends[1] : ends[2]].reshape(-1)
        key_scale_w = pack_all[:, ends[2] : ends[3]].reshape(-1)
        router_full = pack_all[:, ends[3] : ends[3] + router_weight.size].reshape(
            -1, router_weight.shape[1]
        )
    else:
        (
            attention_full,
            query_scale_w,
            key_scale_w,
            query_full,
            key_full,
            value_full,
            output_full,
            feed_full,
            router_full,
        ) = (
            lax.all_gather(attention_gain, "col", axis=0, tiled=True),
            lax.all_gather(query_gain, "col", axis=0, tiled=True),
            lax.all_gather(key_gain, "col", axis=0, tiled=True),
            lax.all_gather(query_weight, "col", axis=0, tiled=True),
            lax.all_gather(key_weight, "col", axis=0, tiled=True),
            lax.all_gather(value_weight, "col", axis=0, tiled=True),
            lax.all_gather(output_weight, "col", axis=1, tiled=True),
            lax.all_gather(feed_gain, "col", axis=0, tiled=True),
            lax.all_gather(router_weight, "col", axis=0, tiled=True),
        )
        sequence = lax.all_gather(layer_input, "row", axis=0, tiled=True)
    length = sequence.shape[0]
    model_width = sequence.shape[1]
    local_width = query_full.shape[1]
    seq_float = sequence.astype(jnp.float32)
    seq_scale = rms_scale(seq_float)
    attention_float = attention_full.astype(jnp.float32)
    normed = (seq_float * seq_scale * attention_float).astype(jnp.bfloat16)
    query_raw = wide_dot(normed, query_full)
    key_raw = wide_dot(normed, key_full)
    values = wide_dot(normed, value_full).astype(jnp.bfloat16)
    query_total, key_total = lax.psum(
        (jnp.sum(query_raw * query_raw, axis=-1), jnp.sum(key_raw * key_raw, axis=-1)), "row"
    )
    query_rs = lax.rsqrt(query_total / model_width + EPS)[:, None]
    key_rs = lax.rsqrt(key_total / model_width + EPS)[:, None]
    query_gain_f = query_scale_w.astype(jnp.float32)
    key_gain_f = key_scale_w.astype(jnp.float32)
    cosine, sine_table = rope_tables(length)
    mixed_heads, queries, keys_rotated, lse_all = attend(
        query_raw, key_raw, values, query_rs, key_rs, query_gain_f, key_gain_f, cosine, sine_table
    )
    if near:
        branch = branch_near(mixed_heads, output_full, 5)
    else:
        branch = lax.psum_scatter(
            wide_dot(mixed_heads, output_full).astype(jnp.bfloat16), "row", scatter_dimension=0, tiled=True
        ).astype(jnp.float32)
    hidden = layer_input.astype(jnp.float32) + branch
    feed_scale = rms_scale(hidden)
    feed_float = feed_full.astype(jnp.float32)
    feed_normed = (hidden * feed_scale * feed_float).astype(jnp.bfloat16)
    logits = wide_dot(feed_normed, router_full)
    logit_top = jnp.max(logits, axis=-1, keepdims=True)
    logit_exp = jnp.exp(logits - logit_top)
    router_probs = logit_exp / jnp.sum(logit_exp, axis=-1, keepdims=True)
    experts = router_full.shape[1]
    experts_local = gate_weight.shape[0]
    ranks = lax.axis_size("col") * rows_count
    gate_hits = expert_index[:, :, None] == jnp.arange(experts, dtype=jnp.int32)
    gate_probs = jnp.sum(jnp.where(gate_hits, router_probs[:, None, :], 0.0), axis=-1)

    if not near:
        index_all = lax.all_gather(expert_index, ("col", "row"), axis=0, tiled=True)
    own = (index_all - lax.axis_index("col") * experts_local).reshape(ranks, tokens, -1)
    matches = own[..., None] == jnp.arange(experts_local, dtype=jnp.int32)
    hit = jnp.sum(matches.astype(jnp.float32), axis=2)
    earlier = jnp.tril(jnp.ones((tokens, tokens), jnp.bfloat16), -1)
    rank = jnp.einsum(
        "tu,sue->ste", earlier, hit.astype(jnp.bfloat16), preferred_element_type=jnp.float32
    )
    slot = jnp.where(hit > 0, rank, -1.0)
    places = jnp.arange(SLOTS, dtype=jnp.float32)
    slot_t = jnp.swapaxes(slot, 1, 2)
    width = experts_local * SLOTS
    picked = slot_t[:, :, None, :] == places[None, None, :, None]
    pick = picked.astype(jnp.bfloat16).reshape(ranks, width, tokens)
    lanes = jnp.arange(width, dtype=jnp.int32)
    widen = (lanes[None, :] // SLOTS == jnp.arange(experts_local)[:, None]).astype(jnp.bfloat16)
    spread = jnp.einsum(
        "ste,ew->stw", slot.astype(jnp.bfloat16), widen, preferred_element_type=jnp.float32
    ) == (lanes % SLOTS).astype(jnp.float32)
    spread_plain = spread.astype(jnp.bfloat16)

    def weigh(probs_all):
        probs_own = jnp.sum(
            jnp.where(matches, probs_all.reshape(ranks, tokens, -1, 1), 0.0), axis=2
        )
        probs_wide = jnp.einsum(
            "ste,ew->stw", probs_own.astype(jnp.bfloat16), widen, preferred_element_type=jnp.float32
        )
        spread_probs = jnp.where(spread, probs_wide, 0.0).astype(jnp.bfloat16)
        probs_t = jnp.swapaxes(probs_own, 1, 2)
        row_probs = jnp.sum(jnp.where(picked, probs_t[:, :, None, :], 0.0), axis=-1)
        row_probs = jnp.swapaxes(row_probs, 0, 1).reshape(experts_local, ranks * SLOTS, 1)
        return spread_probs, row_probs

    if near:
        expert_grads, plain_act, feed_all, probs_all = grads_in(
            pick, cotangent_all, down_weight, feed_normed, gate_probs.T, 2
        )
        spread_probs, row_probs = weigh(jnp.swapaxes(probs_all, 1, 2))
        expert_rows, activated, weighted_act, grad_gate, grad_up, row_gates = feed_in(
            pick, feed_all, gate_weight, up_weight, plain_act, row_probs
        )
    else:
        probs_all = lax.all_gather(gate_probs, ("col", "row"), axis=0, tiled=True)
        spread_probs, row_probs = weigh(probs_all)
        expert_grads = gather_rows(pick, cotangent)
        expert_rows = gather_rows(pick, feed_normed)
        gate_val = jnp.einsum(
            "erd,edf->erf", expert_rows, gate_weight, preferred_element_type=jnp.float32
        )
        up_val = jnp.einsum(
            "erd,edf->erf", expert_rows, up_weight, preferred_element_type=jnp.float32
        )
        plain_act = jnp.einsum(
            "erd,efd->erf", expert_grads, down_weight, preferred_element_type=jnp.float32
        )
        sigmoid_val = jax.nn.sigmoid(gate_val)
        silu_val = gate_val * sigmoid_val
        activated = silu_val * up_val
        grad_act = plain_act * row_probs
        grad_up = (grad_act * silu_val).astype(jnp.bfloat16)
        grad_gate = (
            grad_act * up_val * sigmoid_val * (1.0 + gate_val * (1.0 - sigmoid_val))
        ).astype(jnp.bfloat16)
        row_gates = jnp.sum(activated * plain_act, axis=-1)
        weighted_act = (activated * row_probs).astype(jnp.bfloat16)
        activated = activated.astype(jnp.bfloat16)
    row_gates = jnp.swapaxes(row_gates.reshape(experts_local, ranks, SLOTS), 0, 1)
    own_gates = jnp.sum(jnp.where(picked, row_gates[..., None], 0.0), axis=2)
    if near:
        grad_feed_part = restore(
            spread_plain, [grad_gate, grad_up], [gate_weight, up_weight], (True, True)
        )
        grad_feed, gates_in, grad_gate_weight, grad_up_weight, grad_down_weight = feed_back(
            grad_feed_part, own_gates, expert_rows, grad_gate, grad_up, weighted_act, expert_grads, 3
        )
        grad_gate_weight = grad_gate_weight.astype(jnp.float32)
        grad_up_weight = grad_up_weight.astype(jnp.float32)
        grad_down_weight = grad_down_weight.astype(jnp.float32)
        gates_in = jnp.sum(gates_in.reshape(-1, rows_count, experts_local, tokens), axis=1)
        grad_probs = gates_in.reshape(experts, tokens).T
    else:
        own_gates = lax.psum_scatter(
            jnp.swapaxes(own_gates, 1, 2).reshape(-1, rows_count, tokens, experts_local),
            "row",
            scatter_dimension=1,
        )
        grad_probs = lax.all_to_all(own_gates, "col", split_axis=0, concat_axis=2, tiled=True)[0]
        back_rows = (
            jnp.einsum("erf,edf->erd", grad_gate, gate_weight, preferred_element_type=jnp.float32)
            + jnp.einsum("erf,edf->erd", grad_up, up_weight, preferred_element_type=jnp.float32)
        ).astype(jnp.bfloat16)
        grad_feed = return_rows(spread_plain, back_rows).astype(jnp.float32)
        out_rows = jnp.einsum(
            "erf,efd->erd", activated, down_weight, preferred_element_type=jnp.float32
        ).astype(jnp.bfloat16)
        mixture = return_rows(spread_probs, out_rows).astype(jnp.float32)
        grad_gate_weight = jnp.einsum(
            "erd,erf->edf", expert_rows, grad_gate, preferred_element_type=jnp.float32
        )
        grad_up_weight = jnp.einsum(
            "erd,erf->edf", expert_rows, grad_up, preferred_element_type=jnp.float32
        )
        grad_down_weight = jnp.einsum(
            "erf,erd->efd", weighted_act, expert_grads, preferred_element_type=jnp.float32
        )
    grad_out = cotangent.astype(jnp.float32)
    grad_logits = (
        router_probs * (grad_probs - jnp.sum(router_probs * grad_probs, axis=-1, keepdims=True))
    ).astype(jnp.bfloat16)
    router_grad = inner_rows(feed_normed, grad_logits)
    grad_feed = grad_feed + outer_cols(grad_logits, router_full)
    feed_gain_term = jnp.sum(grad_feed * hidden * feed_scale, axis=0)
    feed_weighted = grad_feed * feed_float
    grad_hidden = (
        grad_out
        + feed_scale * feed_weighted
        - hidden * feed_scale**3 * jnp.mean(feed_weighted * hidden, axis=-1, keepdims=True)
    )
    if near:
        mixture_part, grad_branch = restore_out(
            spread_probs, activated, down_weight, grad_hidden.astype(jnp.bfloat16), 6
        )
    else:
        grad_branch = lax.all_gather(grad_hidden.astype(jnp.bfloat16), "row", axis=0, tiled=True)
    output_grad = inner_rows(mixed_heads, grad_branch)
    grad_mixed = outer_cols(grad_branch, output_full).astype(jnp.bfloat16)
    (
        grad_value_low, query_weighted, key_weighted, query_gain_term, key_gain_term, query_inner, key_inner
    ) = attend_back(
        queries, keys_rotated, values, grad_mixed, lse_all, query_raw, key_raw, query_rs, key_rs,
        query_gain_f, key_gain_f, cosine, sine_table,
    )
    query_gain_term, key_gain_term = query_gain_term.reshape(-1), key_gain_term.reshape(-1)
    query_inner, key_inner = (
        lax.psum(jnp.sum(query_inner, axis=(0, 2)), "row"),
        lax.psum(jnp.sum(key_inner, axis=(0, 2)), "row"),
    )
    grad_query_raw = (
        query_rs * query_weighted - query_raw * query_rs**3 * (query_inner / model_width)[:, None]
    ).astype(jnp.bfloat16)
    grad_key_raw = (
        key_rs * key_weighted - key_raw * key_rs**3 * (key_inner / model_width)[:, None]
    ).astype(jnp.bfloat16)
    query_grad = inner_rows(normed, grad_query_raw)
    key_grad = inner_rows(normed, grad_key_raw)
    value_grad = inner_rows(normed, grad_value_low)
    grad_normed = (
        outer_cols(grad_query_raw, query_full)
        + outer_cols(grad_key_raw, key_full)
        + outer_cols(grad_value_low, value_full)
    )
    attention_weighted = grad_normed * attention_float
    grad_seq_part = seq_scale * attention_weighted - seq_float * seq_scale**3 * jnp.mean(
        attention_weighted * seq_float, axis=-1, keepdims=True
    )
    attention_gain_term = jnp.sum(grad_normed * seq_float * seq_scale, axis=0)
    if near:
        cols = lax.axis_size("col")
        pack = jnp.concatenate(
            [
                attention_gain_term.reshape(cols, -1),
                feed_gain_term.reshape(cols, -1),
                query_gain_term.reshape(cols, -1),
                key_gain_term.reshape(cols, -1),
                router_grad.reshape(cols, -1),
            ],
            axis=1,
        )
        pack = jnp.pad(pack, ((0, 0), (0, PACK_ROWS * 128 - pack.shape[1])))
        pack = pack.astype(jnp.bfloat16).reshape(cols, PACK_ROWS, 128)
        (
            mixture, summed, grad_query_weight, grad_key_weight, grad_value_weight, grad_output_weight, packs
        ) = finish_near(
            mixture_part,
            grad_seq_part.astype(jnp.bfloat16).reshape(rows_count, tokens, model_width),
            [grad.astype(jnp.bfloat16) for grad in (query_grad, key_grad, value_grad, output_grad)],
            pack,
            4,
        )
        input_grad = grad_hidden + summed
        packs = packs.reshape(cols, rows_count, -1).astype(jnp.float32)
        whole = jnp.sum(packs, axis=(0, 1))
        heads_sum = jnp.sum(
            lax.dynamic_index_in_dim(packs, lax.axis_index("row"), 1, keepdims=False), axis=0
        )
        grad_attention_gain = whole[: ends[0]]
        grad_feed_gain = whole[ends[0] : ends[1]]
        grad_query_gain = heads_sum[ends[1] : ends[2]]
        grad_key_gain = heads_sum[ends[2] : ends[3]]
        grad_router_weight = whole[ends[3] : ends[3] + router_weight.size].reshape(router_weight.shape)
    else:
        stacked = jnp.concatenate(
            [
                grad_seq_part.reshape(rows_count, tokens, model_width),
                jnp.broadcast_to(attention_gain_term[None, None, :], (rows_count, 1, model_width)),
            ],
            axis=1,
        ).reshape(rows_count * (tokens + 1), model_width)
        summed = lax.psum_scatter(
            stacked.astype(jnp.bfloat16), "row", scatter_dimension=0, tiled=True
        ).astype(jnp.float32)
        input_grad = grad_hidden + summed[:tokens]
        attention_gain_total = summed[tokens]
        feed_gain_total, router_total = (
            lax.psum(feed_gain_term.astype(jnp.bfloat16), "row").astype(jnp.float32),
            lax.psum(router_grad.astype(jnp.bfloat16), "row").astype(jnp.float32),
        )
        (
            grad_attention_gain,
            grad_query_gain,
            grad_key_gain,
            grad_query_weight,
            grad_key_weight,
            grad_value_weight,
            grad_output_weight,
            grad_feed_gain,
            grad_router_weight,
        ) = (
            lax.psum_scatter(
                attention_gain_total.astype(jnp.bfloat16), "col", scatter_dimension=0, tiled=True
            ).astype(jnp.float32),
            lax.psum_scatter(
                query_gain_term.astype(jnp.bfloat16), "col", scatter_dimension=0, tiled=True
            ).astype(jnp.float32),
            lax.psum_scatter(
                key_gain_term.astype(jnp.bfloat16), "col", scatter_dimension=0, tiled=True
            ).astype(jnp.float32),
            lax.psum_scatter(
                query_grad.astype(jnp.bfloat16), "col", scatter_dimension=0, tiled=True
            ).astype(jnp.float32),
            lax.psum_scatter(
                key_grad.astype(jnp.bfloat16), "col", scatter_dimension=0, tiled=True
            ).astype(jnp.float32),
            lax.psum_scatter(
                value_grad.astype(jnp.bfloat16), "col", scatter_dimension=0, tiled=True
            ).astype(jnp.float32),
            lax.psum_scatter(
                output_grad.astype(jnp.bfloat16), "col", scatter_dimension=1, tiled=True
            ).astype(jnp.float32),
            lax.psum_scatter(
                feed_gain_total.astype(jnp.bfloat16), "col", scatter_dimension=0, tiled=True
            ).astype(jnp.float32),
            lax.psum_scatter(
                router_total.astype(jnp.bfloat16), "col", scatter_dimension=0, tiled=True
            ).astype(jnp.float32),
        )
    layer_output = hidden + mixture
    return (
        layer_output,
        input_grad,
        grad_attention_gain,
        grad_query_gain,
        grad_key_gain,
        grad_query_weight,
        grad_key_weight,
        grad_value_weight,
        grad_output_weight,
        grad_feed_gain,
        grad_router_weight,
        grad_gate_weight,
        grad_up_weight,
        grad_down_weight,
    )


def solution(mesh):
    placed = (
        P(("col", "row"), None),
        P(("col", "row"), None),
        P(("col", "row"), None),
        P("col"),
        P(("row", "col")),
        P(("row", "col")),
        P("col", "row"),
        P("col", "row"),
        P("col", "row"),
        P("row", "col"),
        P("col"),
        P("col", None),
        P("col", None, "row"),
        P("col", None, "row"),
        P("col", "row", None),
    )
    return jax.shard_map(
        local,
        mesh=mesh,
        in_specs=placed,
        out_specs=(
            P(("col", "row"), None),
            P(("col", "row"), None),
            P("col"),
            P(("row", "col")),
            P(("row", "col")),
            P("col", "row"),
            P("col", "row"),
            P("col", "row"),
            P("row", "col"),
            P("col"),
            P("col", None),
            P("col", None, "row"),
            P("col", None, "row"),
            P("col", "row", None),
        ),
        check_vma=False,
    )
```

```python
import functools

import jax
import jax.numpy as jnp
from jax import lax
from jax.experimental import pallas as pl
from jax.experimental.pallas import tpu as pltpu
from jax.sharding import PartitionSpec as P

HD = 128
SLOTS = 40
BLOCK = 512
CHUNK = 256
UNROLL = 4
PACK_ROWS = 144


EPS = 1e-05
THETA = 10000.0
MASKED = -1e30


def wide_dot(left, right):
    return jnp.dot(left, right, preferred_element_type=jnp.float32)


def inner_rows(left, right):
    return lax.dot_general(
        left, right, (((0,), (0,)), ((), ())), preferred_element_type=jnp.float32
    )


def outer_cols(left, right):
    return lax.dot_general(
        left, right, (((1,), (1,)), ((), ())), preferred_element_type=jnp.float32
    )


def rms_scale(field):
    return lax.rsqrt(jnp.mean(field * field, axis=-1, keepdims=True) + EPS)


def rope_tables(length):
    half_size = HD // 2
    freqs = THETA ** (-(jnp.arange(half_size, dtype=jnp.float32) * 2.0) / HD)
    angles = jnp.arange(length, dtype=jnp.float32)[:, None] * freqs[None, :]
    cosine = jnp.concatenate([jnp.cos(angles), jnp.cos(angles)], axis=-1)
    sine_table = jnp.concatenate([-jnp.sin(angles), jnp.sin(angles)], axis=-1)
    return (cosine, sine_table)


def dispatch_body(pick_ref, field_ref, rows_ref):
    groups = rows_ref.shape[0]
    first = wide_dot(pick_ref[0], field_ref[0]).reshape(groups, SLOTS, -1)
    second = wide_dot(pick_ref[1], field_ref[1]).reshape(groups, SLOTS, -1)
    rows_ref[...] = jnp.concatenate([first, second], axis=1).astype(jnp.bfloat16)


def dispatch(pick, field):
    ranks, width, tokens = pick.shape
    groups, depth = width // SLOTS, field.shape[1]
    return pl.pallas_call(
        dispatch_body,
        grid=(ranks // 2, depth // BLOCK),
        in_specs=[
            pl.BlockSpec((2, width, tokens), lambda i, k: (i, 0, 0)),
            pl.BlockSpec((2, tokens, BLOCK), lambda i, k: (i, 0, k)),
        ],
        out_specs=pl.BlockSpec((groups, 2 * SLOTS, BLOCK), lambda i, k: (0, i, k)),
        out_shape=jax.ShapeDtypeStruct((groups, ranks * SLOTS, depth), jnp.bfloat16),
    )(pick, field.reshape(ranks, tokens, depth))


def combine_body(spread_ref, rows_ref, field_ref):
    rows = rows_ref[...].astype(jnp.float32)
    width = rows.shape[0] * SLOTS
    for side in range(2):
        part = rows[:, side * SLOTS : (side + 1) * SLOTS].reshape(width, -1).astype(jnp.bfloat16)
        field_ref[side] = wide_dot(spread_ref[side], part).astype(jnp.bfloat16)


def combine(spread, rows):
    ranks, tokens, width = spread.shape
    groups, depth = width // SLOTS, rows.shape[2]
    field = pl.pallas_call(
        combine_body,
        grid=(ranks // 2, depth // BLOCK),
        in_specs=[
            pl.BlockSpec((2, tokens, width), lambda i, k: (i, 0, 0)),
            pl.BlockSpec((groups, 2 * SLOTS, BLOCK), lambda i, k: (0, i, k)),
        ],
        out_specs=pl.BlockSpec((2, tokens, BLOCK), lambda i, k: (i, 0, k)),
        out_shape=jax.ShapeDtypeStruct((ranks, tokens, depth), jnp.bfloat16),
    )(spread, rows)
    return field.reshape(ranks * tokens, depth)


def scatter_all(field):
    part = lax.psum_scatter(field, "col", scatter_dimension=0, tiled=True)
    return lax.psum_scatter(part, "row", scatter_dimension=0, tiled=True)


def pieces_of(ranks, depth):
    count = max(1, ranks // 32)
    step = depth // count
    return [(at, at + step) for at in range(0, depth, step)]


def gather_rows(pick, field):
    rows = []
    for start, stop in pieces_of(pick.shape[0], field.shape[1]):
        part = field[:, start:stop]
        if rows:
            part = lax.optimization_barrier((part, rows[-1]))[0]
        whole = lax.all_gather(part, ("col", "row"), axis=0, tiled=True)
        rows.append(dispatch(pick, whole))
    return rows[0] if len(rows) == 1 else jnp.concatenate(rows, axis=2)


def return_rows(spread, rows):
    sums = []
    for start, stop in pieces_of(spread.shape[0], rows.shape[2]):
        part = rows[:, :, start:stop]
        if sums:
            part = lax.optimization_barrier((part, sums[-1]))[0]
        sums.append(scatter_all(combine(spread, part)))
    return sums[0] if len(sums) == 1 else jnp.concatenate(sums, axis=1)


MESH = pl.DeviceIdType.MESH


def seat():
    r, c = lax.axis_index("row"), lax.axis_index("col")
    y, x = r // 2, r % 2
    z, core = c // 2, c % 2
    first = y * (1 - core) + x * core
    second = x * (1 - core) + y * core
    return r, c, y, x, z, core, first, second


def partners():
    r, c, y, x, z, core, first, second = seat()
    pair = (r, z * 2 + (1 - core))
    flip_y = (1 - y) * 2 + x
    flip_x = y * 2 + (1 - x)
    along_first = (flip_y * (1 - core) + flip_x * core, c)
    along_second = (flip_x * (1 - core) + flip_y * core, c)
    up = [(r, ((z + k) % 4) * 2 + core) for k in range(1, 4)]
    return pair, along_first, along_second, up


RANKS = 32


def nth(offset):
    spot = (lax.axis_index("col") * 4 + lax.axis_index("row") + offset) % RANKS
    return spot, (spot % 4, spot // 4)


def meet():
    barrier = pltpu.get_barrier_semaphore()

    @pl.loop(1, RANKS)
    def _(offset):
        pl.semaphore_signal(barrier, inc=1, device_id=nth(offset)[1], device_id_type=MESH)

    pl.semaphore_wait(barrier, RANKS - 1)


def small_copy(src_of, small_all, small_send, small_recv, offset):
    spot, device = nth(offset)
    return send(
        src_of(spot), small_all.at[nth(0)[0]], small_send.at[offset], small_recv.at[offset], device
    )


def row_of(core, first, second):
    y = first * (1 - core) + second * core
    x = second * (1 - core) + first * core
    return y, x


def send(src, dst, send_sem, recv_sem, device):
    return pltpu.make_async_remote_copy(
        src_ref=src, dst_ref=dst, send_sem=send_sem, recv_sem=recv_sem, device_id=device, device_id_type=MESH
    )


GSTEPS = 4
QUEUE = (2, 1, 3)
ARRIVE = (1, 3, 2)


def spread_out(own_ref, all_ref, sems):
    r, c, y, x, z, core, first, second = seat()
    pair, along_first, along_second, up = partners()
    here_sem, u_send, u_recv, d_send, d_recv, g_send, g_recv, f_send, f_recv, p_send, p_recv = sems
    step = own_ref.shape[0] // GSTEPS

    def rows(q):
        return pl.ds(pl.multiple_of(q * step, step), step)

    def place(k, s, f, q):
        sec = second * (1 - s) + (1 - second) * s
        fir = first * (1 - f) + (1 - first) * f
        yy, xx = row_of(core, fir, sec)
        return all_ref.at[(z + 4 - k) % 4, core, yy, xx, rows(q)]

    above, below = (r, ((z + 1) % 4) * 2 + core), (r, ((z + 3) % 4) * 2 + core)

    def source(k, q):
        return own_ref.at[rows(q)] if k == 0 else place(k, 0, 0, q)

    def up_copy(d, q):
        return send(source(d, q), place(d, 0, 0, q), u_send.at[d, q], u_recv.at[d, q], above)

    def down_copy(d, q):
        k = (4 - d) % 4
        return send(source(k, q), place(k, 0, 0, q), d_send.at[d, q], d_recv.at[d, q], below)

    def came_up(d, q):
        there = place(d, 0, 0, q)
        return send(there, there, u_send.at[d - 1, q], u_recv.at[d - 1, q], above)

    def came_down(d, q):
        there = place(4 - d, 0, 0, q)
        return send(there, there, d_send.at[d - 1, q], d_recv.at[d - 1, q], below)

    bottom, top = 1 - jnp.minimum(z, 1), z // 3
    arrived = [bottom * (3 - i) + top * (1 + i) + (1 - bottom - top) * ARRIVE[i] for i in range(3)]

    def g_copy(k, q, src):
        return send(src, place(k, 0, 0, q), g_send.at[k, q], g_recv.at[k, q], along_second)

    def f_copy(k, s, q, src):
        return send(src, place(k, s, 0, q), f_send.at[s, k, q], f_recv.at[s, k, q], along_first)

    def p_copy(k, s, f, q, src):
        return send(src, place(k, s, f, q), p_send.at[f, s, k, q], p_recv.at[f, s, k, q], pair)

    here = pltpu.make_async_copy(own_ref, all_ref.at[z, core, y, x], here_sem)

    def begin():
        here.start()

        @pl.loop(0, GSTEPS)
        def _(q):
            src = own_ref.at[rows(q)]

            @pl.when(z < 3)
            def _():
                up_copy(0, q).start()

            @pl.when(z > 0)
            def _():
                down_copy(0, q).start()

            g_copy(0, q, src).start()
            f_copy(0, 0, q, src).start()
            p_copy(0, 0, 0, q, src).start()

    def forward(q):
        def pass_on(k):
            src = place(k, 0, 0, q)
            g_copy(k, q, src).start()
            f_copy(k, 0, q, src).start()
            p_copy(k, 0, 0, q, src).start()

        for d in (1, 2, 3):

            @pl.when(z >= d)
            def _():
                came_up(d, q).wait_recv()
                if d < 3:

                    @pl.when(z < 3)
                    def _():
                        up_copy(d, q).start()

                pass_on(d)

            @pl.when(z + d <= 3)
            def _():
                came_down(d, q).wait_recv()
                if d < 3:

                    @pl.when(z > 0)
                    def _():
                        down_copy(d, q).start()

                pass_on(4 - d)

        for k in (0, *arrived):
            src = place(k, 1, 0, q)
            g_copy(k, q, src).wait_recv()
            f_copy(k, 1, q, src).start()
            p_copy(k, 1, 0, q, src).start()
        for k in (0, *arrived):
            src = place(k, 0, 1, q)
            f_copy(k, 0, q, src).wait_recv()
            p_copy(k, 0, 1, q, src).start()

    def finish():
        @pl.loop(0, GSTEPS)
        def _(q):
            for k in (0, *arrived):
                src = place(k, 1, 1, q)
                f_copy(k, 1, q, src).wait_recv()
                p_copy(k, 1, 1, q, src).start()

        here.wait()

        @pl.loop(0, GSTEPS)
        def _(q):
            for d in range(3):

                @pl.when((z < 3) & (z >= d))
                def _():
                    up_copy(d, q).wait_send()

                @pl.when((z > 0) & (z + d <= 3))
                def _():
                    down_copy(d, q).wait_send()

            for k in range(4):
                src = own_ref.at[rows(q)]
                g_copy(k, q, src).wait_send()
                for s in range(2):
                    f_copy(k, s, q, src).wait_send()
                    for f in range(2):
                        p_copy(k, s, f, q, src).wait()

    return begin, forward, finish


def spread_sems():
    dma = pltpu.SemaphoreType.DMA
    shapes = [(3, GSTEPS), (3, GSTEPS), (4, GSTEPS), (2, 4, GSTEPS), (2, 2, 4, GSTEPS)]
    return [dma(())] + [dma(shape) for shape in shapes for _ in range(2)]


def small_out(small_ref, small_all, sems):
    here_sem, small_send, small_recv = sems
    local = pltpu.make_async_copy(small_ref, small_all.at[nth(0)[0]], here_sem)

    def copy(offset):
        return small_copy(lambda spot: small_ref, small_all, small_send, small_recv, offset)

    def begin():
        local.start()

        @pl.loop(1, RANKS)
        def _(offset):
            copy(offset).start()

    def finish():
        local.wait()

        @pl.loop(1, RANKS)
        def _(offset):
            copy(offset).wait()

    return begin, finish


def small_sems():
    dma = pltpu.SemaphoreType.DMA
    return [dma(()), dma((RANKS,)), dma((RANKS,))]


ANYWHERE = pl.BlockSpec(memory_space=pl.ANY)


def start_body(x_ref, q_ref, k_ref, v_ref, o_ref, pack_ref, own_ref, small_ref,
               x_all, q_all, k_all, v_all, o_all, pack_all, all_ref, small_all, *sems):
    r, c, y, x, z, core, first, second = seat()
    pair, along_first, along_second, up = partners()
    begin, forward, finish = spread_out(own_ref, all_ref, sems[:11])
    small_begin, small_finish = small_out(small_ref, small_all, sems[11:14])
    here_sem, x_send, x_recv, w_send, w_recv, v_send, v_recv = sems[14:]
    weights = [(q_ref, q_all), (k_ref, k_all), (v_ref, v_all), (o_ref, o_all), (pack_ref, pack_all)]

    def block(index, col):
        ref, whole = weights[index]
        if index == 4:
            return whole.at[col]
        if index == 3:
            width = ref.shape[1]
            return whole.at[:, pl.ds(pl.multiple_of(col * width, width), width)]
        height = ref.shape[0]
        return whole.at[pl.ds(pl.multiple_of(col * height, height), height)]

    def w_copy(index, k):
        return send(
            weights[index][0], block(index, c), w_send.at[index, k - 1], w_recv.at[index, k - 1], up[k - 1]
        )

    def pair_copy(index, k):
        col = ((z + 4 - k) % 4) * 2 + core
        src = weights[index][0] if k == 0 else block(index, col)
        return send(src, block(index, col), v_send.at[index, k], v_recv.at[index, k], pair)

    locals_ = [pltpu.make_async_copy(x_ref, x_all.at[r], here_sem.at[5])] + [
        pltpu.make_async_copy(weights[i][0], block(i, c), here_sem.at[i]) for i in range(5)
    ]
    y1, x1 = row_of(core, first, 1 - second)
    near_row = y1 * 2 + x1
    x_first = send(x_ref, x_all.at[r], x_send.at[0], x_recv.at[0], along_first)
    x_second = send(x_ref, x_all.at[r], x_send.at[1], x_recv.at[1], along_second)
    x_relay = send(x_all.at[near_row], x_all.at[near_row], x_send.at[2], x_recv.at[2], along_first)

    meet()
    small_begin()
    x_second.start()
    x_first.start()
    begin()
    for index in (4, 0, 1, 2, 3):
        for k in QUEUE:
            w_copy(index, k).start()
        pair_copy(index, 0).start()
    for item in locals_:
        item.start()
    x_second.wait_recv()
    x_relay.start()

    @pl.loop(0, GSTEPS)
    def _(q):
        forward(q)

    for index in (4, 0, 1, 2, 3):
        for k in ARRIVE:
            w_copy(index, k).wait_recv()
            pair_copy(index, k).start()
    finish()
    small_finish()
    for item in locals_:
        item.wait()
    x_first.wait()
    x_second.wait_send()
    x_relay.wait()
    for index in range(5):
        for k in range(4):
            if k:
                w_copy(index, k).wait_send()
            pair_copy(index, k).wait()


def start_near(x, weights, pack, own, small, collective_id):
    tokens, depth = own.shape
    dma = pltpu.SemaphoreType.DMA
    height, width = weights[0].shape
    shaped = lambda shape, like: jax.ShapeDtypeStruct(shape, like.dtype)
    outs = pl.pallas_call(
        start_body,
        out_shape=(
            shaped((4, *x.shape), x),
            *[shaped((8 * height, width), w) for w in weights[:3]],
            shaped((weights[3].shape[0], 8 * weights[3].shape[1]), weights[3]),
            shaped((8, *pack.shape), pack),
            shaped((4, 2, 2, 2, tokens, depth), own),
            shaped((RANKS, *small.shape), small),
        ),
        in_specs=[ANYWHERE] * 8,
        out_specs=[ANYWHERE] * 8,
        scratch_shapes=spread_sems()
        + small_sems()
        + [dma((6,)), dma((3,)), dma((3,)), dma((5, 3)), dma((5, 3)), dma((5, 4)), dma((5, 4))],
        compiler_params=pltpu.CompilerParams(collective_id=collective_id, has_side_effects=True),
    )(x, *weights, pack, own, small)
    x_all, q, k, v, o, pack_all, whole, small_all = outs
    return x_all.reshape(-1, x.shape[1]), q, k, v, o, pack_all, whole.reshape(RANKS, tokens, depth), small_all


def finish_body(part_ref, field_ref, q_ref, k_ref, v_ref, o_ref, pack_ref,
                mixture_ref, out_ref, q_out, k_out, v_out, o_out, pack_all,
                mine, first_in, second_in, total,
                q_mine, k_mine, v_mine, o_mine, q_pair, k_pair, v_pair, o_pair, q_z, k_z, v_z, o_z,
                q_sum, k_sum, v_sum, o_sum,
                load_sem, f_send, f_recv, g_send, g_recv, w_load, p_send, p_recv, z_send, z_recv, out_sem,
                *rest):
    r, c, y, x, z, core, first, second = seat()
    pair, along_first, along_second, up = partners()
    small_begin, small_finish = small_each(pack_ref, pack_all, rest[:3], lambda spot: spot // 4)
    begin, tick, finish = shrink(part_ref, *rest[3:9], rest[9:18])
    mixture = rest[8]
    tokens, depth = out_ref.shape
    other = 1 - core
    grads = [q_ref, k_ref, v_ref, o_ref]
    kept, pairs, zs = [q_mine, k_mine, v_mine, o_mine], [q_pair, k_pair, v_pair, o_pair], [q_z, k_z, v_z, o_z]
    sums, outs = [q_sum, k_sum, v_sum, o_sum], [q_out, k_out, v_out, o_out]

    def block(index, col):
        ref = grads[index]
        if index == 3:
            width = ref.shape[1] // 8
            return ref.at[:, pl.ds(pl.multiple_of(col * width, width), width)]
        height = ref.shape[0] // 8
        return ref.at[pl.ds(pl.multiple_of(col * height, height), height)]

    def row(fir, sec):
        yy, xx = row_of(core, fir, sec)
        return yy * 2 + xx

    def load(fir, sec):
        return pltpu.make_async_copy(field_ref.at[row(fir, sec)], mine.at[fir, sec], load_sem.at[fir, sec])

    def f_copy(sec):
        return send(field_ref.at[row(1 - first, sec)], first_in.at[sec], f_send.at[sec], f_recv.at[sec], along_first)

    g_copy = send(mine.at[first, 1 - second], second_in, g_send, g_recv, along_second)

    def w_load_copy(index, zz):
        return pltpu.make_async_copy(block(index, zz * 2 + core), kept[index].at[zz], w_load.at[index, zz])

    def w_give(index, zz):
        return send(
            block(index, zz * 2 + other), pairs[index].at[zz], p_send.at[index, zz], p_recv.at[index, zz], pair
        )

    def w_z(index, k):
        return send(
            kept[index].at[(z + k) % 4], zs[index].at[k - 1], z_send.at[index, k - 1], z_recv.at[index, k - 1], up[k - 1]
        )

    def add(ref, extras):
        @pl.loop(0, ref.shape[0] // TILE)
        def _(t):
            here = pl.ds(pl.multiple_of(t * TILE, TILE), TILE)
            value = ref[here].astype(jnp.float32)
            for extra in extras:
                value = value + extra[here].astype(jnp.float32)
            ref[here] = value.astype(jnp.bfloat16)

    def add_out(ref, extras, result):
        @pl.loop(0, ref.shape[0] // TILE)
        def _(t):
            here = pl.ds(pl.multiple_of(t * TILE, TILE), TILE)
            value = ref[here].astype(jnp.float32)
            for extra in extras:
                value = value + extra[here].astype(jnp.float32)
            result[here] = value

    meet()
    for index in range(4):
        for k in (2, 1, 3, 0):
            w_give(index, (z + k) % 4).start()
            w_load_copy(index, (z + k) % 4).start()
    begin()
    f_copy(1 - second).start()
    f_copy(second).start()
    load(first, 1 - second).start()
    load(first, second).start()
    small_begin()
    for index in range(4):
        for k in QUEUE:
            zz = (z + k) % 4
            w_load_copy(index, zz).wait()
            w_give(index, zz).wait_recv()
            add(kept[index].at[zz], [pairs[index].at[zz]])
            w_z(index, k).start()

    @pl.loop(0, RSTEPS + LAGS[2])
    def _(i):
        tick(i)

        @pl.when(i == 2)
        def _():
            load(first, 1 - second).wait()
            f_copy(1 - second).wait_recv()
            add(mine.at[first, 1 - second], [first_in.at[1 - second]])
            g_copy.start()

    for index in range(4):
        w_load_copy(index, z).wait()
        w_give(index, z).wait_recv()
        for k in ARRIVE:
            w_z(index, k).wait_recv()
        add_out(
            kept[index].at[z], [pairs[index].at[z]] + [zs[index].at[k] for k in range(3)], sums[index]
        )
        pltpu.make_async_copy(sums[index], outs[index], out_sem.at[index]).start()
    load(first, second).wait()
    f_copy(second).wait_recv()
    g_copy.wait_recv()
    add_out(mine.at[first, second], [first_in.at[second], second_in], total)
    pltpu.make_async_copy(total, out_ref, out_sem.at[4]).start()

    @pl.loop(RSTEPS + LAGS[2], TICKS)
    def _(i):
        tick(i)

    pltpu.make_async_copy(mixture, mixture_ref, out_sem.at[5]).start()
    finish()
    for sec in range(2):
        f_copy(sec).wait_send()
    g_copy.wait_send()
    for index in range(4):
        for k in range(4):
            w_give(index, (z + k) % 4).wait_send()
            if k:
                w_z(index, k).wait_send()
        pltpu.make_async_copy(sums[index], outs[index], out_sem.at[index]).wait()
    small_finish()
    pltpu.make_async_copy(total, out_ref, out_sem.at[4]).wait()
    pltpu.make_async_copy(mixture, mixture_ref, out_sem.at[5]).wait()


def finish_near(part, field, grads, pack, collective_id):
    rows_count, tokens, depth = field.shape
    dma = pltpu.SemaphoreType.DMA
    blocks = [(g.shape[0] // 8, g.shape[1]) for g in grads[:3]] + [(grads[3].shape[0], grads[3].shape[1] // 8)]
    half = lambda *shape: pltpu.VMEM(shape, jnp.bfloat16)
    return pl.pallas_call(
        finish_body,
        out_shape=(
            jax.ShapeDtypeStruct((tokens, depth), jnp.float32),
            jax.ShapeDtypeStruct((tokens, depth), jnp.float32),
            *[jax.ShapeDtypeStruct(b, jnp.float32) for b in blocks],
            jax.ShapeDtypeStruct((RANKS, *pack.shape[1:]), pack.dtype),
        ),
        in_specs=[ANYWHERE] * 7,
        out_specs=[ANYWHERE] * 7,
        scratch_shapes=[
            half(2, 2, tokens, depth), half(2, tokens, depth), half(tokens, depth),
            pltpu.VMEM((tokens, depth), jnp.float32),
            *[half(4, *b) for b in blocks], *[half(4, *b) for b in blocks], *[half(3, *b) for b in blocks],
            *[pltpu.VMEM(b, jnp.float32) for b in blocks],
            dma((2, 2)), dma((2,)), dma((2,)), dma(()), dma(()),
            dma((4, 4)), dma((4, 4)), dma((4, 4)), dma((4, 3)), dma((4, 3)), dma((6,)),
        ]
        + small_sems()
        + shrink_scratch(tokens, depth),
        compiler_params=pltpu.CompilerParams(
            collective_id=collective_id, has_side_effects=True, vmem_limit_bytes=63 * 1024 * 1024
        ),
    )(part.reshape(4, 2, 2, 2, tokens, depth), field, *grads, pack)


RSTEPS = 8
TILE = 16
LAGS = (0, 1, 2, 4)
TICKS = RSTEPS + LAGS[3]


def shrink(part_ref, sums, near_own, first_in, second_in, z_in, total, sems):
    r, c, y, x, z, core, first, second = seat()
    pair, along_first, along_second, up = partners()
    load_sem, p_send, p_recv, f_send, f_recv, g_send, g_recv, z_send, z_recv = sems
    tokens = total.shape[0]
    step = tokens // RSTEPS
    other = 1 - core

    def rows(q):
        return pl.ds(pl.multiple_of(q * step, step), step)

    def spot(kind):
        fir = (1 - first) if kind < 2 else first
        sec = (1 - second) if kind in (0, 2) else second
        return fir, sec

    def load(kind, q):
        yy, xx = row_of(core, *spot(kind))
        return pltpu.make_async_copy(
            part_ref.at[:, core, yy, xx, rows(q)], near_own.at[q % 2, kind], load_sem.at[kind, q % 2]
        )

    def give(fir, sec, q):
        yy, xx = row_of(other, fir, sec)
        return send(
            part_ref.at[:, other, yy, xx, rows(q)],
            sums.at[fir, sec, :, rows(q)],
            p_send.at[fir, sec, q],
            p_recv.at[fir, sec, q],
            pair,
        )

    def f_copy(sec, q):
        return send(
            sums.at[1 - first, sec, :, rows(q)],
            first_in.at[sec, :, rows(q)],
            f_send.at[sec, q],
            f_recv.at[sec, q],
            along_first,
        )

    def g_copy(q):
        return send(
            sums.at[first, 1 - second, :, rows(q)], second_in.at[:, rows(q)], g_send.at[q], g_recv.at[q], along_second
        )

    def z_copy(k, q):
        return send(
            sums.at[first, second, (z + k) % 4, rows(q)],
            z_in.at[k - 1, rows(q)],
            z_send.at[k - 1, q],
            z_recv.at[k - 1, q],
            up[k - 1],
        )

    def begin():
        @pl.loop(0, RSTEPS)
        def _(q):
            for fir, sec in ((1 - second, 1 - first), (1 - second, first), (second, 1 - first), (second, first)):
                give(fir, sec, q).start()

        for kind in range(4):
            load(kind, 0).start()

    def add(kind, q, extra):
        fir, sec = spot(kind)

        @pl.when(q + 1 < RSTEPS)
        def _():
            load(kind, q + 1).start()

        load(kind, q).wait()
        give(fir, sec, q).wait_recv()

        @pl.loop(0, 4 * (step // TILE))
        def _(t):
            zz, at = t // (step // TILE), t % (step // TILE)
            here = pl.ds(pl.multiple_of(q * step + at * TILE, TILE), TILE)
            near = pl.ds(pl.multiple_of(at * TILE, TILE), TILE)
            value = sums[fir, sec, zz, here].astype(jnp.float32)
            value = value + near_own[q % 2, kind, zz, near].astype(jnp.float32)
            for ref in extra:
                value = value + ref[zz, here].astype(jnp.float32)
            sums[fir, sec, zz, here] = value.astype(jnp.bfloat16)

    def stage_first(q):
        for kind, sec in ((0, 1 - second), (1, second)):
            add(kind, q, [])
            f_copy(sec, q).start()

    def stage_second(q):
        f_copy(1 - second, q).wait_recv()
        add(2, q, [first_in.at[1 - second]])
        g_copy(q).start()

    def stage_z(q):
        f_copy(second, q).wait_recv()
        g_copy(q).wait_recv()
        add(3, q, [first_in.at[second], second_in])
        for k in QUEUE:
            z_copy(k, q).start()

    def stage_out(q):
        for k in ARRIVE:
            z_copy(k, q).wait_recv()

        @pl.loop(0, step // TILE)
        def _(t):
            here = pl.ds(pl.multiple_of(q * step + t * TILE, TILE), TILE)
            value = sums[first, second, z, here].astype(jnp.float32)
            for k in range(3):
                value = value + z_in[k, here].astype(jnp.float32)
            total[here] = value

    def tick(i):
        for stage, lag in zip((stage_first, stage_second, stage_z, stage_out), LAGS):

            @pl.when((i >= lag) & (i < RSTEPS + lag))
            def _(stage=stage, lag=lag):
                stage(i - lag)

    def finish():
        @pl.loop(0, RSTEPS)
        def _(q):
            for fir in range(2):
                for sec in range(2):
                    give(fir, sec, q).wait_send()
            for sec in range(2):
                f_copy(sec, q).wait_send()
            g_copy(q).wait_send()
            for k in QUEUE:
                z_copy(k, q).wait_send()

    return begin, tick, finish


def shrink_scratch(tokens, depth):
    dma = pltpu.SemaphoreType.DMA
    low = lambda *shape: pltpu.VMEM((*shape, depth), jnp.bfloat16)
    buffers = [
        low(2, 2, 4, tokens), low(2, 4, 4, tokens // RSTEPS), low(2, 4, tokens), low(4, tokens), low(3, tokens),
        pltpu.VMEM((tokens, depth), jnp.float32),
    ]
    shapes = [(2, 2, RSTEPS), (2, RSTEPS), (RSTEPS,), (3, RSTEPS)]
    return buffers + [dma((4, 2))] + [dma(shape) for shape in shapes for _ in range(2)]


def small_each(small_ref, small_all, sems, pick):
    here_sem, small_send, small_recv = sems
    local = pltpu.make_async_copy(small_ref.at[pick(nth(0)[0])], small_all.at[nth(0)[0]], here_sem)

    def copy(offset):
        return small_copy(lambda spot: small_ref.at[pick(spot)], small_all, small_send, small_recv, offset)

    def begin():
        local.start()

        @pl.loop(1, RANKS)
        def _(offset):
            copy(offset).start()

    def finish():
        local.wait()

        @pl.loop(1, RANKS)
        def _(offset):
            copy(offset).wait()

    return begin, finish


def feed_back_body(part_ref, small_ref, rows_ref, gate_ref, up_ref, act_ref, grads_ref,
                   out_ref, small_all, gate_out, up_out, down_out, *scratch):
    begin, tick, finish = shrink(part_ref, *scratch[:6], scratch[6:15])
    total, out_sem = scratch[5], scratch[15]
    small_begin, small_finish = small_each(small_ref, small_all, scratch[16:], lambda spot: spot)
    e, k = pl.program_id(0), pl.program_id(1)
    step = e * pl.num_programs(1) + k
    last = pl.num_programs(0) * pl.num_programs(1) - 1

    @pl.when(step == 0)
    def _():
        meet()
        small_begin()
        begin()

    rows = rows_ref[0]
    gate_out[0] = inner_rows(rows, gate_ref[0]).astype(jnp.bfloat16)
    up_out[0] = inner_rows(rows, up_ref[0]).astype(jnp.bfloat16)
    down_out[0] = inner_rows(act_ref[0], grads_ref[0]).astype(jnp.bfloat16)

    @pl.when(k == 0)
    def _():
        tick(e)

    @pl.when(step == last)
    def _():
        @pl.loop(RSTEPS, TICKS)
        def _(i):
            tick(i)

        done = pltpu.make_async_copy(total, out_ref, out_sem)
        done.start()
        finish()
        small_finish()
        done.wait()


def feed_back(part, small, rows, grad_gate, grad_up, act, grads, collective_id):
    tokens, depth = part.shape[0] // RANKS, part.shape[1]
    groups, length, inner = grad_gate.shape
    assert groups == RSTEPS
    dma = pltpu.SemaphoreType.DMA
    slab = pl.BlockSpec((1, length, CHUNK), lambda e, k: (e, 0, k))
    held = pl.BlockSpec((1, length, inner), lambda e, k: (e, 0, 0))
    return pl.pallas_call(
        feed_back_body,
        grid=(groups, depth // CHUNK),
        in_specs=[ANYWHERE, ANYWHERE, slab, held, held, held, slab],
        out_specs=[
            ANYWHERE,
            ANYWHERE,
            pl.BlockSpec((1, CHUNK, inner), lambda e, k: (e, k, 0)),
            pl.BlockSpec((1, CHUNK, inner), lambda e, k: (e, k, 0)),
            pl.BlockSpec((1, inner, CHUNK), lambda e, k: (e, 0, k)),
        ],
        out_shape=(
            jax.ShapeDtypeStruct((tokens, depth), jnp.float32),
            jax.ShapeDtypeStruct(small.shape, small.dtype),
            jax.ShapeDtypeStruct((groups, depth, inner), jnp.bfloat16),
            jax.ShapeDtypeStruct((groups, depth, inner), jnp.bfloat16),
            jax.ShapeDtypeStruct((groups, inner, depth), jnp.bfloat16),
        ),
        scratch_shapes=shrink_scratch(tokens, depth) + [dma(())] + small_sems(),
        compiler_params=pltpu.CompilerParams(
            collective_id=collective_id, has_side_effects=True, vmem_limit_bytes=63 * 1024 * 1024
        ),
    )(part.reshape(4, 2, 2, 2, tokens, depth), small, rows, grad_gate, grad_up, act, grads)


def widen_body(*refs):
    half = len(refs) // 2
    for low, wide in zip(refs[:half], refs[half:]):
        wide[...] = low[...].astype(jnp.float32)


def widen_all(*arrays):
    specs = [pl.BlockSpec((1, *array.shape[1:]), lambda e: (e, 0, 0)) for array in arrays]
    return pl.pallas_call(
        widen_body,
        grid=(arrays[0].shape[0],),
        in_specs=specs,
        out_specs=specs,
        out_shape=[jax.ShapeDtypeStruct(array.shape, jnp.float32) for array in arrays],
        compiler_params=pltpu.CompilerParams(vmem_limit_bytes=40 * 1024 * 1024),
    )(*arrays)


def fill_rows(pick_ref, field_ref, rows_ref):
    ranks, groups = pick_ref.shape[0], rows_ref.shape[0]

    @pl.loop(0, ranks // 2, unroll=UNROLL)
    def _(i):
        parts = [
            wide_dot(pick_ref[2 * i + side], field_ref[2 * i + side]).reshape(groups, SLOTS, CHUNK)
            for side in range(2)
        ]
        here = pl.ds(pl.multiple_of(i * 2 * SLOTS, 2 * SLOTS), 2 * SLOTS)
        rows_ref[:, here] = jnp.concatenate(parts, axis=1).astype(jnp.bfloat16)


def add_products(k, rows_ref, pairs):
    groups = rows_ref.shape[0]

    def products(e, first):
        for product, total in pairs:
            term = product(rows_ref[e], e)
            if first:
                total[e] = term
            else:
                total[e] += term

    @pl.when(k == 0)
    def _():
        @pl.loop(0, groups)
        def _(e):
            products(e, True)

    @pl.when(k > 0)
    def _():
        @pl.loop(0, groups)
        def _(e):
            products(e, False)


def grads_in_body(pick_ref, field_ref, down_ref, own_ref, small_ref,
                  rows_ref, plain_ref, all_ref, small_all, total, *sems):
    begin, forward, finish = spread_out(own_ref, all_ref, sems[:11])
    small_begin, small_finish = small_out(small_ref, small_all, sems[11:])
    k, last = pl.program_id(0), pl.num_programs(0) - 1

    @pl.when(k == 0)
    def _():
        meet()
        small_begin()
        begin()

    fill_rows(pick_ref, field_ref, rows_ref)
    add_products(k, rows_ref, [(lambda rows, e: outer_cols(rows, down_ref[e]), total)])

    @pl.when(k % 2 == 1)
    def _():
        forward(k // 2)

    @pl.when(k == last)
    def _():
        pltpu.sync_copy(total, plain_ref)
        finish()
        small_finish()


def grads_in(pick, field, down, own, small, collective_id):
    ranks, width, tokens = pick.shape
    groups, depth = width // SLOTS, field.shape[-1]
    length, inner = ranks * SLOTS, down.shape[1]
    steps = depth // CHUNK
    rows, plain, whole, small_all = pl.pallas_call(
        grads_in_body,
        grid=(steps,),
        in_specs=[
            pl.BlockSpec((ranks, width, tokens), lambda k: (0, 0, 0), pipeline_mode=pl.Buffered(1)),
            pl.BlockSpec((ranks, tokens, CHUNK), lambda k: (0, 0, k)),
            pl.BlockSpec((groups, inner, CHUNK), lambda k: (0, 0, k)),
            ANYWHERE,
            ANYWHERE,
        ],
        out_specs=[pl.BlockSpec((groups, length, CHUNK), lambda k: (0, 0, k))] + [ANYWHERE] * 3,
        out_shape=[
            jax.ShapeDtypeStruct((groups, length, depth), jnp.bfloat16),
            jax.ShapeDtypeStruct((groups, length, inner), jnp.float32),
            jax.ShapeDtypeStruct((4, 2, 2, 2, *own.shape), own.dtype),
            jax.ShapeDtypeStruct((RANKS, *small.shape), small.dtype),
        ],
        scratch_shapes=[pltpu.VMEM((groups, length, inner), jnp.float32)] + spread_sems() + small_sems(),
        compiler_params=pltpu.CompilerParams(
            collective_id=collective_id, has_side_effects=True, vmem_limit_bytes=62 * 1024 * 1024
        ),
    )(pick, field, down, own, small)
    return rows, plain, whole.reshape(RANKS, *own.shape), small_all


def feed_in_body(steps, pick_ref, field_ref, gate_ref, up_ref, plain_ref, probs_ref,
                 rows_ref, act_ref, weighted_ref, grad_gate_ref, grad_up_ref, gates_ref, gate_sum, up_sum):
    k = pl.program_id(0)

    @pl.when(k < steps)
    def _():
        fill_rows(pick_ref, field_ref, rows_ref)
        add_products(
            k,
            rows_ref,
            [
                (lambda rows, e: wide_dot(rows, gate_ref[e]), gate_sum),
                (lambda rows, e: wide_dot(rows, up_ref[e]), up_sum),
            ],
        )

    @pl.when(k >= steps)
    def _():
        e = k - steps
        length = act_ref.shape[1]

        @pl.loop(0, length // 128)
        def _(t):
            here = pl.ds(pl.multiple_of(t * 128, 128), 128)
            gate_val, up_val = gate_sum[e, here], up_sum[e, here]
            plain, probs = plain_ref[0, here], probs_ref[0, here]
            sigmoid_val = jax.nn.sigmoid(gate_val)
            silu_val = gate_val * sigmoid_val
            activated = silu_val * up_val
            grad_act = plain * probs
            grad_up_ref[0, here] = (grad_act * silu_val).astype(jnp.bfloat16)
            grad_gate_ref[0, here] = (
                grad_act * up_val * (sigmoid_val * (1.0 + gate_val * (1.0 - sigmoid_val)))
            ).astype(jnp.bfloat16)
            gates_ref[0, here] = jnp.sum(activated * plain, axis=-1, keepdims=True)
            weighted_ref[0, here] = (activated * probs).astype(jnp.bfloat16)
            act_ref[0, here] = activated.astype(jnp.bfloat16)


def feed_in(pick, field, gate, up, plain, probs):
    ranks, width, tokens = pick.shape
    groups, depth = width // SLOTS, field.shape[-1]
    length, inner = ranks * SLOTS, gate.shape[2]
    steps = depth // CHUNK
    held = lambda k: jnp.minimum(k, steps - 1)
    late = lambda k: (jnp.maximum(k - steps, 0), 0, 0)
    wide = pl.BlockSpec((1, length, inner), late)
    thin = pl.BlockSpec((1, length, 1), late)
    low = jax.ShapeDtypeStruct((groups, length, inner), jnp.bfloat16)
    return pl.pallas_call(
        functools.partial(feed_in_body, steps),
        grid=(steps + groups,),
        in_specs=[
            pl.BlockSpec((ranks, width, tokens), lambda k: (0, 0, 0), pipeline_mode=pl.Buffered(1)),
            pl.BlockSpec((ranks, tokens, CHUNK), lambda k: (0, 0, held(k))),
            pl.BlockSpec((groups, CHUNK, inner), lambda k: (0, held(k), 0)),
            pl.BlockSpec((groups, CHUNK, inner), lambda k: (0, held(k), 0)),
            wide,
            thin,
        ],
        out_specs=[pl.BlockSpec((groups, length, CHUNK), lambda k: (0, 0, held(k))), wide, wide, wide, wide, thin],
        out_shape=[
            jax.ShapeDtypeStruct((groups, length, depth), jnp.bfloat16),
            low, low, low, low,
            jax.ShapeDtypeStruct((groups, length, 1), jnp.float32),
        ],
        scratch_shapes=[pltpu.VMEM((groups, length, inner), jnp.float32)] * 2,
        compiler_params=pltpu.CompilerParams(vmem_limit_bytes=63 * 1024 * 1024),
        cost_estimate=pl.CostEstimate(
            flops=2 * groups * length * depth * (tokens + 2 * inner), bytes_accessed=120 << 20, transcendentals=0
        ),
    )(pick, field, gate, up, plain, probs)


def fill_field(flipped, spread_ref, lefts, weights, field_ref, rows):
    groups = rows.shape[0]
    ranks = spread_ref.shape[0]

    @pl.loop(0, groups)
    def _(e):
        total = None
        for left, weight, flip in zip(lefts, weights, flipped):
            term = outer_cols(left[e], weight[e]) if flip else wide_dot(left[e], weight[e])
            total = term if total is None else total + term
        rows[e] = total

    @pl.loop(0, ranks, unroll=2 * UNROLL)
    def _(s):
        part = rows[:, pl.ds(pl.multiple_of(s * SLOTS, SLOTS), SLOTS)]
        part = part.reshape(groups * SLOTS, CHUNK).astype(jnp.bfloat16)
        field_ref[s] = wide_dot(spread_ref[s], part).astype(jnp.bfloat16)


def restore_body(flipped, spread_ref, *refs):
    count = len(flipped)
    fill_field(flipped, spread_ref, refs[:count], refs[count : 2 * count], *refs[2 * count :])


def restore_specs(spread, lefts, weights, flipped):
    ranks, tokens, width = spread.shape
    groups = width // SLOTS
    length, inner = ranks * SLOTS, lefts[0].shape[2]
    depth = weights[0].shape[1] if flipped[0] else weights[0].shape[2]
    once = pl.Buffered(1)
    in_specs = (
        [pl.BlockSpec((ranks, tokens, width), lambda k: (0, 0, 0), pipeline_mode=once)]
        + [pl.BlockSpec((groups, length, inner), lambda k: (0, 0, 0), pipeline_mode=once)] * len(lefts)
        + [
            pl.BlockSpec((groups, CHUNK, inner), lambda k: (0, k, 0))
            if flip
            else pl.BlockSpec((groups, inner, CHUNK), lambda k: (0, 0, k))
            for flip in flipped
        ]
    )
    out_spec = pl.BlockSpec((ranks, tokens, CHUNK), lambda k: (0, 0, k))
    out_shape = jax.ShapeDtypeStruct((ranks, tokens, depth), jnp.bfloat16)
    return depth // CHUNK, in_specs, out_spec, out_shape, pltpu.VMEM((groups, length, CHUNK), jnp.float32)


def restore(spread, lefts, weights, flipped):
    steps, in_specs, out_spec, out_shape, rows = restore_specs(spread, lefts, weights, flipped)
    field = pl.pallas_call(
        functools.partial(restore_body, flipped),
        grid=(steps,),
        in_specs=in_specs,
        out_specs=out_spec,
        out_shape=out_shape,
        scratch_shapes=[rows],
        compiler_params=pltpu.CompilerParams(vmem_limit_bytes=63 * 1024 * 1024),
    )(spread, *lefts, *weights)
    return field.reshape(-1, field.shape[2])


PARTS = 4


def restore_out_body(spread_ref, left_ref, weight_ref, own_ref, field_ref, all_ref, rows,
                     here_sem, f_send, f_recv, g_send, g_recv, h_send, h_recv):
    r, c, y, x, z, core, first, second = seat()
    pair, along_first, along_second, up = partners()
    y1, x1 = row_of(core, first, 1 - second)
    near_row = y1 * 2 + x1
    step = own_ref.shape[0] // PARTS
    k = pl.program_id(0)
    here = pltpu.make_async_copy(own_ref, all_ref.at[r], here_sem)

    def part(ref, q):
        return ref.at[pl.ds(q * step, step)]

    def f_copy(q):
        return send(part(own_ref, q), part(all_ref.at[r], q), f_send.at[q], f_recv.at[q], along_first)

    def g_copy(q):
        return send(part(own_ref, q), part(all_ref.at[r], q), g_send.at[q], g_recv.at[q], along_second)

    def h_copy(q):
        there = part(all_ref.at[near_row], q)
        return send(there, there, h_send.at[q], h_recv.at[q], along_first)

    @pl.when(k == 0)
    def _():
        meet()
        here.start()
        for q in range(PARTS):
            g_copy(q).start()
            f_copy(q).start()

    fill_field((False,), spread_ref, [left_ref], [weight_ref], field_ref, rows)

    for q in range(PARTS):

        @pl.when(k == q + 1)
        def _():
            g_copy(q).wait_recv()
            h_copy(q).start()

    @pl.when(k == pl.num_programs(0) - 1)
    def _():
        here.wait()
        for q in range(PARTS):
            g_copy(q).wait_send()
            f_copy(q).wait()
            h_copy(q).wait()


def restore_out(spread, left, weight, own, collective_id):
    steps, in_specs, out_spec, out_shape, rows = restore_specs(spread, [left], [weight], (False,))
    dma = pltpu.SemaphoreType.DMA
    field, whole = pl.pallas_call(
        restore_out_body,
        grid=(steps,),
        in_specs=in_specs + [ANYWHERE],
        out_specs=[out_spec, ANYWHERE],
        out_shape=[out_shape, jax.ShapeDtypeStruct((4, *own.shape), own.dtype)],
        scratch_shapes=[rows, dma(())] + [dma((PARTS,))] * 6,
        compiler_params=pltpu.CompilerParams(
            collective_id=collective_id, has_side_effects=True, vmem_limit_bytes=63 * 1024 * 1024
        ),
    )(spread, left, weight, own)
    return field.reshape(-1, field.shape[2]), whole.reshape(-1, own.shape[1])


def branch_body(mixed_ref, weight_ref, out_ref, away, near, first_in, second_in,
                f_send, f_recv, g_send, g_recv):
    r, c, y, x, z, core, first, second = seat()
    pair, along_first, along_second, up = partners()
    tokens, depth = out_ref.shape
    width = depth // PARTS

    def columns(j):
        return pl.ds(j * width, width)

    def product(fir, sec, j):
        yy, xx = row_of(core, fir, sec)
        rows = pl.ds(pl.multiple_of((yy * 2 + xx) * tokens, tokens), tokens)
        return wide_dot(mixed_ref[rows], weight_ref[:, columns(j)])

    def f_copy(sec, j):
        return send(
            away.at[sec, :, columns(j)], first_in.at[sec, :, columns(j)], f_send.at[sec, j], f_recv.at[sec, j], along_first
        )

    def g_copy(j):
        return send(near.at[:, columns(j)], second_in.at[:, columns(j)], g_send.at[j], g_recv.at[j], along_second)

    meet()
    for j in range(PARTS):
        away[1 - second, :, columns(j)] = product(1 - first, 1 - second, j).astype(jnp.bfloat16)
        f_copy(1 - second, j).start()
    for j in range(PARTS):
        away[second, :, columns(j)] = product(1 - first, second, j).astype(jnp.bfloat16)
        f_copy(second, j).start()
    for j in range(PARTS):
        value = product(first, 1 - second, j)
        f_copy(1 - second, j).wait_recv()
        value = value + first_in[1 - second, :, columns(j)].astype(jnp.float32)
        near[:, columns(j)] = value.astype(jnp.bfloat16)
        g_copy(j).start()
    for j in range(PARTS):
        out_ref[:, columns(j)] = product(first, second, j)
    for j in range(PARTS):
        f_copy(second, j).wait_recv()
        g_copy(j).wait_recv()
        out_ref[:, columns(j)] += first_in[second, :, columns(j)].astype(jnp.float32) + second_in[
            :, columns(j)
        ].astype(jnp.float32)
    for j in range(PARTS):
        g_copy(j).wait_send()
        for sec in range(2):
            f_copy(sec, j).wait_send()


def branch_near(mixed, weight, collective_id):
    tokens, depth = mixed.shape[0] // 4, weight.shape[1]
    dma = pltpu.SemaphoreType.DMA
    inside = pl.BlockSpec(memory_space=pltpu.VMEM)
    low = lambda *shape: pltpu.VMEM((*shape, tokens, depth), jnp.bfloat16)
    return pl.pallas_call(
        branch_body,
        in_specs=[inside] * 2,
        out_specs=inside,
        out_shape=jax.ShapeDtypeStruct((tokens, depth), jnp.float32),
        scratch_shapes=[
            low(2), low(), low(2), low(), dma((2, PARTS)), dma((2, PARTS)), dma((PARTS,)), dma((PARTS,))
        ],
        compiler_params=pltpu.CompilerParams(
            collective_id=collective_id, has_side_effects=True, vmem_limit_bytes=40 * 1024 * 1024
        ),
    )(mixed, weight)


def causal_scores(query_rows, key_rows):
    scores = outer_cols(query_rows, key_rows) * HD ** (-0.5)
    count, length = scores.shape
    position = lax.broadcasted_iota(jnp.int32, scores.shape, 0) + (length - count)
    return jnp.where(position >= lax.broadcasted_iota(jnp.int32, scores.shape, 1), scores, MASKED)


def attend_body(q_raw, k_raw, v_ref, q_rs, k_rs, q_gain, k_gain, cos_ref, sin_ref,
                mixed_ref, q_out, k_out, lse_ref):
    length = v_ref.shape[0]
    block = min(256, length)
    for raw, scale, gain, out in ((q_raw, q_rs, q_gain, q_out), (k_raw, k_rs, k_gain, k_out)):
        normed = raw[...] * scale[...] * gain[...]
        turned = normed * cos_ref[...] + pltpu.roll(normed, HD // 2, 1) * sin_ref[...]
        out[...] = turned.astype(jnp.bfloat16)
    for start in range(0, length, block):
        here, seen = pl.ds(start, block), pl.ds(0, start + block)
        scores = causal_scores(q_out[here], k_out[seen])
        row_top = jnp.max(scores, axis=-1, keepdims=True)
        exponent = jnp.exp(scores - row_top)
        row_total = jnp.sum(exponent, axis=-1, keepdims=True)
        weights = (exponent / row_total).astype(jnp.bfloat16)
        mixed_ref[here] = wide_dot(weights, v_ref[seen]).astype(jnp.bfloat16)
        lse_ref[0, here] = row_top + jnp.log(row_total)


def attend(q_raw, k_raw, values, q_rs, k_rs, q_gain, k_gain, cosine, sine):
    length, width = q_raw.shape
    heads = width // HD
    slab = pl.BlockSpec((length, HD), lambda h: (0, h))
    thin = pl.BlockSpec((length, 1), lambda h: (0, 0))
    line = pl.BlockSpec((1, HD), lambda h: (0, h))
    table = pl.BlockSpec((length, HD), lambda h: (0, 0))
    low = jax.ShapeDtypeStruct((length, width), jnp.bfloat16)
    return pl.pallas_call(
        attend_body,
        grid=(heads,),
        in_specs=[slab, slab, slab, thin, thin, line, line, table, table],
        out_specs=[slab, slab, slab, pl.BlockSpec((1, length, 1), lambda h: (h, 0, 0))],
        out_shape=[low, low, low, jax.ShapeDtypeStruct((heads, length, 1), jnp.float32)],
        cost_estimate=pl.CostEstimate(
            flops=4 * heads * length * length * HD, bytes_accessed=8 << 20, transcendentals=heads * length * length
        ),
    )(q_raw, k_raw, values, q_rs, k_rs, q_gain[None], k_gain[None], cosine, sine)


def attend_back_body(q_ref, k_ref, v_ref, grad_ref, lse_ref, q_raw, k_raw, q_rs, k_rs, q_gain, k_gain, cos_ref, sin_ref,
                     v_grad, q_grad, k_grad, q_term, k_term, q_inner, k_inner, dq, dk, dv):
    length = v_ref.shape[0]
    block = min(256, length)
    dk[...] = jnp.zeros_like(dk)
    dv[...] = jnp.zeros_like(dv)
    for start in range(0, length, block):
        here, seen = pl.ds(start, block), pl.ds(0, start + block)
        query_rows, key_rows, grads = q_ref[here], k_ref[seen], grad_ref[here]
        probs = jnp.exp(causal_scores(query_rows, key_rows) - lse_ref[0, here])
        dv[seen] += inner_rows(probs.astype(jnp.bfloat16), grads)
        weights = outer_cols(grads, v_ref[seen])
        delta = jnp.sum(probs * weights, axis=-1, keepdims=True)
        scores = (probs * (weights - delta)).astype(jnp.bfloat16)
        dq[here] = wide_dot(scores, key_rows) * HD ** (-0.5)
        dk[seen] += inner_rows(scores, query_rows) * HD ** (-0.5)
    v_grad[...] = dv[...].astype(jnp.bfloat16)
    for raw, scale, gain, grad, out, term, inner in (
        (q_raw, q_rs, q_gain, dq, q_grad, q_term, q_inner),
        (k_raw, k_rs, k_gain, dk, k_grad, k_term, k_inner),
    ):
        field, value = raw[...], grad[...]
        normed = value * cos_ref[...] + pltpu.roll(value * sin_ref[...], HD // 2, 1)
        weighted = normed * gain[...]
        out[...] = weighted
        term[...] = jnp.sum(normed * field * scale[...], axis=0, keepdims=True)
        inner[0] = jnp.sum(weighted * field, axis=-1, keepdims=True)


def attend_back(queries, keys, values, grads, lse, q_raw, k_raw, q_rs, k_rs, q_gain, k_gain, cosine, sine):
    length, width = q_raw.shape
    heads = width // HD
    slab = pl.BlockSpec((length, HD), lambda h: (0, h))
    thin = pl.BlockSpec((length, 1), lambda h: (0, 0))
    line = pl.BlockSpec((1, HD), lambda h: (0, h))
    table = pl.BlockSpec((length, HD), lambda h: (0, 0))
    column = pl.BlockSpec((1, length, 1), lambda h: (h, 0, 0))
    wide = jax.ShapeDtypeStruct((length, width), jnp.float32)
    return pl.pallas_call(
        attend_back_body,
        grid=(heads,),
        in_specs=[slab] * 4 + [column, slab, slab, thin, thin, line, line, table, table],
        out_specs=[slab, slab, slab, line, line, column, column],
        out_shape=[
            jax.ShapeDtypeStruct((length, width), jnp.bfloat16),
            wide,
            wide,
            jax.ShapeDtypeStruct((1, width), jnp.float32),
            jax.ShapeDtypeStruct((1, width), jnp.float32),
            jax.ShapeDtypeStruct((heads, length, 1), jnp.float32),
            jax.ShapeDtypeStruct((heads, length, 1), jnp.float32),
        ],
        scratch_shapes=[pltpu.VMEM((length, HD), jnp.float32)] * 3,
        cost_estimate=pl.CostEstimate(
            flops=10 * heads * length * length * HD, bytes_accessed=16 << 20, transcendentals=heads * length * length
        ),
    )(queries, keys, values, grads, lse, q_raw, k_raw, q_rs, k_rs, q_gain[None], k_gain[None], cosine, sine)


def local(
    layer_input,
    cotangent,
    expert_index,
    attention_gain,
    query_gain,
    key_gain,
    query_weight,
    key_weight,
    value_weight,
    output_weight,
    feed_gain,
    router_weight,
    gate_weight,
    up_weight,
    down_weight,
):
    tokens = layer_input.shape[0]
    rows_count = lax.axis_size("row")
    near = rows_count == 4 and lax.axis_size("col") == 8
    if near:
        head_part = query_gain.shape[0]
        slice_width = attention_gain.shape[0]
        pack = jnp.concatenate(
            [attention_gain, feed_gain, query_gain, key_gain, router_weight.reshape(-1)]
        )
        pack = jnp.pad(pack, (0, PACK_ROWS * 128 - pack.shape[0])).reshape(PACK_ROWS, 128)
        (
            sequence, query_full, key_full, value_full, output_full, pack_all, cotangent_all, index_all
        ) = start_near(
            layer_input,
            [query_weight, key_weight, value_weight, output_weight],
            pack,
            cotangent,
            expert_index.T,
            1,
        )
        index_all = jnp.swapaxes(index_all, 1, 2)
        pack_all = pack_all.reshape(8, -1)
        ends = [slice_width, 2 * slice_width, 2 * slice_width + head_part, 2 * slice_width + 2 * head_part]
        attention_full = pack_all[:, : ends[0]].reshape(-1)
        feed_full = pack_all[:, ends[0] : ends[1]].reshape(-1)
        query_scale_w = pack_all[:, ends[1] : ends[2]].reshape(-1)
        key_scale_w = pack_all[:, ends[2] : ends[3]].reshape(-1)
        router_full = pack_all[:, ends[3] : ends[3] + router_weight.size].reshape(
            -1, router_weight.shape[1]
        )
    else:
        (
            attention_full,
            query_scale_w,
            key_scale_w,
            query_full,
            key_full,
            value_full,
            output_full,
            feed_full,
            router_full,
        ) = (
            lax.all_gather(attention_gain, "col", axis=0, tiled=True),
            lax.all_gather(query_gain, "col", axis=0, tiled=True),
            lax.all_gather(key_gain, "col", axis=0, tiled=True),
            lax.all_gather(query_weight, "col", axis=0, tiled=True),
            lax.all_gather(key_weight, "col", axis=0, tiled=True),
            lax.all_gather(value_weight, "col", axis=0, tiled=True),
            lax.all_gather(output_weight, "col", axis=1, tiled=True),
            lax.all_gather(feed_gain, "col", axis=0, tiled=True),
            lax.all_gather(router_weight, "col", axis=0, tiled=True),
        )
        sequence = lax.all_gather(layer_input, "row", axis=0, tiled=True)
    length = sequence.shape[0]
    model_width = sequence.shape[1]
    local_width = query_full.shape[1]
    seq_float = sequence.astype(jnp.float32)
    seq_scale = rms_scale(seq_float)
    attention_float = attention_full.astype(jnp.float32)
    normed = (seq_float * seq_scale * attention_float).astype(jnp.bfloat16)
    query_raw = wide_dot(normed, query_full)
    key_raw = wide_dot(normed, key_full)
    values = wide_dot(normed, value_full).astype(jnp.bfloat16)
    query_total, key_total = lax.psum(
        (jnp.sum(query_raw * query_raw, axis=-1), jnp.sum(key_raw * key_raw, axis=-1)), "row"
    )
    query_rs = lax.rsqrt(query_total / model_width + EPS)[:, None]
    key_rs = lax.rsqrt(key_total / model_width + EPS)[:, None]
    query_gain_f = query_scale_w.astype(jnp.float32)
    key_gain_f = key_scale_w.astype(jnp.float32)
    cosine, sine_table = rope_tables(length)
    mixed_heads, queries, keys_rotated, lse_all = attend(
        query_raw, key_raw, values, query_rs, key_rs, query_gain_f, key_gain_f, cosine, sine_table
    )
    if near:
        branch = branch_near(mixed_heads, output_full, 5)
    else:
        branch = lax.psum_scatter(
            wide_dot(mixed_heads, output_full).astype(jnp.bfloat16), "row", scatter_dimension=0, tiled=True
        ).astype(jnp.float32)
    hidden = layer_input.astype(jnp.float32) + branch
    feed_scale = rms_scale(hidden)
    feed_float = feed_full.astype(jnp.float32)
    feed_normed = (hidden * feed_scale * feed_float).astype(jnp.bfloat16)
    logits = wide_dot(feed_normed, router_full)
    logit_top = jnp.max(logits, axis=-1, keepdims=True)
    logit_exp = jnp.exp(logits - logit_top)
    router_probs = logit_exp / jnp.sum(logit_exp, axis=-1, keepdims=True)
    experts = router_full.shape[1]
    experts_local = gate_weight.shape[0]
    ranks = lax.axis_size("col") * rows_count
    gate_hits = expert_index[:, :, None] == jnp.arange(experts, dtype=jnp.int32)
    gate_probs = jnp.sum(jnp.where(gate_hits, router_probs[:, None, :], 0.0), axis=-1)

    if not near:
        index_all = lax.all_gather(expert_index, ("col", "row"), axis=0, tiled=True)
    own = (index_all - lax.axis_index("col") * experts_local).reshape(ranks, tokens, -1)
    matches = own[..., None] == jnp.arange(experts_local, dtype=jnp.int32)
    hit = jnp.sum(matches.astype(jnp.float32), axis=2)
    earlier = jnp.tril(jnp.ones((tokens, tokens), jnp.bfloat16), -1)
    rank = jnp.einsum(
        "tu,sue->ste", earlier, hit.astype(jnp.bfloat16), preferred_element_type=jnp.float32
    )
    slot = jnp.where(hit > 0, rank, -1.0)
    places = jnp.arange(SLOTS, dtype=jnp.float32)
    slot_t = jnp.swapaxes(slot, 1, 2)
    width = experts_local * SLOTS
    picked = slot_t[:, :, None, :] == places[None, None, :, None]
    pick = picked.astype(jnp.bfloat16).reshape(ranks, width, tokens)
    lanes = jnp.arange(width, dtype=jnp.int32)
    widen = (lanes[None, :] // SLOTS == jnp.arange(experts_local)[:, None]).astype(jnp.bfloat16)
    spread = jnp.einsum(
        "ste,ew->stw", slot.astype(jnp.bfloat16), widen, preferred_element_type=jnp.float32
    ) == (lanes % SLOTS).astype(jnp.float32)
    spread_plain = spread.astype(jnp.bfloat16)

    def weigh(probs_all):
        probs_own = jnp.sum(
            jnp.where(matches, probs_all.reshape(ranks, tokens, -1, 1), 0.0), axis=2
        )
        probs_wide = jnp.einsum(
            "ste,ew->stw", probs_own.astype(jnp.bfloat16), widen, preferred_element_type=jnp.float32
        )
        spread_probs = jnp.where(spread, probs_wide, 0.0).astype(jnp.bfloat16)
        probs_t = jnp.swapaxes(probs_own, 1, 2)
        row_probs = jnp.sum(jnp.where(picked, probs_t[:, :, None, :], 0.0), axis=-1)
        row_probs = jnp.swapaxes(row_probs, 0, 1).reshape(experts_local, ranks * SLOTS, 1)
        return spread_probs, row_probs

    if near:
        expert_grads, plain_act, feed_all, probs_all = grads_in(
            pick, cotangent_all, down_weight, feed_normed, gate_probs.T, 2
        )
        spread_probs, row_probs = weigh(jnp.swapaxes(probs_all, 1, 2))
        expert_rows, activated, weighted_act, grad_gate, grad_up, row_gates = feed_in(
            pick, feed_all, gate_weight, up_weight, plain_act, row_probs
        )
    else:
        probs_all = lax.all_gather(gate_probs, ("col", "row"), axis=0, tiled=True)
        spread_probs, row_probs = weigh(probs_all)
        expert_grads = gather_rows(pick, cotangent)
        expert_rows = gather_rows(pick, feed_normed)
        gate_val = jnp.einsum(
            "erd,edf->erf", expert_rows, gate_weight, preferred_element_type=jnp.float32
        )
        up_val = jnp.einsum(
            "erd,edf->erf", expert_rows, up_weight, preferred_element_type=jnp.float32
        )
        plain_act = jnp.einsum(
            "erd,efd->erf", expert_grads, down_weight, preferred_element_type=jnp.float32
        )
        sigmoid_val = jax.nn.sigmoid(gate_val)
        silu_val = gate_val * sigmoid_val
        activated = silu_val * up_val
        grad_act = plain_act * row_probs
        grad_up = (grad_act * silu_val).astype(jnp.bfloat16)
        grad_gate = (
            grad_act * up_val * sigmoid_val * (1.0 + gate_val * (1.0 - sigmoid_val))
        ).astype(jnp.bfloat16)
        row_gates = jnp.sum(activated * plain_act, axis=-1)
        weighted_act = (activated * row_probs).astype(jnp.bfloat16)
        activated = activated.astype(jnp.bfloat16)
    row_gates = jnp.swapaxes(row_gates.reshape(experts_local, ranks, SLOTS), 0, 1)
    own_gates = jnp.sum(jnp.where(picked, row_gates[..., None], 0.0), axis=2)
    if near:
        grad_feed_part = restore(
            spread_plain, [grad_gate, grad_up], [gate_weight, up_weight], (True, True)
        )
        grad_feed, gates_in, grad_gate_weight, grad_up_weight, grad_down_weight = feed_back(
            grad_feed_part, own_gates, expert_rows, grad_gate, grad_up, weighted_act, expert_grads, 3
        )
        grad_gate_weight, grad_up_weight, grad_down_weight = widen_all(
            grad_gate_weight, grad_up_weight, grad_down_weight
        )
        gates_in = jnp.sum(gates_in.reshape(-1, rows_count, experts_local, tokens), axis=1)
        grad_probs = gates_in.reshape(experts, tokens).T
    else:
        own_gates = lax.psum_scatter(
            jnp.swapaxes(own_gates, 1, 2).reshape(-1, rows_count, tokens, experts_local),
            "row",
            scatter_dimension=1,
        )
        grad_probs = lax.all_to_all(own_gates, "col", split_axis=0, concat_axis=2, tiled=True)[0]
        back_rows = (
            jnp.einsum("erf,edf->erd", grad_gate, gate_weight, preferred_element_type=jnp.float32)
            + jnp.einsum("erf,edf->erd", grad_up, up_weight, preferred_element_type=jnp.float32)
        ).astype(jnp.bfloat16)
        grad_feed = return_rows(spread_plain, back_rows).astype(jnp.float32)
        out_rows = jnp.einsum(
            "erf,efd->erd", activated, down_weight, preferred_element_type=jnp.float32
        ).astype(jnp.bfloat16)
        mixture = return_rows(spread_probs, out_rows).astype(jnp.float32)
        grad_gate_weight = jnp.einsum(
            "erd,erf->edf", expert_rows, grad_gate, preferred_element_type=jnp.float32
        )
        grad_up_weight = jnp.einsum(
            "erd,erf->edf", expert_rows, grad_up, preferred_element_type=jnp.float32
        )
        grad_down_weight = jnp.einsum(
            "erf,erd->efd", weighted_act, expert_grads, preferred_element_type=jnp.float32
        )
    grad_out = cotangent.astype(jnp.float32)
    grad_logits = (
        router_probs * (grad_probs - jnp.sum(router_probs * grad_probs, axis=-1, keepdims=True))
    ).astype(jnp.bfloat16)
    router_grad = inner_rows(feed_normed, grad_logits)
    grad_feed = grad_feed + outer_cols(grad_logits, router_full)
    feed_gain_term = jnp.sum(grad_feed * hidden * feed_scale, axis=0)
    feed_weighted = grad_feed * feed_float
    grad_hidden = (
        grad_out
        + feed_scale * feed_weighted
        - hidden * feed_scale**3 * jnp.mean(feed_weighted * hidden, axis=-1, keepdims=True)
    )
    if near:
        mixture_part, grad_branch = restore_out(
            spread_probs, activated, down_weight, grad_hidden.astype(jnp.bfloat16), 6
        )
    else:
        grad_branch = lax.all_gather(grad_hidden.astype(jnp.bfloat16), "row", axis=0, tiled=True)
    output_grad = inner_rows(mixed_heads, grad_branch)
    grad_mixed = outer_cols(grad_branch, output_full).astype(jnp.bfloat16)
    (
        grad_value_low, query_weighted, key_weighted, query_gain_term, key_gain_term, query_inner, key_inner
    ) = attend_back(
        queries, keys_rotated, values, grad_mixed, lse_all, query_raw, key_raw, query_rs, key_rs,
        query_gain_f, key_gain_f, cosine, sine_table,
    )
    query_gain_term, key_gain_term = query_gain_term.reshape(-1), key_gain_term.reshape(-1)
    query_inner, key_inner = (
        lax.psum(jnp.sum(query_inner, axis=(0, 2)), "row"),
        lax.psum(jnp.sum(key_inner, axis=(0, 2)), "row"),
    )
    grad_query_raw = (
        query_rs * query_weighted - query_raw * query_rs**3 * (query_inner / model_width)[:, None]
    ).astype(jnp.bfloat16)
    grad_key_raw = (
        key_rs * key_weighted - key_raw * key_rs**3 * (key_inner / model_width)[:, None]
    ).astype(jnp.bfloat16)
    query_grad = inner_rows(normed, grad_query_raw)
    key_grad = inner_rows(normed, grad_key_raw)
    value_grad = inner_rows(normed, grad_value_low)
    grad_normed = (
        outer_cols(grad_query_raw, query_full)
        + outer_cols(grad_key_raw, key_full)
        + outer_cols(grad_value_low, value_full)
    )
    attention_weighted = grad_normed * attention_float
    grad_seq_part = seq_scale * attention_weighted - seq_float * seq_scale**3 * jnp.mean(
        attention_weighted * seq_float, axis=-1, keepdims=True
    )
    attention_gain_term = jnp.sum(grad_normed * seq_float * seq_scale, axis=0)
    if near:
        cols = lax.axis_size("col")
        pack = jnp.concatenate(
            [
                attention_gain_term.reshape(cols, -1),
                feed_gain_term.reshape(cols, -1),
                query_gain_term.reshape(cols, -1),
                key_gain_term.reshape(cols, -1),
                router_grad.reshape(cols, -1),
            ],
            axis=1,
        )
        pack = jnp.pad(pack, ((0, 0), (0, PACK_ROWS * 128 - pack.shape[1])))
        pack = pack.astype(jnp.bfloat16).reshape(cols, PACK_ROWS, 128)
        (
            mixture, summed, grad_query_weight, grad_key_weight, grad_value_weight, grad_output_weight, packs
        ) = finish_near(
            mixture_part,
            grad_seq_part.astype(jnp.bfloat16).reshape(rows_count, tokens, model_width),
            [grad.astype(jnp.bfloat16) for grad in (query_grad, key_grad, value_grad, output_grad)],
            pack,
            4,
        )
        input_grad = grad_hidden + summed
        packs = packs.reshape(cols, rows_count, -1).astype(jnp.float32)
        whole = jnp.sum(packs, axis=(0, 1))
        heads_sum = jnp.sum(
            lax.dynamic_index_in_dim(packs, lax.axis_index("row"), 1, keepdims=False), axis=0
        )
        grad_attention_gain = whole[: ends[0]]
        grad_feed_gain = whole[ends[0] : ends[1]]
        grad_query_gain = heads_sum[ends[1] : ends[2]]
        grad_key_gain = heads_sum[ends[2] : ends[3]]
        grad_router_weight = whole[ends[3] : ends[3] + router_weight.size].reshape(router_weight.shape)
    else:
        stacked = jnp.concatenate(
            [
                grad_seq_part.reshape(rows_count, tokens, model_width),
                jnp.broadcast_to(attention_gain_term[None, None, :], (rows_count, 1, model_width)),
            ],
            axis=1,
        ).reshape(rows_count * (tokens + 1), model_width)
        summed = lax.psum_scatter(
            stacked.astype(jnp.bfloat16), "row", scatter_dimension=0, tiled=True
        ).astype(jnp.float32)
        input_grad = grad_hidden + summed[:tokens]
        attention_gain_total = summed[tokens]
        feed_gain_total, router_total = (
            lax.psum(feed_gain_term.astype(jnp.bfloat16), "row").astype(jnp.float32),
            lax.psum(router_grad.astype(jnp.bfloat16), "row").astype(jnp.float32),
        )
        (
            grad_attention_gain,
            grad_query_gain,
            grad_key_gain,
            grad_query_weight,
            grad_key_weight,
            grad_value_weight,
            grad_output_weight,
            grad_feed_gain,
            grad_router_weight,
        ) = (
            lax.psum_scatter(
                attention_gain_total.astype(jnp.bfloat16), "col", scatter_dimension=0, tiled=True
            ).astype(jnp.float32),
            lax.psum_scatter(
                query_gain_term.astype(jnp.bfloat16), "col", scatter_dimension=0, tiled=True
            ).astype(jnp.float32),
            lax.psum_scatter(
                key_gain_term.astype(jnp.bfloat16), "col", scatter_dimension=0, tiled=True
            ).astype(jnp.float32),
            lax.psum_scatter(
                query_grad.astype(jnp.bfloat16), "col", scatter_dimension=0, tiled=True
            ).astype(jnp.float32),
            lax.psum_scatter(
                key_grad.astype(jnp.bfloat16), "col", scatter_dimension=0, tiled=True
            ).astype(jnp.float32),
            lax.psum_scatter(
                value_grad.astype(jnp.bfloat16), "col", scatter_dimension=0, tiled=True
            ).astype(jnp.float32),
            lax.psum_scatter(
                output_grad.astype(jnp.bfloat16), "col", scatter_dimension=1, tiled=True
            ).astype(jnp.float32),
            lax.psum_scatter(
                feed_gain_total.astype(jnp.bfloat16), "col", scatter_dimension=0, tiled=True
            ).astype(jnp.float32),
            lax.psum_scatter(
                router_total.astype(jnp.bfloat16), "col", scatter_dimension=0, tiled=True
            ).astype(jnp.float32),
        )
    layer_output = hidden + mixture
    return (
        layer_output,
        input_grad,
        grad_attention_gain,
        grad_query_gain,
        grad_key_gain,
        grad_query_weight,
        grad_key_weight,
        grad_value_weight,
        grad_output_weight,
        grad_feed_gain,
        grad_router_weight,
        grad_gate_weight,
        grad_up_weight,
        grad_down_weight,
    )


def solution(mesh):
    placed = (
        P(("col", "row"), None),
        P(("col", "row"), None),
        P(("col", "row"), None),
        P("col"),
        P(("row", "col")),
        P(("row", "col")),
        P("col", "row"),
        P("col", "row"),
        P("col", "row"),
        P("row", "col"),
        P("col"),
        P("col", None),
        P("col", None, "row"),
        P("col", None, "row"),
        P("col", "row", None),
    )
    return jax.shard_map(
        local,
        mesh=mesh,
        in_specs=placed,
        out_specs=(
            P(("col", "row"), None),
            P(("col", "row"), None),
            P("col"),
            P(("row", "col")),
            P(("row", "col")),
            P("col", "row"),
            P("col", "row"),
            P("col", "row"),
            P("row", "col"),
            P("col"),
            P("col", None),
            P("col", None, "row"),
            P("col", None, "row"),
            P("col", "row", None),
        ),
        check_vma=False,
    )
```

```python
import functools

import jax
import jax.numpy as jnp
from jax import lax
from jax.experimental import pallas as pl
from jax.experimental.pallas import tpu as pltpu
from jax.sharding import PartitionSpec as P

HD = 128
SLOTS = 40
BLOCK = 512
CHUNK = 256
UNROLL = 4
PACK_ROWS = 144


EPS = 1e-05
THETA = 10000.0
MASKED = -1e30


def wide_dot(left, right):
    return jnp.dot(left, right, preferred_element_type=jnp.float32)


def inner_rows(left, right):
    return lax.dot_general(
        left, right, (((0,), (0,)), ((), ())), preferred_element_type=jnp.float32
    )


def outer_cols(left, right):
    return lax.dot_general(
        left, right, (((1,), (1,)), ((), ())), preferred_element_type=jnp.float32
    )


def rms_scale(field):
    return lax.rsqrt(jnp.mean(field * field, axis=-1, keepdims=True) + EPS)


def rope_tables(length):
    half_size = HD // 2
    freqs = THETA ** (-(jnp.arange(half_size, dtype=jnp.float32) * 2.0) / HD)
    angles = jnp.arange(length, dtype=jnp.float32)[:, None] * freqs[None, :]
    cosine = jnp.concatenate([jnp.cos(angles), jnp.cos(angles)], axis=-1)
    sine_table = jnp.concatenate([-jnp.sin(angles), jnp.sin(angles)], axis=-1)
    return (cosine, sine_table)


def dispatch_body(pick_ref, field_ref, rows_ref):
    groups = rows_ref.shape[0]
    first = wide_dot(pick_ref[0], field_ref[0]).reshape(groups, SLOTS, -1)
    second = wide_dot(pick_ref[1], field_ref[1]).reshape(groups, SLOTS, -1)
    rows_ref[...] = jnp.concatenate([first, second], axis=1).astype(jnp.bfloat16)


def dispatch(pick, field):
    ranks, width, tokens = pick.shape
    groups, depth = width // SLOTS, field.shape[1]
    return pl.pallas_call(
        dispatch_body,
        grid=(ranks // 2, depth // BLOCK),
        in_specs=[
            pl.BlockSpec((2, width, tokens), lambda i, k: (i, 0, 0)),
            pl.BlockSpec((2, tokens, BLOCK), lambda i, k: (i, 0, k)),
        ],
        out_specs=pl.BlockSpec((groups, 2 * SLOTS, BLOCK), lambda i, k: (0, i, k)),
        out_shape=jax.ShapeDtypeStruct((groups, ranks * SLOTS, depth), jnp.bfloat16),
    )(pick, field.reshape(ranks, tokens, depth))


def combine_body(spread_ref, rows_ref, field_ref):
    rows = rows_ref[...].astype(jnp.float32)
    width = rows.shape[0] * SLOTS
    for side in range(2):
        part = rows[:, side * SLOTS : (side + 1) * SLOTS].reshape(width, -1).astype(jnp.bfloat16)
        field_ref[side] = wide_dot(spread_ref[side], part).astype(jnp.bfloat16)


def combine(spread, rows):
    ranks, tokens, width = spread.shape
    groups, depth = width // SLOTS, rows.shape[2]
    field = pl.pallas_call(
        combine_body,
        grid=(ranks // 2, depth // BLOCK),
        in_specs=[
            pl.BlockSpec((2, tokens, width), lambda i, k: (i, 0, 0)),
            pl.BlockSpec((groups, 2 * SLOTS, BLOCK), lambda i, k: (0, i, k)),
        ],
        out_specs=pl.BlockSpec((2, tokens, BLOCK), lambda i, k: (i, 0, k)),
        out_shape=jax.ShapeDtypeStruct((ranks, tokens, depth), jnp.bfloat16),
    )(spread, rows)
    return field.reshape(ranks * tokens, depth)


def scatter_all(field):
    part = lax.psum_scatter(field, "col", scatter_dimension=0, tiled=True)
    return lax.psum_scatter(part, "row", scatter_dimension=0, tiled=True)


def pieces_of(ranks, depth):
    count = max(1, ranks // 32)
    step = depth // count
    return [(at, at + step) for at in range(0, depth, step)]


def gather_rows(pick, field):
    rows = []
    for start, stop in pieces_of(pick.shape[0], field.shape[1]):
        part = field[:, start:stop]
        if rows:
            part = lax.optimization_barrier((part, rows[-1]))[0]
        whole = lax.all_gather(part, ("col", "row"), axis=0, tiled=True)
        rows.append(dispatch(pick, whole))
    return rows[0] if len(rows) == 1 else jnp.concatenate(rows, axis=2)


def return_rows(spread, rows):
    sums = []
    for start, stop in pieces_of(spread.shape[0], rows.shape[2]):
        part = rows[:, :, start:stop]
        if sums:
            part = lax.optimization_barrier((part, sums[-1]))[0]
        sums.append(scatter_all(combine(spread, part)))
    return sums[0] if len(sums) == 1 else jnp.concatenate(sums, axis=1)


MESH = pl.DeviceIdType.MESH


def seat():
    r, c = lax.axis_index("row"), lax.axis_index("col")
    y, x = r // 2, r % 2
    z, core = c // 2, c % 2
    first = y * (1 - core) + x * core
    second = x * (1 - core) + y * core
    return r, c, y, x, z, core, first, second


def partners():
    r, c, y, x, z, core, first, second = seat()
    pair = (r, z * 2 + (1 - core))
    flip_y = (1 - y) * 2 + x
    flip_x = y * 2 + (1 - x)
    along_first = (flip_y * (1 - core) + flip_x * core, c)
    along_second = (flip_x * (1 - core) + flip_y * core, c)
    up = [(r, ((z + k) % 4) * 2 + core) for k in range(1, 4)]
    return pair, along_first, along_second, up


RANKS = 32


def nth(offset):
    spot = (lax.axis_index("col") * 4 + lax.axis_index("row") + offset) % RANKS
    return spot, (spot % 4, spot // 4)


def meet():
    barrier = pltpu.get_barrier_semaphore()

    @pl.loop(1, RANKS)
    def _(offset):
        pl.semaphore_signal(barrier, inc=1, device_id=nth(offset)[1], device_id_type=MESH)

    pl.semaphore_wait(barrier, RANKS - 1)


def small_copy(src_of, small_all, small_send, small_recv, offset):
    spot, device = nth(offset)
    return send(
        src_of(spot), small_all.at[nth(0)[0]], small_send.at[offset], small_recv.at[offset], device
    )


def row_of(core, first, second):
    y = first * (1 - core) + second * core
    x = second * (1 - core) + first * core
    return y, x


def send(src, dst, send_sem, recv_sem, device):
    return pltpu.make_async_remote_copy(
        src_ref=src, dst_ref=dst, send_sem=send_sem, recv_sem=recv_sem, device_id=device, device_id_type=MESH
    )


GSTEPS = 4
QUEUE = (2, 1, 3)
ARRIVE = (1, 3, 2)


def spread_out(own_ref, all_ref, sems):
    r, c, y, x, z, core, first, second = seat()
    pair, along_first, along_second, up = partners()
    here_sem, u_send, u_recv, d_send, d_recv, g_send, g_recv, f_send, f_recv, p_send, p_recv = sems
    step = own_ref.shape[0] // GSTEPS

    def rows(q):
        return pl.ds(pl.multiple_of(q * step, step), step)

    def place(k, s, f, q):
        sec = second * (1 - s) + (1 - second) * s
        fir = first * (1 - f) + (1 - first) * f
        yy, xx = row_of(core, fir, sec)
        return all_ref.at[(z + 4 - k) % 4, core, yy, xx, rows(q)]

    above, below = (r, ((z + 1) % 4) * 2 + core), (r, ((z + 3) % 4) * 2 + core)

    def source(k, q):
        return own_ref.at[rows(q)] if k == 0 else place(k, 0, 0, q)

    def up_copy(d, q):
        return send(source(d, q), place(d, 0, 0, q), u_send.at[d, q], u_recv.at[d, q], above)

    def down_copy(d, q):
        k = (4 - d) % 4
        return send(source(k, q), place(k, 0, 0, q), d_send.at[d, q], d_recv.at[d, q], below)

    def came_up(d, q):
        there = place(d, 0, 0, q)
        return send(there, there, u_send.at[d - 1, q], u_recv.at[d - 1, q], above)

    def came_down(d, q):
        there = place(4 - d, 0, 0, q)
        return send(there, there, d_send.at[d - 1, q], d_recv.at[d - 1, q], below)

    bottom, top = 1 - jnp.minimum(z, 1), z // 3
    arrived = [bottom * (3 - i) + top * (1 + i) + (1 - bottom - top) * ARRIVE[i] for i in range(3)]

    def g_copy(k, q, src):
        return send(src, place(k, 0, 0, q), g_send.at[k, q], g_recv.at[k, q], along_second)

    def f_copy(k, s, q, src):
        return send(src, place(k, s, 0, q), f_send.at[s, k, q], f_recv.at[s, k, q], along_first)

    def p_copy(k, s, f, q, src):
        return send(src, place(k, s, f, q), p_send.at[f, s, k, q], p_recv.at[f, s, k, q], pair)

    here = pltpu.make_async_copy(own_ref, all_ref.at[z, core, y, x], here_sem)

    def begin():
        here.start()

        @pl.loop(0, GSTEPS)
        def _(q):
            src = own_ref.at[rows(q)]

            @pl.when(z < 3)
            def _():
                up_copy(0, q).start()

            @pl.when(z > 0)
            def _():
                down_copy(0, q).start()

            g_copy(0, q, src).start()
            f_copy(0, 0, q, src).start()
            p_copy(0, 0, 0, q, src).start()

    def along_z(q):
        def pass_on(k):
            src = place(k, 0, 0, q)
            g_copy(k, q, src).start()
            f_copy(k, 0, q, src).start()
            p_copy(k, 0, 0, q, src).start()

        for d in (1, 2, 3):

            @pl.when(z >= d)
            def _():
                came_up(d, q).wait_recv()
                if d < 3:

                    @pl.when(z < 3)
                    def _():
                        up_copy(d, q).start()

                pass_on(d)

            @pl.when(z + d <= 3)
            def _():
                came_down(d, q).wait_recv()
                if d < 3:

                    @pl.when(z > 0)
                    def _():
                        down_copy(d, q).start()

                pass_on(4 - d)

    def forward(q):
        @pl.when(q == 0)
        def _():
            along_z(q)

        @pl.when(q + 1 < GSTEPS)
        def _():
            along_z(q + 1)

        for k in (0, *arrived):
            src = place(k, 1, 0, q)
            g_copy(k, q, src).wait_recv()
            f_copy(k, 1, q, src).start()
            p_copy(k, 1, 0, q, src).start()
        for k in (0, *arrived):
            src = place(k, 0, 1, q)
            f_copy(k, 0, q, src).wait_recv()
            p_copy(k, 0, 1, q, src).start()

    def finish():
        @pl.loop(0, GSTEPS)
        def _(q):
            for k in (0, *arrived):
                src = place(k, 1, 1, q)
                f_copy(k, 1, q, src).wait_recv()
                p_copy(k, 1, 1, q, src).start()

        here.wait()

        @pl.loop(0, GSTEPS)
        def _(q):
            for d in range(3):

                @pl.when((z < 3) & (z >= d))
                def _():
                    up_copy(d, q).wait_send()

                @pl.when((z > 0) & (z + d <= 3))
                def _():
                    down_copy(d, q).wait_send()

            for k in range(4):
                src = own_ref.at[rows(q)]
                g_copy(k, q, src).wait_send()
                for s in range(2):
                    f_copy(k, s, q, src).wait_send()
                    for f in range(2):
                        p_copy(k, s, f, q, src).wait()

    return begin, forward, finish


def spread_sems():
    dma = pltpu.SemaphoreType.DMA
    shapes = [(3, GSTEPS), (3, GSTEPS), (4, GSTEPS), (2, 4, GSTEPS), (2, 2, 4, GSTEPS)]
    return [dma(())] + [dma(shape) for shape in shapes for _ in range(2)]


def small_out(small_ref, small_all, sems):
    here_sem, small_send, small_recv = sems
    local = pltpu.make_async_copy(small_ref, small_all.at[nth(0)[0]], here_sem)

    def copy(offset):
        return small_copy(lambda spot: small_ref, small_all, small_send, small_recv, offset)

    def begin():
        local.start()

        @pl.loop(1, RANKS)
        def _(offset):
            copy(offset).start()

    def finish():
        local.wait()

        @pl.loop(1, RANKS)
        def _(offset):
            copy(offset).wait()

    return begin, finish


def small_sems():
    dma = pltpu.SemaphoreType.DMA
    return [dma(()), dma((RANKS,)), dma((RANKS,))]


ANYWHERE = pl.BlockSpec(memory_space=pl.ANY)


def start_body(x_ref, q_ref, k_ref, v_ref, o_ref, pack_ref, own_ref, small_ref,
               x_all, qkv_all, o_all, pack_all, all_ref, small_all, *sems):
    r, c, y, x, z, core, first, second = seat()
    pair, along_first, along_second, up = partners()
    begin, forward, finish = spread_out(own_ref, all_ref, sems[:11])
    small_begin, small_finish = small_out(small_ref, small_all, sems[11:14])
    here_sem, x_send, x_recv, w_send, w_recv, v_send, v_recv = sems[14:]
    weights = [(q_ref, qkv_all), (k_ref, qkv_all), (v_ref, qkv_all), (o_ref, o_all), (pack_ref, pack_all)]

    def block(index, col):
        ref, whole = weights[index]
        if index == 4:
            return whole.at[col]
        if index == 3:
            width = ref.shape[1]
            return whole.at[:, pl.ds(pl.multiple_of(col * width, width), width)]
        height, width = ref.shape
        return whole.at[pl.ds(pl.multiple_of(col * height, height), height), pl.ds(index * width, width)]

    def w_copy(index, k):
        return send(
            weights[index][0], block(index, c), w_send.at[index, k - 1], w_recv.at[index, k - 1], up[k - 1]
        )

    def pair_copy(index, k):
        col = ((z + 4 - k) % 4) * 2 + core
        src = weights[index][0] if k == 0 else block(index, col)
        return send(src, block(index, col), v_send.at[index, k], v_recv.at[index, k], pair)

    locals_ = [pltpu.make_async_copy(x_ref, x_all.at[r], here_sem.at[5])] + [
        pltpu.make_async_copy(weights[i][0], block(i, c), here_sem.at[i]) for i in range(5)
    ]
    y1, x1 = row_of(core, first, 1 - second)
    near_row = y1 * 2 + x1
    x_first = send(x_ref, x_all.at[r], x_send.at[0], x_recv.at[0], along_first)
    x_second = send(x_ref, x_all.at[r], x_send.at[1], x_recv.at[1], along_second)
    x_relay = send(x_all.at[near_row], x_all.at[near_row], x_send.at[2], x_recv.at[2], along_first)

    meet()
    small_begin()
    x_second.start()
    x_first.start()
    begin()
    for item in locals_:
        item.start()
    x_second.wait_recv()
    x_relay.start()
    for q, group in enumerate(((4, 0), (1,), (2, 3), ())):
        forward(q)
        for index in group:
            for k in QUEUE:
                w_copy(index, k).start()
            pair_copy(index, 0).start()

    for index in (4, 0, 1, 2, 3):
        for k in ARRIVE:
            w_copy(index, k).wait_recv()
            pair_copy(index, k).start()
    finish()
    small_finish()
    for item in locals_:
        item.wait()
    x_first.wait()
    x_second.wait_send()
    x_relay.wait()
    for index in range(5):
        for k in range(4):
            if k:
                w_copy(index, k).wait_send()
            pair_copy(index, k).wait()


def start_near(x, weights, pack, own, small, collective_id):
    tokens, depth = own.shape
    dma = pltpu.SemaphoreType.DMA
    height, width = weights[0].shape
    shaped = lambda shape, like: jax.ShapeDtypeStruct(shape, like.dtype)
    outs = pl.pallas_call(
        start_body,
        out_shape=(
            shaped((4, *x.shape), x),
            shaped((8 * height, 3 * width), weights[0]),
            shaped((weights[3].shape[0], 8 * weights[3].shape[1]), weights[3]),
            shaped((8, *pack.shape), pack),
            shaped((4, 2, 2, 2, tokens, depth), own),
            shaped((RANKS, *small.shape), small),
        ),
        in_specs=[ANYWHERE] * 8,
        out_specs=[ANYWHERE] * 6,
        scratch_shapes=spread_sems()
        + small_sems()
        + [dma((6,)), dma((3,)), dma((3,)), dma((5, 3)), dma((5, 3)), dma((5, 4)), dma((5, 4))],
        compiler_params=pltpu.CompilerParams(collective_id=collective_id, has_side_effects=True),
    )(x, *weights, pack, own, small)
    x_all, qkv, o, pack_all, whole, small_all = outs
    return x_all.reshape(-1, x.shape[1]), qkv, o, pack_all, whole.reshape(RANKS, tokens, depth), small_all


def finish_body(part_ref, field_ref, qkv_ref, o_ref, pack_ref,
                mixture_ref, out_ref, q_out, k_out, v_out, o_out, pack_all,
                mine, first_in, second_in, total,
                qkv_mine, o_mine, qkv_pair, o_pair, qkv_z, o_z, qkv_sum, o_sum,
                load_sem, f_send, f_recv, g_send, g_recv, w_load, p_send, p_recv, z_send, z_recv, out_sem,
                *rest):
    r, c, y, x, z, core, first, second = seat()
    pair, along_first, along_second, up = partners()
    small_begin, small_finish = small_each(pack_ref, pack_all, rest[:3], lambda spot: spot // 4)
    begin, tick, finish = shrink(part_ref, *rest[3:9], rest[9:18])
    mixture = rest[8]
    tokens, depth = out_ref.shape
    other = 1 - core
    grads, kept, pairs = [qkv_ref, o_ref], [qkv_mine, o_mine], [qkv_pair, o_pair]
    zs, sums = [qkv_z, o_z], [qkv_sum, o_sum]
    width = q_out.shape[1]
    results = [
        [
            pltpu.make_async_copy(qkv_sum.at[:, pl.ds(i * width, width)], out, out_sem.at[i])
            for i, out in enumerate((q_out, k_out, v_out))
        ],
        [pltpu.make_async_copy(o_sum, o_out, out_sem.at[3])],
    ]

    def block(index, col):
        ref = grads[index]
        if index == 1:
            width = ref.shape[1] // 8
            return ref.at[:, pl.ds(pl.multiple_of(col * width, width), width)]
        height = ref.shape[0] // 8
        return ref.at[pl.ds(pl.multiple_of(col * height, height), height)]

    def row(fir, sec):
        yy, xx = row_of(core, fir, sec)
        return yy * 2 + xx

    def load(fir, sec):
        return pltpu.make_async_copy(field_ref.at[row(fir, sec)], mine.at[fir, sec], load_sem.at[fir, sec])

    def f_copy(sec):
        return send(field_ref.at[row(1 - first, sec)], first_in.at[sec], f_send.at[sec], f_recv.at[sec], along_first)

    g_copy = send(mine.at[first, 1 - second], second_in, g_send, g_recv, along_second)

    def w_load_copy(index, zz):
        return pltpu.make_async_copy(block(index, zz * 2 + core), kept[index].at[zz], w_load.at[index, zz])

    def w_give(index, zz):
        return send(
            block(index, zz * 2 + other), pairs[index].at[zz], p_send.at[index, zz], p_recv.at[index, zz], pair
        )

    def w_z(index, k):
        return send(
            kept[index].at[(z + k) % 4], zs[index].at[k - 1], z_send.at[index, k - 1], z_recv.at[index, k - 1], up[k - 1]
        )

    def add(ref, extras):
        @pl.loop(0, ref.shape[0] // TILE)
        def _(t):
            here = pl.ds(pl.multiple_of(t * TILE, TILE), TILE)
            value = ref[here].astype(jnp.float32)
            for extra in extras:
                value = value + extra[here].astype(jnp.float32)
            ref[here] = value.astype(jnp.bfloat16)

    def add_out(ref, extras, result):
        @pl.loop(0, ref.shape[0] // TILE)
        def _(t):
            here = pl.ds(pl.multiple_of(t * TILE, TILE), TILE)
            value = ref[here].astype(jnp.float32)
            for extra in extras:
                value = value + extra[here].astype(jnp.float32)
            result[here] = value

    meet()
    for index in range(2):
        for k in (2, 1, 3, 0):
            w_give(index, (z + k) % 4).start()
            w_load_copy(index, (z + k) % 4).start()
    begin()
    f_copy(1 - second).start()
    f_copy(second).start()
    load(first, 1 - second).start()
    load(first, second).start()
    small_begin()
    for index in range(2):
        for k in QUEUE:
            zz = (z + k) % 4
            w_load_copy(index, zz).wait()
            w_give(index, zz).wait_recv()
            add(kept[index].at[zz], [pairs[index].at[zz]])
            w_z(index, k).start()

    @pl.loop(0, RSTEPS + LAGS[2])
    def _(i):
        tick(i)

        @pl.when(i == 2)
        def _():
            load(first, 1 - second).wait()
            f_copy(1 - second).wait_recv()
            add(mine.at[first, 1 - second], [first_in.at[1 - second]])
            g_copy.start()

    for index in range(2):
        w_load_copy(index, z).wait()
        w_give(index, z).wait_recv()
        for k in ARRIVE:
            w_z(index, k).wait_recv()
        add_out(
            kept[index].at[z], [pairs[index].at[z]] + [zs[index].at[k] for k in range(3)], sums[index]
        )
        for result in results[index]:
            result.start()
    load(first, second).wait()
    f_copy(second).wait_recv()
    g_copy.wait_recv()
    add_out(mine.at[first, second], [first_in.at[second], second_in], total)
    pltpu.make_async_copy(total, out_ref, out_sem.at[4]).start()

    @pl.loop(RSTEPS + LAGS[2], TICKS)
    def _(i):
        tick(i)

    pltpu.make_async_copy(mixture, mixture_ref, out_sem.at[5]).start()
    finish()
    for sec in range(2):
        f_copy(sec).wait_send()
    g_copy.wait_send()
    for index in range(2):
        for k in range(4):
            w_give(index, (z + k) % 4).wait_send()
            if k:
                w_z(index, k).wait_send()
        for result in results[index]:
            result.wait()
    small_finish()
    pltpu.make_async_copy(total, out_ref, out_sem.at[4]).wait()
    pltpu.make_async_copy(mixture, mixture_ref, out_sem.at[5]).wait()


def finish_near(part, field, grads, pack, collective_id):
    rows_count, tokens, depth = field.shape
    dma = pltpu.SemaphoreType.DMA
    blocks = [(grads[0].shape[0] // 8, grads[0].shape[1]), (grads[1].shape[0], grads[1].shape[1] // 8)]
    results = [(blocks[0][0], blocks[0][1] // 3)] * 3 + [blocks[1]]
    half = lambda *shape: pltpu.VMEM(shape, jnp.bfloat16)
    return pl.pallas_call(
        finish_body,
        out_shape=(
            jax.ShapeDtypeStruct((tokens, depth), jnp.float32),
            jax.ShapeDtypeStruct((tokens, depth), jnp.float32),
            *[jax.ShapeDtypeStruct(b, jnp.float32) for b in results],
            jax.ShapeDtypeStruct((RANKS, *pack.shape[1:]), pack.dtype),
        ),
        in_specs=[ANYWHERE] * 5,
        out_specs=[ANYWHERE] * 7,
        scratch_shapes=[
            half(2, 2, tokens, depth), half(2, tokens, depth), half(tokens, depth),
            pltpu.VMEM((tokens, depth), jnp.float32),
            *[half(4, *b) for b in blocks], *[half(4, *b) for b in blocks], *[half(3, *b) for b in blocks],
            *[pltpu.VMEM(b, jnp.float32) for b in blocks],
            dma((2, 2)), dma((2,)), dma((2,)), dma(()), dma(()),
            dma((2, 4)), dma((2, 4)), dma((2, 4)), dma((2, 3)), dma((2, 3)), dma((6,)),
        ]
        + small_sems()
        + shrink_scratch(tokens, depth),
        compiler_params=pltpu.CompilerParams(
            collective_id=collective_id, has_side_effects=True, vmem_limit_bytes=63 * 1024 * 1024
        ),
    )(part.reshape(4, 2, 2, 2, tokens, depth), field, *grads, pack)


RSTEPS = 8
TILE = 16
LAGS = (0, 1, 2, 4)
TICKS = RSTEPS + LAGS[3]


def shrink(part_ref, sums, near_own, first_in, second_in, z_in, total, sems):
    r, c, y, x, z, core, first, second = seat()
    pair, along_first, along_second, up = partners()
    load_sem, p_send, p_recv, f_send, f_recv, g_send, g_recv, z_send, z_recv = sems
    tokens = total.shape[0]
    step = tokens // RSTEPS
    other = 1 - core

    def rows(q):
        return pl.ds(pl.multiple_of(q * step, step), step)

    def spot(kind):
        fir = (1 - first) if kind < 2 else first
        sec = (1 - second) if kind in (0, 2) else second
        return fir, sec

    def load(kind, q):
        yy, xx = row_of(core, *spot(kind))
        return pltpu.make_async_copy(
            part_ref.at[:, core, yy, xx, rows(q)], near_own.at[q % 2, kind], load_sem.at[kind, q % 2]
        )

    def give(fir, sec, q):
        yy, xx = row_of(other, fir, sec)
        return send(
            part_ref.at[:, other, yy, xx, rows(q)],
            sums.at[fir, sec, :, rows(q)],
            p_send.at[fir, sec, q],
            p_recv.at[fir, sec, q],
            pair,
        )

    def f_copy(sec, q):
        return send(
            sums.at[1 - first, sec, :, rows(q)],
            first_in.at[sec, :, rows(q)],
            f_send.at[sec, q],
            f_recv.at[sec, q],
            along_first,
        )

    def g_copy(q):
        return send(
            sums.at[first, 1 - second, :, rows(q)], second_in.at[:, rows(q)], g_send.at[q], g_recv.at[q], along_second
        )

    def z_copy(k, q):
        return send(
            sums.at[first, second, (z + k) % 4, rows(q)],
            z_in.at[k - 1, rows(q)],
            z_send.at[k - 1, q],
            z_recv.at[k - 1, q],
            up[k - 1],
        )

    def begin():
        @pl.loop(0, RSTEPS)
        def _(q):
            for fir, sec in ((1 - second, 1 - first), (1 - second, first), (second, 1 - first), (second, first)):
                give(fir, sec, q).start()

        for kind in range(4):
            load(kind, 0).start()

    def add(kind, q, extra):
        fir, sec = spot(kind)

        @pl.when(q + 1 < RSTEPS)
        def _():
            load(kind, q + 1).start()

        load(kind, q).wait()
        give(fir, sec, q).wait_recv()

        @pl.loop(0, 4 * (step // TILE))
        def _(t):
            zz, at = t // (step // TILE), t % (step // TILE)
            here = pl.ds(pl.multiple_of(q * step + at * TILE, TILE), TILE)
            near = pl.ds(pl.multiple_of(at * TILE, TILE), TILE)
            value = sums[fir, sec, zz, here].astype(jnp.float32)
            value = value + near_own[q % 2, kind, zz, near].astype(jnp.float32)
            for ref in extra:
                value = value + ref[zz, here].astype(jnp.float32)
            sums[fir, sec, zz, here] = value.astype(jnp.bfloat16)

    def stage_first(q):
        for kind, sec in ((0, 1 - second), (1, second)):
            add(kind, q, [])
            f_copy(sec, q).start()

    def stage_second(q):
        f_copy(1 - second, q).wait_recv()
        add(2, q, [first_in.at[1 - second]])
        g_copy(q).start()

    def stage_z(q):
        f_copy(second, q).wait_recv()
        g_copy(q).wait_recv()
        add(3, q, [first_in.at[second], second_in])
        for k in QUEUE:
            z_copy(k, q).start()

    def stage_out(q):
        for k in ARRIVE:
            z_copy(k, q).wait_recv()

        @pl.loop(0, step // TILE)
        def _(t):
            here = pl.ds(pl.multiple_of(q * step + t * TILE, TILE), TILE)
            value = sums[first, second, z, here].astype(jnp.float32)
            for k in range(3):
                value = value + z_in[k, here].astype(jnp.float32)
            total[here] = value

    def tick(i):
        for stage, lag in zip((stage_first, stage_second, stage_z, stage_out), LAGS):

            @pl.when((i >= lag) & (i < RSTEPS + lag))
            def _(stage=stage, lag=lag):
                stage(i - lag)

    def finish():
        @pl.loop(0, RSTEPS)
        def _(q):
            for fir in range(2):
                for sec in range(2):
                    give(fir, sec, q).wait_send()
            for sec in range(2):
                f_copy(sec, q).wait_send()
            g_copy(q).wait_send()
            for k in QUEUE:
                z_copy(k, q).wait_send()

    return begin, tick, finish


def shrink_scratch(tokens, depth):
    dma = pltpu.SemaphoreType.DMA
    low = lambda *shape: pltpu.VMEM((*shape, depth), jnp.bfloat16)
    buffers = [
        low(2, 2, 4, tokens), low(2, 4, 4, tokens // RSTEPS), low(2, 4, tokens), low(4, tokens), low(3, tokens),
        pltpu.VMEM((tokens, depth), jnp.float32),
    ]
    shapes = [(2, 2, RSTEPS), (2, RSTEPS), (RSTEPS,), (3, RSTEPS)]
    return buffers + [dma((4, 2))] + [dma(shape) for shape in shapes for _ in range(2)]


def small_each(small_ref, small_all, sems, pick):
    here_sem, small_send, small_recv = sems
    local = pltpu.make_async_copy(small_ref.at[pick(nth(0)[0])], small_all.at[nth(0)[0]], here_sem)

    def copy(offset):
        return small_copy(lambda spot: small_ref.at[pick(spot)], small_all, small_send, small_recv, offset)

    def begin():
        local.start()

        @pl.loop(1, RANKS)
        def _(offset):
            copy(offset).start()

    def finish():
        local.wait()

        @pl.loop(1, RANKS)
        def _(offset):
            copy(offset).wait()

    return begin, finish


def feed_back_body(part_ref, small_ref, rows_ref, gate_ref, up_ref, act_ref, grads_ref,
                   out_ref, small_all, gate_out, up_out, down_out, *scratch):
    begin, tick, finish = shrink(part_ref, *scratch[:6], scratch[6:15])
    total, out_sem = scratch[5], scratch[15]
    small_begin, small_finish = small_each(small_ref, small_all, scratch[16:], lambda spot: spot)
    e, k = pl.program_id(0), pl.program_id(1)
    step = e * pl.num_programs(1) + k
    last = pl.num_programs(0) * pl.num_programs(1) - 1

    @pl.when(step == 0)
    def _():
        meet()
        small_begin()
        begin()

    rows = rows_ref[0]
    gate_out[0] = inner_rows(rows, gate_ref[0]).astype(jnp.bfloat16)
    up_out[0] = inner_rows(rows, up_ref[0]).astype(jnp.bfloat16)
    down_out[0] = inner_rows(act_ref[0], grads_ref[0]).astype(jnp.bfloat16)

    @pl.when(k == 0)
    def _():
        tick(e)

    @pl.when(step == last)
    def _():
        @pl.loop(RSTEPS, TICKS)
        def _(i):
            tick(i)

        done = pltpu.make_async_copy(total, out_ref, out_sem)
        done.start()
        finish()
        small_finish()
        done.wait()


def feed_back(part, small, rows, grad_gate, grad_up, act, grads, collective_id):
    tokens, depth = part.shape[0] // RANKS, part.shape[1]
    groups, length, inner = grad_gate.shape
    assert groups == RSTEPS
    dma = pltpu.SemaphoreType.DMA
    slab = pl.BlockSpec((1, length, CHUNK), lambda e, k: (e, 0, k))
    held = pl.BlockSpec((1, length, inner), lambda e, k: (e, 0, 0))
    return pl.pallas_call(
        feed_back_body,
        grid=(groups, depth // CHUNK),
        in_specs=[ANYWHERE, ANYWHERE, slab, held, held, held, slab],
        out_specs=[
            ANYWHERE,
            ANYWHERE,
            pl.BlockSpec((1, CHUNK, inner), lambda e, k: (e, k, 0)),
            pl.BlockSpec((1, CHUNK, inner), lambda e, k: (e, k, 0)),
            pl.BlockSpec((1, inner, CHUNK), lambda e, k: (e, 0, k)),
        ],
        out_shape=(
            jax.ShapeDtypeStruct((tokens, depth), jnp.float32),
            jax.ShapeDtypeStruct(small.shape, small.dtype),
            jax.ShapeDtypeStruct((groups, depth, inner), jnp.bfloat16),
            jax.ShapeDtypeStruct((groups, depth, inner), jnp.bfloat16),
            jax.ShapeDtypeStruct((groups, inner, depth), jnp.bfloat16),
        ),
        scratch_shapes=shrink_scratch(tokens, depth) + [dma(())] + small_sems(),
        compiler_params=pltpu.CompilerParams(
            collective_id=collective_id, has_side_effects=True, vmem_limit_bytes=63 * 1024 * 1024
        ),
    )(part.reshape(4, 2, 2, 2, tokens, depth), small, rows, grad_gate, grad_up, act, grads)


def widen_body(*refs):
    half = len(refs) // 2
    for low, wide in zip(refs[:half], refs[half:]):
        wide[...] = low[...].astype(jnp.float32)


def widen_all(*arrays):
    specs = [pl.BlockSpec((1, *array.shape[1:]), lambda e: (e, 0, 0)) for array in arrays]
    return pl.pallas_call(
        widen_body,
        grid=(arrays[0].shape[0],),
        in_specs=specs,
        out_specs=specs,
        out_shape=[jax.ShapeDtypeStruct(array.shape, jnp.float32) for array in arrays],
        compiler_params=pltpu.CompilerParams(vmem_limit_bytes=40 * 1024 * 1024),
    )(*arrays)


def fill_rows(pick_ref, field_ref, rows_ref):
    ranks, groups = pick_ref.shape[0], rows_ref.shape[0]

    @pl.loop(0, ranks // 2, unroll=UNROLL)
    def _(i):
        parts = [
            wide_dot(pick_ref[2 * i + side], field_ref[2 * i + side]).reshape(groups, SLOTS, CHUNK)
            for side in range(2)
        ]
        here = pl.ds(pl.multiple_of(i * 2 * SLOTS, 2 * SLOTS), 2 * SLOTS)
        rows_ref[:, here] = jnp.concatenate(parts, axis=1).astype(jnp.bfloat16)


def add_products(k, rows_ref, pairs):
    groups = rows_ref.shape[0]

    def products(e, first):
        for product, total in pairs:
            term = product(rows_ref[e], e)
            if first:
                total[e] = term
            else:
                total[e] += term

    @pl.when(k == 0)
    def _():
        @pl.loop(0, groups)
        def _(e):
            products(e, True)

    @pl.when(k > 0)
    def _():
        @pl.loop(0, groups)
        def _(e):
            products(e, False)


def grads_in_body(pick_ref, field_ref, down_ref, own_ref, small_ref,
                  rows_ref, plain_ref, all_ref, small_all, total, *sems):
    begin, forward, finish = spread_out(own_ref, all_ref, sems[:11])
    small_begin, small_finish = small_out(small_ref, small_all, sems[11:])
    k, last = pl.program_id(0), pl.num_programs(0) - 1

    @pl.when(k == 0)
    def _():
        meet()
        small_begin()
        begin()

    fill_rows(pick_ref, field_ref, rows_ref)
    add_products(k, rows_ref, [(lambda rows, e: outer_cols(rows, down_ref[e]), total)])

    @pl.when(k % 2 == 1)
    def _():
        forward(k // 2)

    @pl.when(k == last)
    def _():
        pltpu.sync_copy(total, plain_ref)
        finish()
        small_finish()


def grads_in(pick, field, down, own, small, collective_id):
    ranks, width, tokens = pick.shape
    groups, depth = width // SLOTS, field.shape[-1]
    length, inner = ranks * SLOTS, down.shape[1]
    steps = depth // CHUNK
    rows, plain, whole, small_all = pl.pallas_call(
        grads_in_body,
        grid=(steps,),
        in_specs=[
            pl.BlockSpec((ranks, width, tokens), lambda k: (0, 0, 0), pipeline_mode=pl.Buffered(1)),
            pl.BlockSpec((ranks, tokens, CHUNK), lambda k: (0, 0, k)),
            pl.BlockSpec((groups, inner, CHUNK), lambda k: (0, 0, k)),
            ANYWHERE,
            ANYWHERE,
        ],
        out_specs=[pl.BlockSpec((groups, length, CHUNK), lambda k: (0, 0, k))] + [ANYWHERE] * 3,
        out_shape=[
            jax.ShapeDtypeStruct((groups, length, depth), jnp.bfloat16),
            jax.ShapeDtypeStruct((groups, length, inner), jnp.float32),
            jax.ShapeDtypeStruct((4, 2, 2, 2, *own.shape), own.dtype),
            jax.ShapeDtypeStruct((RANKS, *small.shape), small.dtype),
        ],
        scratch_shapes=[pltpu.VMEM((groups, length, inner), jnp.float32)] + spread_sems() + small_sems(),
        compiler_params=pltpu.CompilerParams(
            collective_id=collective_id, has_side_effects=True, vmem_limit_bytes=62 * 1024 * 1024
        ),
    )(pick, field, down, own, small)
    return rows, plain, whole.reshape(RANKS, *own.shape), small_all


def feed_in_body(steps, pick_ref, field_ref, gate_ref, up_ref, plain_ref, probs_ref,
                 rows_ref, act_ref, weighted_ref, grad_gate_ref, grad_up_ref, gates_ref, gate_sum, up_sum):
    k = pl.program_id(0)

    @pl.when(k < steps)
    def _():
        fill_rows(pick_ref, field_ref, rows_ref)
        add_products(
            k,
            rows_ref,
            [
                (lambda rows, e: wide_dot(rows, gate_ref[e]), gate_sum),
                (lambda rows, e: wide_dot(rows, up_ref[e]), up_sum),
            ],
        )

    @pl.when(k >= steps)
    def _():
        e = k - steps
        length = act_ref.shape[1]

        @pl.loop(0, length // 128)
        def _(t):
            here = pl.ds(pl.multiple_of(t * 128, 128), 128)
            gate_val, up_val = gate_sum[e, here], up_sum[e, here]
            plain, probs = plain_ref[0, here], probs_ref[0, here]
            sigmoid_val = jax.nn.sigmoid(gate_val)
            silu_val = gate_val * sigmoid_val
            activated = silu_val * up_val
            grad_act = plain * probs
            grad_up_ref[0, here] = (grad_act * silu_val).astype(jnp.bfloat16)
            grad_gate_ref[0, here] = (
                grad_act * up_val * (sigmoid_val * (1.0 + gate_val * (1.0 - sigmoid_val)))
            ).astype(jnp.bfloat16)
            gates_ref[0, here] = jnp.sum(activated * plain, axis=-1, keepdims=True)
            weighted_ref[0, here] = (activated * probs).astype(jnp.bfloat16)
            act_ref[0, here] = activated.astype(jnp.bfloat16)


def feed_in(pick, field, gate, up, plain, probs):
    ranks, width, tokens = pick.shape
    groups, depth = width // SLOTS, field.shape[-1]
    length, inner = ranks * SLOTS, gate.shape[2]
    steps = depth // CHUNK
    held = lambda k: jnp.minimum(k, steps - 1)
    late = lambda k: (jnp.maximum(k - steps, 0), 0, 0)
    wide = pl.BlockSpec((1, length, inner), late)
    thin = pl.BlockSpec((1, length, 1), late)
    low = jax.ShapeDtypeStruct((groups, length, inner), jnp.bfloat16)
    return pl.pallas_call(
        functools.partial(feed_in_body, steps),
        grid=(steps + groups,),
        in_specs=[
            pl.BlockSpec((ranks, width, tokens), lambda k: (0, 0, 0), pipeline_mode=pl.Buffered(1)),
            pl.BlockSpec((ranks, tokens, CHUNK), lambda k: (0, 0, held(k))),
            pl.BlockSpec((groups, CHUNK, inner), lambda k: (0, held(k), 0)),
            pl.BlockSpec((groups, CHUNK, inner), lambda k: (0, held(k), 0)),
            wide,
            thin,
        ],
        out_specs=[pl.BlockSpec((groups, length, CHUNK), lambda k: (0, 0, held(k))), wide, wide, wide, wide, thin],
        out_shape=[
            jax.ShapeDtypeStruct((groups, length, depth), jnp.bfloat16),
            low, low, low, low,
            jax.ShapeDtypeStruct((groups, length, 1), jnp.float32),
        ],
        scratch_shapes=[pltpu.VMEM((groups, length, inner), jnp.float32)] * 2,
        compiler_params=pltpu.CompilerParams(vmem_limit_bytes=63 * 1024 * 1024),
        cost_estimate=pl.CostEstimate(
            flops=2 * groups * length * depth * (tokens + 2 * inner), bytes_accessed=120 << 20, transcendentals=0
        ),
    )(pick, field, gate, up, plain, probs)


def fill_field(flipped, spread_ref, lefts, weights, field_ref, rows):
    groups = rows.shape[0]
    ranks = spread_ref.shape[0]

    @pl.loop(0, groups)
    def _(e):
        total = None
        for left, weight, flip in zip(lefts, weights, flipped):
            term = outer_cols(left[e], weight[e]) if flip else wide_dot(left[e], weight[e])
            total = term if total is None else total + term
        rows[e] = total

    @pl.loop(0, ranks, unroll=2 * UNROLL)
    def _(s):
        part = rows[:, pl.ds(pl.multiple_of(s * SLOTS, SLOTS), SLOTS)]
        part = part.reshape(groups * SLOTS, CHUNK).astype(jnp.bfloat16)
        field_ref[s] = wide_dot(spread_ref[s], part).astype(jnp.bfloat16)


def restore_body(flipped, spread_ref, *refs):
    count = len(flipped)
    fill_field(flipped, spread_ref, refs[:count], refs[count : 2 * count], *refs[2 * count :])


def restore_specs(spread, lefts, weights, flipped):
    ranks, tokens, width = spread.shape
    groups = width // SLOTS
    length, inner = ranks * SLOTS, lefts[0].shape[2]
    depth = weights[0].shape[1] if flipped[0] else weights[0].shape[2]
    once = pl.Buffered(1)
    in_specs = (
        [pl.BlockSpec((ranks, tokens, width), lambda k: (0, 0, 0), pipeline_mode=once)]
        + [pl.BlockSpec((groups, length, inner), lambda k: (0, 0, 0), pipeline_mode=once)] * len(lefts)
        + [
            pl.BlockSpec((groups, CHUNK, inner), lambda k: (0, k, 0))
            if flip
            else pl.BlockSpec((groups, inner, CHUNK), lambda k: (0, 0, k))
            for flip in flipped
        ]
    )
    out_spec = pl.BlockSpec((ranks, tokens, CHUNK), lambda k: (0, 0, k))
    out_shape = jax.ShapeDtypeStruct((ranks, tokens, depth), jnp.bfloat16)
    return depth // CHUNK, in_specs, out_spec, out_shape, pltpu.VMEM((groups, length, CHUNK), jnp.float32)


def restore(spread, lefts, weights, flipped):
    steps, in_specs, out_spec, out_shape, rows = restore_specs(spread, lefts, weights, flipped)
    field = pl.pallas_call(
        functools.partial(restore_body, flipped),
        grid=(steps,),
        in_specs=in_specs,
        out_specs=out_spec,
        out_shape=out_shape,
        scratch_shapes=[rows],
        compiler_params=pltpu.CompilerParams(vmem_limit_bytes=63 * 1024 * 1024),
    )(spread, *lefts, *weights)
    return field.reshape(-1, field.shape[2])


PARTS = 4


def restore_out_body(spread_ref, left_ref, weight_ref, own_ref, field_ref, all_ref, rows,
                     here_sem, f_send, f_recv, g_send, g_recv, h_send, h_recv):
    r, c, y, x, z, core, first, second = seat()
    pair, along_first, along_second, up = partners()
    y1, x1 = row_of(core, first, 1 - second)
    near_row = y1 * 2 + x1
    step = own_ref.shape[0] // PARTS
    k = pl.program_id(0)
    here = pltpu.make_async_copy(own_ref, all_ref.at[r], here_sem)

    def part(ref, q):
        return ref.at[pl.ds(q * step, step)]

    def f_copy(q):
        return send(part(own_ref, q), part(all_ref.at[r], q), f_send.at[q], f_recv.at[q], along_first)

    def g_copy(q):
        return send(part(own_ref, q), part(all_ref.at[r], q), g_send.at[q], g_recv.at[q], along_second)

    def h_copy(q):
        there = part(all_ref.at[near_row], q)
        return send(there, there, h_send.at[q], h_recv.at[q], along_first)

    @pl.when(k == 0)
    def _():
        meet()
        here.start()
        for q in range(PARTS):
            g_copy(q).start()
            f_copy(q).start()

    fill_field((False,), spread_ref, [left_ref], [weight_ref], field_ref, rows)

    for q in range(PARTS):

        @pl.when(k == q + 1)
        def _():
            g_copy(q).wait_recv()
            h_copy(q).start()

    @pl.when(k == pl.num_programs(0) - 1)
    def _():
        here.wait()
        for q in range(PARTS):
            g_copy(q).wait_send()
            f_copy(q).wait()
            h_copy(q).wait()


def restore_out(spread, left, weight, own, collective_id):
    steps, in_specs, out_spec, out_shape, rows = restore_specs(spread, [left], [weight], (False,))
    dma = pltpu.SemaphoreType.DMA
    field, whole = pl.pallas_call(
        restore_out_body,
        grid=(steps,),
        in_specs=in_specs + [ANYWHERE],
        out_specs=[out_spec, ANYWHERE],
        out_shape=[out_shape, jax.ShapeDtypeStruct((4, *own.shape), own.dtype)],
        scratch_shapes=[rows, dma(())] + [dma((PARTS,))] * 6,
        compiler_params=pltpu.CompilerParams(
            collective_id=collective_id, has_side_effects=True, vmem_limit_bytes=63 * 1024 * 1024
        ),
    )(spread, left, weight, own)
    return field.reshape(-1, field.shape[2]), whole.reshape(-1, own.shape[1])


def branch_body(mixed_ref, weight_ref, out_ref, away, near, first_in, second_in,
                f_send, f_recv, g_send, g_recv):
    r, c, y, x, z, core, first, second = seat()
    pair, along_first, along_second, up = partners()
    tokens, depth = out_ref.shape
    width = depth // PARTS

    def columns(j):
        return pl.ds(j * width, width)

    def product(fir, sec, j):
        yy, xx = row_of(core, fir, sec)
        rows = pl.ds(pl.multiple_of((yy * 2 + xx) * tokens, tokens), tokens)
        return wide_dot(mixed_ref[rows], weight_ref[:, columns(j)])

    def f_copy(sec, j):
        return send(
            away.at[sec, :, columns(j)], first_in.at[sec, :, columns(j)], f_send.at[sec, j], f_recv.at[sec, j], along_first
        )

    def g_copy(j):
        return send(near.at[:, columns(j)], second_in.at[:, columns(j)], g_send.at[j], g_recv.at[j], along_second)

    meet()
    for j in range(PARTS):
        away[1 - second, :, columns(j)] = product(1 - first, 1 - second, j).astype(jnp.bfloat16)
        f_copy(1 - second, j).start()
    for j in range(PARTS):
        away[second, :, columns(j)] = product(1 - first, second, j).astype(jnp.bfloat16)
        f_copy(second, j).start()
    for j in range(PARTS):
        value = product(first, 1 - second, j)
        f_copy(1 - second, j).wait_recv()
        value = value + first_in[1 - second, :, columns(j)].astype(jnp.float32)
        near[:, columns(j)] = value.astype(jnp.bfloat16)
        g_copy(j).start()
    for j in range(PARTS):
        out_ref[:, columns(j)] = product(first, second, j)
    for j in range(PARTS):
        f_copy(second, j).wait_recv()
        g_copy(j).wait_recv()
        out_ref[:, columns(j)] += first_in[second, :, columns(j)].astype(jnp.float32) + second_in[
            :, columns(j)
        ].astype(jnp.float32)
    for j in range(PARTS):
        g_copy(j).wait_send()
        for sec in range(2):
            f_copy(sec, j).wait_send()


def branch_near(mixed, weight, collective_id):
    tokens, depth = mixed.shape[0] // 4, weight.shape[1]
    dma = pltpu.SemaphoreType.DMA
    inside = pl.BlockSpec(memory_space=pltpu.VMEM)
    low = lambda *shape: pltpu.VMEM((*shape, tokens, depth), jnp.bfloat16)
    return pl.pallas_call(
        branch_body,
        in_specs=[inside] * 2,
        out_specs=inside,
        out_shape=jax.ShapeDtypeStruct((tokens, depth), jnp.float32),
        scratch_shapes=[
            low(2), low(), low(2), low(), dma((2, PARTS)), dma((2, PARTS)), dma((PARTS,)), dma((PARTS,))
        ],
        compiler_params=pltpu.CompilerParams(
            collective_id=collective_id, has_side_effects=True, vmem_limit_bytes=40 * 1024 * 1024
        ),
    )(mixed, weight)


def causal_scores(query_rows, key_rows):
    scores = outer_cols(query_rows, key_rows) * HD ** (-0.5)
    count, length = scores.shape
    position = lax.broadcasted_iota(jnp.int32, scores.shape, 0) + (length - count)
    return jnp.where(position >= lax.broadcasted_iota(jnp.int32, scores.shape, 1), scores, MASKED)


def attend_body(q_raw, k_raw, v_ref, q_rs, k_rs, q_gain, k_gain, cos_ref, sin_ref,
                mixed_ref, q_out, k_out, v_out, lse_ref):
    length = v_ref.shape[0]
    block = min(256, length)
    v_out[...] = v_ref[...].astype(jnp.bfloat16)
    for raw, scale, gain, out in ((q_raw, q_rs, q_gain, q_out), (k_raw, k_rs, k_gain, k_out)):
        normed = raw[...] * scale[...] * gain[...]
        turned = normed * cos_ref[...] + pltpu.roll(normed, HD // 2, 1) * sin_ref[...]
        out[...] = turned.astype(jnp.bfloat16)
    for start in range(0, length, block):
        here, seen = pl.ds(start, block), pl.ds(0, start + block)
        scores = causal_scores(q_out[here], k_out[seen])
        row_top = jnp.max(scores, axis=-1, keepdims=True)
        exponent = jnp.exp(scores - row_top)
        row_total = jnp.sum(exponent, axis=-1, keepdims=True)
        weights = (exponent / row_total).astype(jnp.bfloat16)
        mixed_ref[here] = wide_dot(weights, v_out[seen]).astype(jnp.bfloat16)
        lse_ref[0, here] = row_top + jnp.log(row_total)


def three_slabs(length, heads):
    return [pl.BlockSpec((length, HD), lambda h, at=at: (0, at * heads + h)) for at in range(3)]


def attend(raw, q_rs, k_rs, q_gain, k_gain, cosine, sine):
    length, width = raw.shape[0], raw.shape[1] // 3
    heads = width // HD
    slab = pl.BlockSpec((length, HD), lambda h: (0, h))
    thin = pl.BlockSpec((length, 1), lambda h: (0, 0))
    line = pl.BlockSpec((1, HD), lambda h: (0, h))
    table = pl.BlockSpec((length, HD), lambda h: (0, 0))
    low = jax.ShapeDtypeStruct((length, width), jnp.bfloat16)
    return pl.pallas_call(
        attend_body,
        grid=(heads,),
        in_specs=three_slabs(length, heads) + [thin, thin, line, line, table, table],
        out_specs=[slab, slab, slab, slab, pl.BlockSpec((1, length, 1), lambda h: (h, 0, 0))],
        out_shape=[low, low, low, low, jax.ShapeDtypeStruct((heads, length, 1), jnp.float32)],
        cost_estimate=pl.CostEstimate(
            flops=4 * heads * length * length * HD, bytes_accessed=8 << 20, transcendentals=heads * length * length
        ),
    )(raw, raw, raw, q_rs, k_rs, q_gain[None], k_gain[None], cosine, sine)


def attend_back_body(q_ref, k_ref, v_ref, grad_ref, lse_ref, q_raw, k_raw, q_rs, k_rs, q_gain, k_gain, cos_ref, sin_ref,
                     v_grad, q_grad, k_grad, q_term, k_term, q_inner, k_inner, dq, dk, dv):
    length = v_ref.shape[0]
    block = min(256, length)
    dk[...] = jnp.zeros_like(dk)
    dv[...] = jnp.zeros_like(dv)
    for start in range(0, length, block):
        here, seen = pl.ds(start, block), pl.ds(0, start + block)
        query_rows, key_rows, grads = q_ref[here], k_ref[seen], grad_ref[here]
        probs = jnp.exp(causal_scores(query_rows, key_rows) - lse_ref[0, here])
        dv[seen] += inner_rows(probs.astype(jnp.bfloat16), grads)
        weights = outer_cols(grads, v_ref[seen])
        delta = jnp.sum(probs * weights, axis=-1, keepdims=True)
        scores = (probs * (weights - delta)).astype(jnp.bfloat16)
        dq[here] = wide_dot(scores, key_rows) * HD ** (-0.5)
        dk[seen] += inner_rows(scores, query_rows) * HD ** (-0.5)
    v_grad[...] = dv[...].astype(jnp.bfloat16)
    for raw, scale, gain, grad, out, term, inner in (
        (q_raw, q_rs, q_gain, dq, q_grad, q_term, q_inner),
        (k_raw, k_rs, k_gain, dk, k_grad, k_term, k_inner),
    ):
        field, value = raw[...], grad[...]
        normed = value * cos_ref[...] + pltpu.roll(value * sin_ref[...], HD // 2, 1)
        weighted = normed * gain[...]
        out[...] = weighted
        term[...] = jnp.sum(normed * field * scale[...], axis=0, keepdims=True)
        inner[0] = jnp.sum(weighted * field, axis=-1, keepdims=True)


def attend_back(queries, keys, values, grads, lse, raw, q_rs, k_rs, q_gain, k_gain, cosine, sine):
    length, width = raw.shape[0], raw.shape[1] // 3
    heads = width // HD
    slab = pl.BlockSpec((length, HD), lambda h: (0, h))
    thin = pl.BlockSpec((length, 1), lambda h: (0, 0))
    line = pl.BlockSpec((1, HD), lambda h: (0, h))
    table = pl.BlockSpec((length, HD), lambda h: (0, 0))
    column = pl.BlockSpec((1, length, 1), lambda h: (h, 0, 0))
    wide = jax.ShapeDtypeStruct((length, width), jnp.float32)
    return pl.pallas_call(
        attend_back_body,
        grid=(heads,),
        in_specs=[slab] * 4 + [column] + three_slabs(length, heads)[:2] + [thin, thin, line, line, table, table],
        out_specs=[slab, slab, slab, line, line, column, column],
        out_shape=[
            jax.ShapeDtypeStruct((length, width), jnp.bfloat16),
            wide,
            wide,
            jax.ShapeDtypeStruct((1, width), jnp.float32),
            jax.ShapeDtypeStruct((1, width), jnp.float32),
            jax.ShapeDtypeStruct((heads, length, 1), jnp.float32),
            jax.ShapeDtypeStruct((heads, length, 1), jnp.float32),
        ],
        scratch_shapes=[pltpu.VMEM((length, HD), jnp.float32)] * 3,
        cost_estimate=pl.CostEstimate(
            flops=10 * heads * length * length * HD, bytes_accessed=16 << 20, transcendentals=heads * length * length
        ),
    )(queries, keys, values, grads, lse, raw, raw, q_rs, k_rs, q_gain[None], k_gain[None], cosine, sine)


def local(
    layer_input,
    cotangent,
    expert_index,
    attention_gain,
    query_gain,
    key_gain,
    query_weight,
    key_weight,
    value_weight,
    output_weight,
    feed_gain,
    router_weight,
    gate_weight,
    up_weight,
    down_weight,
):
    tokens = layer_input.shape[0]
    rows_count = lax.axis_size("row")
    near = rows_count == 4 and lax.axis_size("col") == 8
    if near:
        head_part = query_gain.shape[0]
        slice_width = attention_gain.shape[0]
        pack = jnp.concatenate(
            [attention_gain, feed_gain, query_gain, key_gain, router_weight.reshape(-1)]
        )
        pack = jnp.pad(pack, (0, PACK_ROWS * 128 - pack.shape[0])).reshape(PACK_ROWS, 128)
        (
            sequence, qkv_full, output_full, pack_all, cotangent_all, index_all
        ) = start_near(
            layer_input,
            [query_weight, key_weight, value_weight, output_weight],
            pack,
            cotangent,
            expert_index.T,
            1,
        )
        index_all = jnp.swapaxes(index_all, 1, 2)
        pack_all = pack_all.reshape(8, -1)
        ends = [slice_width, 2 * slice_width, 2 * slice_width + head_part, 2 * slice_width + 2 * head_part]
        attention_full = pack_all[:, : ends[0]].reshape(-1)
        feed_full = pack_all[:, ends[0] : ends[1]].reshape(-1)
        query_scale_w = pack_all[:, ends[1] : ends[2]].reshape(-1)
        key_scale_w = pack_all[:, ends[2] : ends[3]].reshape(-1)
        router_full = pack_all[:, ends[3] : ends[3] + router_weight.size].reshape(
            -1, router_weight.shape[1]
        )
    else:
        (
            attention_full,
            query_scale_w,
            key_scale_w,
            query_full,
            key_full,
            value_full,
            output_full,
            feed_full,
            router_full,
        ) = (
            lax.all_gather(attention_gain, "col", axis=0, tiled=True),
            lax.all_gather(query_gain, "col", axis=0, tiled=True),
            lax.all_gather(key_gain, "col", axis=0, tiled=True),
            lax.all_gather(query_weight, "col", axis=0, tiled=True),
            lax.all_gather(key_weight, "col", axis=0, tiled=True),
            lax.all_gather(value_weight, "col", axis=0, tiled=True),
            lax.all_gather(output_weight, "col", axis=1, tiled=True),
            lax.all_gather(feed_gain, "col", axis=0, tiled=True),
            lax.all_gather(router_weight, "col", axis=0, tiled=True),
        )
        qkv_full = jnp.concatenate([query_full, key_full, value_full], axis=1)
        sequence = lax.all_gather(layer_input, "row", axis=0, tiled=True)
    length = sequence.shape[0]
    model_width = sequence.shape[1]
    local_width = qkv_full.shape[1] // 3
    seq_float = sequence.astype(jnp.float32)
    seq_scale = rms_scale(seq_float)
    attention_float = attention_full.astype(jnp.float32)
    normed = (seq_float * seq_scale * attention_float).astype(jnp.bfloat16)
    raw = wide_dot(normed, qkv_full)
    query_raw, key_raw = raw[:, :local_width], raw[:, local_width : 2 * local_width]
    query_total, key_total = lax.psum(
        (jnp.sum(query_raw * query_raw, axis=-1), jnp.sum(key_raw * key_raw, axis=-1)), "row"
    )
    query_rs = lax.rsqrt(query_total / model_width + EPS)[:, None]
    key_rs = lax.rsqrt(key_total / model_width + EPS)[:, None]
    query_gain_f = query_scale_w.astype(jnp.float32)
    key_gain_f = key_scale_w.astype(jnp.float32)
    cosine, sine_table = rope_tables(length)
    mixed_heads, queries, keys_rotated, values, lse_all = attend(
        raw, query_rs, key_rs, query_gain_f, key_gain_f, cosine, sine_table
    )
    if near:
        branch = branch_near(mixed_heads, output_full, 5)
    else:
        branch = lax.psum_scatter(
            wide_dot(mixed_heads, output_full).astype(jnp.bfloat16), "row", scatter_dimension=0, tiled=True
        ).astype(jnp.float32)
    hidden = layer_input.astype(jnp.float32) + branch
    feed_scale = rms_scale(hidden)
    feed_float = feed_full.astype(jnp.float32)
    feed_normed = (hidden * feed_scale * feed_float).astype(jnp.bfloat16)
    logits = wide_dot(feed_normed, router_full)
    logit_top = jnp.max(logits, axis=-1, keepdims=True)
    logit_exp = jnp.exp(logits - logit_top)
    router_probs = logit_exp / jnp.sum(logit_exp, axis=-1, keepdims=True)
    experts = router_full.shape[1]
    experts_local = gate_weight.shape[0]
    ranks = lax.axis_size("col") * rows_count
    gate_hits = expert_index[:, :, None] == jnp.arange(experts, dtype=jnp.int32)
    gate_probs = jnp.sum(jnp.where(gate_hits, router_probs[:, None, :], 0.0), axis=-1)

    if not near:
        index_all = lax.all_gather(expert_index, ("col", "row"), axis=0, tiled=True)
    own = (index_all - lax.axis_index("col") * experts_local).reshape(ranks, tokens, -1)
    matches = own[..., None] == jnp.arange(experts_local, dtype=jnp.int32)
    hit = jnp.sum(matches.astype(jnp.float32), axis=2)
    earlier = jnp.tril(jnp.ones((tokens, tokens), jnp.bfloat16), -1)
    rank = jnp.einsum(
        "tu,sue->ste", earlier, hit.astype(jnp.bfloat16), preferred_element_type=jnp.float32
    )
    slot = jnp.where(hit > 0, rank, -1.0)
    places = jnp.arange(SLOTS, dtype=jnp.float32)
    slot_t = jnp.swapaxes(slot, 1, 2)
    width = experts_local * SLOTS
    picked = slot_t[:, :, None, :] == places[None, None, :, None]
    pick = picked.astype(jnp.bfloat16).reshape(ranks, width, tokens)
    lanes = jnp.arange(width, dtype=jnp.int32)
    widen = (lanes[None, :] // SLOTS == jnp.arange(experts_local)[:, None]).astype(jnp.bfloat16)
    spread = jnp.einsum(
        "ste,ew->stw", slot.astype(jnp.bfloat16), widen, preferred_element_type=jnp.float32
    ) == (lanes % SLOTS).astype(jnp.float32)
    spread_plain = spread.astype(jnp.bfloat16)

    def weigh(probs_all):
        probs_own = jnp.sum(
            jnp.where(matches, probs_all.reshape(ranks, tokens, -1, 1), 0.0), axis=2
        )
        probs_wide = jnp.einsum(
            "ste,ew->stw", probs_own.astype(jnp.bfloat16), widen, preferred_element_type=jnp.float32
        )
        spread_probs = jnp.where(spread, probs_wide, 0.0).astype(jnp.bfloat16)
        probs_t = jnp.swapaxes(probs_own, 1, 2)
        row_probs = jnp.sum(jnp.where(picked, probs_t[:, :, None, :], 0.0), axis=-1)
        row_probs = jnp.swapaxes(row_probs, 0, 1).reshape(experts_local, ranks * SLOTS, 1)
        return spread_probs, row_probs

    if near:
        expert_grads, plain_act, feed_all, probs_all = grads_in(
            pick, cotangent_all, down_weight, feed_normed, gate_probs.T, 2
        )
        spread_probs, row_probs = weigh(jnp.swapaxes(probs_all, 1, 2))
        expert_rows, activated, weighted_act, grad_gate, grad_up, row_gates = feed_in(
            pick, feed_all, gate_weight, up_weight, plain_act, row_probs
        )
    else:
        probs_all = lax.all_gather(gate_probs, ("col", "row"), axis=0, tiled=True)
        spread_probs, row_probs = weigh(probs_all)
        expert_grads = gather_rows(pick, cotangent)
        expert_rows = gather_rows(pick, feed_normed)
        gate_val = jnp.einsum(
            "erd,edf->erf", expert_rows, gate_weight, preferred_element_type=jnp.float32
        )
        up_val = jnp.einsum(
            "erd,edf->erf", expert_rows, up_weight, preferred_element_type=jnp.float32
        )
        plain_act = jnp.einsum(
            "erd,efd->erf", expert_grads, down_weight, preferred_element_type=jnp.float32
        )
        sigmoid_val = jax.nn.sigmoid(gate_val)
        silu_val = gate_val * sigmoid_val
        activated = silu_val * up_val
        grad_act = plain_act * row_probs
        grad_up = (grad_act * silu_val).astype(jnp.bfloat16)
        grad_gate = (
            grad_act * up_val * sigmoid_val * (1.0 + gate_val * (1.0 - sigmoid_val))
        ).astype(jnp.bfloat16)
        row_gates = jnp.sum(activated * plain_act, axis=-1)
        weighted_act = (activated * row_probs).astype(jnp.bfloat16)
        activated = activated.astype(jnp.bfloat16)
    row_gates = jnp.swapaxes(row_gates.reshape(experts_local, ranks, SLOTS), 0, 1)
    own_gates = jnp.sum(jnp.where(picked, row_gates[..., None], 0.0), axis=2)
    if near:
        grad_feed_part = restore(
            spread_plain, [grad_gate, grad_up], [gate_weight, up_weight], (True, True)
        )
        grad_feed, gates_in, grad_gate_weight, grad_up_weight, grad_down_weight = feed_back(
            grad_feed_part, own_gates, expert_rows, grad_gate, grad_up, weighted_act, expert_grads, 3
        )
        grad_gate_weight, grad_up_weight, grad_down_weight = widen_all(
            grad_gate_weight, grad_up_weight, grad_down_weight
        )
        gates_in = jnp.sum(gates_in.reshape(-1, rows_count, experts_local, tokens), axis=1)
        grad_probs = gates_in.reshape(experts, tokens).T
    else:
        own_gates = lax.psum_scatter(
            jnp.swapaxes(own_gates, 1, 2).reshape(-1, rows_count, tokens, experts_local),
            "row",
            scatter_dimension=1,
        )
        grad_probs = lax.all_to_all(own_gates, "col", split_axis=0, concat_axis=2, tiled=True)[0]
        back_rows = (
            jnp.einsum("erf,edf->erd", grad_gate, gate_weight, preferred_element_type=jnp.float32)
            + jnp.einsum("erf,edf->erd", grad_up, up_weight, preferred_element_type=jnp.float32)
        ).astype(jnp.bfloat16)
        grad_feed = return_rows(spread_plain, back_rows).astype(jnp.float32)
        out_rows = jnp.einsum(
            "erf,efd->erd", activated, down_weight, preferred_element_type=jnp.float32
        ).astype(jnp.bfloat16)
        mixture = return_rows(spread_probs, out_rows).astype(jnp.float32)
        grad_gate_weight = jnp.einsum(
            "erd,erf->edf", expert_rows, grad_gate, preferred_element_type=jnp.float32
        )
        grad_up_weight = jnp.einsum(
            "erd,erf->edf", expert_rows, grad_up, preferred_element_type=jnp.float32
        )
        grad_down_weight = jnp.einsum(
            "erf,erd->efd", weighted_act, expert_grads, preferred_element_type=jnp.float32
        )
    grad_out = cotangent.astype(jnp.float32)
    grad_logits = (
        router_probs * (grad_probs - jnp.sum(router_probs * grad_probs, axis=-1, keepdims=True))
    ).astype(jnp.bfloat16)
    router_grad = inner_rows(feed_normed, grad_logits)
    grad_feed = grad_feed + outer_cols(grad_logits, router_full)
    feed_gain_term = jnp.sum(grad_feed * hidden * feed_scale, axis=0)
    feed_weighted = grad_feed * feed_float
    grad_hidden = (
        grad_out
        + feed_scale * feed_weighted
        - hidden * feed_scale**3 * jnp.mean(feed_weighted * hidden, axis=-1, keepdims=True)
    )
    if near:
        mixture_part, grad_branch = restore_out(
            spread_probs, activated, down_weight, grad_hidden.astype(jnp.bfloat16), 6
        )
    else:
        grad_branch = lax.all_gather(grad_hidden.astype(jnp.bfloat16), "row", axis=0, tiled=True)
    output_grad = inner_rows(mixed_heads, grad_branch)
    grad_mixed = outer_cols(grad_branch, output_full).astype(jnp.bfloat16)
    (
        grad_value_low, query_weighted, key_weighted, query_gain_term, key_gain_term, query_inner, key_inner
    ) = attend_back(
        queries, keys_rotated, values, grad_mixed, lse_all, raw, query_rs, key_rs,
        query_gain_f, key_gain_f, cosine, sine_table,
    )
    query_gain_term, key_gain_term = query_gain_term.reshape(-1), key_gain_term.reshape(-1)
    query_inner, key_inner = (
        lax.psum(jnp.sum(query_inner, axis=(0, 2)), "row"),
        lax.psum(jnp.sum(key_inner, axis=(0, 2)), "row"),
    )
    grad_query_raw = (
        query_rs * query_weighted - query_raw * query_rs**3 * (query_inner / model_width)[:, None]
    ).astype(jnp.bfloat16)
    grad_key_raw = (
        key_rs * key_weighted - key_raw * key_rs**3 * (key_inner / model_width)[:, None]
    ).astype(jnp.bfloat16)
    raw_grads = jnp.concatenate([grad_query_raw, grad_key_raw, grad_value_low], axis=1)
    qkv_grad = inner_rows(normed, raw_grads)
    grad_normed = outer_cols(raw_grads, qkv_full)
    attention_weighted = grad_normed * attention_float
    grad_seq_part = seq_scale * attention_weighted - seq_float * seq_scale**3 * jnp.mean(
        attention_weighted * seq_float, axis=-1, keepdims=True
    )
    attention_gain_term = jnp.sum(grad_normed * seq_float * seq_scale, axis=0)
    if near:
        cols = lax.axis_size("col")
        pack = jnp.concatenate(
            [
                attention_gain_term.reshape(cols, -1),
                feed_gain_term.reshape(cols, -1),
                query_gain_term.reshape(cols, -1),
                key_gain_term.reshape(cols, -1),
                router_grad.reshape(cols, -1),
            ],
            axis=1,
        )
        pack = jnp.pad(pack, ((0, 0), (0, PACK_ROWS * 128 - pack.shape[1])))
        pack = pack.astype(jnp.bfloat16).reshape(cols, PACK_ROWS, 128)
        (
            mixture, summed, grad_query_weight, grad_key_weight, grad_value_weight, grad_output_weight, packs
        ) = finish_near(
            mixture_part,
            grad_seq_part.astype(jnp.bfloat16).reshape(rows_count, tokens, model_width),
            [grad.astype(jnp.bfloat16) for grad in (qkv_grad, output_grad)],
            pack,
            4,
        )
        input_grad = grad_hidden + summed
        packs = packs.reshape(cols, rows_count, -1).astype(jnp.float32)
        whole = jnp.sum(packs, axis=(0, 1))
        heads_sum = jnp.sum(
            lax.dynamic_index_in_dim(packs, lax.axis_index("row"), 1, keepdims=False), axis=0
        )
        grad_attention_gain = whole[: ends[0]]
        grad_feed_gain = whole[ends[0] : ends[1]]
        grad_query_gain = heads_sum[ends[1] : ends[2]]
        grad_key_gain = heads_sum[ends[2] : ends[3]]
        grad_router_weight = whole[ends[3] : ends[3] + router_weight.size].reshape(router_weight.shape)
    else:
        stacked = jnp.concatenate(
            [
                grad_seq_part.reshape(rows_count, tokens, model_width),
                jnp.broadcast_to(attention_gain_term[None, None, :], (rows_count, 1, model_width)),
            ],
            axis=1,
        ).reshape(rows_count * (tokens + 1), model_width)
        summed = lax.psum_scatter(
            stacked.astype(jnp.bfloat16), "row", scatter_dimension=0, tiled=True
        ).astype(jnp.float32)
        input_grad = grad_hidden + summed[:tokens]
        attention_gain_total = summed[tokens]
        query_grad, key_grad, value_grad = jnp.split(qkv_grad, 3, axis=1)
        feed_gain_total, router_total = (
            lax.psum(feed_gain_term.astype(jnp.bfloat16), "row").astype(jnp.float32),
            lax.psum(router_grad.astype(jnp.bfloat16), "row").astype(jnp.float32),
        )
        (
            grad_attention_gain,
            grad_query_gain,
            grad_key_gain,
            grad_query_weight,
            grad_key_weight,
            grad_value_weight,
            grad_output_weight,
            grad_feed_gain,
            grad_router_weight,
        ) = (
            lax.psum_scatter(
                attention_gain_total.astype(jnp.bfloat16), "col", scatter_dimension=0, tiled=True
            ).astype(jnp.float32),
            lax.psum_scatter(
                query_gain_term.astype(jnp.bfloat16), "col", scatter_dimension=0, tiled=True
            ).astype(jnp.float32),
            lax.psum_scatter(
                key_gain_term.astype(jnp.bfloat16), "col", scatter_dimension=0, tiled=True
            ).astype(jnp.float32),
            lax.psum_scatter(
                query_grad.astype(jnp.bfloat16), "col", scatter_dimension=0, tiled=True
            ).astype(jnp.float32),
            lax.psum_scatter(
                key_grad.astype(jnp.bfloat16), "col", scatter_dimension=0, tiled=True
            ).astype(jnp.float32),
            lax.psum_scatter(
                value_grad.astype(jnp.bfloat16), "col", scatter_dimension=0, tiled=True
            ).astype(jnp.float32),
            lax.psum_scatter(
                output_grad.astype(jnp.bfloat16), "col", scatter_dimension=1, tiled=True
            ).astype(jnp.float32),
            lax.psum_scatter(
                feed_gain_total.astype(jnp.bfloat16), "col", scatter_dimension=0, tiled=True
            ).astype(jnp.float32),
            lax.psum_scatter(
                router_total.astype(jnp.bfloat16), "col", scatter_dimension=0, tiled=True
            ).astype(jnp.float32),
        )
    layer_output = hidden + mixture
    return (
        layer_output,
        input_grad,
        grad_attention_gain,
        grad_query_gain,
        grad_key_gain,
        grad_query_weight,
        grad_key_weight,
        grad_value_weight,
        grad_output_weight,
        grad_feed_gain,
        grad_router_weight,
        grad_gate_weight,
        grad_up_weight,
        grad_down_weight,
    )


def solution(mesh):
    placed = (
        P(("col", "row"), None),
        P(("col", "row"), None),
        P(("col", "row"), None),
        P("col"),
        P(("row", "col")),
        P(("row", "col")),
        P("col", "row"),
        P("col", "row"),
        P("col", "row"),
        P("row", "col"),
        P("col"),
        P("col", None),
        P("col", None, "row"),
        P("col", None, "row"),
        P("col", "row", None),
    )
    return jax.shard_map(
        local,
        mesh=mesh,
        in_specs=placed,
        out_specs=(
            P(("col", "row"), None),
            P(("col", "row"), None),
            P("col"),
            P(("row", "col")),
            P(("row", "col")),
            P("col", "row"),
            P("col", "row"),
            P("col", "row"),
            P("row", "col"),
            P("col"),
            P("col", None),
            P("col", None, "row"),
            P("col", None, "row"),
            P("col", "row", None),
        ),
        check_vma=False,
    )
```

```python
import functools

import jax
import jax.numpy as jnp
from jax import lax
from jax.experimental import pallas as pl
from jax.experimental.pallas import tpu as pltpu
from jax.sharding import PartitionSpec as P

HD = 128
SLOTS = 40
BLOCK = 512
CHUNK = 256
UNROLL = 4
PACK_ROWS = 144


EPS = 1e-05
THETA = 10000.0
MASKED = -1e30


def wide_dot(left, right):
    return jnp.dot(left, right, preferred_element_type=jnp.float32)


def inner_rows(left, right):
    return lax.dot_general(
        left, right, (((0,), (0,)), ((), ())), preferred_element_type=jnp.float32
    )


def outer_cols(left, right):
    return lax.dot_general(
        left, right, (((1,), (1,)), ((), ())), preferred_element_type=jnp.float32
    )


def rms_scale(field):
    return lax.rsqrt(jnp.mean(field * field, axis=-1, keepdims=True) + EPS)


def rope_tables(length):
    half_size = HD // 2
    freqs = THETA ** (-(jnp.arange(half_size, dtype=jnp.float32) * 2.0) / HD)
    angles = jnp.arange(length, dtype=jnp.float32)[:, None] * freqs[None, :]
    cosine = jnp.concatenate([jnp.cos(angles), jnp.cos(angles)], axis=-1)
    sine_table = jnp.concatenate([-jnp.sin(angles), jnp.sin(angles)], axis=-1)
    return (cosine, sine_table)


def dispatch_body(pick_ref, field_ref, rows_ref):
    groups = rows_ref.shape[0]
    first = wide_dot(pick_ref[0], field_ref[0]).reshape(groups, SLOTS, -1)
    second = wide_dot(pick_ref[1], field_ref[1]).reshape(groups, SLOTS, -1)
    rows_ref[...] = jnp.concatenate([first, second], axis=1).astype(jnp.bfloat16)


def dispatch(pick, field):
    ranks, width, tokens = pick.shape
    groups, depth = width // SLOTS, field.shape[1]
    return pl.pallas_call(
        dispatch_body,
        grid=(ranks // 2, depth // BLOCK),
        in_specs=[
            pl.BlockSpec((2, width, tokens), lambda i, k: (i, 0, 0)),
            pl.BlockSpec((2, tokens, BLOCK), lambda i, k: (i, 0, k)),
        ],
        out_specs=pl.BlockSpec((groups, 2 * SLOTS, BLOCK), lambda i, k: (0, i, k)),
        out_shape=jax.ShapeDtypeStruct((groups, ranks * SLOTS, depth), jnp.bfloat16),
    )(pick, field.reshape(ranks, tokens, depth))


def combine_body(spread_ref, rows_ref, field_ref):
    rows = rows_ref[...].astype(jnp.float32)
    width = rows.shape[0] * SLOTS
    for side in range(2):
        part = rows[:, side * SLOTS : (side + 1) * SLOTS].reshape(width, -1).astype(jnp.bfloat16)
        field_ref[side] = wide_dot(spread_ref[side], part).astype(jnp.bfloat16)


def combine(spread, rows):
    ranks, tokens, width = spread.shape
    groups, depth = width // SLOTS, rows.shape[2]
    field = pl.pallas_call(
        combine_body,
        grid=(ranks // 2, depth // BLOCK),
        in_specs=[
            pl.BlockSpec((2, tokens, width), lambda i, k: (i, 0, 0)),
            pl.BlockSpec((groups, 2 * SLOTS, BLOCK), lambda i, k: (0, i, k)),
        ],
        out_specs=pl.BlockSpec((2, tokens, BLOCK), lambda i, k: (i, 0, k)),
        out_shape=jax.ShapeDtypeStruct((ranks, tokens, depth), jnp.bfloat16),
    )(spread, rows)
    return field.reshape(ranks * tokens, depth)


def scatter_all(field):
    part = lax.psum_scatter(field, "col", scatter_dimension=0, tiled=True)
    return lax.psum_scatter(part, "row", scatter_dimension=0, tiled=True)


def pieces_of(ranks, depth):
    count = max(1, ranks // 32)
    step = depth // count
    return [(at, at + step) for at in range(0, depth, step)]


def gather_rows(pick, field):
    rows = []
    for start, stop in pieces_of(pick.shape[0], field.shape[1]):
        part = field[:, start:stop]
        if rows:
            part = lax.optimization_barrier((part, rows[-1]))[0]
        whole = lax.all_gather(part, ("col", "row"), axis=0, tiled=True)
        rows.append(dispatch(pick, whole))
    return rows[0] if len(rows) == 1 else jnp.concatenate(rows, axis=2)


def return_rows(spread, rows):
    sums = []
    for start, stop in pieces_of(spread.shape[0], rows.shape[2]):
        part = rows[:, :, start:stop]
        if sums:
            part = lax.optimization_barrier((part, sums[-1]))[0]
        sums.append(scatter_all(combine(spread, part)))
    return sums[0] if len(sums) == 1 else jnp.concatenate(sums, axis=1)


MESH = pl.DeviceIdType.MESH


def seat():
    r, c = lax.axis_index("row"), lax.axis_index("col")
    y, x = r // 2, r % 2
    z, core = c // 2, c % 2
    first = y * (1 - core) + x * core
    second = x * (1 - core) + y * core
    return r, c, y, x, z, core, first, second


def partners():
    r, c, y, x, z, core, first, second = seat()
    pair = (r, z * 2 + (1 - core))
    flip_y = (1 - y) * 2 + x
    flip_x = y * 2 + (1 - x)
    along_first = (flip_y * (1 - core) + flip_x * core, c)
    along_second = (flip_x * (1 - core) + flip_y * core, c)
    up = [(r, ((z + k) % 4) * 2 + core) for k in range(1, 4)]
    return pair, along_first, along_second, up


RANKS = 32


def nth(offset):
    spot = (lax.axis_index("col") * 4 + lax.axis_index("row") + offset) % RANKS
    return spot, (spot % 4, spot // 4)


def meet():
    barrier = pltpu.get_barrier_semaphore()

    @pl.loop(1, RANKS)
    def _(offset):
        pl.semaphore_signal(barrier, inc=1, device_id=nth(offset)[1], device_id_type=MESH)

    pl.semaphore_wait(barrier, RANKS - 1)


def small_copy(src_of, small_all, small_send, small_recv, offset):
    spot, device = nth(offset)
    return send(
        src_of(spot), small_all.at[nth(0)[0]], small_send.at[offset], small_recv.at[offset], device
    )


def row_of(core, first, second):
    y = first * (1 - core) + second * core
    x = second * (1 - core) + first * core
    return y, x


def send(src, dst, send_sem, recv_sem, device):
    return pltpu.make_async_remote_copy(
        src_ref=src, dst_ref=dst, send_sem=send_sem, recv_sem=recv_sem, device_id=device, device_id_type=MESH
    )


GSTEPS = 4
QUEUE = (2, 1, 3)
ARRIVE = (1, 3, 2)


def spread_out(own_ref, all_ref, sems):
    r, c, y, x, z, core, first, second = seat()
    pair, along_first, along_second, up = partners()
    here_sem, u_send, u_recv, d_send, d_recv, g_send, g_recv, f_send, f_recv, p_send, p_recv = sems
    step = own_ref.shape[0] // GSTEPS

    def rows(q):
        return pl.ds(pl.multiple_of(q * step, step), step)

    def place(k, s, f, q):
        sec = second * (1 - s) + (1 - second) * s
        fir = first * (1 - f) + (1 - first) * f
        yy, xx = row_of(core, fir, sec)
        return all_ref.at[(z + 4 - k) % 4, core, yy, xx, rows(q)]

    above, below = (r, ((z + 1) % 4) * 2 + core), (r, ((z + 3) % 4) * 2 + core)

    def source(k, q):
        return own_ref.at[rows(q)] if k == 0 else place(k, 0, 0, q)

    def up_copy(d, q):
        return send(source(d, q), place(d, 0, 0, q), u_send.at[d, q], u_recv.at[d, q], above)

    def down_copy(d, q):
        k = (4 - d) % 4
        return send(source(k, q), place(k, 0, 0, q), d_send.at[d, q], d_recv.at[d, q], below)

    def came_up(d, q):
        there = place(d, 0, 0, q)
        return send(there, there, u_send.at[d - 1, q], u_recv.at[d - 1, q], above)

    def came_down(d, q):
        there = place(4 - d, 0, 0, q)
        return send(there, there, d_send.at[d - 1, q], d_recv.at[d - 1, q], below)

    bottom, top = 1 - jnp.minimum(z, 1), z // 3
    arrived = [bottom * (3 - i) + top * (1 + i) + (1 - bottom - top) * ARRIVE[i] for i in range(3)]

    def g_copy(k, q, src):
        return send(src, place(k, 0, 0, q), g_send.at[k, q], g_recv.at[k, q], along_second)

    def f_copy(k, s, q, src):
        return send(src, place(k, s, 0, q), f_send.at[s, k, q], f_recv.at[s, k, q], along_first)

    def p_copy(k, s, f, q, src):
        return send(src, place(k, s, f, q), p_send.at[f, s, k, q], p_recv.at[f, s, k, q], pair)

    here = pltpu.make_async_copy(own_ref, all_ref.at[z, core, y, x], here_sem)

    def begin():
        here.start()

        @pl.loop(0, GSTEPS)
        def _(q):
            src = own_ref.at[rows(q)]

            @pl.when(z < 3)
            def _():
                up_copy(0, q).start()

            @pl.when(z > 0)
            def _():
                down_copy(0, q).start()

            g_copy(0, q, src).start()
            f_copy(0, 0, q, src).start()
            p_copy(0, 0, 0, q, src).start()

    def along_z(q):
        def pass_on(k):
            src = place(k, 0, 0, q)
            g_copy(k, q, src).start()
            f_copy(k, 0, q, src).start()
            p_copy(k, 0, 0, q, src).start()

        for d in (1, 2, 3):

            @pl.when(z >= d)
            def _():
                came_up(d, q).wait_recv()
                if d < 3:

                    @pl.when(z < 3)
                    def _():
                        up_copy(d, q).start()

                pass_on(d)

            @pl.when(z + d <= 3)
            def _():
                came_down(d, q).wait_recv()
                if d < 3:

                    @pl.when(z > 0)
                    def _():
                        down_copy(d, q).start()

                pass_on(4 - d)

    def forward(q, between=None):
        @pl.when(q == 0)
        def _():
            along_z(q)

        @pl.when(q + 1 < GSTEPS)
        def _():
            along_z(q + 1)

        if between is not None:
            between()

        for k in (0, *arrived):
            src = place(k, 1, 0, q)
            g_copy(k, q, src).wait_recv()
            f_copy(k, 1, q, src).start()
            p_copy(k, 1, 0, q, src).start()
        for k in (0, *arrived):
            src = place(k, 0, 1, q)
            f_copy(k, 0, q, src).wait_recv()
            p_copy(k, 0, 1, q, src).start()

    def finish():
        @pl.loop(0, GSTEPS)
        def _(q):
            for k in (0, *arrived):
                src = place(k, 1, 1, q)
                f_copy(k, 1, q, src).wait_recv()
                p_copy(k, 1, 1, q, src).start()

        here.wait()

        @pl.loop(0, GSTEPS)
        def _(q):
            for d in range(3):

                @pl.when((z < 3) & (z >= d))
                def _():
                    up_copy(d, q).wait_send()

                @pl.when((z > 0) & (z + d <= 3))
                def _():
                    down_copy(d, q).wait_send()

            for k in range(4):
                src = own_ref.at[rows(q)]
                g_copy(k, q, src).wait_send()
                for s in range(2):
                    f_copy(k, s, q, src).wait_send()
                    for f in range(2):
                        p_copy(k, s, f, q, src).wait()

    return begin, forward, finish


def spread_sems():
    dma = pltpu.SemaphoreType.DMA
    shapes = [(3, GSTEPS), (3, GSTEPS), (4, GSTEPS), (2, 4, GSTEPS), (2, 2, 4, GSTEPS)]
    return [dma(())] + [dma(shape) for shape in shapes for _ in range(2)]


def small_out(small_ref, small_all, sems):
    here_sem, small_send, small_recv = sems
    local = pltpu.make_async_copy(small_ref, small_all.at[nth(0)[0]], here_sem)

    def copy(offset):
        return small_copy(lambda spot: small_ref, small_all, small_send, small_recv, offset)

    def begin():
        local.start()

        @pl.loop(1, RANKS)
        def _(offset):
            copy(offset).start()

    def finish():
        local.wait()

        @pl.loop(1, RANKS)
        def _(offset):
            copy(offset).wait()

    return begin, finish


def small_sems():
    dma = pltpu.SemaphoreType.DMA
    return [dma(()), dma((RANKS,)), dma((RANKS,))]


ANYWHERE = pl.BlockSpec(memory_space=pl.ANY)


def start_body(x_ref, q_ref, k_ref, v_ref, o_ref, pack_ref, own_ref, small_ref,
               x_all, qkv_all, o_all, pack_all, all_ref, small_all, *sems):
    r, c, y, x, z, core, first, second = seat()
    pair, along_first, along_second, up = partners()
    begin, forward, finish = spread_out(own_ref, all_ref, sems[:11])
    small_begin, small_finish = small_out(small_ref, small_all, sems[11:14])
    here_sem, x_send, x_recv, w_send, w_recv, v_send, v_recv = sems[14:]
    weights = [(q_ref, qkv_all), (k_ref, qkv_all), (v_ref, qkv_all), (o_ref, o_all), (pack_ref, pack_all)]

    def block(index, col):
        ref, whole = weights[index]
        if index == 4:
            return whole.at[col]
        if index == 3:
            width = ref.shape[1]
            return whole.at[:, pl.ds(pl.multiple_of(col * width, width), width)]
        height, width = ref.shape
        return whole.at[pl.ds(pl.multiple_of(col * height, height), height), pl.ds(index * width, width)]

    def w_copy(index, k):
        return send(
            weights[index][0], block(index, c), w_send.at[index, k - 1], w_recv.at[index, k - 1], up[k - 1]
        )

    def pair_copy(index, k):
        col = ((z + 4 - k) % 4) * 2 + core
        src = weights[index][0] if k == 0 else block(index, col)
        return send(src, block(index, col), v_send.at[index, k], v_recv.at[index, k], pair)

    locals_ = [pltpu.make_async_copy(x_ref, x_all.at[r], here_sem.at[5])] + [
        pltpu.make_async_copy(weights[i][0], block(i, c), here_sem.at[i]) for i in range(5)
    ]
    y1, x1 = row_of(core, first, 1 - second)
    near_row = y1 * 2 + x1
    x_first = send(x_ref, x_all.at[r], x_send.at[0], x_recv.at[0], along_first)
    x_second = send(x_ref, x_all.at[r], x_send.at[1], x_recv.at[1], along_second)
    x_relay = send(x_all.at[near_row], x_all.at[near_row], x_send.at[2], x_recv.at[2], along_first)

    meet()
    small_begin()
    x_second.start()
    x_first.start()
    begin()
    for item in locals_:
        item.start()
    x_second.wait_recv()
    x_relay.start()
    def weights_out(group):
        for index in group:
            for k in QUEUE:
                w_copy(index, k).start()
            pair_copy(index, 0).start()

    for q, group in enumerate(((4, 0), (1, 2), (3,), ())):
        forward(q, functools.partial(weights_out, group))

    for index in (4, 0, 1, 2, 3):
        for k in ARRIVE:
            w_copy(index, k).wait_recv()
            pair_copy(index, k).start()
    finish()
    small_finish()
    for item in locals_:
        item.wait()
    x_first.wait()
    x_second.wait_send()
    x_relay.wait()
    for index in range(5):
        for k in range(4):
            if k:
                w_copy(index, k).wait_send()
            pair_copy(index, k).wait()


def start_near(x, weights, pack, own, small, collective_id):
    tokens, depth = own.shape
    dma = pltpu.SemaphoreType.DMA
    height, width = weights[0].shape
    shaped = lambda shape, like: jax.ShapeDtypeStruct(shape, like.dtype)
    outs = pl.pallas_call(
        start_body,
        out_shape=(
            shaped((4, *x.shape), x),
            shaped((8 * height, 3 * width), weights[0]),
            shaped((weights[3].shape[0], 8 * weights[3].shape[1]), weights[3]),
            shaped((8, *pack.shape), pack),
            shaped((4, 2, 2, 2, tokens, depth), own),
            shaped((RANKS, *small.shape), small),
        ),
        in_specs=[ANYWHERE] * 8,
        out_specs=[ANYWHERE] * 6,
        scratch_shapes=spread_sems()
        + small_sems()
        + [dma((6,)), dma((3,)), dma((3,)), dma((5, 3)), dma((5, 3)), dma((5, 4)), dma((5, 4))],
        compiler_params=pltpu.CompilerParams(collective_id=collective_id, has_side_effects=True),
    )(x, *weights, pack, own, small)
    x_all, qkv, o, pack_all, whole, small_all = outs
    return x_all.reshape(-1, x.shape[1]), qkv, o, pack_all, whole.reshape(RANKS, tokens, depth), small_all


def finish_body(part_ref, field_ref, qkv_ref, o_ref, pack_ref,
                mixture_ref, out_ref, q_out, k_out, v_out, o_out, pack_all,
                mine, first_in, second_in, total,
                qkv_mine, o_mine, qkv_pair, o_pair, qkv_z, o_z, qkv_sum, o_sum,
                load_sem, f_send, f_recv, g_send, g_recv, w_load, p_send, p_recv, z_send, z_recv, out_sem,
                *rest):
    r, c, y, x, z, core, first, second = seat()
    pair, along_first, along_second, up = partners()
    small_begin, small_finish = small_each(pack_ref, pack_all, rest[:3], lambda spot: spot // 4)
    begin, tick, finish = shrink(part_ref, *rest[3:9], rest[9:18])
    mixture = rest[8]
    tokens, depth = out_ref.shape
    other = 1 - core
    grads, kept, pairs = [qkv_ref, o_ref], [qkv_mine, o_mine], [qkv_pair, o_pair]
    zs, sums = [qkv_z, o_z], [qkv_sum, o_sum]
    width = q_out.shape[1]
    results = [
        [
            pltpu.make_async_copy(qkv_sum.at[:, pl.ds(i * width, width)], out, out_sem.at[i])
            for i, out in enumerate((q_out, k_out, v_out))
        ],
        [pltpu.make_async_copy(o_sum, o_out, out_sem.at[3])],
    ]

    def block(index, col):
        ref = grads[index]
        if index == 1:
            width = ref.shape[1] // 8
            return ref.at[:, pl.ds(pl.multiple_of(col * width, width), width)]
        height = ref.shape[0] // 8
        return ref.at[pl.ds(pl.multiple_of(col * height, height), height)]

    def row(fir, sec):
        yy, xx = row_of(core, fir, sec)
        return yy * 2 + xx

    def load(fir, sec):
        return pltpu.make_async_copy(field_ref.at[row(fir, sec)], mine.at[fir, sec], load_sem.at[fir, sec])

    def f_copy(sec):
        return send(field_ref.at[row(1 - first, sec)], first_in.at[sec], f_send.at[sec], f_recv.at[sec], along_first)

    g_copy = send(mine.at[first, 1 - second], second_in, g_send, g_recv, along_second)

    def w_load_copy(index, zz):
        return pltpu.make_async_copy(block(index, zz * 2 + core), kept[index].at[zz], w_load.at[index, zz])

    def w_give(index, zz):
        return send(
            block(index, zz * 2 + other), pairs[index].at[zz], p_send.at[index, zz], p_recv.at[index, zz], pair
        )

    above, below = (r, ((z + 1) % 4) * 2 + core), (r, ((z + 3) % 4) * 2 + core)

    def up_copy(index, dest):
        return send(
            kept[index].at[dest], zs[index].at[dest], z_send.at[index, dest], z_recv.at[index, dest], above
        )

    def down_copy(index, dest, slot):
        return send(kept[index].at[dest], zs[index].at[slot], z_send.at[index, dest], z_recv.at[index, slot], below)

    def chain(stage):
        @pl.when(z == stage)
        def _():
            for index in range(2):
                for dest in range(3, stage, -1):
                    if stage > 0:
                        up_copy(index, dest).wait_recv()
                        add(kept[index].at[dest], [zs[index].at[dest]])
                    up_copy(index, dest).start()

        @pl.when(z == 3 - stage)
        def _():
            for index in range(2):
                for dest in range(3 - stage):
                    if stage > 0:
                        down_copy(index, dest, dest).wait_recv()
                        add(kept[index].at[dest], [zs[index].at[dest]])
                    down_copy(index, dest, 4 if dest == 2 - stage else dest).start()

    def add(ref, extras):
        @pl.loop(0, ref.shape[0] // TILE)
        def _(t):
            here = pl.ds(pl.multiple_of(t * TILE, TILE), TILE)
            value = ref[here].astype(jnp.float32)
            for extra in extras:
                value = value + extra[here].astype(jnp.float32)
            ref[here] = value.astype(jnp.bfloat16)

    def add_out(ref, extras, result):
        @pl.loop(0, ref.shape[0] // TILE)
        def _(t):
            here = pl.ds(pl.multiple_of(t * TILE, TILE), TILE)
            value = ref[here].astype(jnp.float32)
            for extra in extras:
                value = value + extra[here].astype(jnp.float32)
            result[here] = value

    meet()
    for index in range(2):
        for k in (2, 1, 3, 0):
            w_give(index, (z + k) % 4).start()
            w_load_copy(index, (z + k) % 4).start()
    begin()
    f_copy(1 - second).start()
    f_copy(second).start()
    load(first, 1 - second).start()
    load(first, second).start()
    small_begin()
    for index in range(2):
        for k in (2, 1, 3, 0):
            zz = (z + k) % 4
            w_load_copy(index, zz).wait()
            w_give(index, zz).wait_recv()
            add(kept[index].at[zz], [pairs[index].at[zz]])
    chain(0)

    @pl.loop(0, RSTEPS + LAGS[2])
    def _(i):
        tick(i)

        @pl.when(i == 2)
        def _():
            chain(1)

        @pl.when(i == 4)
        def _():
            chain(2)

        @pl.when(i == 1)
        def _():
            load(first, 1 - second).wait()
            f_copy(1 - second).wait_recv()
            add(mine.at[first, 1 - second], [first_in.at[1 - second]])
            g_copy.start()

    for index in range(2):
        @pl.when(z == 0)
        def _():
            down_copy(index, 0, 4).wait_recv()
            add_out(kept[index].at[z], [zs[index].at[4]], sums[index])

        @pl.when(z == 3)
        def _():
            up_copy(index, 3).wait_recv()
            add_out(kept[index].at[z], [zs[index].at[3]], sums[index])

        @pl.when((z > 0) & (z < 3))
        def _():
            up_copy(index, z).wait_recv()
            down_copy(index, z, 4).wait_recv()
            add_out(kept[index].at[z], [zs[index].at[z], zs[index].at[4]], sums[index])

        for result in results[index]:
            result.start()
    load(first, second).wait()
    f_copy(second).wait_recv()
    g_copy.wait_recv()
    add_out(mine.at[first, second], [first_in.at[second], second_in], total)
    pltpu.make_async_copy(total, out_ref, out_sem.at[4]).start()

    @pl.loop(RSTEPS + LAGS[2], TICKS)
    def _(i):
        tick(i)

    pltpu.make_async_copy(mixture, mixture_ref, out_sem.at[5]).start()
    finish()
    for sec in range(2):
        f_copy(sec).wait_send()
    g_copy.wait_send()
    for index in range(2):
        for k in range(4):
            w_give(index, (z + k) % 4).wait_send()
            if k:
                up_copy(index, (z + k) % 4).wait_send()
        for result in results[index]:
            result.wait()
    small_finish()
    pltpu.make_async_copy(total, out_ref, out_sem.at[4]).wait()
    pltpu.make_async_copy(mixture, mixture_ref, out_sem.at[5]).wait()


def finish_near(part, field, grads, pack, collective_id):
    rows_count, tokens, depth = field.shape
    dma = pltpu.SemaphoreType.DMA
    blocks = [(grads[0].shape[0] // 8, grads[0].shape[1]), (grads[1].shape[0], grads[1].shape[1] // 8)]
    results = [(blocks[0][0], blocks[0][1] // 3)] * 3 + [blocks[1]]
    half = lambda *shape: pltpu.VMEM(shape, jnp.bfloat16)
    return pl.pallas_call(
        finish_body,
        out_shape=(
            jax.ShapeDtypeStruct((tokens, depth), jnp.float32),
            jax.ShapeDtypeStruct((tokens, depth), jnp.float32),
            *[jax.ShapeDtypeStruct(b, jnp.float32) for b in results],
            jax.ShapeDtypeStruct((RANKS, *pack.shape[1:]), pack.dtype),
        ),
        in_specs=[ANYWHERE] * 5,
        out_specs=[ANYWHERE] * 7,
        scratch_shapes=[
            half(2, 2, tokens, depth), half(2, tokens, depth), half(tokens, depth),
            pltpu.VMEM((tokens, depth), jnp.float32),
            *[half(4, *b) for b in blocks], *[half(4, *b) for b in blocks], *[half(5, *b) for b in blocks],
            *[pltpu.VMEM(b, jnp.float32) for b in blocks],
            dma((2, 2)), dma((2,)), dma((2,)), dma(()), dma(()),
            dma((2, 4)), dma((2, 4)), dma((2, 4)), dma((2, 4)), dma((2, 5)), dma((6,)),
        ]
        + small_sems()
        + shrink_scratch(tokens, depth),
        compiler_params=pltpu.CompilerParams(
            collective_id=collective_id, has_side_effects=True, vmem_limit_bytes=63 * 1024 * 1024
        ),
    )(part.reshape(4, 2, 2, 2, tokens, depth), field, *grads, pack)


RSTEPS = 8
TILE = 16
LAGS = (0, 1, 2, 4)
TICKS = RSTEPS + LAGS[3]


def shrink(part_ref, sums, near_own, first_in, second_in, z_in, total, sems):
    r, c, y, x, z, core, first, second = seat()
    pair, along_first, along_second, up = partners()
    load_sem, p_send, p_recv, f_send, f_recv, g_send, g_recv, z_send, z_recv = sems
    tokens = total.shape[0]
    step = tokens // RSTEPS
    other = 1 - core

    def rows(q):
        return pl.ds(pl.multiple_of(q * step, step), step)

    def spot(kind):
        fir = (1 - first) if kind < 2 else first
        sec = (1 - second) if kind in (0, 2) else second
        return fir, sec

    def load(kind, q):
        yy, xx = row_of(core, *spot(kind))
        return pltpu.make_async_copy(
            part_ref.at[:, core, yy, xx, rows(q)], near_own.at[q % 2, kind], load_sem.at[kind, q % 2]
        )

    def give(fir, sec, q):
        yy, xx = row_of(other, fir, sec)
        return send(
            part_ref.at[:, other, yy, xx, rows(q)],
            sums.at[fir, sec, :, rows(q)],
            p_send.at[fir, sec, q],
            p_recv.at[fir, sec, q],
            pair,
        )

    def f_copy(sec, q):
        return send(
            sums.at[1 - first, sec, :, rows(q)],
            first_in.at[sec, :, rows(q)],
            f_send.at[sec, q],
            f_recv.at[sec, q],
            along_first,
        )

    def g_copy(q):
        return send(
            sums.at[first, 1 - second, :, rows(q)], second_in.at[:, rows(q)], g_send.at[q], g_recv.at[q], along_second
        )

    def z_copy(k, q):
        return send(
            sums.at[first, second, (z + k) % 4, rows(q)],
            z_in.at[k - 1, rows(q)],
            z_send.at[k - 1, q],
            z_recv.at[k - 1, q],
            up[k - 1],
        )

    def begin():
        @pl.loop(0, RSTEPS)
        def _(q):
            for fir, sec in ((1 - second, 1 - first), (1 - second, first), (second, 1 - first), (second, first)):
                give(fir, sec, q).start()

        for kind in range(4):
            load(kind, 0).start()

    def add(kind, q, extra):
        fir, sec = spot(kind)

        @pl.when(q + 1 < RSTEPS)
        def _():
            load(kind, q + 1).start()

        load(kind, q).wait()
        give(fir, sec, q).wait_recv()

        @pl.loop(0, 4 * (step // TILE))
        def _(t):
            zz, at = t // (step // TILE), t % (step // TILE)
            here = pl.ds(pl.multiple_of(q * step + at * TILE, TILE), TILE)
            near = pl.ds(pl.multiple_of(at * TILE, TILE), TILE)
            value = sums[fir, sec, zz, here].astype(jnp.float32)
            value = value + near_own[q % 2, kind, zz, near].astype(jnp.float32)
            for ref in extra:
                value = value + ref[zz, here].astype(jnp.float32)
            sums[fir, sec, zz, here] = value.astype(jnp.bfloat16)

    def stage_first(q):
        for kind, sec in ((0, 1 - second), (1, second)):
            add(kind, q, [])
            f_copy(sec, q).start()

    def stage_second(q):
        f_copy(1 - second, q).wait_recv()
        add(2, q, [first_in.at[1 - second]])
        g_copy(q).start()

    def stage_z(q):
        f_copy(second, q).wait_recv()
        g_copy(q).wait_recv()
        add(3, q, [first_in.at[second], second_in])
        for k in QUEUE:
            z_copy(k, q).start()

    def stage_out(q):
        for k in ARRIVE:
            z_copy(k, q).wait_recv()

        @pl.loop(0, step // TILE)
        def _(t):
            here = pl.ds(pl.multiple_of(q * step + t * TILE, TILE), TILE)
            value = sums[first, second, z, here].astype(jnp.float32)
            for k in range(3):
                value = value + z_in[k, here].astype(jnp.float32)
            total[here] = value

    def tick(i):
        for stage, lag in zip((stage_first, stage_second, stage_z, stage_out), LAGS):

            @pl.when((i >= lag) & (i < RSTEPS + lag))
            def _(stage=stage, lag=lag):
                stage(i - lag)

    def finish():
        @pl.loop(0, RSTEPS)
        def _(q):
            for fir in range(2):
                for sec in range(2):
                    give(fir, sec, q).wait_send()
            for sec in range(2):
                f_copy(sec, q).wait_send()
            g_copy(q).wait_send()
            for k in QUEUE:
                z_copy(k, q).wait_send()

    return begin, tick, finish


def shrink_scratch(tokens, depth):
    dma = pltpu.SemaphoreType.DMA
    low = lambda *shape: pltpu.VMEM((*shape, depth), jnp.bfloat16)
    buffers = [
        low(2, 2, 4, tokens), low(2, 4, 4, tokens // RSTEPS), low(2, 4, tokens), low(4, tokens), low(3, tokens),
        pltpu.VMEM((tokens, depth), jnp.float32),
    ]
    shapes = [(2, 2, RSTEPS), (2, RSTEPS), (RSTEPS,), (3, RSTEPS)]
    return buffers + [dma((4, 2))] + [dma(shape) for shape in shapes for _ in range(2)]


def small_each(small_ref, small_all, sems, pick):
    here_sem, small_send, small_recv = sems
    local = pltpu.make_async_copy(small_ref.at[pick(nth(0)[0])], small_all.at[nth(0)[0]], here_sem)

    def copy(offset):
        return small_copy(lambda spot: small_ref.at[pick(spot)], small_all, small_send, small_recv, offset)

    def begin():
        local.start()

        @pl.loop(1, RANKS)
        def _(offset):
            copy(offset).start()

    def finish():
        local.wait()

        @pl.loop(1, RANKS)
        def _(offset):
            copy(offset).wait()

    return begin, finish


def feed_back_body(part_ref, small_ref, rows_ref, gate_ref, up_ref, act_ref, grads_ref,
                   out_ref, small_all, gate_out, up_out, down_out, *scratch):
    begin, tick, finish = shrink(part_ref, *scratch[:6], scratch[6:15])
    total, out_sem = scratch[5], scratch[15]
    small_begin, small_finish = small_each(small_ref, small_all, scratch[16:], lambda spot: spot)
    e, k = pl.program_id(0), pl.program_id(1)
    step = e * pl.num_programs(1) + k
    last = pl.num_programs(0) * pl.num_programs(1) - 1

    @pl.when(step == 0)
    def _():
        meet()
        small_begin()
        begin()

    rows = rows_ref[0]
    gate_out[0] = inner_rows(rows, gate_ref[0]).astype(jnp.bfloat16)
    up_out[0] = inner_rows(rows, up_ref[0]).astype(jnp.bfloat16)
    down_out[0] = inner_rows(act_ref[0], grads_ref[0]).astype(jnp.bfloat16)

    @pl.when(k == 0)
    def _():
        tick(e)

    @pl.when(step == last)
    def _():
        @pl.loop(RSTEPS, TICKS)
        def _(i):
            tick(i)

        done = pltpu.make_async_copy(total, out_ref, out_sem)
        done.start()
        finish()
        small_finish()
        done.wait()


def feed_back(part, small, rows, grad_gate, grad_up, act, grads, collective_id):
    tokens, depth = part.shape[0] // RANKS, part.shape[1]
    groups, length, inner = grad_gate.shape
    assert groups == RSTEPS
    dma = pltpu.SemaphoreType.DMA
    slab = pl.BlockSpec((1, length, CHUNK), lambda e, k: (e, 0, k))
    held = pl.BlockSpec((1, length, inner), lambda e, k: (e, 0, 0))
    return pl.pallas_call(
        feed_back_body,
        grid=(groups, depth // CHUNK),
        in_specs=[ANYWHERE, ANYWHERE, slab, held, held, held, slab],
        out_specs=[
            ANYWHERE,
            ANYWHERE,
            pl.BlockSpec((1, CHUNK, inner), lambda e, k: (e, k, 0)),
            pl.BlockSpec((1, CHUNK, inner), lambda e, k: (e, k, 0)),
            pl.BlockSpec((1, inner, CHUNK), lambda e, k: (e, 0, k)),
        ],
        out_shape=(
            jax.ShapeDtypeStruct((tokens, depth), jnp.float32),
            jax.ShapeDtypeStruct(small.shape, small.dtype),
            jax.ShapeDtypeStruct((groups, depth, inner), jnp.bfloat16),
            jax.ShapeDtypeStruct((groups, depth, inner), jnp.bfloat16),
            jax.ShapeDtypeStruct((groups, inner, depth), jnp.bfloat16),
        ),
        scratch_shapes=shrink_scratch(tokens, depth) + [dma(())] + small_sems(),
        compiler_params=pltpu.CompilerParams(
            collective_id=collective_id, has_side_effects=True, vmem_limit_bytes=63 * 1024 * 1024
        ),
    )(part.reshape(4, 2, 2, 2, tokens, depth), small, rows, grad_gate, grad_up, act, grads)


def widen_body(*refs):
    half = len(refs) // 2
    for low, wide in zip(refs[:half], refs[half:]):
        wide[...] = low[...].astype(jnp.float32)


def widen_all(*arrays):
    specs = [pl.BlockSpec((1, *array.shape[1:]), lambda e: (e, 0, 0)) for array in arrays]
    return pl.pallas_call(
        widen_body,
        grid=(arrays[0].shape[0],),
        in_specs=specs,
        out_specs=specs,
        out_shape=[jax.ShapeDtypeStruct(array.shape, jnp.float32) for array in arrays],
        compiler_params=pltpu.CompilerParams(vmem_limit_bytes=40 * 1024 * 1024),
    )(*arrays)


def fill_rows(pick_ref, field_ref, rows_ref):
    ranks, groups = pick_ref.shape[0], rows_ref.shape[0]

    @pl.loop(0, ranks // 2, unroll=UNROLL)
    def _(i):
        parts = [
            wide_dot(pick_ref[2 * i + side], field_ref[2 * i + side]).reshape(groups, SLOTS, CHUNK)
            for side in range(2)
        ]
        here = pl.ds(pl.multiple_of(i * 2 * SLOTS, 2 * SLOTS), 2 * SLOTS)
        rows_ref[:, here] = jnp.concatenate(parts, axis=1).astype(jnp.bfloat16)


def add_products(k, rows_ref, pairs):
    groups = rows_ref.shape[0]

    def products(e, first):
        for product, total in pairs:
            term = product(rows_ref[e], e)
            if first:
                total[e] = term
            else:
                total[e] += term

    @pl.when(k == 0)
    def _():
        @pl.loop(0, groups)
        def _(e):
            products(e, True)

    @pl.when(k > 0)
    def _():
        @pl.loop(0, groups)
        def _(e):
            products(e, False)


def grads_in_body(pick_ref, field_ref, down_ref, own_ref, small_ref,
                  rows_ref, plain_ref, all_ref, small_all, total, *sems):
    begin, forward, finish = spread_out(own_ref, all_ref, sems[:11])
    small_begin, small_finish = small_out(small_ref, small_all, sems[11:])
    k, last = pl.program_id(0), pl.num_programs(0) - 1

    @pl.when(k == 0)
    def _():
        meet()
        small_begin()
        begin()

    fill_rows(pick_ref, field_ref, rows_ref)
    add_products(k, rows_ref, [(lambda rows, e: outer_cols(rows, down_ref[e]), total)])

    @pl.when(k % 2 == 1)
    def _():
        forward(k // 2)

    @pl.when(k == last)
    def _():
        pltpu.sync_copy(total, plain_ref)
        finish()
        small_finish()


def grads_in(pick, field, down, own, small, collective_id):
    ranks, width, tokens = pick.shape
    groups, depth = width // SLOTS, field.shape[-1]
    length, inner = ranks * SLOTS, down.shape[1]
    steps = depth // CHUNK
    rows, plain, whole, small_all = pl.pallas_call(
        grads_in_body,
        grid=(steps,),
        in_specs=[
            pl.BlockSpec((ranks, width, tokens), lambda k: (0, 0, 0), pipeline_mode=pl.Buffered(1)),
            pl.BlockSpec((ranks, tokens, CHUNK), lambda k: (0, 0, k)),
            pl.BlockSpec((groups, inner, CHUNK), lambda k: (0, 0, k)),
            ANYWHERE,
            ANYWHERE,
        ],
        out_specs=[pl.BlockSpec((groups, length, CHUNK), lambda k: (0, 0, k))] + [ANYWHERE] * 3,
        out_shape=[
            jax.ShapeDtypeStruct((groups, length, depth), jnp.bfloat16),
            jax.ShapeDtypeStruct((groups, length, inner), jnp.float32),
            jax.ShapeDtypeStruct((4, 2, 2, 2, *own.shape), own.dtype),
            jax.ShapeDtypeStruct((RANKS, *small.shape), small.dtype),
        ],
        scratch_shapes=[pltpu.VMEM((groups, length, inner), jnp.float32)] + spread_sems() + small_sems(),
        compiler_params=pltpu.CompilerParams(
            collective_id=collective_id, has_side_effects=True, vmem_limit_bytes=62 * 1024 * 1024
        ),
    )(pick, field, down, own, small)
    return rows, plain, whole.reshape(RANKS, *own.shape), small_all


def feed_in_body(steps, pick_ref, field_ref, gate_ref, up_ref, plain_ref, probs_ref,
                 rows_ref, act_ref, weighted_ref, grad_gate_ref, grad_up_ref, gates_ref, gate_sum, up_sum):
    k = pl.program_id(0)

    @pl.when(k < steps)
    def _():
        fill_rows(pick_ref, field_ref, rows_ref)
        add_products(
            k,
            rows_ref,
            [
                (lambda rows, e: wide_dot(rows, gate_ref[e]), gate_sum),
                (lambda rows, e: wide_dot(rows, up_ref[e]), up_sum),
            ],
        )

    @pl.when(k >= steps)
    def _():
        e = k - steps
        length = act_ref.shape[1]

        @pl.loop(0, length // 128)
        def _(t):
            here = pl.ds(pl.multiple_of(t * 128, 128), 128)
            gate_val, up_val = gate_sum[e, here], up_sum[e, here]
            plain, probs = plain_ref[0, here], probs_ref[0, here]
            sigmoid_val = jax.nn.sigmoid(gate_val)
            silu_val = gate_val * sigmoid_val
            activated = silu_val * up_val
            grad_act = plain * probs
            grad_up_ref[0, here] = (grad_act * silu_val).astype(jnp.bfloat16)
            grad_gate_ref[0, here] = (
                grad_act * up_val * (sigmoid_val * (1.0 + gate_val * (1.0 - sigmoid_val)))
            ).astype(jnp.bfloat16)
            gates_ref[0, here] = jnp.sum(activated * plain, axis=-1, keepdims=True)
            weighted_ref[0, here] = (activated * probs).astype(jnp.bfloat16)
            act_ref[0, here] = activated.astype(jnp.bfloat16)


def feed_in(pick, field, gate, up, plain, probs):
    ranks, width, tokens = pick.shape
    groups, depth = width // SLOTS, field.shape[-1]
    length, inner = ranks * SLOTS, gate.shape[2]
    steps = depth // CHUNK
    held = lambda k: jnp.minimum(k, steps - 1)
    late = lambda k: (jnp.maximum(k - steps, 0), 0, 0)
    wide = pl.BlockSpec((1, length, inner), late)
    thin = pl.BlockSpec((1, length, 1), late)
    low = jax.ShapeDtypeStruct((groups, length, inner), jnp.bfloat16)
    return pl.pallas_call(
        functools.partial(feed_in_body, steps),
        grid=(steps + groups,),
        in_specs=[
            pl.BlockSpec((ranks, width, tokens), lambda k: (0, 0, 0), pipeline_mode=pl.Buffered(1)),
            pl.BlockSpec((ranks, tokens, CHUNK), lambda k: (0, 0, held(k))),
            pl.BlockSpec((groups, CHUNK, inner), lambda k: (0, held(k), 0)),
            pl.BlockSpec((groups, CHUNK, inner), lambda k: (0, held(k), 0)),
            wide,
            thin,
        ],
        out_specs=[pl.BlockSpec((groups, length, CHUNK), lambda k: (0, 0, held(k))), wide, wide, wide, wide, thin],
        out_shape=[
            jax.ShapeDtypeStruct((groups, length, depth), jnp.bfloat16),
            low, low, low, low,
            jax.ShapeDtypeStruct((groups, length, 1), jnp.float32),
        ],
        scratch_shapes=[pltpu.VMEM((groups, length, inner), jnp.float32)] * 2,
        compiler_params=pltpu.CompilerParams(vmem_limit_bytes=63 * 1024 * 1024),
        cost_estimate=pl.CostEstimate(
            flops=2 * groups * length * depth * (tokens + 2 * inner), bytes_accessed=120 << 20, transcendentals=0
        ),
    )(pick, field, gate, up, plain, probs)


def fill_field(flipped, spread_ref, lefts, weights, field_ref, rows):
    groups = rows.shape[0]
    ranks = spread_ref.shape[0]

    @pl.loop(0, groups)
    def _(e):
        total = None
        for left, weight, flip in zip(lefts, weights, flipped):
            term = outer_cols(left[e], weight[e]) if flip else wide_dot(left[e], weight[e])
            total = term if total is None else total + term
        rows[e] = total

    @pl.loop(0, ranks, unroll=2 * UNROLL)
    def _(s):
        part = rows[:, pl.ds(pl.multiple_of(s * SLOTS, SLOTS), SLOTS)]
        part = part.reshape(groups * SLOTS, CHUNK).astype(jnp.bfloat16)
        field_ref[s] = wide_dot(spread_ref[s], part).astype(jnp.bfloat16)


def restore_body(flipped, spread_ref, *refs):
    count = len(flipped)
    fill_field(flipped, spread_ref, refs[:count], refs[count : 2 * count], *refs[2 * count :])


def restore_specs(spread, lefts, weights, flipped):
    ranks, tokens, width = spread.shape
    groups = width // SLOTS
    length, inner = ranks * SLOTS, lefts[0].shape[2]
    depth = weights[0].shape[1] if flipped[0] else weights[0].shape[2]
    once = pl.Buffered(1)
    in_specs = (
        [pl.BlockSpec((ranks, tokens, width), lambda k: (0, 0, 0), pipeline_mode=once)]
        + [pl.BlockSpec((groups, length, inner), lambda k: (0, 0, 0), pipeline_mode=once)] * len(lefts)
        + [
            pl.BlockSpec((groups, CHUNK, inner), lambda k: (0, k, 0))
            if flip
            else pl.BlockSpec((groups, inner, CHUNK), lambda k: (0, 0, k))
            for flip in flipped
        ]
    )
    out_spec = pl.BlockSpec((ranks, tokens, CHUNK), lambda k: (0, 0, k))
    out_shape = jax.ShapeDtypeStruct((ranks, tokens, depth), jnp.bfloat16)
    return depth // CHUNK, in_specs, out_spec, out_shape, pltpu.VMEM((groups, length, CHUNK), jnp.float32)


def restore(spread, lefts, weights, flipped):
    steps, in_specs, out_spec, out_shape, rows = restore_specs(spread, lefts, weights, flipped)
    field = pl.pallas_call(
        functools.partial(restore_body, flipped),
        grid=(steps,),
        in_specs=in_specs,
        out_specs=out_spec,
        out_shape=out_shape,
        scratch_shapes=[rows],
        compiler_params=pltpu.CompilerParams(vmem_limit_bytes=63 * 1024 * 1024),
    )(spread, *lefts, *weights)
    return field.reshape(-1, field.shape[2])


PARTS = 4


def restore_out_body(spread_ref, left_ref, weight_ref, own_ref, field_ref, all_ref, rows,
                     here_sem, f_send, f_recv, g_send, g_recv, h_send, h_recv):
    r, c, y, x, z, core, first, second = seat()
    pair, along_first, along_second, up = partners()
    y1, x1 = row_of(core, first, 1 - second)
    near_row = y1 * 2 + x1
    step = own_ref.shape[0] // PARTS
    k = pl.program_id(0)
    here = pltpu.make_async_copy(own_ref, all_ref.at[r], here_sem)

    def part(ref, q):
        return ref.at[pl.ds(q * step, step)]

    def f_copy(q):
        return send(part(own_ref, q), part(all_ref.at[r], q), f_send.at[q], f_recv.at[q], along_first)

    def g_copy(q):
        return send(part(own_ref, q), part(all_ref.at[r], q), g_send.at[q], g_recv.at[q], along_second)

    def h_copy(q):
        there = part(all_ref.at[near_row], q)
        return send(there, there, h_send.at[q], h_recv.at[q], along_first)

    @pl.when(k == 0)
    def _():
        meet()
        here.start()
        for q in range(PARTS):
            g_copy(q).start()
            f_copy(q).start()

    fill_field((False,), spread_ref, [left_ref], [weight_ref], field_ref, rows)

    for q in range(PARTS):

        @pl.when(k == q + 1)
        def _():
            g_copy(q).wait_recv()
            h_copy(q).start()

    @pl.when(k == pl.num_programs(0) - 1)
    def _():
        here.wait()
        for q in range(PARTS):
            g_copy(q).wait_send()
            f_copy(q).wait()
            h_copy(q).wait()


def restore_out(spread, left, weight, own, collective_id):
    steps, in_specs, out_spec, out_shape, rows = restore_specs(spread, [left], [weight], (False,))
    dma = pltpu.SemaphoreType.DMA
    field, whole = pl.pallas_call(
        restore_out_body,
        grid=(steps,),
        in_specs=in_specs + [ANYWHERE],
        out_specs=[out_spec, ANYWHERE],
        out_shape=[out_shape, jax.ShapeDtypeStruct((4, *own.shape), own.dtype)],
        scratch_shapes=[rows, dma(())] + [dma((PARTS,))] * 6,
        compiler_params=pltpu.CompilerParams(
            collective_id=collective_id, has_side_effects=True, vmem_limit_bytes=63 * 1024 * 1024
        ),
    )(spread, left, weight, own)
    return field.reshape(-1, field.shape[2]), whole.reshape(-1, own.shape[1])


def branch_body(mixed_ref, weight_ref, out_ref, away, near, first_in, second_in,
                f_send, f_recv, g_send, g_recv):
    r, c, y, x, z, core, first, second = seat()
    pair, along_first, along_second, up = partners()
    tokens, depth = out_ref.shape
    width = depth // PARTS

    def columns(j):
        return pl.ds(j * width, width)

    def product(fir, sec, j):
        yy, xx = row_of(core, fir, sec)
        rows = pl.ds(pl.multiple_of((yy * 2 + xx) * tokens, tokens), tokens)
        return wide_dot(mixed_ref[rows], weight_ref[:, columns(j)])

    def f_copy(sec, j):
        return send(
            away.at[sec, :, columns(j)], first_in.at[sec, :, columns(j)], f_send.at[sec, j], f_recv.at[sec, j], along_first
        )

    def g_copy(j):
        return send(near.at[:, columns(j)], second_in.at[:, columns(j)], g_send.at[j], g_recv.at[j], along_second)

    meet()
    for j in range(PARTS):
        away[1 - second, :, columns(j)] = product(1 - first, 1 - second, j).astype(jnp.bfloat16)
        f_copy(1 - second, j).start()
    for j in range(PARTS):
        away[second, :, columns(j)] = product(1 - first, second, j).astype(jnp.bfloat16)
        f_copy(second, j).start()
    for j in range(PARTS):
        value = product(first, 1 - second, j)
        f_copy(1 - second, j).wait_recv()
        value = value + first_in[1 - second, :, columns(j)].astype(jnp.float32)
        near[:, columns(j)] = value.astype(jnp.bfloat16)
        g_copy(j).start()
    for j in range(PARTS):
        out_ref[:, columns(j)] = product(first, second, j)
    for j in range(PARTS):
        f_copy(second, j).wait_recv()
        g_copy(j).wait_recv()
        out_ref[:, columns(j)] += first_in[second, :, columns(j)].astype(jnp.float32) + second_in[
            :, columns(j)
        ].astype(jnp.float32)
    for j in range(PARTS):
        g_copy(j).wait_send()
        for sec in range(2):
            f_copy(sec, j).wait_send()


def branch_near(mixed, weight, collective_id):
    tokens, depth = mixed.shape[0] // 4, weight.shape[1]
    dma = pltpu.SemaphoreType.DMA
    inside = pl.BlockSpec(memory_space=pltpu.VMEM)
    low = lambda *shape: pltpu.VMEM((*shape, tokens, depth), jnp.bfloat16)
    return pl.pallas_call(
        branch_body,
        in_specs=[inside] * 2,
        out_specs=inside,
        out_shape=jax.ShapeDtypeStruct((tokens, depth), jnp.float32),
        scratch_shapes=[
            low(2), low(), low(2), low(), dma((2, PARTS)), dma((2, PARTS)), dma((PARTS,)), dma((PARTS,))
        ],
        compiler_params=pltpu.CompilerParams(
            collective_id=collective_id, has_side_effects=True, vmem_limit_bytes=40 * 1024 * 1024
        ),
    )(mixed, weight)


def causal_scores(query_rows, key_rows):
    scores = outer_cols(query_rows, key_rows) * HD ** (-0.5)
    count, length = scores.shape
    position = lax.broadcasted_iota(jnp.int32, scores.shape, 0) + (length - count)
    return jnp.where(position >= lax.broadcasted_iota(jnp.int32, scores.shape, 1), scores, MASKED)


def attend_body(q_raw, k_raw, v_ref, q_rs, k_rs, q_gain, k_gain, cos_ref, sin_ref,
                mixed_ref, q_out, k_out, v_out, lse_ref):
    length = v_ref.shape[0]
    block = min(256, length)
    v_out[...] = v_ref[...].astype(jnp.bfloat16)
    for raw, scale, gain, out in ((q_raw, q_rs, q_gain, q_out), (k_raw, k_rs, k_gain, k_out)):
        normed = raw[...] * scale[...] * gain[...]
        turned = normed * cos_ref[...] + pltpu.roll(normed, HD // 2, 1) * sin_ref[...]
        out[...] = turned.astype(jnp.bfloat16)
    for start in range(0, length, block):
        here, seen = pl.ds(start, block), pl.ds(0, start + block)
        scores = causal_scores(q_out[here], k_out[seen])
        row_top = jnp.max(scores, axis=-1, keepdims=True)
        exponent = jnp.exp(scores - row_top)
        row_total = jnp.sum(exponent, axis=-1, keepdims=True)
        weights = (exponent / row_total).astype(jnp.bfloat16)
        mixed_ref[here] = wide_dot(weights, v_out[seen]).astype(jnp.bfloat16)
        lse_ref[0, here] = row_top + jnp.log(row_total)


def three_slabs(length, heads):
    return [pl.BlockSpec((length, HD), lambda h, at=at: (0, at * heads + h)) for at in range(3)]


def attend(raw, q_rs, k_rs, q_gain, k_gain, cosine, sine):
    length, width = raw.shape[0], raw.shape[1] // 3
    heads = width // HD
    slab = pl.BlockSpec((length, HD), lambda h: (0, h))
    thin = pl.BlockSpec((length, 1), lambda h: (0, 0))
    line = pl.BlockSpec((1, HD), lambda h: (0, h))
    table = pl.BlockSpec((length, HD), lambda h: (0, 0))
    low = jax.ShapeDtypeStruct((length, width), jnp.bfloat16)
    return pl.pallas_call(
        attend_body,
        grid=(heads,),
        in_specs=three_slabs(length, heads) + [thin, thin, line, line, table, table],
        out_specs=[slab, slab, slab, slab, pl.BlockSpec((1, length, 1), lambda h: (h, 0, 0))],
        out_shape=[low, low, low, low, jax.ShapeDtypeStruct((heads, length, 1), jnp.float32)],
        cost_estimate=pl.CostEstimate(
            flops=4 * heads * length * length * HD, bytes_accessed=8 << 20, transcendentals=heads * length * length
        ),
    )(raw, raw, raw, q_rs, k_rs, q_gain[None], k_gain[None], cosine, sine)


def attend_back_body(q_ref, k_ref, v_ref, grad_ref, lse_ref, q_raw, k_raw, q_rs, k_rs, q_gain, k_gain, cos_ref, sin_ref,
                     v_grad, q_grad, k_grad, q_term, k_term, q_inner, k_inner, dq, dk, dv):
    length = v_ref.shape[0]
    block = min(256, length)
    dk[...] = jnp.zeros_like(dk)
    dv[...] = jnp.zeros_like(dv)
    for start in range(0, length, block):
        here, seen = pl.ds(start, block), pl.ds(0, start + block)
        query_rows, key_rows, grads = q_ref[here], k_ref[seen], grad_ref[here]
        probs = jnp.exp(causal_scores(query_rows, key_rows) - lse_ref[0, here])
        dv[seen] += inner_rows(probs.astype(jnp.bfloat16), grads)
        weights = outer_cols(grads, v_ref[seen])
        delta = jnp.sum(probs * weights, axis=-1, keepdims=True)
        scores = (probs * (weights - delta)).astype(jnp.bfloat16)
        dq[here] = wide_dot(scores, key_rows) * HD ** (-0.5)
        dk[seen] += inner_rows(scores, query_rows) * HD ** (-0.5)
    v_grad[...] = dv[...].astype(jnp.bfloat16)
    for raw, scale, gain, grad, out, term, inner in (
        (q_raw, q_rs, q_gain, dq, q_grad, q_term, q_inner),
        (k_raw, k_rs, k_gain, dk, k_grad, k_term, k_inner),
    ):
        field, value = raw[...], grad[...]
        normed = value * cos_ref[...] + pltpu.roll(value * sin_ref[...], HD // 2, 1)
        weighted = normed * gain[...]
        out[...] = weighted
        term[...] = jnp.sum(normed * field * scale[...], axis=0, keepdims=True)
        inner[0] = jnp.sum(weighted * field, axis=-1, keepdims=True)


def attend_back(queries, keys, values, grads, lse, raw, q_rs, k_rs, q_gain, k_gain, cosine, sine):
    length, width = raw.shape[0], raw.shape[1] // 3
    heads = width // HD
    slab = pl.BlockSpec((length, HD), lambda h: (0, h))
    thin = pl.BlockSpec((length, 1), lambda h: (0, 0))
    line = pl.BlockSpec((1, HD), lambda h: (0, h))
    table = pl.BlockSpec((length, HD), lambda h: (0, 0))
    column = pl.BlockSpec((1, length, 1), lambda h: (h, 0, 0))
    wide = jax.ShapeDtypeStruct((length, width), jnp.float32)
    return pl.pallas_call(
        attend_back_body,
        grid=(heads,),
        in_specs=[slab] * 4 + [column] + three_slabs(length, heads)[:2] + [thin, thin, line, line, table, table],
        out_specs=[slab, slab, slab, line, line, column, column],
        out_shape=[
            jax.ShapeDtypeStruct((length, width), jnp.bfloat16),
            wide,
            wide,
            jax.ShapeDtypeStruct((1, width), jnp.float32),
            jax.ShapeDtypeStruct((1, width), jnp.float32),
            jax.ShapeDtypeStruct((heads, length, 1), jnp.float32),
            jax.ShapeDtypeStruct((heads, length, 1), jnp.float32),
        ],
        scratch_shapes=[pltpu.VMEM((length, HD), jnp.float32)] * 3,
        cost_estimate=pl.CostEstimate(
            flops=10 * heads * length * length * HD, bytes_accessed=16 << 20, transcendentals=heads * length * length
        ),
    )(queries, keys, values, grads, lse, raw, raw, q_rs, k_rs, q_gain[None], k_gain[None], cosine, sine)


def local(
    layer_input,
    cotangent,
    expert_index,
    attention_gain,
    query_gain,
    key_gain,
    query_weight,
    key_weight,
    value_weight,
    output_weight,
    feed_gain,
    router_weight,
    gate_weight,
    up_weight,
    down_weight,
):
    tokens = layer_input.shape[0]
    rows_count = lax.axis_size("row")
    near = rows_count == 4 and lax.axis_size("col") == 8
    if near:
        head_part = query_gain.shape[0]
        slice_width = attention_gain.shape[0]
        pack = jnp.concatenate(
            [attention_gain, feed_gain, query_gain, key_gain, router_weight.reshape(-1)]
        )
        pack = jnp.pad(pack, (0, PACK_ROWS * 128 - pack.shape[0])).reshape(PACK_ROWS, 128)
        (
            sequence, qkv_full, output_full, pack_all, cotangent_all, index_all
        ) = start_near(
            layer_input,
            [query_weight, key_weight, value_weight, output_weight],
            pack,
            cotangent,
            expert_index.T,
            1,
        )
        index_all = jnp.swapaxes(index_all, 1, 2)
        pack_all = pack_all.reshape(8, -1)
        ends = [slice_width, 2 * slice_width, 2 * slice_width + head_part, 2 * slice_width + 2 * head_part]
        attention_full = pack_all[:, : ends[0]].reshape(-1)
        feed_full = pack_all[:, ends[0] : ends[1]].reshape(-1)
        query_scale_w = pack_all[:, ends[1] : ends[2]].reshape(-1)
        key_scale_w = pack_all[:, ends[2] : ends[3]].reshape(-1)
        router_full = pack_all[:, ends[3] : ends[3] + router_weight.size].reshape(
            -1, router_weight.shape[1]
        )
    else:
        (
            attention_full,
            query_scale_w,
            key_scale_w,
            query_full,
            key_full,
            value_full,
            output_full,
            feed_full,
            router_full,
        ) = (
            lax.all_gather(attention_gain, "col", axis=0, tiled=True),
            lax.all_gather(query_gain, "col", axis=0, tiled=True),
            lax.all_gather(key_gain, "col", axis=0, tiled=True),
            lax.all_gather(query_weight, "col", axis=0, tiled=True),
            lax.all_gather(key_weight, "col", axis=0, tiled=True),
            lax.all_gather(value_weight, "col", axis=0, tiled=True),
            lax.all_gather(output_weight, "col", axis=1, tiled=True),
            lax.all_gather(feed_gain, "col", axis=0, tiled=True),
            lax.all_gather(router_weight, "col", axis=0, tiled=True),
        )
        qkv_full = jnp.concatenate([query_full, key_full, value_full], axis=1)
        sequence = lax.all_gather(layer_input, "row", axis=0, tiled=True)
    length = sequence.shape[0]
    model_width = sequence.shape[1]
    local_width = qkv_full.shape[1] // 3
    seq_float = sequence.astype(jnp.float32)
    seq_scale = rms_scale(seq_float)
    attention_float = attention_full.astype(jnp.float32)
    normed = (seq_float * seq_scale * attention_float).astype(jnp.bfloat16)
    raw = wide_dot(normed, qkv_full)
    query_raw, key_raw = raw[:, :local_width], raw[:, local_width : 2 * local_width]
    query_total, key_total = lax.psum(
        (jnp.sum(query_raw * query_raw, axis=-1), jnp.sum(key_raw * key_raw, axis=-1)), "row"
    )
    query_rs = lax.rsqrt(query_total / model_width + EPS)[:, None]
    key_rs = lax.rsqrt(key_total / model_width + EPS)[:, None]
    query_gain_f = query_scale_w.astype(jnp.float32)
    key_gain_f = key_scale_w.astype(jnp.float32)
    cosine, sine_table = rope_tables(length)
    mixed_heads, queries, keys_rotated, values, lse_all = attend(
        raw, query_rs, key_rs, query_gain_f, key_gain_f, cosine, sine_table
    )
    if near:
        branch = branch_near(mixed_heads, output_full, 5)
    else:
        branch = lax.psum_scatter(
            wide_dot(mixed_heads, output_full).astype(jnp.bfloat16), "row", scatter_dimension=0, tiled=True
        ).astype(jnp.float32)
    hidden = layer_input.astype(jnp.float32) + branch
    feed_scale = rms_scale(hidden)
    feed_float = feed_full.astype(jnp.float32)
    feed_normed = (hidden * feed_scale * feed_float).astype(jnp.bfloat16)
    logits = wide_dot(feed_normed, router_full)
    logit_top = jnp.max(logits, axis=-1, keepdims=True)
    logit_exp = jnp.exp(logits - logit_top)
    router_probs = logit_exp / jnp.sum(logit_exp, axis=-1, keepdims=True)
    experts = router_full.shape[1]
    experts_local = gate_weight.shape[0]
    ranks = lax.axis_size("col") * rows_count
    gate_hits = expert_index[:, :, None] == jnp.arange(experts, dtype=jnp.int32)
    gate_probs = jnp.sum(jnp.where(gate_hits, router_probs[:, None, :], 0.0), axis=-1)

    if not near:
        index_all = lax.all_gather(expert_index, ("col", "row"), axis=0, tiled=True)
    own = (index_all - lax.axis_index("col") * experts_local).reshape(ranks, tokens, -1)
    matches = own[..., None] == jnp.arange(experts_local, dtype=jnp.int32)
    hit = jnp.sum(matches.astype(jnp.float32), axis=2)
    earlier = jnp.tril(jnp.ones((tokens, tokens), jnp.bfloat16), -1)
    rank = jnp.einsum(
        "tu,sue->ste", earlier, hit.astype(jnp.bfloat16), preferred_element_type=jnp.float32
    )
    slot = jnp.where(hit > 0, rank, -1.0)
    places = jnp.arange(SLOTS, dtype=jnp.float32)
    slot_t = jnp.swapaxes(slot, 1, 2)
    width = experts_local * SLOTS
    picked = slot_t[:, :, None, :] == places[None, None, :, None]
    pick = picked.astype(jnp.bfloat16).reshape(ranks, width, tokens)
    lanes = jnp.arange(width, dtype=jnp.int32)
    widen = (lanes[None, :] // SLOTS == jnp.arange(experts_local)[:, None]).astype(jnp.bfloat16)
    spread = jnp.einsum(
        "ste,ew->stw", slot.astype(jnp.bfloat16), widen, preferred_element_type=jnp.float32
    ) == (lanes % SLOTS).astype(jnp.float32)
    spread_plain = spread.astype(jnp.bfloat16)

    def weigh(probs_all):
        probs_own = jnp.sum(
            jnp.where(matches, probs_all.reshape(ranks, tokens, -1, 1), 0.0), axis=2
        )
        probs_wide = jnp.einsum(
            "ste,ew->stw", probs_own.astype(jnp.bfloat16), widen, preferred_element_type=jnp.float32
        )
        spread_probs = jnp.where(spread, probs_wide, 0.0).astype(jnp.bfloat16)
        probs_t = jnp.swapaxes(probs_own, 1, 2)
        row_probs = jnp.sum(jnp.where(picked, probs_t[:, :, None, :], 0.0), axis=-1)
        row_probs = jnp.swapaxes(row_probs, 0, 1).reshape(experts_local, ranks * SLOTS, 1)
        return spread_probs, row_probs

    if near:
        expert_grads, plain_act, feed_all, probs_all = grads_in(
            pick, cotangent_all, down_weight, feed_normed, gate_probs.T, 2
        )
        spread_probs, row_probs = weigh(jnp.swapaxes(probs_all, 1, 2))
        expert_rows, activated, weighted_act, grad_gate, grad_up, row_gates = feed_in(
            pick, feed_all, gate_weight, up_weight, plain_act, row_probs
        )
    else:
        probs_all = lax.all_gather(gate_probs, ("col", "row"), axis=0, tiled=True)
        spread_probs, row_probs = weigh(probs_all)
        expert_grads = gather_rows(pick, cotangent)
        expert_rows = gather_rows(pick, feed_normed)
        gate_val = jnp.einsum(
            "erd,edf->erf", expert_rows, gate_weight, preferred_element_type=jnp.float32
        )
        up_val = jnp.einsum(
            "erd,edf->erf", expert_rows, up_weight, preferred_element_type=jnp.float32
        )
        plain_act = jnp.einsum(
            "erd,efd->erf", expert_grads, down_weight, preferred_element_type=jnp.float32
        )
        sigmoid_val = jax.nn.sigmoid(gate_val)
        silu_val = gate_val * sigmoid_val
        activated = silu_val * up_val
        grad_act = plain_act * row_probs
        grad_up = (grad_act * silu_val).astype(jnp.bfloat16)
        grad_gate = (
            grad_act * up_val * sigmoid_val * (1.0 + gate_val * (1.0 - sigmoid_val))
        ).astype(jnp.bfloat16)
        row_gates = jnp.sum(activated * plain_act, axis=-1)
        weighted_act = (activated * row_probs).astype(jnp.bfloat16)
        activated = activated.astype(jnp.bfloat16)
    row_gates = jnp.swapaxes(row_gates.reshape(experts_local, ranks, SLOTS), 0, 1)
    own_gates = jnp.sum(jnp.where(picked, row_gates[..., None], 0.0), axis=2)
    if near:
        grad_feed_part = restore(
            spread_plain, [grad_gate, grad_up], [gate_weight, up_weight], (True, True)
        )
        grad_feed, gates_in, grad_gate_weight, grad_up_weight, grad_down_weight = feed_back(
            grad_feed_part, own_gates, expert_rows, grad_gate, grad_up, weighted_act, expert_grads, 3
        )
        grad_gate_weight, grad_up_weight, grad_down_weight = widen_all(
            grad_gate_weight, grad_up_weight, grad_down_weight
        )
        gates_in = jnp.sum(gates_in.reshape(-1, rows_count, experts_local, tokens), axis=1)
        grad_probs = gates_in.reshape(experts, tokens).T
    else:
        own_gates = lax.psum_scatter(
            jnp.swapaxes(own_gates, 1, 2).reshape(-1, rows_count, tokens, experts_local),
            "row",
            scatter_dimension=1,
        )
        grad_probs = lax.all_to_all(own_gates, "col", split_axis=0, concat_axis=2, tiled=True)[0]
        back_rows = (
            jnp.einsum("erf,edf->erd", grad_gate, gate_weight, preferred_element_type=jnp.float32)
            + jnp.einsum("erf,edf->erd", grad_up, up_weight, preferred_element_type=jnp.float32)
        ).astype(jnp.bfloat16)
        grad_feed = return_rows(spread_plain, back_rows).astype(jnp.float32)
        out_rows = jnp.einsum(
            "erf,efd->erd", activated, down_weight, preferred_element_type=jnp.float32
        ).astype(jnp.bfloat16)
        mixture = return_rows(spread_probs, out_rows).astype(jnp.float32)
        grad_gate_weight = jnp.einsum(
            "erd,erf->edf", expert_rows, grad_gate, preferred_element_type=jnp.float32
        )
        grad_up_weight = jnp.einsum(
            "erd,erf->edf", expert_rows, grad_up, preferred_element_type=jnp.float32
        )
        grad_down_weight = jnp.einsum(
            "erf,erd->efd", weighted_act, expert_grads, preferred_element_type=jnp.float32
        )
    grad_out = cotangent.astype(jnp.float32)
    grad_logits = (
        router_probs * (grad_probs - jnp.sum(router_probs * grad_probs, axis=-1, keepdims=True))
    ).astype(jnp.bfloat16)
    router_grad = inner_rows(feed_normed, grad_logits)
    grad_feed = grad_feed + outer_cols(grad_logits, router_full)
    feed_gain_term = jnp.sum(grad_feed * hidden * feed_scale, axis=0)
    feed_weighted = grad_feed * feed_float
    grad_hidden = (
        grad_out
        + feed_scale * feed_weighted
        - hidden * feed_scale**3 * jnp.mean(feed_weighted * hidden, axis=-1, keepdims=True)
    )
    if near:
        mixture_part, grad_branch = restore_out(
            spread_probs, activated, down_weight, grad_hidden.astype(jnp.bfloat16), 6
        )
    else:
        grad_branch = lax.all_gather(grad_hidden.astype(jnp.bfloat16), "row", axis=0, tiled=True)
    output_grad = inner_rows(mixed_heads, grad_branch)
    grad_mixed = outer_cols(grad_branch, output_full).astype(jnp.bfloat16)
    (
        grad_value_low, query_weighted, key_weighted, query_gain_term, key_gain_term, query_inner, key_inner
    ) = attend_back(
        queries, keys_rotated, values, grad_mixed, lse_all, raw, query_rs, key_rs,
        query_gain_f, key_gain_f, cosine, sine_table,
    )
    query_gain_term, key_gain_term = query_gain_term.reshape(-1), key_gain_term.reshape(-1)
    query_inner, key_inner = (
        lax.psum(jnp.sum(query_inner, axis=(0, 2)), "row"),
        lax.psum(jnp.sum(key_inner, axis=(0, 2)), "row"),
    )
    grad_query_raw = (
        query_rs * query_weighted - query_raw * query_rs**3 * (query_inner / model_width)[:, None]
    ).astype(jnp.bfloat16)
    grad_key_raw = (
        key_rs * key_weighted - key_raw * key_rs**3 * (key_inner / model_width)[:, None]
    ).astype(jnp.bfloat16)
    raw_grads = jnp.concatenate([grad_query_raw, grad_key_raw, grad_value_low], axis=1)
    qkv_grad = inner_rows(normed, raw_grads)
    grad_normed = outer_cols(raw_grads, qkv_full)
    attention_weighted = grad_normed * attention_float
    grad_seq_part = seq_scale * attention_weighted - seq_float * seq_scale**3 * jnp.mean(
        attention_weighted * seq_float, axis=-1, keepdims=True
    )
    attention_gain_term = jnp.sum(grad_normed * seq_float * seq_scale, axis=0)
    if near:
        cols = lax.axis_size("col")
        pack = jnp.concatenate(
            [
                attention_gain_term.reshape(cols, -1),
                feed_gain_term.reshape(cols, -1),
                query_gain_term.reshape(cols, -1),
                key_gain_term.reshape(cols, -1),
                router_grad.reshape(cols, -1),
            ],
            axis=1,
        )
        pack = jnp.pad(pack, ((0, 0), (0, PACK_ROWS * 128 - pack.shape[1])))
        pack = pack.astype(jnp.bfloat16).reshape(cols, PACK_ROWS, 128)
        (
            mixture, summed, grad_query_weight, grad_key_weight, grad_value_weight, grad_output_weight, packs
        ) = finish_near(
            mixture_part,
            grad_seq_part.astype(jnp.bfloat16).reshape(rows_count, tokens, model_width),
            [grad.astype(jnp.bfloat16) for grad in (qkv_grad, output_grad)],
            pack,
            4,
        )
        input_grad = grad_hidden + summed
        packs = packs.reshape(cols, rows_count, -1).astype(jnp.float32)
        whole = jnp.sum(packs, axis=(0, 1))
        heads_sum = jnp.sum(
            lax.dynamic_index_in_dim(packs, lax.axis_index("row"), 1, keepdims=False), axis=0
        )
        grad_attention_gain = whole[: ends[0]]
        grad_feed_gain = whole[ends[0] : ends[1]]
        grad_query_gain = heads_sum[ends[1] : ends[2]]
        grad_key_gain = heads_sum[ends[2] : ends[3]]
        grad_router_weight = whole[ends[3] : ends[3] + router_weight.size].reshape(router_weight.shape)
    else:
        stacked = jnp.concatenate(
            [
                grad_seq_part.reshape(rows_count, tokens, model_width),
                jnp.broadcast_to(attention_gain_term[None, None, :], (rows_count, 1, model_width)),
            ],
            axis=1,
        ).reshape(rows_count * (tokens + 1), model_width)
        summed = lax.psum_scatter(
            stacked.astype(jnp.bfloat16), "row", scatter_dimension=0, tiled=True
        ).astype(jnp.float32)
        input_grad = grad_hidden + summed[:tokens]
        attention_gain_total = summed[tokens]
        query_grad, key_grad, value_grad = jnp.split(qkv_grad, 3, axis=1)
        feed_gain_total, router_total = (
            lax.psum(feed_gain_term.astype(jnp.bfloat16), "row").astype(jnp.float32),
            lax.psum(router_grad.astype(jnp.bfloat16), "row").astype(jnp.float32),
        )
        (
            grad_attention_gain,
            grad_query_gain,
            grad_key_gain,
            grad_query_weight,
            grad_key_weight,
            grad_value_weight,
            grad_output_weight,
            grad_feed_gain,
            grad_router_weight,
        ) = (
            lax.psum_scatter(
                attention_gain_total.astype(jnp.bfloat16), "col", scatter_dimension=0, tiled=True
            ).astype(jnp.float32),
            lax.psum_scatter(
                query_gain_term.astype(jnp.bfloat16), "col", scatter_dimension=0, tiled=True
            ).astype(jnp.float32),
            lax.psum_scatter(
                key_gain_term.astype(jnp.bfloat16), "col", scatter_dimension=0, tiled=True
            ).astype(jnp.float32),
            lax.psum_scatter(
                query_grad.astype(jnp.bfloat16), "col", scatter_dimension=0, tiled=True
            ).astype(jnp.float32),
            lax.psum_scatter(
                key_grad.astype(jnp.bfloat16), "col", scatter_dimension=0, tiled=True
            ).astype(jnp.float32),
            lax.psum_scatter(
                value_grad.astype(jnp.bfloat16), "col", scatter_dimension=0, tiled=True
            ).astype(jnp.float32),
            lax.psum_scatter(
                output_grad.astype(jnp.bfloat16), "col", scatter_dimension=1, tiled=True
            ).astype(jnp.float32),
            lax.psum_scatter(
                feed_gain_total.astype(jnp.bfloat16), "col", scatter_dimension=0, tiled=True
            ).astype(jnp.float32),
            lax.psum_scatter(
                router_total.astype(jnp.bfloat16), "col", scatter_dimension=0, tiled=True
            ).astype(jnp.float32),
        )
    layer_output = hidden + mixture
    return (
        layer_output,
        input_grad,
        grad_attention_gain,
        grad_query_gain,
        grad_key_gain,
        grad_query_weight,
        grad_key_weight,
        grad_value_weight,
        grad_output_weight,
        grad_feed_gain,
        grad_router_weight,
        grad_gate_weight,
        grad_up_weight,
        grad_down_weight,
    )


def solution(mesh):
    placed = (
        P(("col", "row"), None),
        P(("col", "row"), None),
        P(("col", "row"), None),
        P("col"),
        P(("row", "col")),
        P(("row", "col")),
        P("col", "row"),
        P("col", "row"),
        P("col", "row"),
        P("row", "col"),
        P("col"),
        P("col", None),
        P("col", None, "row"),
        P("col", None, "row"),
        P("col", "row", None),
    )
    return jax.shard_map(
        local,
        mesh=mesh,
        in_specs=placed,
        out_specs=(
            P(("col", "row"), None),
            P(("col", "row"), None),
            P("col"),
            P(("row", "col")),
            P(("row", "col")),
            P("col", "row"),
            P("col", "row"),
            P("col", "row"),
            P("row", "col"),
            P("col"),
            P("col", None),
            P("col", None, "row"),
            P("col", None, "row"),
            P("col", "row", None),
        ),
        check_vma=False,
    )
```

```python
import functools

import jax
import jax.numpy as jnp
from jax import lax
from jax.experimental import pallas as pl
from jax.experimental.pallas import tpu as pltpu
from jax.sharding import PartitionSpec as P

HD = 128
SLOTS = 40
BLOCK = 512
CHUNK = 256
UNROLL = 4
PACK_ROWS = 144


EPS = 1e-05
THETA = 10000.0
MASKED = -1e30


def wide_dot(left, right):
    return jnp.dot(left, right, preferred_element_type=jnp.float32)


def inner_rows(left, right):
    return lax.dot_general(
        left, right, (((0,), (0,)), ((), ())), preferred_element_type=jnp.float32
    )


def outer_cols(left, right):
    return lax.dot_general(
        left, right, (((1,), (1,)), ((), ())), preferred_element_type=jnp.float32
    )


def rms_scale(field):
    return lax.rsqrt(jnp.mean(field * field, axis=-1, keepdims=True) + EPS)


def rope_tables(length):
    half_size = HD // 2
    freqs = THETA ** (-(jnp.arange(half_size, dtype=jnp.float32) * 2.0) / HD)
    angles = jnp.arange(length, dtype=jnp.float32)[:, None] * freqs[None, :]
    cosine = jnp.concatenate([jnp.cos(angles), jnp.cos(angles)], axis=-1)
    sine_table = jnp.concatenate([-jnp.sin(angles), jnp.sin(angles)], axis=-1)
    return (cosine, sine_table)


def dispatch_body(pick_ref, field_ref, rows_ref):
    groups = rows_ref.shape[0]
    first = wide_dot(pick_ref[0], field_ref[0]).reshape(groups, SLOTS, -1)
    second = wide_dot(pick_ref[1], field_ref[1]).reshape(groups, SLOTS, -1)
    rows_ref[...] = jnp.concatenate([first, second], axis=1).astype(jnp.bfloat16)


def dispatch(pick, field):
    ranks, width, tokens = pick.shape
    groups, depth = width // SLOTS, field.shape[1]
    return pl.pallas_call(
        dispatch_body,
        grid=(ranks // 2, depth // BLOCK),
        in_specs=[
            pl.BlockSpec((2, width, tokens), lambda i, k: (i, 0, 0)),
            pl.BlockSpec((2, tokens, BLOCK), lambda i, k: (i, 0, k)),
        ],
        out_specs=pl.BlockSpec((groups, 2 * SLOTS, BLOCK), lambda i, k: (0, i, k)),
        out_shape=jax.ShapeDtypeStruct((groups, ranks * SLOTS, depth), jnp.bfloat16),
    )(pick, field.reshape(ranks, tokens, depth))


def combine_body(spread_ref, rows_ref, field_ref):
    rows = rows_ref[...].astype(jnp.float32)
    width = rows.shape[0] * SLOTS
    for side in range(2):
        part = rows[:, side * SLOTS : (side + 1) * SLOTS].reshape(width, -1).astype(jnp.bfloat16)
        field_ref[side] = wide_dot(spread_ref[side], part).astype(jnp.bfloat16)


def combine(spread, rows):
    ranks, tokens, width = spread.shape
    groups, depth = width // SLOTS, rows.shape[2]
    field = pl.pallas_call(
        combine_body,
        grid=(ranks // 2, depth // BLOCK),
        in_specs=[
            pl.BlockSpec((2, tokens, width), lambda i, k: (i, 0, 0)),
            pl.BlockSpec((groups, 2 * SLOTS, BLOCK), lambda i, k: (0, i, k)),
        ],
        out_specs=pl.BlockSpec((2, tokens, BLOCK), lambda i, k: (i, 0, k)),
        out_shape=jax.ShapeDtypeStruct((ranks, tokens, depth), jnp.bfloat16),
    )(spread, rows)
    return field.reshape(ranks * tokens, depth)


def scatter_all(field):
    part = lax.psum_scatter(field, "col", scatter_dimension=0, tiled=True)
    return lax.psum_scatter(part, "row", scatter_dimension=0, tiled=True)


def pieces_of(ranks, depth):
    count = max(1, ranks // 32)
    step = depth // count
    return [(at, at + step) for at in range(0, depth, step)]


def gather_rows(pick, field):
    rows = []
    for start, stop in pieces_of(pick.shape[0], field.shape[1]):
        part = field[:, start:stop]
        if rows:
            part = lax.optimization_barrier((part, rows[-1]))[0]
        whole = lax.all_gather(part, ("col", "row"), axis=0, tiled=True)
        rows.append(dispatch(pick, whole))
    return rows[0] if len(rows) == 1 else jnp.concatenate(rows, axis=2)


def return_rows(spread, rows):
    sums = []
    for start, stop in pieces_of(spread.shape[0], rows.shape[2]):
        part = rows[:, :, start:stop]
        if sums:
            part = lax.optimization_barrier((part, sums[-1]))[0]
        sums.append(scatter_all(combine(spread, part)))
    return sums[0] if len(sums) == 1 else jnp.concatenate(sums, axis=1)


MESH = pl.DeviceIdType.MESH


def seat():
    r, c = lax.axis_index("row"), lax.axis_index("col")
    y, x = r // 2, r % 2
    z, core = c // 2, c % 2
    first = y * (1 - core) + x * core
    second = x * (1 - core) + y * core
    return r, c, y, x, z, core, first, second


def partners():
    r, c, y, x, z, core, first, second = seat()
    pair = (r, z * 2 + (1 - core))
    flip_y = (1 - y) * 2 + x
    flip_x = y * 2 + (1 - x)
    along_first = (flip_y * (1 - core) + flip_x * core, c)
    along_second = (flip_x * (1 - core) + flip_y * core, c)
    up = [(r, ((z + k) % 4) * 2 + core) for k in range(1, 4)]
    return pair, along_first, along_second, up


RANKS = 32


def nth(offset):
    spot = (lax.axis_index("col") * 4 + lax.axis_index("row") + offset) % RANKS
    return spot, (spot % 4, spot // 4)


def meet():
    barrier = pltpu.get_barrier_semaphore()

    @pl.loop(1, RANKS)
    def _(offset):
        pl.semaphore_signal(barrier, inc=1, device_id=nth(offset)[1], device_id_type=MESH)

    pl.semaphore_wait(barrier, RANKS - 1)


def small_copy(src_of, small_all, small_send, small_recv, offset):
    spot, device = nth(offset)
    return send(
        src_of(spot), small_all.at[nth(0)[0]], small_send.at[offset], small_recv.at[offset], device
    )


def row_of(core, first, second):
    y = first * (1 - core) + second * core
    x = second * (1 - core) + first * core
    return y, x


def send(src, dst, send_sem, recv_sem, device):
    return pltpu.make_async_remote_copy(
        src_ref=src, dst_ref=dst, send_sem=send_sem, recv_sem=recv_sem, device_id=device, device_id_type=MESH
    )


GSTEPS = 8
QUEUE = (2, 1, 3)
ARRIVE = (1, 3, 2)


def spread_out(own_ref, all_ref, sems):
    r, c, y, x, z, core, first, second = seat()
    pair, along_first, along_second, up = partners()
    here_sem, u_send, u_recv, d_send, d_recv, g_send, g_recv, f_send, f_recv, p_send, p_recv = sems
    step = own_ref.shape[0] // GSTEPS

    def rows(q):
        return pl.ds(pl.multiple_of(q * step, step), step)

    def place(k, s, f, q):
        sec = second * (1 - s) + (1 - second) * s
        fir = first * (1 - f) + (1 - first) * f
        yy, xx = row_of(core, fir, sec)
        return all_ref.at[(z + 4 - k) % 4, core, yy, xx, rows(q)]

    above, below = (r, ((z + 1) % 4) * 2 + core), (r, ((z + 3) % 4) * 2 + core)

    def source(k, q):
        return own_ref.at[rows(q)] if k == 0 else place(k, 0, 0, q)

    def up_copy(d, q):
        return send(source(d, q), place(d, 0, 0, q), u_send.at[d, q], u_recv.at[d, q], above)

    def down_copy(d, q):
        k = (4 - d) % 4
        return send(source(k, q), place(k, 0, 0, q), d_send.at[d, q], d_recv.at[d, q], below)

    def came_up(d, q):
        there = place(d, 0, 0, q)
        return send(there, there, u_send.at[d - 1, q], u_recv.at[d - 1, q], above)

    def came_down(d, q):
        there = place(4 - d, 0, 0, q)
        return send(there, there, d_send.at[d - 1, q], d_recv.at[d - 1, q], below)

    bottom, top = 1 - jnp.minimum(z, 1), z // 3
    arrived = [bottom * (3 - i) + top * (1 + i) + (1 - bottom - top) * ARRIVE[i] for i in range(3)]

    def g_copy(k, q, src):
        return send(src, place(k, 0, 0, q), g_send.at[k, q], g_recv.at[k, q], along_second)

    def f_copy(k, s, q, src):
        return send(src, place(k, s, 0, q), f_send.at[s, k, q], f_recv.at[s, k, q], along_first)

    def p_copy(k, s, f, q, src):
        return send(src, place(k, s, f, q), p_send.at[f, s, k, q], p_recv.at[f, s, k, q], pair)

    here = pltpu.make_async_copy(own_ref, all_ref.at[z, core, y, x], here_sem)

    def begin():
        here.start()

        @pl.loop(0, GSTEPS)
        def _(q):
            src = own_ref.at[rows(q)]

            @pl.when(z < 3)
            def _():
                up_copy(0, q).start()

            @pl.when(z > 0)
            def _():
                down_copy(0, q).start()

            g_copy(0, q, src).start()
            f_copy(0, 0, q, src).start()
            p_copy(0, 0, 0, q, src).start()

    def along_z(q):
        def pass_on(k):
            src = place(k, 0, 0, q)
            g_copy(k, q, src).start()
            f_copy(k, 0, q, src).start()
            p_copy(k, 0, 0, q, src).start()

        for d in (1, 2, 3):

            @pl.when(z >= d)
            def _():
                came_up(d, q).wait_recv()
                if d < 3:

                    @pl.when(z < 3)
                    def _():
                        up_copy(d, q).start()

                pass_on(d)

            @pl.when(z + d <= 3)
            def _():
                came_down(d, q).wait_recv()
                if d < 3:

                    @pl.when(z > 0)
                    def _():
                        down_copy(d, q).start()

                pass_on(4 - d)

    def forward(q, between=None):
        @pl.when(q == 0)
        def _():
            along_z(q)

        @pl.when(q + 1 < GSTEPS)
        def _():
            along_z(q + 1)

        if between is not None:
            between()

        for k in (0, *arrived):
            src = place(k, 1, 0, q)
            g_copy(k, q, src).wait_recv()
            f_copy(k, 1, q, src).start()
            p_copy(k, 1, 0, q, src).start()
        for k in (0, *arrived):
            src = place(k, 0, 1, q)
            f_copy(k, 0, q, src).wait_recv()
            p_copy(k, 0, 1, q, src).start()

    def finish():
        @pl.loop(0, GSTEPS)
        def _(q):
            for k in (0, *arrived):
                src = place(k, 1, 1, q)
                f_copy(k, 1, q, src).wait_recv()
                p_copy(k, 1, 1, q, src).start()

        here.wait()

        @pl.loop(0, GSTEPS)
        def _(q):
            for d in range(3):

                @pl.when((z < 3) & (z >= d))
                def _():
                    up_copy(d, q).wait_send()

                @pl.when((z > 0) & (z + d <= 3))
                def _():
                    down_copy(d, q).wait_send()

            for k in range(4):
                src = own_ref.at[rows(q)]
                g_copy(k, q, src).wait_send()
                for s in range(2):
                    f_copy(k, s, q, src).wait_send()
                    for f in range(2):
                        p_copy(k, s, f, q, src).wait()

    return begin, forward, finish


def spread_sems():
    dma = pltpu.SemaphoreType.DMA
    shapes = [(3, GSTEPS), (3, GSTEPS), (4, GSTEPS), (2, 4, GSTEPS), (2, 2, 4, GSTEPS)]
    return [dma(())] + [dma(shape) for shape in shapes for _ in range(2)]


def small_out(small_ref, small_all, sems):
    here_sem, small_send, small_recv = sems
    local = pltpu.make_async_copy(small_ref, small_all.at[nth(0)[0]], here_sem)

    def copy(offset):
        return small_copy(lambda spot: small_ref, small_all, small_send, small_recv, offset)

    def begin():
        local.start()

        @pl.loop(1, RANKS)
        def _(offset):
            copy(offset).start()

    def finish():
        local.wait()

        @pl.loop(1, RANKS)
        def _(offset):
            copy(offset).wait()

    return begin, finish


def small_sems():
    dma = pltpu.SemaphoreType.DMA
    return [dma(()), dma((RANKS,)), dma((RANKS,))]


ANYWHERE = pl.BlockSpec(memory_space=pl.ANY)


def start_body(x_ref, q_ref, k_ref, v_ref, o_ref, pack_ref, own_ref, small_ref,
               x_all, qkv_all, o_all, pack_all, all_ref, small_all, *sems):
    r, c, y, x, z, core, first, second = seat()
    pair, along_first, along_second, up = partners()
    begin, forward, finish = spread_out(own_ref, all_ref, sems[:11])
    small_begin, small_finish = small_out(small_ref, small_all, sems[11:14])
    here_sem, x_send, x_recv, w_send, w_recv, v_send, v_recv = sems[14:]
    weights = [(q_ref, qkv_all), (k_ref, qkv_all), (v_ref, qkv_all), (o_ref, o_all), (pack_ref, pack_all)]

    def block(index, col):
        ref, whole = weights[index]
        if index == 4:
            return whole.at[col]
        if index == 3:
            width = ref.shape[1]
            return whole.at[:, pl.ds(pl.multiple_of(col * width, width), width)]
        height, width = ref.shape
        return whole.at[pl.ds(pl.multiple_of(col * height, height), height), pl.ds(index * width, width)]

    def w_copy(index, k):
        return send(
            weights[index][0], block(index, c), w_send.at[index, k - 1], w_recv.at[index, k - 1], up[k - 1]
        )

    def pair_copy(index, k):
        col = ((z + 4 - k) % 4) * 2 + core
        src = weights[index][0] if k == 0 else block(index, col)
        return send(src, block(index, col), v_send.at[index, k], v_recv.at[index, k], pair)

    locals_ = [pltpu.make_async_copy(x_ref, x_all.at[r], here_sem.at[5])] + [
        pltpu.make_async_copy(weights[i][0], block(i, c), here_sem.at[i]) for i in range(5)
    ]
    y1, x1 = row_of(core, first, 1 - second)
    near_row = y1 * 2 + x1
    x_first = send(x_ref, x_all.at[r], x_send.at[0], x_recv.at[0], along_first)
    x_second = send(x_ref, x_all.at[r], x_send.at[1], x_recv.at[1], along_second)
    x_relay = send(x_all.at[near_row], x_all.at[near_row], x_send.at[2], x_recv.at[2], along_first)

    meet()
    small_begin()
    x_second.start()
    x_first.start()
    begin()
    for item in locals_:
        item.start()
    x_second.wait_recv()
    x_relay.start()
    def weights_out(group):
        for index in group:
            for k in QUEUE:
                w_copy(index, k).start()
            pair_copy(index, 0).start()

    @pl.loop(0, GSTEPS)
    def _(q):
        def between():
            for at, group in enumerate(((4,), (0,), (1,), (2,), (3,))):

                @pl.when(q == at)
                def _(group=group):
                    weights_out(group)

        forward(q, between)

    for index in (4, 0, 1, 2, 3):
        for k in ARRIVE:
            w_copy(index, k).wait_recv()
            pair_copy(index, k).start()
    finish()
    small_finish()
    for item in locals_:
        item.wait()
    x_first.wait()
    x_second.wait_send()
    x_relay.wait()
    for index in range(5):
        for k in range(4):
            if k:
                w_copy(index, k).wait_send()
            pair_copy(index, k).wait()


def start_near(x, weights, pack, own, small, collective_id):
    tokens, depth = own.shape
    dma = pltpu.SemaphoreType.DMA
    height, width = weights[0].shape
    shaped = lambda shape, like: jax.ShapeDtypeStruct(shape, like.dtype)
    outs = pl.pallas_call(
        start_body,
        out_shape=(
            shaped((4, *x.shape), x),
            shaped((8 * height, 3 * width), weights[0]),
            shaped((weights[3].shape[0], 8 * weights[3].shape[1]), weights[3]),
            shaped((8, *pack.shape), pack),
            shaped((4, 2, 2, 2, tokens, depth), own),
            shaped((RANKS, *small.shape), small),
        ),
        in_specs=[ANYWHERE] * 8,
        out_specs=[ANYWHERE] * 6,
        scratch_shapes=spread_sems()
        + small_sems()
        + [dma((6,)), dma((3,)), dma((3,)), dma((5, 3)), dma((5, 3)), dma((5, 4)), dma((5, 4))],
        compiler_params=pltpu.CompilerParams(collective_id=collective_id, has_side_effects=True),
    )(x, *weights, pack, own, small)
    x_all, qkv, o, pack_all, whole, small_all = outs
    return x_all.reshape(-1, x.shape[1]), qkv, o, pack_all, whole.reshape(RANKS, tokens, depth), small_all


def finish_body(part_ref, field_ref, qkv_ref, o_ref, pack_ref,
                mixture_ref, out_ref, q_out, k_out, v_out, o_out, pack_all,
                mine, first_in, second_in, total,
                qkv_mine, o_mine, qkv_pair, o_pair, qkv_z, o_z, qkv_sum, o_sum,
                load_sem, f_send, f_recv, g_send, g_recv, w_load, p_send, p_recv, z_send, z_recv, out_sem,
                *rest):
    r, c, y, x, z, core, first, second = seat()
    pair, along_first, along_second, up = partners()
    small_begin, small_finish = small_each(pack_ref, pack_all, rest[:3], lambda spot: spot // 4)
    begin, tick, finish = shrink(part_ref, *rest[3:9], rest[9:18])
    mixture = rest[8]
    tokens, depth = out_ref.shape
    other = 1 - core
    grads, kept, pairs = [qkv_ref, o_ref], [qkv_mine, o_mine], [qkv_pair, o_pair]
    zs, sums = [qkv_z, o_z], [qkv_sum, o_sum]
    width = q_out.shape[1]
    results = [
        [
            pltpu.make_async_copy(qkv_sum.at[:, pl.ds(i * width, width)], out, out_sem.at[i])
            for i, out in enumerate((q_out, k_out, v_out))
        ],
        [pltpu.make_async_copy(o_sum, o_out, out_sem.at[3])],
    ]

    def block(index, col):
        ref = grads[index]
        if index == 1:
            width = ref.shape[1] // 8
            return ref.at[:, pl.ds(pl.multiple_of(col * width, width), width)]
        height = ref.shape[0] // 8
        return ref.at[pl.ds(pl.multiple_of(col * height, height), height)]

    def row(fir, sec):
        yy, xx = row_of(core, fir, sec)
        return yy * 2 + xx

    def load(fir, sec):
        return pltpu.make_async_copy(field_ref.at[row(fir, sec)], mine.at[fir, sec], load_sem.at[fir, sec])

    def f_copy(sec):
        return send(field_ref.at[row(1 - first, sec)], first_in.at[sec], f_send.at[sec], f_recv.at[sec], along_first)

    g_copy = send(mine.at[first, 1 - second], second_in, g_send, g_recv, along_second)

    def w_load_copy(index, zz):
        return pltpu.make_async_copy(block(index, zz * 2 + core), kept[index].at[zz], w_load.at[index, zz])

    def w_give(index, zz):
        return send(
            block(index, zz * 2 + other), pairs[index].at[zz], p_send.at[index, zz], p_recv.at[index, zz], pair
        )

    above, below = (r, ((z + 1) % 4) * 2 + core), (r, ((z + 3) % 4) * 2 + core)

    def up_copy(index, dest):
        return send(
            kept[index].at[dest], zs[index].at[dest], z_send.at[index, dest], z_recv.at[index, dest], above
        )

    def down_copy(index, dest, slot):
        return send(kept[index].at[dest], zs[index].at[slot], z_send.at[index, dest], z_recv.at[index, slot], below)

    def chain(stage):
        @pl.when(z == stage)
        def _():
            for index in range(2):
                for dest in range(3, stage, -1):
                    if stage > 0:
                        up_copy(index, dest).wait_recv()
                        add(kept[index].at[dest], [zs[index].at[dest]])
                    up_copy(index, dest).start()

        @pl.when(z == 3 - stage)
        def _():
            for index in range(2):
                for dest in range(3 - stage):
                    if stage > 0:
                        down_copy(index, dest, dest).wait_recv()
                        add(kept[index].at[dest], [zs[index].at[dest]])
                    down_copy(index, dest, 4 if dest == 2 - stage else dest).start()

    def add(ref, extras):
        @pl.loop(0, ref.shape[0] // TILE)
        def _(t):
            here = pl.ds(pl.multiple_of(t * TILE, TILE), TILE)
            value = ref[here].astype(jnp.float32)
            for extra in extras:
                value = value + extra[here].astype(jnp.float32)
            ref[here] = value.astype(jnp.bfloat16)

    def add_out(ref, extras, result):
        @pl.loop(0, ref.shape[0] // TILE)
        def _(t):
            here = pl.ds(pl.multiple_of(t * TILE, TILE), TILE)
            value = ref[here].astype(jnp.float32)
            for extra in extras:
                value = value + extra[here].astype(jnp.float32)
            result[here] = value

    meet()
    for index in range(2):
        for k in (2, 1, 3, 0):
            w_give(index, (z + k) % 4).start()
            w_load_copy(index, (z + k) % 4).start()
    begin()
    f_copy(1 - second).start()
    f_copy(second).start()
    load(first, 1 - second).start()
    load(first, second).start()
    small_begin()
    for index in range(2):
        for k in (2, 1, 3, 0):
            zz = (z + k) % 4
            w_load_copy(index, zz).wait()
            w_give(index, zz).wait_recv()
            add(kept[index].at[zz], [pairs[index].at[zz]])
    chain(0)

    @pl.loop(0, RSTEPS + LAGS[2])
    def _(i):
        tick(i)

        @pl.when(i == 4)
        def _():
            chain(1)

        @pl.when(i == 8)
        def _():
            chain(2)

        @pl.when(i == 2)
        def _():
            load(first, 1 - second).wait()
            f_copy(1 - second).wait_recv()
            add(mine.at[first, 1 - second], [first_in.at[1 - second]])
            g_copy.start()

    for index in range(2):
        @pl.when(z == 0)
        def _():
            down_copy(index, 0, 4).wait_recv()
            add_out(kept[index].at[z], [zs[index].at[4]], sums[index])

        @pl.when(z == 3)
        def _():
            up_copy(index, 3).wait_recv()
            add_out(kept[index].at[z], [zs[index].at[3]], sums[index])

        @pl.when((z > 0) & (z < 3))
        def _():
            up_copy(index, z).wait_recv()
            down_copy(index, z, 4).wait_recv()
            add_out(kept[index].at[z], [zs[index].at[z], zs[index].at[4]], sums[index])

        for result in results[index]:
            result.start()
    load(first, second).wait()
    f_copy(second).wait_recv()
    g_copy.wait_recv()
    add_out(mine.at[first, second], [first_in.at[second], second_in], total)
    pltpu.make_async_copy(total, out_ref, out_sem.at[4]).start()

    @pl.loop(RSTEPS + LAGS[2], TICKS)
    def _(i):
        tick(i)

    pltpu.make_async_copy(mixture, mixture_ref, out_sem.at[5]).start()
    finish()
    for sec in range(2):
        f_copy(sec).wait_send()
    g_copy.wait_send()
    for index in range(2):
        for k in range(4):
            w_give(index, (z + k) % 4).wait_send()
            if k:
                up_copy(index, (z + k) % 4).wait_send()
        for result in results[index]:
            result.wait()
    small_finish()
    pltpu.make_async_copy(total, out_ref, out_sem.at[4]).wait()
    pltpu.make_async_copy(mixture, mixture_ref, out_sem.at[5]).wait()


def finish_near(part, field, grads, pack, collective_id):
    rows_count, tokens, depth = field.shape
    dma = pltpu.SemaphoreType.DMA
    blocks = [(grads[0].shape[0] // 8, grads[0].shape[1]), (grads[1].shape[0], grads[1].shape[1] // 8)]
    results = [(blocks[0][0], blocks[0][1] // 3)] * 3 + [blocks[1]]
    half = lambda *shape: pltpu.VMEM(shape, jnp.bfloat16)
    return pl.pallas_call(
        finish_body,
        out_shape=(
            jax.ShapeDtypeStruct((tokens, depth), jnp.float32),
            jax.ShapeDtypeStruct((tokens, depth), jnp.float32),
            *[jax.ShapeDtypeStruct(b, jnp.float32) for b in results],
            jax.ShapeDtypeStruct((RANKS, *pack.shape[1:]), pack.dtype),
        ),
        in_specs=[ANYWHERE] * 5,
        out_specs=[ANYWHERE] * 7,
        scratch_shapes=[
            half(2, 2, tokens, depth), half(2, tokens, depth), half(tokens, depth),
            pltpu.VMEM((tokens, depth), jnp.float32),
            *[half(4, *b) for b in blocks], *[half(4, *b) for b in blocks], *[half(5, *b) for b in blocks],
            *[pltpu.VMEM(b, jnp.float32) for b in blocks],
            dma((2, 2)), dma((2,)), dma((2,)), dma(()), dma(()),
            dma((2, 4)), dma((2, 4)), dma((2, 4)), dma((2, 4)), dma((2, 5)), dma((6,)),
        ]
        + small_sems()
        + shrink_scratch(tokens, depth),
        compiler_params=pltpu.CompilerParams(
            collective_id=collective_id, has_side_effects=True, vmem_limit_bytes=63 * 1024 * 1024
        ),
    )(part.reshape(4, 2, 2, 2, tokens, depth), field, *grads, pack)


RSTEPS = 16
TILE = 16
LAGS = (0, 1, 3, 6)
TICKS = RSTEPS + LAGS[3]


def shrink(part_ref, sums, near_own, first_in, second_in, z_in, total, sems):
    r, c, y, x, z, core, first, second = seat()
    pair, along_first, along_second, up = partners()
    load_sem, p_send, p_recv, f_send, f_recv, g_send, g_recv, z_send, z_recv = sems
    tokens = total.shape[0]
    step = tokens // RSTEPS
    other = 1 - core

    def rows(q):
        return pl.ds(pl.multiple_of(q * step, step), step)

    def spot(kind):
        fir = (1 - first) if kind < 2 else first
        sec = (1 - second) if kind in (0, 2) else second
        return fir, sec

    def load(kind, q):
        yy, xx = row_of(core, *spot(kind))
        return pltpu.make_async_copy(
            part_ref.at[:, core, yy, xx, rows(q)], near_own.at[q % 2, kind], load_sem.at[kind, q % 2]
        )

    def give(fir, sec, q):
        yy, xx = row_of(other, fir, sec)
        return send(
            part_ref.at[:, other, yy, xx, rows(q)],
            sums.at[fir, sec, :, rows(q)],
            p_send.at[fir, sec, q],
            p_recv.at[fir, sec, q],
            pair,
        )

    def f_copy(sec, q):
        return send(
            sums.at[1 - first, sec, :, rows(q)],
            first_in.at[sec, :, rows(q)],
            f_send.at[sec, q],
            f_recv.at[sec, q],
            along_first,
        )

    def g_copy(q):
        return send(
            sums.at[first, 1 - second, :, rows(q)], second_in.at[:, rows(q)], g_send.at[q], g_recv.at[q], along_second
        )

    def z_copy(k, q):
        return send(
            sums.at[first, second, (z + k) % 4, rows(q)],
            z_in.at[k - 1, rows(q)],
            z_send.at[k - 1, q],
            z_recv.at[k - 1, q],
            up[k - 1],
        )

    def begin():
        @pl.loop(0, RSTEPS)
        def _(q):
            for fir, sec in ((1 - second, 1 - first), (1 - second, first), (second, 1 - first), (second, first)):
                give(fir, sec, q).start()

        for kind in range(4):
            load(kind, 0).start()

    def add(kind, q, extra):
        fir, sec = spot(kind)

        @pl.when(q + 1 < RSTEPS)
        def _():
            load(kind, q + 1).start()

        load(kind, q).wait()
        give(fir, sec, q).wait_recv()

        @pl.loop(0, 4 * (step // TILE))
        def _(t):
            zz, at = t // (step // TILE), t % (step // TILE)
            here = pl.ds(pl.multiple_of(q * step + at * TILE, TILE), TILE)
            near = pl.ds(pl.multiple_of(at * TILE, TILE), TILE)
            value = sums[fir, sec, zz, here].astype(jnp.float32)
            value = value + near_own[q % 2, kind, zz, near].astype(jnp.float32)
            for ref in extra:
                value = value + ref[zz, here].astype(jnp.float32)
            sums[fir, sec, zz, here] = value.astype(jnp.bfloat16)

    def stage_first(q):
        for kind, sec in ((0, 1 - second), (1, second)):
            add(kind, q, [])
            f_copy(sec, q).start()

    def stage_second(q):
        f_copy(1 - second, q).wait_recv()
        add(2, q, [first_in.at[1 - second]])
        g_copy(q).start()

    def stage_z(q):
        f_copy(second, q).wait_recv()
        g_copy(q).wait_recv()
        add(3, q, [first_in.at[second], second_in])
        for k in QUEUE:
            z_copy(k, q).start()

    def stage_out(q):
        for k in ARRIVE:
            z_copy(k, q).wait_recv()

        @pl.loop(0, step // TILE)
        def _(t):
            here = pl.ds(pl.multiple_of(q * step + t * TILE, TILE), TILE)
            value = sums[first, second, z, here].astype(jnp.float32)
            for k in range(3):
                value = value + z_in[k, here].astype(jnp.float32)
            total[here] = value

    def tick(i):
        for stage, lag in zip((stage_first, stage_second, stage_z, stage_out), LAGS):

            @pl.when((i >= lag) & (i < RSTEPS + lag))
            def _(stage=stage, lag=lag):
                stage(i - lag)

    def finish():
        @pl.loop(0, RSTEPS)
        def _(q):
            for fir in range(2):
                for sec in range(2):
                    give(fir, sec, q).wait_send()
            for sec in range(2):
                f_copy(sec, q).wait_send()
            g_copy(q).wait_send()
            for k in QUEUE:
                z_copy(k, q).wait_send()

    return begin, tick, finish


def shrink_scratch(tokens, depth):
    dma = pltpu.SemaphoreType.DMA
    low = lambda *shape: pltpu.VMEM((*shape, depth), jnp.bfloat16)
    buffers = [
        low(2, 2, 4, tokens), low(2, 4, 4, tokens // RSTEPS), low(2, 4, tokens), low(4, tokens), low(3, tokens),
        pltpu.VMEM((tokens, depth), jnp.float32),
    ]
    shapes = [(2, 2, RSTEPS), (2, RSTEPS), (RSTEPS,), (3, RSTEPS)]
    return buffers + [dma((4, 2))] + [dma(shape) for shape in shapes for _ in range(2)]


def small_each(small_ref, small_all, sems, pick):
    here_sem, small_send, small_recv = sems
    local = pltpu.make_async_copy(small_ref.at[pick(nth(0)[0])], small_all.at[nth(0)[0]], here_sem)

    def copy(offset):
        return small_copy(lambda spot: small_ref.at[pick(spot)], small_all, small_send, small_recv, offset)

    def begin():
        local.start()

        @pl.loop(1, RANKS)
        def _(offset):
            copy(offset).start()

    def finish():
        local.wait()

        @pl.loop(1, RANKS)
        def _(offset):
            copy(offset).wait()

    return begin, finish


def feed_back_body(part_ref, small_ref, rows_ref, gate_ref, up_ref, act_ref, grads_ref,
                   out_ref, small_all, gate_out, up_out, down_out, *scratch):
    begin, tick, finish = shrink(part_ref, *scratch[:6], scratch[6:15])
    total, out_sem = scratch[5], scratch[15]
    small_begin, small_finish = small_each(small_ref, small_all, scratch[16:], lambda spot: spot)
    e, k = pl.program_id(0), pl.program_id(1)
    step = e * pl.num_programs(1) + k
    last = pl.num_programs(0) * pl.num_programs(1) - 1

    @pl.when(step == 0)
    def _():
        meet()
        small_begin()
        begin()

    rows = rows_ref[0]
    gate_out[0] = inner_rows(rows, gate_ref[0]).astype(jnp.bfloat16)
    up_out[0] = inner_rows(rows, up_ref[0]).astype(jnp.bfloat16)
    down_out[0] = inner_rows(act_ref[0], grads_ref[0]).astype(jnp.bfloat16)

    for half in range(2):

        @pl.when(k == half * (pl.num_programs(1) // 2))
        def _():
            tick(2 * e + half)

    @pl.when(step == last)
    def _():
        @pl.loop(RSTEPS, TICKS)
        def _(i):
            tick(i)

        done = pltpu.make_async_copy(total, out_ref, out_sem)
        done.start()
        finish()
        small_finish()
        done.wait()


def feed_back(part, small, rows, grad_gate, grad_up, act, grads, collective_id):
    tokens, depth = part.shape[0] // RANKS, part.shape[1]
    groups, length, inner = grad_gate.shape
    assert 2 * groups == RSTEPS
    dma = pltpu.SemaphoreType.DMA
    slab = pl.BlockSpec((1, length, CHUNK), lambda e, k: (e, 0, k))
    held = pl.BlockSpec((1, length, inner), lambda e, k: (e, 0, 0))
    return pl.pallas_call(
        feed_back_body,
        grid=(groups, depth // CHUNK),
        in_specs=[ANYWHERE, ANYWHERE, slab, held, held, held, slab],
        out_specs=[
            ANYWHERE,
            ANYWHERE,
            pl.BlockSpec((1, CHUNK, inner), lambda e, k: (e, k, 0)),
            pl.BlockSpec((1, CHUNK, inner), lambda e, k: (e, k, 0)),
            pl.BlockSpec((1, inner, CHUNK), lambda e, k: (e, 0, k)),
        ],
        out_shape=(
            jax.ShapeDtypeStruct((tokens, depth), jnp.float32),
            jax.ShapeDtypeStruct(small.shape, small.dtype),
            jax.ShapeDtypeStruct((groups, depth, inner), jnp.bfloat16),
            jax.ShapeDtypeStruct((groups, depth, inner), jnp.bfloat16),
            jax.ShapeDtypeStruct((groups, inner, depth), jnp.bfloat16),
        ),
        scratch_shapes=shrink_scratch(tokens, depth) + [dma(())] + small_sems(),
        compiler_params=pltpu.CompilerParams(
            collective_id=collective_id, has_side_effects=True, vmem_limit_bytes=63 * 1024 * 1024
        ),
    )(part.reshape(4, 2, 2, 2, tokens, depth), small, rows, grad_gate, grad_up, act, grads)


def widen_body(*refs):
    half = len(refs) // 2
    for low, wide in zip(refs[:half], refs[half:]):
        wide[...] = low[...].astype(jnp.float32)


def widen_all(*arrays):
    specs = [pl.BlockSpec((1, *array.shape[1:]), lambda e: (e, 0, 0)) for array in arrays]
    return pl.pallas_call(
        widen_body,
        grid=(arrays[0].shape[0],),
        in_specs=specs,
        out_specs=specs,
        out_shape=[jax.ShapeDtypeStruct(array.shape, jnp.float32) for array in arrays],
        compiler_params=pltpu.CompilerParams(vmem_limit_bytes=40 * 1024 * 1024),
    )(*arrays)


def fill_rows(pick_ref, field_ref, rows_ref):
    ranks, groups = pick_ref.shape[0], rows_ref.shape[0]

    @pl.loop(0, ranks // 2, unroll=UNROLL)
    def _(i):
        parts = [
            wide_dot(pick_ref[2 * i + side], field_ref[2 * i + side]).reshape(groups, SLOTS, CHUNK)
            for side in range(2)
        ]
        here = pl.ds(pl.multiple_of(i * 2 * SLOTS, 2 * SLOTS), 2 * SLOTS)
        rows_ref[:, here] = jnp.concatenate(parts, axis=1).astype(jnp.bfloat16)


def add_products(k, rows_ref, pairs):
    groups = rows_ref.shape[0]

    def products(e, first):
        for product, total in pairs:
            term = product(rows_ref[e], e)
            if first:
                total[e] = term
            else:
                total[e] += term

    @pl.when(k == 0)
    def _():
        @pl.loop(0, groups)
        def _(e):
            products(e, True)

    @pl.when(k > 0)
    def _():
        @pl.loop(0, groups)
        def _(e):
            products(e, False)


def grads_in_body(pick_ref, field_ref, down_ref, own_ref, small_ref,
                  rows_ref, plain_ref, all_ref, small_all, total, *sems):
    begin, forward, finish = spread_out(own_ref, all_ref, sems[:11])
    small_begin, small_finish = small_out(small_ref, small_all, sems[11:])
    k, last = pl.program_id(0), pl.num_programs(0) - 1

    @pl.when(k == 0)
    def _():
        meet()
        small_begin()
        begin()

    fill_rows(pick_ref, field_ref, rows_ref)
    add_products(k, rows_ref, [(lambda rows, e: outer_cols(rows, down_ref[e]), total)])

    forward(k)

    @pl.when(k == last)
    def _():
        pltpu.sync_copy(total, plain_ref)
        finish()
        small_finish()


def grads_in(pick, field, down, own, small, collective_id):
    ranks, width, tokens = pick.shape
    groups, depth = width // SLOTS, field.shape[-1]
    length, inner = ranks * SLOTS, down.shape[1]
    steps = depth // CHUNK
    assert steps == GSTEPS
    rows, plain, whole, small_all = pl.pallas_call(
        grads_in_body,
        grid=(steps,),
        in_specs=[
            pl.BlockSpec((ranks, width, tokens), lambda k: (0, 0, 0), pipeline_mode=pl.Buffered(1)),
            pl.BlockSpec((ranks, tokens, CHUNK), lambda k: (0, 0, k)),
            pl.BlockSpec((groups, inner, CHUNK), lambda k: (0, 0, k)),
            ANYWHERE,
            ANYWHERE,
        ],
        out_specs=[pl.BlockSpec((groups, length, CHUNK), lambda k: (0, 0, k))] + [ANYWHERE] * 3,
        out_shape=[
            jax.ShapeDtypeStruct((groups, length, depth), jnp.bfloat16),
            jax.ShapeDtypeStruct((groups, length, inner), jnp.float32),
            jax.ShapeDtypeStruct((4, 2, 2, 2, *own.shape), own.dtype),
            jax.ShapeDtypeStruct((RANKS, *small.shape), small.dtype),
        ],
        scratch_shapes=[pltpu.VMEM((groups, length, inner), jnp.float32)] + spread_sems() + small_sems(),
        compiler_params=pltpu.CompilerParams(
            collective_id=collective_id, has_side_effects=True, vmem_limit_bytes=62 * 1024 * 1024
        ),
    )(pick, field, down, own, small)
    return rows, plain, whole.reshape(RANKS, *own.shape), small_all


def feed_in_body(steps, pick_ref, field_ref, gate_ref, up_ref, plain_ref, probs_ref,
                 rows_ref, act_ref, weighted_ref, grad_gate_ref, grad_up_ref, gates_ref, gate_sum, up_sum):
    k = pl.program_id(0)

    @pl.when(k < steps)
    def _():
        fill_rows(pick_ref, field_ref, rows_ref)
        add_products(
            k,
            rows_ref,
            [
                (lambda rows, e: wide_dot(rows, gate_ref[e]), gate_sum),
                (lambda rows, e: wide_dot(rows, up_ref[e]), up_sum),
            ],
        )

    @pl.when(k >= steps)
    def _():
        e = k - steps
        length = act_ref.shape[1]

        @pl.loop(0, length // 128)
        def _(t):
            here = pl.ds(pl.multiple_of(t * 128, 128), 128)
            gate_val, up_val = gate_sum[e, here], up_sum[e, here]
            plain, probs = plain_ref[0, here], probs_ref[0, here]
            sigmoid_val = jax.nn.sigmoid(gate_val)
            silu_val = gate_val * sigmoid_val
            activated = silu_val * up_val
            grad_act = plain * probs
            grad_up_ref[0, here] = (grad_act * silu_val).astype(jnp.bfloat16)
            grad_gate_ref[0, here] = (
                grad_act * up_val * (sigmoid_val * (1.0 + gate_val * (1.0 - sigmoid_val)))
            ).astype(jnp.bfloat16)
            gates_ref[0, here] = jnp.sum(activated * plain, axis=-1, keepdims=True)
            weighted_ref[0, here] = (activated * probs).astype(jnp.bfloat16)
            act_ref[0, here] = activated.astype(jnp.bfloat16)


def feed_in(pick, field, gate, up, plain, probs):
    ranks, width, tokens = pick.shape
    groups, depth = width // SLOTS, field.shape[-1]
    length, inner = ranks * SLOTS, gate.shape[2]
    steps = depth // CHUNK
    held = lambda k: jnp.minimum(k, steps - 1)
    late = lambda k: (jnp.maximum(k - steps, 0), 0, 0)
    wide = pl.BlockSpec((1, length, inner), late)
    thin = pl.BlockSpec((1, length, 1), late)
    low = jax.ShapeDtypeStruct((groups, length, inner), jnp.bfloat16)
    return pl.pallas_call(
        functools.partial(feed_in_body, steps),
        grid=(steps + groups,),
        in_specs=[
            pl.BlockSpec((ranks, width, tokens), lambda k: (0, 0, 0), pipeline_mode=pl.Buffered(1)),
            pl.BlockSpec((ranks, tokens, CHUNK), lambda k: (0, 0, held(k))),
            pl.BlockSpec((groups, CHUNK, inner), lambda k: (0, held(k), 0)),
            pl.BlockSpec((groups, CHUNK, inner), lambda k: (0, held(k), 0)),
            wide,
            thin,
        ],
        out_specs=[pl.BlockSpec((groups, length, CHUNK), lambda k: (0, 0, held(k))), wide, wide, wide, wide, thin],
        out_shape=[
            jax.ShapeDtypeStruct((groups, length, depth), jnp.bfloat16),
            low, low, low, low,
            jax.ShapeDtypeStruct((groups, length, 1), jnp.float32),
        ],
        scratch_shapes=[pltpu.VMEM((groups, length, inner), jnp.float32)] * 2,
        compiler_params=pltpu.CompilerParams(vmem_limit_bytes=63 * 1024 * 1024),
        cost_estimate=pl.CostEstimate(
            flops=2 * groups * length * depth * (tokens + 2 * inner), bytes_accessed=120 << 20, transcendentals=0
        ),
    )(pick, field, gate, up, plain, probs)


def fill_field(flipped, spread_ref, lefts, weights, field_ref, rows):
    groups = rows.shape[0]
    ranks = spread_ref.shape[0]

    @pl.loop(0, groups)
    def _(e):
        total = None
        for left, weight, flip in zip(lefts, weights, flipped):
            term = outer_cols(left[e], weight[e]) if flip else wide_dot(left[e], weight[e])
            total = term if total is None else total + term
        rows[e] = total

    @pl.loop(0, ranks, unroll=2 * UNROLL)
    def _(s):
        part = rows[:, pl.ds(pl.multiple_of(s * SLOTS, SLOTS), SLOTS)]
        part = part.reshape(groups * SLOTS, CHUNK).astype(jnp.bfloat16)
        field_ref[s] = wide_dot(spread_ref[s], part).astype(jnp.bfloat16)


def restore_body(flipped, spread_ref, *refs):
    count = len(flipped)
    fill_field(flipped, spread_ref, refs[:count], refs[count : 2 * count], *refs[2 * count :])


def restore_specs(spread, lefts, weights, flipped):
    ranks, tokens, width = spread.shape
    groups = width // SLOTS
    length, inner = ranks * SLOTS, lefts[0].shape[2]
    depth = weights[0].shape[1] if flipped[0] else weights[0].shape[2]
    once = pl.Buffered(1)
    in_specs = (
        [pl.BlockSpec((ranks, tokens, width), lambda k: (0, 0, 0), pipeline_mode=once)]
        + [pl.BlockSpec((groups, length, inner), lambda k: (0, 0, 0), pipeline_mode=once)] * len(lefts)
        + [
            pl.BlockSpec((groups, CHUNK, inner), lambda k: (0, k, 0))
            if flip
            else pl.BlockSpec((groups, inner, CHUNK), lambda k: (0, 0, k))
            for flip in flipped
        ]
    )
    out_spec = pl.BlockSpec((ranks, tokens, CHUNK), lambda k: (0, 0, k))
    out_shape = jax.ShapeDtypeStruct((ranks, tokens, depth), jnp.bfloat16)
    return depth // CHUNK, in_specs, out_spec, out_shape, pltpu.VMEM((groups, length, CHUNK), jnp.float32)


def restore(spread, lefts, weights, flipped):
    steps, in_specs, out_spec, out_shape, rows = restore_specs(spread, lefts, weights, flipped)
    field = pl.pallas_call(
        functools.partial(restore_body, flipped),
        grid=(steps,),
        in_specs=in_specs,
        out_specs=out_spec,
        out_shape=out_shape,
        scratch_shapes=[rows],
        compiler_params=pltpu.CompilerParams(vmem_limit_bytes=63 * 1024 * 1024),
    )(spread, *lefts, *weights)
    return field.reshape(-1, field.shape[2])


PARTS = 4


def restore_out_body(spread_ref, left_ref, weight_ref, own_ref, field_ref, all_ref, rows,
                     here_sem, f_send, f_recv, g_send, g_recv, h_send, h_recv):
    r, c, y, x, z, core, first, second = seat()
    pair, along_first, along_second, up = partners()
    y1, x1 = row_of(core, first, 1 - second)
    near_row = y1 * 2 + x1
    step = own_ref.shape[0] // PARTS
    k = pl.program_id(0)
    here = pltpu.make_async_copy(own_ref, all_ref.at[r], here_sem)

    def part(ref, q):
        return ref.at[pl.ds(q * step, step)]

    def f_copy(q):
        return send(part(own_ref, q), part(all_ref.at[r], q), f_send.at[q], f_recv.at[q], along_first)

    def g_copy(q):
        return send(part(own_ref, q), part(all_ref.at[r], q), g_send.at[q], g_recv.at[q], along_second)

    def h_copy(q):
        there = part(all_ref.at[near_row], q)
        return send(there, there, h_send.at[q], h_recv.at[q], along_first)

    @pl.when(k == 0)
    def _():
        meet()
        here.start()
        for q in range(PARTS):
            g_copy(q).start()
            f_copy(q).start()

    fill_field((False,), spread_ref, [left_ref], [weight_ref], field_ref, rows)

    for q in range(PARTS):

        @pl.when(k == q + 1)
        def _():
            g_copy(q).wait_recv()
            h_copy(q).start()

    @pl.when(k == pl.num_programs(0) - 1)
    def _():
        here.wait()
        for q in range(PARTS):
            g_copy(q).wait_send()
            f_copy(q).wait()
            h_copy(q).wait()


def restore_out(spread, left, weight, own, collective_id):
    steps, in_specs, out_spec, out_shape, rows = restore_specs(spread, [left], [weight], (False,))
    dma = pltpu.SemaphoreType.DMA
    field, whole = pl.pallas_call(
        restore_out_body,
        grid=(steps,),
        in_specs=in_specs + [ANYWHERE],
        out_specs=[out_spec, ANYWHERE],
        out_shape=[out_shape, jax.ShapeDtypeStruct((4, *own.shape), own.dtype)],
        scratch_shapes=[rows, dma(())] + [dma((PARTS,))] * 6,
        compiler_params=pltpu.CompilerParams(
            collective_id=collective_id, has_side_effects=True, vmem_limit_bytes=63 * 1024 * 1024
        ),
    )(spread, left, weight, own)
    return field.reshape(-1, field.shape[2]), whole.reshape(-1, own.shape[1])


def branch_body(mixed_ref, weight_ref, out_ref, away, near, first_in, second_in,
                f_send, f_recv, g_send, g_recv):
    r, c, y, x, z, core, first, second = seat()
    pair, along_first, along_second, up = partners()
    tokens, depth = out_ref.shape
    width = depth // PARTS

    def columns(j):
        return pl.ds(j * width, width)

    def product(fir, sec, j):
        yy, xx = row_of(core, fir, sec)
        rows = pl.ds(pl.multiple_of((yy * 2 + xx) * tokens, tokens), tokens)
        return wide_dot(mixed_ref[rows], weight_ref[:, columns(j)])

    def f_copy(sec, j):
        return send(
            away.at[sec, :, columns(j)], first_in.at[sec, :, columns(j)], f_send.at[sec, j], f_recv.at[sec, j], along_first
        )

    def g_copy(j):
        return send(near.at[:, columns(j)], second_in.at[:, columns(j)], g_send.at[j], g_recv.at[j], along_second)

    meet()
    for j in range(PARTS):
        away[1 - second, :, columns(j)] = product(1 - first, 1 - second, j).astype(jnp.bfloat16)
        f_copy(1 - second, j).start()
    for j in range(PARTS):
        away[second, :, columns(j)] = product(1 - first, second, j).astype(jnp.bfloat16)
        f_copy(second, j).start()
    for j in range(PARTS):
        value = product(first, 1 - second, j)
        f_copy(1 - second, j).wait_recv()
        value = value + first_in[1 - second, :, columns(j)].astype(jnp.float32)
        near[:, columns(j)] = value.astype(jnp.bfloat16)
        g_copy(j).start()
    for j in range(PARTS):
        out_ref[:, columns(j)] = product(first, second, j)
    for j in range(PARTS):
        f_copy(second, j).wait_recv()
        g_copy(j).wait_recv()
        out_ref[:, columns(j)] += first_in[second, :, columns(j)].astype(jnp.float32) + second_in[
            :, columns(j)
        ].astype(jnp.float32)
    for j in range(PARTS):
        g_copy(j).wait_send()
        for sec in range(2):
            f_copy(sec, j).wait_send()


def branch_near(mixed, weight, collective_id):
    tokens, depth = mixed.shape[0] // 4, weight.shape[1]
    dma = pltpu.SemaphoreType.DMA
    inside = pl.BlockSpec(memory_space=pltpu.VMEM)
    low = lambda *shape: pltpu.VMEM((*shape, tokens, depth), jnp.bfloat16)
    return pl.pallas_call(
        branch_body,
        in_specs=[inside] * 2,
        out_specs=inside,
        out_shape=jax.ShapeDtypeStruct((tokens, depth), jnp.float32),
        scratch_shapes=[
            low(2), low(), low(2), low(), dma((2, PARTS)), dma((2, PARTS)), dma((PARTS,)), dma((PARTS,))
        ],
        compiler_params=pltpu.CompilerParams(
            collective_id=collective_id, has_side_effects=True, vmem_limit_bytes=40 * 1024 * 1024
        ),
    )(mixed, weight)


def causal_scores(query_rows, key_rows):
    scores = outer_cols(query_rows, key_rows) * HD ** (-0.5)
    count, length = scores.shape
    position = lax.broadcasted_iota(jnp.int32, scores.shape, 0) + (length - count)
    return jnp.where(position >= lax.broadcasted_iota(jnp.int32, scores.shape, 1), scores, MASKED)


def attend_body(q_raw, k_raw, v_ref, q_rs, k_rs, q_gain, k_gain, cos_ref, sin_ref,
                mixed_ref, q_out, k_out, v_out, lse_ref):
    length = v_ref.shape[0]
    block = min(256, length)
    v_out[...] = v_ref[...].astype(jnp.bfloat16)
    for raw, scale, gain, out in ((q_raw, q_rs, q_gain, q_out), (k_raw, k_rs, k_gain, k_out)):
        normed = raw[...] * scale[...] * gain[...]
        turned = normed * cos_ref[...] + pltpu.roll(normed, HD // 2, 1) * sin_ref[...]
        out[...] = turned.astype(jnp.bfloat16)
    for start in range(0, length, block):
        here, seen = pl.ds(start, block), pl.ds(0, start + block)
        scores = causal_scores(q_out[here], k_out[seen])
        row_top = jnp.max(scores, axis=-1, keepdims=True)
        exponent = jnp.exp(scores - row_top)
        row_total = jnp.sum(exponent, axis=-1, keepdims=True)
        weights = (exponent / row_total).astype(jnp.bfloat16)
        mixed_ref[here] = wide_dot(weights, v_out[seen]).astype(jnp.bfloat16)
        lse_ref[0, here] = row_top + jnp.log(row_total)


def three_slabs(length, heads):
    return [pl.BlockSpec((length, HD), lambda h, at=at: (0, at * heads + h)) for at in range(3)]


def attend(raw, q_rs, k_rs, q_gain, k_gain, cosine, sine):
    length, width = raw.shape[0], raw.shape[1] // 3
    heads = width // HD
    slab = pl.BlockSpec((length, HD), lambda h: (0, h))
    thin = pl.BlockSpec((length, 1), lambda h: (0, 0))
    line = pl.BlockSpec((1, HD), lambda h: (0, h))
    table = pl.BlockSpec((length, HD), lambda h: (0, 0))
    low = jax.ShapeDtypeStruct((length, width), jnp.bfloat16)
    return pl.pallas_call(
        attend_body,
        grid=(heads,),
        in_specs=three_slabs(length, heads) + [thin, thin, line, line, table, table],
        out_specs=[slab, slab, slab, slab, pl.BlockSpec((1, length, 1), lambda h: (h, 0, 0))],
        out_shape=[low, low, low, low, jax.ShapeDtypeStruct((heads, length, 1), jnp.float32)],
        cost_estimate=pl.CostEstimate(
            flops=4 * heads * length * length * HD, bytes_accessed=8 << 20, transcendentals=heads * length * length
        ),
    )(raw, raw, raw, q_rs, k_rs, q_gain[None], k_gain[None], cosine, sine)


def attend_back_body(q_ref, k_ref, v_ref, grad_ref, lse_ref, q_raw, k_raw, q_rs, k_rs, q_gain, k_gain, cos_ref, sin_ref,
                     v_grad, q_grad, k_grad, q_term, k_term, q_inner, k_inner, dq, dk, dv):
    length = v_ref.shape[0]
    block = min(256, length)
    dk[...] = jnp.zeros_like(dk)
    dv[...] = jnp.zeros_like(dv)
    for start in range(0, length, block):
        here, seen = pl.ds(start, block), pl.ds(0, start + block)
        query_rows, key_rows, grads = q_ref[here], k_ref[seen], grad_ref[here]
        probs = jnp.exp(causal_scores(query_rows, key_rows) - lse_ref[0, here])
        dv[seen] += inner_rows(probs.astype(jnp.bfloat16), grads)
        weights = outer_cols(grads, v_ref[seen])
        delta = jnp.sum(probs * weights, axis=-1, keepdims=True)
        scores = (probs * (weights - delta)).astype(jnp.bfloat16)
        dq[here] = wide_dot(scores, key_rows) * HD ** (-0.5)
        dk[seen] += inner_rows(scores, query_rows) * HD ** (-0.5)
    v_grad[...] = dv[...].astype(jnp.bfloat16)
    for raw, scale, gain, grad, out, term, inner in (
        (q_raw, q_rs, q_gain, dq, q_grad, q_term, q_inner),
        (k_raw, k_rs, k_gain, dk, k_grad, k_term, k_inner),
    ):
        field, value = raw[...], grad[...]
        normed = value * cos_ref[...] + pltpu.roll(value * sin_ref[...], HD // 2, 1)
        weighted = normed * gain[...]
        out[...] = weighted
        term[...] = jnp.sum(normed * field * scale[...], axis=0, keepdims=True)
        inner[0] = jnp.sum(weighted * field, axis=-1, keepdims=True)


def attend_back(queries, keys, values, grads, lse, raw, q_rs, k_rs, q_gain, k_gain, cosine, sine):
    length, width = raw.shape[0], raw.shape[1] // 3
    heads = width // HD
    slab = pl.BlockSpec((length, HD), lambda h: (0, h))
    thin = pl.BlockSpec((length, 1), lambda h: (0, 0))
    line = pl.BlockSpec((1, HD), lambda h: (0, h))
    table = pl.BlockSpec((length, HD), lambda h: (0, 0))
    column = pl.BlockSpec((1, length, 1), lambda h: (h, 0, 0))
    wide = jax.ShapeDtypeStruct((length, width), jnp.float32)
    return pl.pallas_call(
        attend_back_body,
        grid=(heads,),
        in_specs=[slab] * 4 + [column] + three_slabs(length, heads)[:2] + [thin, thin, line, line, table, table],
        out_specs=[slab, slab, slab, line, line, column, column],
        out_shape=[
            jax.ShapeDtypeStruct((length, width), jnp.bfloat16),
            wide,
            wide,
            jax.ShapeDtypeStruct((1, width), jnp.float32),
            jax.ShapeDtypeStruct((1, width), jnp.float32),
            jax.ShapeDtypeStruct((heads, length, 1), jnp.float32),
            jax.ShapeDtypeStruct((heads, length, 1), jnp.float32),
        ],
        scratch_shapes=[pltpu.VMEM((length, HD), jnp.float32)] * 3,
        cost_estimate=pl.CostEstimate(
            flops=10 * heads * length * length * HD, bytes_accessed=16 << 20, transcendentals=heads * length * length
        ),
    )(queries, keys, values, grads, lse, raw, raw, q_rs, k_rs, q_gain[None], k_gain[None], cosine, sine)


def local(
    layer_input,
    cotangent,
    expert_index,
    attention_gain,
    query_gain,
    key_gain,
    query_weight,
    key_weight,
    value_weight,
    output_weight,
    feed_gain,
    router_weight,
    gate_weight,
    up_weight,
    down_weight,
):
    tokens = layer_input.shape[0]
    rows_count = lax.axis_size("row")
    near = rows_count == 4 and lax.axis_size("col") == 8
    if near:
        head_part = query_gain.shape[0]
        slice_width = attention_gain.shape[0]
        pack = jnp.concatenate(
            [attention_gain, feed_gain, query_gain, key_gain, router_weight.reshape(-1)]
        )
        pack = jnp.pad(pack, (0, PACK_ROWS * 128 - pack.shape[0])).reshape(PACK_ROWS, 128)
        (
            sequence, qkv_full, output_full, pack_all, cotangent_all, index_all
        ) = start_near(
            layer_input,
            [query_weight, key_weight, value_weight, output_weight],
            pack,
            cotangent,
            expert_index.T,
            1,
        )
        index_all = jnp.swapaxes(index_all, 1, 2)
        pack_all = pack_all.reshape(8, -1)
        ends = [slice_width, 2 * slice_width, 2 * slice_width + head_part, 2 * slice_width + 2 * head_part]
        attention_full = pack_all[:, : ends[0]].reshape(-1)
        feed_full = pack_all[:, ends[0] : ends[1]].reshape(-1)
        query_scale_w = pack_all[:, ends[1] : ends[2]].reshape(-1)
        key_scale_w = pack_all[:, ends[2] : ends[3]].reshape(-1)
        router_full = pack_all[:, ends[3] : ends[3] + router_weight.size].reshape(
            -1, router_weight.shape[1]
        )
    else:
        (
            attention_full,
            query_scale_w,
            key_scale_w,
            query_full,
            key_full,
            value_full,
            output_full,
            feed_full,
            router_full,
        ) = (
            lax.all_gather(attention_gain, "col", axis=0, tiled=True),
            lax.all_gather(query_gain, "col", axis=0, tiled=True),
            lax.all_gather(key_gain, "col", axis=0, tiled=True),
            lax.all_gather(query_weight, "col", axis=0, tiled=True),
            lax.all_gather(key_weight, "col", axis=0, tiled=True),
            lax.all_gather(value_weight, "col", axis=0, tiled=True),
            lax.all_gather(output_weight, "col", axis=1, tiled=True),
            lax.all_gather(feed_gain, "col", axis=0, tiled=True),
            lax.all_gather(router_weight, "col", axis=0, tiled=True),
        )
        qkv_full = jnp.concatenate([query_full, key_full, value_full], axis=1)
        sequence = lax.all_gather(layer_input, "row", axis=0, tiled=True)
    length = sequence.shape[0]
    model_width = sequence.shape[1]
    local_width = qkv_full.shape[1] // 3
    seq_float = sequence.astype(jnp.float32)
    seq_scale = rms_scale(seq_float)
    attention_float = attention_full.astype(jnp.float32)
    normed = (seq_float * seq_scale * attention_float).astype(jnp.bfloat16)
    raw = wide_dot(normed, qkv_full)
    query_raw, key_raw = raw[:, :local_width], raw[:, local_width : 2 * local_width]
    query_total, key_total = lax.psum(
        (jnp.sum(query_raw * query_raw, axis=-1), jnp.sum(key_raw * key_raw, axis=-1)), "row"
    )
    query_rs = lax.rsqrt(query_total / model_width + EPS)[:, None]
    key_rs = lax.rsqrt(key_total / model_width + EPS)[:, None]
    query_gain_f = query_scale_w.astype(jnp.float32)
    key_gain_f = key_scale_w.astype(jnp.float32)
    cosine, sine_table = rope_tables(length)
    mixed_heads, queries, keys_rotated, values, lse_all = attend(
        raw, query_rs, key_rs, query_gain_f, key_gain_f, cosine, sine_table
    )
    if near:
        branch = branch_near(mixed_heads, output_full, 5)
    else:
        branch = lax.psum_scatter(
            wide_dot(mixed_heads, output_full).astype(jnp.bfloat16), "row", scatter_dimension=0, tiled=True
        ).astype(jnp.float32)
    hidden = layer_input.astype(jnp.float32) + branch
    feed_scale = rms_scale(hidden)
    feed_float = feed_full.astype(jnp.float32)
    feed_normed = (hidden * feed_scale * feed_float).astype(jnp.bfloat16)
    logits = wide_dot(feed_normed, router_full)
    logit_top = jnp.max(logits, axis=-1, keepdims=True)
    logit_exp = jnp.exp(logits - logit_top)
    router_probs = logit_exp / jnp.sum(logit_exp, axis=-1, keepdims=True)
    experts = router_full.shape[1]
    experts_local = gate_weight.shape[0]
    ranks = lax.axis_size("col") * rows_count
    gate_hits = expert_index[:, :, None] == jnp.arange(experts, dtype=jnp.int32)
    gate_probs = jnp.sum(jnp.where(gate_hits, router_probs[:, None, :], 0.0), axis=-1)

    if not near:
        index_all = lax.all_gather(expert_index, ("col", "row"), axis=0, tiled=True)
    own = (index_all - lax.axis_index("col") * experts_local).reshape(ranks, tokens, -1)
    matches = own[..., None] == jnp.arange(experts_local, dtype=jnp.int32)
    hit = jnp.sum(matches.astype(jnp.float32), axis=2)
    earlier = jnp.tril(jnp.ones((tokens, tokens), jnp.bfloat16), -1)
    rank = jnp.einsum(
        "tu,sue->ste", earlier, hit.astype(jnp.bfloat16), preferred_element_type=jnp.float32
    )
    slot = jnp.where(hit > 0, rank, -1.0)
    places = jnp.arange(SLOTS, dtype=jnp.float32)
    slot_t = jnp.swapaxes(slot, 1, 2)
    width = experts_local * SLOTS
    picked = slot_t[:, :, None, :] == places[None, None, :, None]
    pick = picked.astype(jnp.bfloat16).reshape(ranks, width, tokens)
    lanes = jnp.arange(width, dtype=jnp.int32)
    widen = (lanes[None, :] // SLOTS == jnp.arange(experts_local)[:, None]).astype(jnp.bfloat16)
    spread = jnp.einsum(
        "ste,ew->stw", slot.astype(jnp.bfloat16), widen, preferred_element_type=jnp.float32
    ) == (lanes % SLOTS).astype(jnp.float32)
    spread_plain = spread.astype(jnp.bfloat16)

    def weigh(probs_all):
        probs_own = jnp.sum(
            jnp.where(matches, probs_all.reshape(ranks, tokens, -1, 1), 0.0), axis=2
        )
        probs_wide = jnp.einsum(
            "ste,ew->stw", probs_own.astype(jnp.bfloat16), widen, preferred_element_type=jnp.float32
        )
        spread_probs = jnp.where(spread, probs_wide, 0.0).astype(jnp.bfloat16)
        probs_t = jnp.swapaxes(probs_own, 1, 2)
        row_probs = jnp.sum(jnp.where(picked, probs_t[:, :, None, :], 0.0), axis=-1)
        row_probs = jnp.swapaxes(row_probs, 0, 1).reshape(experts_local, ranks * SLOTS, 1)
        return spread_probs, row_probs

    if near:
        expert_grads, plain_act, feed_all, probs_all = grads_in(
            pick, cotangent_all, down_weight, feed_normed, gate_probs.T, 2
        )
        spread_probs, row_probs = weigh(jnp.swapaxes(probs_all, 1, 2))
        expert_rows, activated, weighted_act, grad_gate, grad_up, row_gates = feed_in(
            pick, feed_all, gate_weight, up_weight, plain_act, row_probs
        )
    else:
        probs_all = lax.all_gather(gate_probs, ("col", "row"), axis=0, tiled=True)
        spread_probs, row_probs = weigh(probs_all)
        expert_grads = gather_rows(pick, cotangent)
        expert_rows = gather_rows(pick, feed_normed)
        gate_val = jnp.einsum(
            "erd,edf->erf", expert_rows, gate_weight, preferred_element_type=jnp.float32
        )
        up_val = jnp.einsum(
            "erd,edf->erf", expert_rows, up_weight, preferred_element_type=jnp.float32
        )
        plain_act = jnp.einsum(
            "erd,efd->erf", expert_grads, down_weight, preferred_element_type=jnp.float32
        )
        sigmoid_val = jax.nn.sigmoid(gate_val)
        silu_val = gate_val * sigmoid_val
        activated = silu_val * up_val
        grad_act = plain_act * row_probs
        grad_up = (grad_act * silu_val).astype(jnp.bfloat16)
        grad_gate = (
            grad_act * up_val * sigmoid_val * (1.0 + gate_val * (1.0 - sigmoid_val))
        ).astype(jnp.bfloat16)
        row_gates = jnp.sum(activated * plain_act, axis=-1)
        weighted_act = (activated * row_probs).astype(jnp.bfloat16)
        activated = activated.astype(jnp.bfloat16)
    row_gates = jnp.swapaxes(row_gates.reshape(experts_local, ranks, SLOTS), 0, 1)
    own_gates = jnp.sum(jnp.where(picked, row_gates[..., None], 0.0), axis=2)
    if near:
        grad_feed_part = restore(
            spread_plain, [grad_gate, grad_up], [gate_weight, up_weight], (True, True)
        )
        grad_feed, gates_in, grad_gate_weight, grad_up_weight, grad_down_weight = feed_back(
            grad_feed_part, own_gates, expert_rows, grad_gate, grad_up, weighted_act, expert_grads, 3
        )
        grad_gate_weight, grad_up_weight, grad_down_weight = widen_all(
            grad_gate_weight, grad_up_weight, grad_down_weight
        )
        gates_in = jnp.sum(gates_in.reshape(-1, rows_count, experts_local, tokens), axis=1)
        grad_probs = gates_in.reshape(experts, tokens).T
    else:
        own_gates = lax.psum_scatter(
            jnp.swapaxes(own_gates, 1, 2).reshape(-1, rows_count, tokens, experts_local),
            "row",
            scatter_dimension=1,
        )
        grad_probs = lax.all_to_all(own_gates, "col", split_axis=0, concat_axis=2, tiled=True)[0]
        back_rows = (
            jnp.einsum("erf,edf->erd", grad_gate, gate_weight, preferred_element_type=jnp.float32)
            + jnp.einsum("erf,edf->erd", grad_up, up_weight, preferred_element_type=jnp.float32)
        ).astype(jnp.bfloat16)
        grad_feed = return_rows(spread_plain, back_rows).astype(jnp.float32)
        out_rows = jnp.einsum(
            "erf,efd->erd", activated, down_weight, preferred_element_type=jnp.float32
        ).astype(jnp.bfloat16)
        mixture = return_rows(spread_probs, out_rows).astype(jnp.float32)
        grad_gate_weight = jnp.einsum(
            "erd,erf->edf", expert_rows, grad_gate, preferred_element_type=jnp.float32
        )
        grad_up_weight = jnp.einsum(
            "erd,erf->edf", expert_rows, grad_up, preferred_element_type=jnp.float32
        )
        grad_down_weight = jnp.einsum(
            "erf,erd->efd", weighted_act, expert_grads, preferred_element_type=jnp.float32
        )
    grad_out = cotangent.astype(jnp.float32)
    grad_logits = (
        router_probs * (grad_probs - jnp.sum(router_probs * grad_probs, axis=-1, keepdims=True))
    ).astype(jnp.bfloat16)
    router_grad = inner_rows(feed_normed, grad_logits)
    grad_feed = grad_feed + outer_cols(grad_logits, router_full)
    feed_gain_term = jnp.sum(grad_feed * hidden * feed_scale, axis=0)
    feed_weighted = grad_feed * feed_float
    grad_hidden = (
        grad_out
        + feed_scale * feed_weighted
        - hidden * feed_scale**3 * jnp.mean(feed_weighted * hidden, axis=-1, keepdims=True)
    )
    if near:
        mixture_part, grad_branch = restore_out(
            spread_probs, activated, down_weight, grad_hidden.astype(jnp.bfloat16), 6
        )
    else:
        grad_branch = lax.all_gather(grad_hidden.astype(jnp.bfloat16), "row", axis=0, tiled=True)
    output_grad = inner_rows(mixed_heads, grad_branch)
    grad_mixed = outer_cols(grad_branch, output_full).astype(jnp.bfloat16)
    (
        grad_value_low, query_weighted, key_weighted, query_gain_term, key_gain_term, query_inner, key_inner
    ) = attend_back(
        queries, keys_rotated, values, grad_mixed, lse_all, raw, query_rs, key_rs,
        query_gain_f, key_gain_f, cosine, sine_table,
    )
    query_gain_term, key_gain_term = query_gain_term.reshape(-1), key_gain_term.reshape(-1)
    query_inner, key_inner = (
        lax.psum(jnp.sum(query_inner, axis=(0, 2)), "row"),
        lax.psum(jnp.sum(key_inner, axis=(0, 2)), "row"),
    )
    grad_query_raw = (
        query_rs * query_weighted - query_raw * query_rs**3 * (query_inner / model_width)[:, None]
    ).astype(jnp.bfloat16)
    grad_key_raw = (
        key_rs * key_weighted - key_raw * key_rs**3 * (key_inner / model_width)[:, None]
    ).astype(jnp.bfloat16)
    raw_grads = jnp.concatenate([grad_query_raw, grad_key_raw, grad_value_low], axis=1)
    qkv_grad = inner_rows(normed, raw_grads)
    grad_normed = outer_cols(raw_grads, qkv_full)
    attention_weighted = grad_normed * attention_float
    grad_seq_part = seq_scale * attention_weighted - seq_float * seq_scale**3 * jnp.mean(
        attention_weighted * seq_float, axis=-1, keepdims=True
    )
    attention_gain_term = jnp.sum(grad_normed * seq_float * seq_scale, axis=0)
    if near:
        cols = lax.axis_size("col")
        pack = jnp.concatenate(
            [
                attention_gain_term.reshape(cols, -1),
                feed_gain_term.reshape(cols, -1),
                query_gain_term.reshape(cols, -1),
                key_gain_term.reshape(cols, -1),
                router_grad.reshape(cols, -1),
            ],
            axis=1,
        )
        pack = jnp.pad(pack, ((0, 0), (0, PACK_ROWS * 128 - pack.shape[1])))
        pack = pack.astype(jnp.bfloat16).reshape(cols, PACK_ROWS, 128)
        (
            mixture, summed, grad_query_weight, grad_key_weight, grad_value_weight, grad_output_weight, packs
        ) = finish_near(
            mixture_part,
            grad_seq_part.astype(jnp.bfloat16).reshape(rows_count, tokens, model_width),
            [grad.astype(jnp.bfloat16) for grad in (qkv_grad, output_grad)],
            pack,
            4,
        )
        input_grad = grad_hidden + summed
        packs = packs.reshape(cols, rows_count, -1).astype(jnp.float32)
        whole = jnp.sum(packs, axis=(0, 1))
        heads_sum = jnp.sum(
            lax.dynamic_index_in_dim(packs, lax.axis_index("row"), 1, keepdims=False), axis=0
        )
        grad_attention_gain = whole[: ends[0]]
        grad_feed_gain = whole[ends[0] : ends[1]]
        grad_query_gain = heads_sum[ends[1] : ends[2]]
        grad_key_gain = heads_sum[ends[2] : ends[3]]
        grad_router_weight = whole[ends[3] : ends[3] + router_weight.size].reshape(router_weight.shape)
    else:
        stacked = jnp.concatenate(
            [
                grad_seq_part.reshape(rows_count, tokens, model_width),
                jnp.broadcast_to(attention_gain_term[None, None, :], (rows_count, 1, model_width)),
            ],
            axis=1,
        ).reshape(rows_count * (tokens + 1), model_width)
        summed = lax.psum_scatter(
            stacked.astype(jnp.bfloat16), "row", scatter_dimension=0, tiled=True
        ).astype(jnp.float32)
        input_grad = grad_hidden + summed[:tokens]
        attention_gain_total = summed[tokens]
        query_grad, key_grad, value_grad = jnp.split(qkv_grad, 3, axis=1)
        feed_gain_total, router_total = (
            lax.psum(feed_gain_term.astype(jnp.bfloat16), "row").astype(jnp.float32),
            lax.psum(router_grad.astype(jnp.bfloat16), "row").astype(jnp.float32),
        )
        (
            grad_attention_gain,
            grad_query_gain,
            grad_key_gain,
            grad_query_weight,
            grad_key_weight,
            grad_value_weight,
            grad_output_weight,
            grad_feed_gain,
            grad_router_weight,
        ) = (
            lax.psum_scatter(
                attention_gain_total.astype(jnp.bfloat16), "col", scatter_dimension=0, tiled=True
            ).astype(jnp.float32),
            lax.psum_scatter(
                query_gain_term.astype(jnp.bfloat16), "col", scatter_dimension=0, tiled=True
            ).astype(jnp.float32),
            lax.psum_scatter(
                key_gain_term.astype(jnp.bfloat16), "col", scatter_dimension=0, tiled=True
            ).astype(jnp.float32),
            lax.psum_scatter(
                query_grad.astype(jnp.bfloat16), "col", scatter_dimension=0, tiled=True
            ).astype(jnp.float32),
            lax.psum_scatter(
                key_grad.astype(jnp.bfloat16), "col", scatter_dimension=0, tiled=True
            ).astype(jnp.float32),
            lax.psum_scatter(
                value_grad.astype(jnp.bfloat16), "col", scatter_dimension=0, tiled=True
            ).astype(jnp.float32),
            lax.psum_scatter(
                output_grad.astype(jnp.bfloat16), "col", scatter_dimension=1, tiled=True
            ).astype(jnp.float32),
            lax.psum_scatter(
                feed_gain_total.astype(jnp.bfloat16), "col", scatter_dimension=0, tiled=True
            ).astype(jnp.float32),
            lax.psum_scatter(
                router_total.astype(jnp.bfloat16), "col", scatter_dimension=0, tiled=True
            ).astype(jnp.float32),
        )
    layer_output = hidden + mixture
    return (
        layer_output,
        input_grad,
        grad_attention_gain,
        grad_query_gain,
        grad_key_gain,
        grad_query_weight,
        grad_key_weight,
        grad_value_weight,
        grad_output_weight,
        grad_feed_gain,
        grad_router_weight,
        grad_gate_weight,
        grad_up_weight,
        grad_down_weight,
    )


def solution(mesh):
    placed = (
        P(("col", "row"), None),
        P(("col", "row"), None),
        P(("col", "row"), None),
        P("col"),
        P(("row", "col")),
        P(("row", "col")),
        P("col", "row"),
        P("col", "row"),
        P("col", "row"),
        P("row", "col"),
        P("col"),
        P("col", None),
        P("col", None, "row"),
        P("col", None, "row"),
        P("col", "row", None),
    )
    return jax.shard_map(
        local,
        mesh=mesh,
        in_specs=placed,
        out_specs=(
            P(("col", "row"), None),
            P(("col", "row"), None),
            P("col"),
            P(("row", "col")),
            P(("row", "col")),
            P("col", "row"),
            P("col", "row"),
            P("col", "row"),
            P("row", "col"),
            P("col"),
            P("col", None),
            P("col", None, "row"),
            P("col", None, "row"),
            P("col", "row", None),
        ),
        check_vma=False,
    )
```

```python
import functools

import jax
import jax.numpy as jnp
from jax import lax
from jax.experimental import pallas as pl
from jax.experimental.pallas import tpu as pltpu
from jax.sharding import PartitionSpec as P

HD = 128
SLOTS = 40
BLOCK = 512
CHUNK = 256
UNROLL = 4
PACK_ROWS = 144


EPS = 1e-05
THETA = 10000.0
MASKED = -1e30


def wide_dot(left, right):
    return jnp.dot(left, right, preferred_element_type=jnp.float32)


def inner_rows(left, right):
    return lax.dot_general(
        left, right, (((0,), (0,)), ((), ())), preferred_element_type=jnp.float32
    )


def outer_cols(left, right):
    return lax.dot_general(
        left, right, (((1,), (1,)), ((), ())), preferred_element_type=jnp.float32
    )


def rms_scale(field):
    return lax.rsqrt(jnp.mean(field * field, axis=-1, keepdims=True) + EPS)


def rope_tables(length):
    half_size = HD // 2
    freqs = THETA ** (-(jnp.arange(half_size, dtype=jnp.float32) * 2.0) / HD)
    angles = jnp.arange(length, dtype=jnp.float32)[:, None] * freqs[None, :]
    cosine = jnp.concatenate([jnp.cos(angles), jnp.cos(angles)], axis=-1)
    sine_table = jnp.concatenate([-jnp.sin(angles), jnp.sin(angles)], axis=-1)
    return (cosine, sine_table)


def dispatch_body(pick_ref, field_ref, rows_ref):
    groups = rows_ref.shape[0]
    first = wide_dot(pick_ref[0], field_ref[0]).reshape(groups, SLOTS, -1)
    second = wide_dot(pick_ref[1], field_ref[1]).reshape(groups, SLOTS, -1)
    rows_ref[...] = jnp.concatenate([first, second], axis=1).astype(jnp.bfloat16)


def dispatch(pick, field):
    ranks, width, tokens = pick.shape
    groups, depth = width // SLOTS, field.shape[1]
    return pl.pallas_call(
        dispatch_body,
        grid=(ranks // 2, depth // BLOCK),
        in_specs=[
            pl.BlockSpec((2, width, tokens), lambda i, k: (i, 0, 0)),
            pl.BlockSpec((2, tokens, BLOCK), lambda i, k: (i, 0, k)),
        ],
        out_specs=pl.BlockSpec((groups, 2 * SLOTS, BLOCK), lambda i, k: (0, i, k)),
        out_shape=jax.ShapeDtypeStruct((groups, ranks * SLOTS, depth), jnp.bfloat16),
    )(pick, field.reshape(ranks, tokens, depth))


def combine_body(spread_ref, rows_ref, field_ref):
    rows = rows_ref[...].astype(jnp.float32)
    width = rows.shape[0] * SLOTS
    for side in range(2):
        part = rows[:, side * SLOTS : (side + 1) * SLOTS].reshape(width, -1).astype(jnp.bfloat16)
        field_ref[side] = wide_dot(spread_ref[side], part).astype(jnp.bfloat16)


def combine(spread, rows):
    ranks, tokens, width = spread.shape
    groups, depth = width // SLOTS, rows.shape[2]
    field = pl.pallas_call(
        combine_body,
        grid=(ranks // 2, depth // BLOCK),
        in_specs=[
            pl.BlockSpec((2, tokens, width), lambda i, k: (i, 0, 0)),
            pl.BlockSpec((groups, 2 * SLOTS, BLOCK), lambda i, k: (0, i, k)),
        ],
        out_specs=pl.BlockSpec((2, tokens, BLOCK), lambda i, k: (i, 0, k)),
        out_shape=jax.ShapeDtypeStruct((ranks, tokens, depth), jnp.bfloat16),
    )(spread, rows)
    return field.reshape(ranks * tokens, depth)


def scatter_all(field):
    part = lax.psum_scatter(field, "col", scatter_dimension=0, tiled=True)
    return lax.psum_scatter(part, "row", scatter_dimension=0, tiled=True)


def pieces_of(ranks, depth):
    count = max(1, ranks // 32)
    step = depth // count
    return [(at, at + step) for at in range(0, depth, step)]


def gather_rows(pick, field):
    rows = []
    for start, stop in pieces_of(pick.shape[0], field.shape[1]):
        part = field[:, start:stop]
        if rows:
            part = lax.optimization_barrier((part, rows[-1]))[0]
        whole = lax.all_gather(part, ("col", "row"), axis=0, tiled=True)
        rows.append(dispatch(pick, whole))
    return rows[0] if len(rows) == 1 else jnp.concatenate(rows, axis=2)


def return_rows(spread, rows):
    sums = []
    for start, stop in pieces_of(spread.shape[0], rows.shape[2]):
        part = rows[:, :, start:stop]
        if sums:
            part = lax.optimization_barrier((part, sums[-1]))[0]
        sums.append(scatter_all(combine(spread, part)))
    return sums[0] if len(sums) == 1 else jnp.concatenate(sums, axis=1)


MESH = pl.DeviceIdType.MESH


def seat():
    r, c = lax.axis_index("row"), lax.axis_index("col")
    y, x = r // 2, r % 2
    z, core = c // 2, c % 2
    first = y * (1 - core) + x * core
    second = x * (1 - core) + y * core
    return r, c, y, x, z, core, first, second


def partners():
    r, c, y, x, z, core, first, second = seat()
    pair = (r, z * 2 + (1 - core))
    flip_y = (1 - y) * 2 + x
    flip_x = y * 2 + (1 - x)
    along_first = (flip_y * (1 - core) + flip_x * core, c)
    along_second = (flip_x * (1 - core) + flip_y * core, c)
    up = [(r, ((z + k) % 4) * 2 + core) for k in range(1, 4)]
    return pair, along_first, along_second, up


RANKS = 32


def nth(offset):
    spot = (lax.axis_index("col") * 4 + lax.axis_index("row") + offset) % RANKS
    return spot, (spot % 4, spot // 4)


def meet():
    barrier = pltpu.get_barrier_semaphore()

    @pl.loop(1, RANKS)
    def _(offset):
        pl.semaphore_signal(barrier, inc=1, device_id=nth(offset)[1], device_id_type=MESH)

    pl.semaphore_wait(barrier, RANKS - 1)


def small_copy(src_of, small_all, small_send, small_recv, offset):
    spot, device = nth(offset)
    return send(
        src_of(spot), small_all.at[nth(0)[0]], small_send.at[offset], small_recv.at[offset], device
    )


def row_of(core, first, second):
    y = first * (1 - core) + second * core
    x = second * (1 - core) + first * core
    return y, x


def send(src, dst, send_sem, recv_sem, device):
    return pltpu.make_async_remote_copy(
        src_ref=src, dst_ref=dst, send_sem=send_sem, recv_sem=recv_sem, device_id=device, device_id_type=MESH
    )


GSTEPS = 4
QUEUE = (2, 1, 3)
ARRIVE = (1, 3, 2)


def spread_out(own_ref, all_ref, sems):
    r, c, y, x, z, core, first, second = seat()
    pair, along_first, along_second, up = partners()
    here_sem, u_send, u_recv, d_send, d_recv, g_send, g_recv, f_send, f_recv, p_send, p_recv = sems
    step = own_ref.shape[0] // GSTEPS

    def rows(q):
        return pl.ds(pl.multiple_of(q * step, step), step)

    def place(k, s, f, q):
        sec = second * (1 - s) + (1 - second) * s
        fir = first * (1 - f) + (1 - first) * f
        yy, xx = row_of(core, fir, sec)
        return all_ref.at[(z + 4 - k) % 4, core, yy, xx, rows(q)]

    above, below = (r, ((z + 1) % 4) * 2 + core), (r, ((z + 3) % 4) * 2 + core)

    def source(k, q):
        return own_ref.at[rows(q)] if k == 0 else place(k, 0, 0, q)

    def up_copy(d, q):
        return send(source(d, q), place(d, 0, 0, q), u_send.at[d, q], u_recv.at[d, q], above)

    def down_copy(d, q):
        k = (4 - d) % 4
        return send(source(k, q), place(k, 0, 0, q), d_send.at[d, q], d_recv.at[d, q], below)

    def came_up(d, q):
        there = place(d, 0, 0, q)
        return send(there, there, u_send.at[d - 1, q], u_recv.at[d - 1, q], above)

    def came_down(d, q):
        there = place(4 - d, 0, 0, q)
        return send(there, there, d_send.at[d - 1, q], d_recv.at[d - 1, q], below)

    bottom, top = 1 - jnp.minimum(z, 1), z // 3
    arrived = [bottom * (3 - i) + top * (1 + i) + (1 - bottom - top) * ARRIVE[i] for i in range(3)]

    def g_copy(k, q, src):
        return send(src, place(k, 0, 0, q), g_send.at[k, q], g_recv.at[k, q], along_second)

    def f_copy(k, s, q, src):
        return send(src, place(k, s, 0, q), f_send.at[s, k, q], f_recv.at[s, k, q], along_first)

    def p_copy(k, s, f, q, src):
        return send(src, place(k, s, f, q), p_send.at[f, s, k, q], p_recv.at[f, s, k, q], pair)

    here = pltpu.make_async_copy(own_ref, all_ref.at[z, core, y, x], here_sem)

    def begin():
        here.start()

        @pl.loop(0, GSTEPS)
        def _(q):
            src = own_ref.at[rows(q)]

            @pl.when(z < 3)
            def _():
                up_copy(0, q).start()

            @pl.when(z > 0)
            def _():
                down_copy(0, q).start()

            g_copy(0, q, src).start()
            f_copy(0, 0, q, src).start()
            p_copy(0, 0, 0, q, src).start()

    def along_z(q):
        def pass_on(k):
            src = place(k, 0, 0, q)
            g_copy(k, q, src).start()
            f_copy(k, 0, q, src).start()
            p_copy(k, 0, 0, q, src).start()

        for d in (1, 2, 3):

            @pl.when(z >= d)
            def _():
                came_up(d, q).wait_recv()
                if d < 3:

                    @pl.when(z < 3)
                    def _():
                        up_copy(d, q).start()

                pass_on(d)

            @pl.when(z + d <= 3)
            def _():
                came_down(d, q).wait_recv()
                if d < 3:

                    @pl.when(z > 0)
                    def _():
                        down_copy(d, q).start()

                pass_on(4 - d)

    def forward(q, between=None):
        @pl.when(q == 0)
        def _():
            along_z(q)

        @pl.when(q + 1 < GSTEPS)
        def _():
            along_z(q + 1)

        if between is not None:
            between()

        for k in (0, *arrived):
            src = place(k, 1, 0, q)
            g_copy(k, q, src).wait_recv()
            f_copy(k, 1, q, src).start()
            p_copy(k, 1, 0, q, src).start()
        for k in (0, *arrived):
            src = place(k, 0, 1, q)
            f_copy(k, 0, q, src).wait_recv()
            p_copy(k, 0, 1, q, src).start()

    def finish():
        @pl.loop(0, GSTEPS)
        def _(q):
            for k in (0, *arrived):
                src = place(k, 1, 1, q)
                f_copy(k, 1, q, src).wait_recv()
                p_copy(k, 1, 1, q, src).start()

        here.wait()

        @pl.loop(0, GSTEPS)
        def _(q):
            for d in range(3):

                @pl.when((z < 3) & (z >= d))
                def _():
                    up_copy(d, q).wait_send()

                @pl.when((z > 0) & (z + d <= 3))
                def _():
                    down_copy(d, q).wait_send()

            for k in range(4):
                src = own_ref.at[rows(q)]
                g_copy(k, q, src).wait_send()
                for s in range(2):
                    f_copy(k, s, q, src).wait_send()
                    for f in range(2):
                        p_copy(k, s, f, q, src).wait()

    return begin, forward, finish


def spread_sems():
    dma = pltpu.SemaphoreType.DMA
    shapes = [(3, GSTEPS), (3, GSTEPS), (4, GSTEPS), (2, 4, GSTEPS), (2, 2, 4, GSTEPS)]
    return [dma(())] + [dma(shape) for shape in shapes for _ in range(2)]


def small_out(small_ref, small_all, sems):
    here_sem, small_send, small_recv = sems
    local = pltpu.make_async_copy(small_ref, small_all.at[nth(0)[0]], here_sem)

    def copy(offset):
        return small_copy(lambda spot: small_ref, small_all, small_send, small_recv, offset)

    def begin():
        local.start()

        @pl.loop(1, RANKS)
        def _(offset):
            copy(offset).start()

    def finish():
        local.wait()

        @pl.loop(1, RANKS)
        def _(offset):
            copy(offset).wait()

    return begin, finish


def small_sems():
    dma = pltpu.SemaphoreType.DMA
    return [dma(()), dma((RANKS,)), dma((RANKS,))]


ANYWHERE = pl.BlockSpec(memory_space=pl.ANY)


def start_body(x_ref, q_ref, k_ref, v_ref, o_ref, pack_ref, own_ref, small_ref,
               x_all, qkv_all, o_all, pack_all, all_ref, small_all, *sems):
    r, c, y, x, z, core, first, second = seat()
    pair, along_first, along_second, up = partners()
    begin, forward, finish = spread_out(own_ref, all_ref, sems[:11])
    small_begin, small_finish = small_out(small_ref, small_all, sems[11:14])
    here_sem, x_send, x_recv, w_send, w_recv, v_send, v_recv = sems[14:]
    weights = [(q_ref, qkv_all), (k_ref, qkv_all), (v_ref, qkv_all), (o_ref, o_all), (pack_ref, pack_all)]

    def block(index, col):
        ref, whole = weights[index]
        if index == 4:
            return whole.at[col]
        if index == 3:
            width = ref.shape[1]
            return whole.at[:, pl.ds(pl.multiple_of(col * width, width), width)]
        height, width = ref.shape
        return whole.at[pl.ds(pl.multiple_of(col * height, height), height), pl.ds(index * width, width)]

    def w_copy(index, k):
        return send(
            weights[index][0], block(index, c), w_send.at[index, k - 1], w_recv.at[index, k - 1], up[k - 1]
        )

    def pair_copy(index, k):
        col = ((z + 4 - k) % 4) * 2 + core
        src = weights[index][0] if k == 0 else block(index, col)
        return send(src, block(index, col), v_send.at[index, k], v_recv.at[index, k], pair)

    locals_ = [pltpu.make_async_copy(x_ref, x_all.at[r], here_sem.at[5])] + [
        pltpu.make_async_copy(weights[i][0], block(i, c), here_sem.at[i]) for i in range(5)
    ]
    y1, x1 = row_of(core, first, 1 - second)
    near_row = y1 * 2 + x1
    x_first = send(x_ref, x_all.at[r], x_send.at[0], x_recv.at[0], along_first)
    x_second = send(x_ref, x_all.at[r], x_send.at[1], x_recv.at[1], along_second)
    x_relay = send(x_all.at[near_row], x_all.at[near_row], x_send.at[2], x_recv.at[2], along_first)

    meet()
    small_begin()
    x_second.start()
    x_first.start()
    begin()
    for item in locals_:
        item.start()
    x_second.wait_recv()
    x_relay.start()
    def weights_out(group):
        for index in group:
            for k in QUEUE:
                w_copy(index, k).start()
            pair_copy(index, 0).start()

    for q, group in enumerate(((4, 0), (1, 2), (3,), ())):
        forward(q, functools.partial(weights_out, group))

    for index in (4, 0, 1, 2, 3):
        for k in ARRIVE:
            w_copy(index, k).wait_recv()
            pair_copy(index, k).start()
    finish()
    small_finish()
    for item in locals_:
        item.wait()
    x_first.wait()
    x_second.wait_send()
    x_relay.wait()
    for index in range(5):
        for k in range(4):
            if k:
                w_copy(index, k).wait_send()
            pair_copy(index, k).wait()


def start_near(x, weights, pack, own, small, collective_id):
    tokens, depth = own.shape
    dma = pltpu.SemaphoreType.DMA
    height, width = weights[0].shape
    shaped = lambda shape, like: jax.ShapeDtypeStruct(shape, like.dtype)
    outs = pl.pallas_call(
        start_body,
        out_shape=(
            shaped((4, *x.shape), x),
            shaped((8 * height, 3 * width), weights[0]),
            shaped((weights[3].shape[0], 8 * weights[3].shape[1]), weights[3]),
            shaped((8, *pack.shape), pack),
            shaped((4, 2, 2, 2, tokens, depth), own),
            shaped((RANKS, *small.shape), small),
        ),
        in_specs=[ANYWHERE] * 8,
        out_specs=[ANYWHERE] * 6,
        scratch_shapes=spread_sems()
        + small_sems()
        + [dma((6,)), dma((3,)), dma((3,)), dma((5, 3)), dma((5, 3)), dma((5, 4)), dma((5, 4))],
        compiler_params=pltpu.CompilerParams(collective_id=collective_id, has_side_effects=True),
    )(x, *weights, pack, own, small)
    x_all, qkv, o, pack_all, whole, small_all = outs
    return x_all.reshape(-1, x.shape[1]), qkv, o, pack_all, whole.reshape(RANKS, tokens, depth), small_all


def finish_body(part_ref, field_ref, qkv_ref, o_ref, pack_ref,
                mixture_ref, out_ref, q_out, k_out, v_out, o_out, pack_all,
                mine, first_in, second_in, total,
                qkv_mine, o_mine, qkv_pair, o_pair, qkv_z, o_z, qkv_sum, o_sum,
                load_sem, f_send, f_recv, g_send, g_recv, w_load, p_send, p_recv, z_send, z_recv, out_sem,
                *rest):
    r, c, y, x, z, core, first, second = seat()
    pair, along_first, along_second, up = partners()
    small_begin, small_finish = small_each(pack_ref, pack_all, rest[:3], lambda spot: spot // 4)
    begin, tick, finish = shrink(part_ref, *rest[3:9], rest[9:18])
    mixture = rest[8]
    tokens, depth = out_ref.shape
    other = 1 - core
    grads, kept, pairs = [qkv_ref, o_ref], [qkv_mine, o_mine], [qkv_pair, o_pair]
    zs, sums = [qkv_z, o_z], [qkv_sum, o_sum]
    width = q_out.shape[1]
    results = [
        [
            pltpu.make_async_copy(qkv_sum.at[:, pl.ds(i * width, width)], out, out_sem.at[i])
            for i, out in enumerate((q_out, k_out, v_out))
        ],
        [pltpu.make_async_copy(o_sum, o_out, out_sem.at[3])],
    ]

    def block(index, col):
        ref = grads[index]
        if index == 1:
            width = ref.shape[1] // 8
            return ref.at[:, pl.ds(pl.multiple_of(col * width, width), width)]
        height = ref.shape[0] // 8
        return ref.at[pl.ds(pl.multiple_of(col * height, height), height)]

    def row(fir, sec):
        yy, xx = row_of(core, fir, sec)
        return yy * 2 + xx

    def load(fir, sec):
        return pltpu.make_async_copy(field_ref.at[row(fir, sec)], mine.at[fir, sec], load_sem.at[fir, sec])

    def f_copy(sec):
        return send(field_ref.at[row(1 - first, sec)], first_in.at[sec], f_send.at[sec], f_recv.at[sec], along_first)

    g_copy = send(mine.at[first, 1 - second], second_in, g_send, g_recv, along_second)

    def w_load_copy(index, zz):
        return pltpu.make_async_copy(block(index, zz * 2 + core), kept[index].at[zz], w_load.at[index, zz])

    def w_give(index, zz):
        return send(
            block(index, zz * 2 + other), pairs[index].at[zz], p_send.at[index, zz], p_recv.at[index, zz], pair
        )

    above, below = (r, ((z + 1) % 4) * 2 + core), (r, ((z + 3) % 4) * 2 + core)

    def up_copy(index, dest):
        return send(
            kept[index].at[dest], zs[index].at[dest], z_send.at[index, dest], z_recv.at[index, dest], above
        )

    def down_copy(index, dest, slot):
        return send(kept[index].at[dest], zs[index].at[slot], z_send.at[index, dest], z_recv.at[index, slot], below)

    def chain(stage):
        @pl.when(z == stage)
        def _():
            for index in range(2):
                for dest in range(3, stage, -1):
                    if stage > 0:
                        up_copy(index, dest).wait_recv()
                        add(kept[index].at[dest], [zs[index].at[dest]])
                    up_copy(index, dest).start()

        @pl.when(z == 3 - stage)
        def _():
            for index in range(2):
                for dest in range(3 - stage):
                    if stage > 0:
                        down_copy(index, dest, dest).wait_recv()
                        add(kept[index].at[dest], [zs[index].at[dest]])
                    down_copy(index, dest, 4 if dest == 2 - stage else dest).start()

    def add(ref, extras):
        @pl.loop(0, ref.shape[0] // TILE)
        def _(t):
            here = pl.ds(pl.multiple_of(t * TILE, TILE), TILE)
            value = ref[here].astype(jnp.float32)
            for extra in extras:
                value = value + extra[here].astype(jnp.float32)
            ref[here] = value.astype(jnp.bfloat16)

    def add_out(ref, extras, result):
        @pl.loop(0, ref.shape[0] // TILE)
        def _(t):
            here = pl.ds(pl.multiple_of(t * TILE, TILE), TILE)
            value = ref[here].astype(jnp.float32)
            for extra in extras:
                value = value + extra[here].astype(jnp.float32)
            result[here] = value

    meet()
    for index in range(2):
        for k in (2, 1, 3, 0):
            w_give(index, (z + k) % 4).start()
            w_load_copy(index, (z + k) % 4).start()
    begin()
    f_copy(1 - second).start()
    f_copy(second).start()
    load(first, 1 - second).start()
    load(first, second).start()
    small_begin()
    for index in range(2):
        for k in (2, 1, 3, 0):
            zz = (z + k) % 4
            w_load_copy(index, zz).wait()
            w_give(index, zz).wait_recv()
            add(kept[index].at[zz], [pairs[index].at[zz]])
    chain(0)

    @pl.loop(0, RSTEPS + LAGS[2])
    def _(i):
        tick(i)

        @pl.when(i == 2)
        def _():
            chain(1)

        @pl.when(i == 4)
        def _():
            chain(2)

        @pl.when(i == 1)
        def _():
            load(first, 1 - second).wait()
            f_copy(1 - second).wait_recv()
            add(mine.at[first, 1 - second], [first_in.at[1 - second]])
            g_copy.start()

    for index in range(2):
        @pl.when(z == 0)
        def _():
            down_copy(index, 0, 4).wait_recv()
            add_out(kept[index].at[z], [zs[index].at[4]], sums[index])

        @pl.when(z == 3)
        def _():
            up_copy(index, 3).wait_recv()
            add_out(kept[index].at[z], [zs[index].at[3]], sums[index])

        @pl.when((z > 0) & (z < 3))
        def _():
            up_copy(index, z).wait_recv()
            down_copy(index, z, 4).wait_recv()
            add_out(kept[index].at[z], [zs[index].at[z], zs[index].at[4]], sums[index])

        for result in results[index]:
            result.start()
    load(first, second).wait()
    f_copy(second).wait_recv()
    g_copy.wait_recv()
    add_out(mine.at[first, second], [first_in.at[second], second_in], total)
    pltpu.make_async_copy(total, out_ref, out_sem.at[4]).start()

    @pl.loop(RSTEPS + LAGS[2], TICKS)
    def _(i):
        tick(i)

    pltpu.make_async_copy(mixture, mixture_ref, out_sem.at[5]).start()
    finish()
    for sec in range(2):
        f_copy(sec).wait_send()
    g_copy.wait_send()
    for index in range(2):
        for k in range(4):
            w_give(index, (z + k) % 4).wait_send()
            if k:
                up_copy(index, (z + k) % 4).wait_send()
        for result in results[index]:
            result.wait()
    small_finish()
    pltpu.make_async_copy(total, out_ref, out_sem.at[4]).wait()
    pltpu.make_async_copy(mixture, mixture_ref, out_sem.at[5]).wait()


def finish_near(part, field, grads, pack, collective_id):
    rows_count, tokens, depth = field.shape
    dma = pltpu.SemaphoreType.DMA
    blocks = [(grads[0].shape[0] // 8, grads[0].shape[1]), (grads[1].shape[0], grads[1].shape[1] // 8)]
    results = [(blocks[0][0], blocks[0][1] // 3)] * 3 + [blocks[1]]
    half = lambda *shape: pltpu.VMEM(shape, jnp.bfloat16)
    return pl.pallas_call(
        finish_body,
        out_shape=(
            jax.ShapeDtypeStruct((tokens, depth), jnp.float32),
            jax.ShapeDtypeStruct((tokens, depth), jnp.float32),
            *[jax.ShapeDtypeStruct(b, jnp.float32) for b in results],
            jax.ShapeDtypeStruct((RANKS, *pack.shape[1:]), pack.dtype),
        ),
        in_specs=[ANYWHERE] * 5,
        out_specs=[ANYWHERE] * 7,
        scratch_shapes=[
            half(2, 2, tokens, depth), half(2, tokens, depth), half(tokens, depth),
            pltpu.VMEM((tokens, depth), jnp.float32),
            *[half(4, *b) for b in blocks], *[half(4, *b) for b in blocks], *[half(5, *b) for b in blocks],
            *[pltpu.VMEM(b, jnp.float32) for b in blocks],
            dma((2, 2)), dma((2,)), dma((2,)), dma(()), dma(()),
            dma((2, 4)), dma((2, 4)), dma((2, 4)), dma((2, 4)), dma((2, 5)), dma((6,)),
        ]
        + small_sems()
        + shrink_scratch(tokens, depth),
        compiler_params=pltpu.CompilerParams(
            collective_id=collective_id, has_side_effects=True, vmem_limit_bytes=63 * 1024 * 1024
        ),
    )(part.reshape(4, 2, 2, 2, tokens, depth), field, *grads, pack)


RSTEPS = 8
TILE = 16
LAGS = (0, 1, 2, 4)
TICKS = RSTEPS + LAGS[3]


def shrink(part_ref, sums, near_own, first_in, second_in, z_in, total, sems):
    r, c, y, x, z, core, first, second = seat()
    pair, along_first, along_second, up = partners()
    load_sem, p_send, p_recv, f_send, f_recv, g_send, g_recv, z_send, z_recv = sems
    tokens = total.shape[0]
    step = tokens // RSTEPS
    other = 1 - core

    def rows(q):
        return pl.ds(pl.multiple_of(q * step, step), step)

    def spot(kind):
        fir = (1 - first) if kind < 2 else first
        sec = (1 - second) if kind in (0, 2) else second
        return fir, sec

    def load(kind, q):
        yy, xx = row_of(core, *spot(kind))
        return pltpu.make_async_copy(
            part_ref.at[:, core, yy, xx, rows(q)], near_own.at[q % 2, kind], load_sem.at[kind, q % 2]
        )

    def give(fir, sec, q):
        yy, xx = row_of(other, fir, sec)
        return send(
            part_ref.at[:, other, yy, xx, rows(q)],
            sums.at[fir, sec, :, rows(q)],
            p_send.at[fir, sec, q],
            p_recv.at[fir, sec, q],
            pair,
        )

    def f_copy(sec, q):
        return send(
            sums.at[1 - first, sec, :, rows(q)],
            first_in.at[sec, :, rows(q)],
            f_send.at[sec, q],
            f_recv.at[sec, q],
            along_first,
        )

    def g_copy(q):
        return send(
            sums.at[first, 1 - second, :, rows(q)], second_in.at[:, rows(q)], g_send.at[q], g_recv.at[q], along_second
        )

    def z_copy(k, q):
        return send(
            sums.at[first, second, (z + k) % 4, rows(q)],
            z_in.at[k - 1, rows(q)],
            z_send.at[k - 1, q],
            z_recv.at[k - 1, q],
            up[k - 1],
        )

    def begin():
        @pl.loop(0, RSTEPS)
        def _(q):
            for fir, sec in ((1 - second, 1 - first), (1 - second, first), (second, 1 - first), (second, first)):
                give(fir, sec, q).start()

        for kind in range(4):
            load(kind, 0).start()

    def add(kind, q, extra):
        fir, sec = spot(kind)

        @pl.when(q + 1 < RSTEPS)
        def _():
            load(kind, q + 1).start()

        load(kind, q).wait()
        give(fir, sec, q).wait_recv()

        @pl.loop(0, 4 * (step // TILE))
        def _(t):
            zz, at = t // (step // TILE), t % (step // TILE)
            here = pl.ds(pl.multiple_of(q * step + at * TILE, TILE), TILE)
            near = pl.ds(pl.multiple_of(at * TILE, TILE), TILE)
            value = sums[fir, sec, zz, here].astype(jnp.float32)
            value = value + near_own[q % 2, kind, zz, near].astype(jnp.float32)
            for ref in extra:
                value = value + ref[zz, here].astype(jnp.float32)
            sums[fir, sec, zz, here] = value.astype(jnp.bfloat16)

    def stage_first(q):
        for kind, sec in ((0, 1 - second), (1, second)):
            add(kind, q, [])
            f_copy(sec, q).start()

    def stage_second(q):
        f_copy(1 - second, q).wait_recv()
        add(2, q, [first_in.at[1 - second]])
        g_copy(q).start()

    def stage_z(q):
        f_copy(second, q).wait_recv()
        g_copy(q).wait_recv()
        add(3, q, [first_in.at[second], second_in])
        for k in QUEUE:
            z_copy(k, q).start()

    def stage_out(q):
        for k in ARRIVE:
            z_copy(k, q).wait_recv()

        @pl.loop(0, step // TILE)
        def _(t):
            here = pl.ds(pl.multiple_of(q * step + t * TILE, TILE), TILE)
            value = sums[first, second, z, here].astype(jnp.float32)
            for k in range(3):
                value = value + z_in[k, here].astype(jnp.float32)
            total[here] = value

    def tick(i):
        for stage, lag in zip((stage_first, stage_second, stage_z, stage_out), LAGS):

            @pl.when((i >= lag) & (i < RSTEPS + lag))
            def _(stage=stage, lag=lag):
                stage(i - lag)

    def finish():
        @pl.loop(0, RSTEPS)
        def _(q):
            for fir in range(2):
                for sec in range(2):
                    give(fir, sec, q).wait_send()
            for sec in range(2):
                f_copy(sec, q).wait_send()
            g_copy(q).wait_send()
            for k in QUEUE:
                z_copy(k, q).wait_send()

    return begin, tick, finish


def shrink_scratch(tokens, depth):
    dma = pltpu.SemaphoreType.DMA
    low = lambda *shape: pltpu.VMEM((*shape, depth), jnp.bfloat16)
    buffers = [
        low(2, 2, 4, tokens), low(2, 4, 4, tokens // RSTEPS), low(2, 4, tokens), low(4, tokens), low(3, tokens),
        pltpu.VMEM((tokens, depth), jnp.float32),
    ]
    shapes = [(2, 2, RSTEPS), (2, RSTEPS), (RSTEPS,), (3, RSTEPS)]
    return buffers + [dma((4, 2))] + [dma(shape) for shape in shapes for _ in range(2)]


def small_each(small_ref, small_all, sems, pick):
    here_sem, small_send, small_recv = sems
    local = pltpu.make_async_copy(small_ref.at[pick(nth(0)[0])], small_all.at[nth(0)[0]], here_sem)

    def copy(offset):
        return small_copy(lambda spot: small_ref.at[pick(spot)], small_all, small_send, small_recv, offset)

    def begin():
        local.start()

        @pl.loop(1, RANKS)
        def _(offset):
            copy(offset).start()

    def finish():
        local.wait()

        @pl.loop(1, RANKS)
        def _(offset):
            copy(offset).wait()

    return begin, finish


def feed_back_body(part_ref, small_ref, rows_ref, gate_ref, up_ref, act_ref, grads_ref,
                   out_ref, small_all, gate_out, up_out, down_out, *scratch):
    begin, tick, finish = shrink(part_ref, *scratch[:6], scratch[6:15])
    total, out_sem = scratch[5], scratch[15]
    small_begin, small_finish = small_each(small_ref, small_all, scratch[16:], lambda spot: spot)
    e, k = pl.program_id(0), pl.program_id(1)
    step = e * pl.num_programs(1) + k
    last = pl.num_programs(0) * pl.num_programs(1) - 1

    @pl.when(step == 0)
    def _():
        meet()
        small_begin()
        begin()

    rows = rows_ref[0]
    gate_out[0] = inner_rows(rows, gate_ref[0]).astype(jnp.bfloat16)
    up_out[0] = inner_rows(rows, up_ref[0]).astype(jnp.bfloat16)
    down_out[0] = inner_rows(act_ref[0], grads_ref[0]).astype(jnp.bfloat16)

    @pl.when(k == 0)
    def _():
        tick(e)

    @pl.when(step == last)
    def _():
        @pl.loop(RSTEPS, TICKS)
        def _(i):
            tick(i)

        done = pltpu.make_async_copy(total, out_ref, out_sem)
        done.start()
        finish()
        small_finish()
        done.wait()


def feed_back(part, small, rows, grad_gate, grad_up, act, grads, collective_id):
    tokens, depth = part.shape[0] // RANKS, part.shape[1]
    groups, length, inner = grad_gate.shape
    assert groups == RSTEPS
    dma = pltpu.SemaphoreType.DMA
    slab = pl.BlockSpec((1, length, CHUNK), lambda e, k: (e, 0, k))
    held = pl.BlockSpec((1, length, inner), lambda e, k: (e, 0, 0))
    return pl.pallas_call(
        feed_back_body,
        grid=(groups, depth // CHUNK),
        in_specs=[ANYWHERE, ANYWHERE, slab, held, held, held, slab],
        out_specs=[
            ANYWHERE,
            ANYWHERE,
            pl.BlockSpec((1, CHUNK, inner), lambda e, k: (e, k, 0)),
            pl.BlockSpec((1, CHUNK, inner), lambda e, k: (e, k, 0)),
            pl.BlockSpec((1, inner, CHUNK), lambda e, k: (e, 0, k)),
        ],
        out_shape=(
            jax.ShapeDtypeStruct((tokens, depth), jnp.float32),
            jax.ShapeDtypeStruct(small.shape, small.dtype),
            jax.ShapeDtypeStruct((groups, depth, inner), jnp.bfloat16),
            jax.ShapeDtypeStruct((groups, depth, inner), jnp.bfloat16),
            jax.ShapeDtypeStruct((groups, inner, depth), jnp.bfloat16),
        ),
        scratch_shapes=shrink_scratch(tokens, depth) + [dma(())] + small_sems(),
        compiler_params=pltpu.CompilerParams(
            collective_id=collective_id, has_side_effects=True, vmem_limit_bytes=63 * 1024 * 1024
        ),
    )(part.reshape(4, 2, 2, 2, tokens, depth), small, rows, grad_gate, grad_up, act, grads)


def fill_rows(pick_ref, field_ref, rows_ref):
    ranks, groups = pick_ref.shape[0], rows_ref.shape[0]

    @pl.loop(0, ranks // 2, unroll=UNROLL)
    def _(i):
        parts = [
            wide_dot(pick_ref[2 * i + side], field_ref[2 * i + side]).reshape(groups, SLOTS, CHUNK)
            for side in range(2)
        ]
        here = pl.ds(pl.multiple_of(i * 2 * SLOTS, 2 * SLOTS), 2 * SLOTS)
        rows_ref[:, here] = jnp.concatenate(parts, axis=1).astype(jnp.bfloat16)


def add_products(k, rows_ref, pairs):
    groups = rows_ref.shape[0]

    def products(e, first):
        for product, total in pairs:
            term = product(rows_ref[e], e)
            if first:
                total[e] = term
            else:
                total[e] += term

    @pl.when(k == 0)
    def _():
        @pl.loop(0, groups)
        def _(e):
            products(e, True)

    @pl.when(k > 0)
    def _():
        @pl.loop(0, groups)
        def _(e):
            products(e, False)


def grads_in_body(pick_ref, field_ref, down_ref, own_ref, small_ref,
                  rows_ref, plain_ref, all_ref, small_all, total, *sems):
    begin, forward, finish = spread_out(own_ref, all_ref, sems[:11])
    small_begin, small_finish = small_out(small_ref, small_all, sems[11:])
    k, last = pl.program_id(0), pl.num_programs(0) - 1

    @pl.when(k == 0)
    def _():
        meet()
        small_begin()
        begin()

    fill_rows(pick_ref, field_ref, rows_ref)
    add_products(k, rows_ref, [(lambda rows, e: outer_cols(rows, down_ref[e]), total)])

    @pl.when(k % 2 == 1)
    def _():
        forward(k // 2)

    @pl.when(k == last)
    def _():
        pltpu.sync_copy(total, plain_ref)
        finish()
        small_finish()


def grads_in(pick, field, down, own, small, collective_id):
    ranks, width, tokens = pick.shape
    groups, depth = width // SLOTS, field.shape[-1]
    length, inner = ranks * SLOTS, down.shape[1]
    steps = depth // CHUNK
    rows, plain, whole, small_all = pl.pallas_call(
        grads_in_body,
        grid=(steps,),
        in_specs=[
            pl.BlockSpec((ranks, width, tokens), lambda k: (0, 0, 0), pipeline_mode=pl.Buffered(1)),
            pl.BlockSpec((ranks, tokens, CHUNK), lambda k: (0, 0, k)),
            pl.BlockSpec((groups, inner, CHUNK), lambda k: (0, 0, k)),
            ANYWHERE,
            ANYWHERE,
        ],
        out_specs=[pl.BlockSpec((groups, length, CHUNK), lambda k: (0, 0, k))] + [ANYWHERE] * 3,
        out_shape=[
            jax.ShapeDtypeStruct((groups, length, depth), jnp.bfloat16),
            jax.ShapeDtypeStruct((groups, length, inner), jnp.float32),
            jax.ShapeDtypeStruct((4, 2, 2, 2, *own.shape), own.dtype),
            jax.ShapeDtypeStruct((RANKS, *small.shape), small.dtype),
        ],
        scratch_shapes=[pltpu.VMEM((groups, length, inner), jnp.float32)] + spread_sems() + small_sems(),
        compiler_params=pltpu.CompilerParams(
            collective_id=collective_id, has_side_effects=True, vmem_limit_bytes=62 * 1024 * 1024
        ),
    )(pick, field, down, own, small)
    return rows, plain, whole.reshape(RANKS, *own.shape), small_all


def feed_in_body(steps, pick_ref, field_ref, gate_ref, up_ref, plain_ref, probs_ref,
                 rows_ref, act_ref, weighted_ref, grad_gate_ref, grad_up_ref, gates_ref, gate_sum, up_sum):
    k = pl.program_id(0)

    @pl.when(k < steps)
    def _():
        fill_rows(pick_ref, field_ref, rows_ref)
        add_products(
            k,
            rows_ref,
            [
                (lambda rows, e: wide_dot(rows, gate_ref[e]), gate_sum),
                (lambda rows, e: wide_dot(rows, up_ref[e]), up_sum),
            ],
        )

    @pl.when(k >= steps)
    def _():
        e = k - steps
        length = act_ref.shape[1]

        @pl.loop(0, length // 128)
        def _(t):
            here = pl.ds(pl.multiple_of(t * 128, 128), 128)
            gate_val, up_val = gate_sum[e, here], up_sum[e, here]
            plain, probs = plain_ref[0, here], probs_ref[0, here]
            sigmoid_val = jax.nn.sigmoid(gate_val)
            silu_val = gate_val * sigmoid_val
            activated = silu_val * up_val
            grad_act = plain * probs
            grad_up_ref[0, here] = (grad_act * silu_val).astype(jnp.bfloat16)
            grad_gate_ref[0, here] = (
                grad_act * up_val * (sigmoid_val * (1.0 + gate_val * (1.0 - sigmoid_val)))
            ).astype(jnp.bfloat16)
            gates_ref[0, here] = jnp.sum(activated * plain, axis=-1, keepdims=True)
            weighted_ref[0, here] = (activated * probs).astype(jnp.bfloat16)
            act_ref[0, here] = activated.astype(jnp.bfloat16)


def feed_in(pick, field, gate, up, plain, probs):
    ranks, width, tokens = pick.shape
    groups, depth = width // SLOTS, field.shape[-1]
    length, inner = ranks * SLOTS, gate.shape[2]
    steps = depth // CHUNK
    held = lambda k: jnp.minimum(k, steps - 1)
    late = lambda k: (jnp.maximum(k - steps, 0), 0, 0)
    wide = pl.BlockSpec((1, length, inner), late)
    thin = pl.BlockSpec((1, length, 1), late)
    low = jax.ShapeDtypeStruct((groups, length, inner), jnp.bfloat16)
    return pl.pallas_call(
        functools.partial(feed_in_body, steps),
        grid=(steps + groups,),
        in_specs=[
            pl.BlockSpec((ranks, width, tokens), lambda k: (0, 0, 0), pipeline_mode=pl.Buffered(1)),
            pl.BlockSpec((ranks, tokens, CHUNK), lambda k: (0, 0, held(k))),
            pl.BlockSpec((groups, CHUNK, inner), lambda k: (0, held(k), 0)),
            pl.BlockSpec((groups, CHUNK, inner), lambda k: (0, held(k), 0)),
            wide,
            thin,
        ],
        out_specs=[pl.BlockSpec((groups, length, CHUNK), lambda k: (0, 0, held(k))), wide, wide, wide, wide, thin],
        out_shape=[
            jax.ShapeDtypeStruct((groups, length, depth), jnp.bfloat16),
            low, low, low, low,
            jax.ShapeDtypeStruct((groups, length, 1), jnp.float32),
        ],
        scratch_shapes=[pltpu.VMEM((groups, length, inner), jnp.float32)] * 2,
        compiler_params=pltpu.CompilerParams(vmem_limit_bytes=63 * 1024 * 1024),
        cost_estimate=pl.CostEstimate(
            flops=2 * groups * length * depth * (tokens + 2 * inner), bytes_accessed=120 << 20, transcendentals=0
        ),
    )(pick, field, gate, up, plain, probs)


def fill_field(flipped, spread_ref, lefts, weights, field_ref, rows):
    groups = rows.shape[0]
    ranks = spread_ref.shape[0]

    @pl.loop(0, groups)
    def _(e):
        total = None
        for left, weight, flip in zip(lefts, weights, flipped):
            term = outer_cols(left[e], weight[e]) if flip else wide_dot(left[e], weight[e])
            total = term if total is None else total + term
        rows[e] = total

    @pl.loop(0, ranks, unroll=2 * UNROLL)
    def _(s):
        part = rows[:, pl.ds(pl.multiple_of(s * SLOTS, SLOTS), SLOTS)]
        part = part.reshape(groups * SLOTS, CHUNK).astype(jnp.bfloat16)
        field_ref[s] = wide_dot(spread_ref[s], part).astype(jnp.bfloat16)


def restore_body(flipped, spread_ref, *refs):
    count = len(flipped)
    fill_field(flipped, spread_ref, refs[:count], refs[count : 2 * count], *refs[2 * count :])


def restore_specs(spread, lefts, weights, flipped):
    ranks, tokens, width = spread.shape
    groups = width // SLOTS
    length, inner = ranks * SLOTS, lefts[0].shape[2]
    depth = weights[0].shape[1] if flipped[0] else weights[0].shape[2]
    once = pl.Buffered(1)
    in_specs = (
        [pl.BlockSpec((ranks, tokens, width), lambda k: (0, 0, 0), pipeline_mode=once)]
        + [pl.BlockSpec((groups, length, inner), lambda k: (0, 0, 0), pipeline_mode=once)] * len(lefts)
        + [
            pl.BlockSpec((groups, CHUNK, inner), lambda k: (0, k, 0))
            if flip
            else pl.BlockSpec((groups, inner, CHUNK), lambda k: (0, 0, k))
            for flip in flipped
        ]
    )
    out_spec = pl.BlockSpec((ranks, tokens, CHUNK), lambda k: (0, 0, k))
    out_shape = jax.ShapeDtypeStruct((ranks, tokens, depth), jnp.bfloat16)
    return depth // CHUNK, in_specs, out_spec, out_shape, pltpu.VMEM((groups, length, CHUNK), jnp.float32)


def restore(spread, lefts, weights, flipped):
    steps, in_specs, out_spec, out_shape, rows = restore_specs(spread, lefts, weights, flipped)
    field = pl.pallas_call(
        functools.partial(restore_body, flipped),
        grid=(steps,),
        in_specs=in_specs,
        out_specs=out_spec,
        out_shape=out_shape,
        scratch_shapes=[rows],
        compiler_params=pltpu.CompilerParams(vmem_limit_bytes=63 * 1024 * 1024),
    )(spread, *lefts, *weights)
    return field.reshape(-1, field.shape[2])


PARTS = 4


def restore_out_body(spread_ref, left_ref, weight_ref, own_ref, field_ref, all_ref, rows,
                     here_sem, f_send, f_recv, g_send, g_recv, h_send, h_recv):
    r, c, y, x, z, core, first, second = seat()
    pair, along_first, along_second, up = partners()
    y1, x1 = row_of(core, first, 1 - second)
    near_row = y1 * 2 + x1
    step = own_ref.shape[0] // PARTS
    k = pl.program_id(0)
    here = pltpu.make_async_copy(own_ref, all_ref.at[r], here_sem)

    def part(ref, q):
        return ref.at[pl.ds(q * step, step)]

    def f_copy(q):
        return send(part(own_ref, q), part(all_ref.at[r], q), f_send.at[q], f_recv.at[q], along_first)

    def g_copy(q):
        return send(part(own_ref, q), part(all_ref.at[r], q), g_send.at[q], g_recv.at[q], along_second)

    def h_copy(q):
        there = part(all_ref.at[near_row], q)
        return send(there, there, h_send.at[q], h_recv.at[q], along_first)

    @pl.when(k == 0)
    def _():
        meet()
        here.start()
        for q in range(PARTS):
            g_copy(q).start()
            f_copy(q).start()

    fill_field((False,), spread_ref, [left_ref], [weight_ref], field_ref, rows)

    for q in range(PARTS):

        @pl.when(k == q + 1)
        def _():
            g_copy(q).wait_recv()
            h_copy(q).start()

    @pl.when(k == pl.num_programs(0) - 1)
    def _():
        here.wait()
        for q in range(PARTS):
            g_copy(q).wait_send()
            f_copy(q).wait()
            h_copy(q).wait()


def restore_out(spread, left, weight, own, collective_id):
    steps, in_specs, out_spec, out_shape, rows = restore_specs(spread, [left], [weight], (False,))
    dma = pltpu.SemaphoreType.DMA
    field, whole = pl.pallas_call(
        restore_out_body,
        grid=(steps,),
        in_specs=in_specs + [ANYWHERE],
        out_specs=[out_spec, ANYWHERE],
        out_shape=[out_shape, jax.ShapeDtypeStruct((4, *own.shape), own.dtype)],
        scratch_shapes=[rows, dma(())] + [dma((PARTS,))] * 6,
        compiler_params=pltpu.CompilerParams(
            collective_id=collective_id, has_side_effects=True, vmem_limit_bytes=63 * 1024 * 1024
        ),
    )(spread, left, weight, own)
    return field.reshape(-1, field.shape[2]), whole.reshape(-1, own.shape[1])


def branch_body(mixed_ref, weight_ref, out_ref, away, near, first_in, second_in,
                f_send, f_recv, g_send, g_recv):
    r, c, y, x, z, core, first, second = seat()
    pair, along_first, along_second, up = partners()
    tokens, depth = out_ref.shape
    width = depth // PARTS

    def columns(j):
        return pl.ds(j * width, width)

    def product(fir, sec, j):
        yy, xx = row_of(core, fir, sec)
        rows = pl.ds(pl.multiple_of((yy * 2 + xx) * tokens, tokens), tokens)
        return wide_dot(mixed_ref[rows], weight_ref[:, columns(j)])

    def f_copy(sec, j):
        return send(
            away.at[sec, :, columns(j)], first_in.at[sec, :, columns(j)], f_send.at[sec, j], f_recv.at[sec, j], along_first
        )

    def g_copy(j):
        return send(near.at[:, columns(j)], second_in.at[:, columns(j)], g_send.at[j], g_recv.at[j], along_second)

    meet()
    for j in range(PARTS):
        away[1 - second, :, columns(j)] = product(1 - first, 1 - second, j).astype(jnp.bfloat16)
        f_copy(1 - second, j).start()
    for j in range(PARTS):
        away[second, :, columns(j)] = product(1 - first, second, j).astype(jnp.bfloat16)
        f_copy(second, j).start()
    for j in range(PARTS):
        value = product(first, 1 - second, j)
        f_copy(1 - second, j).wait_recv()
        value = value + first_in[1 - second, :, columns(j)].astype(jnp.float32)
        near[:, columns(j)] = value.astype(jnp.bfloat16)
        g_copy(j).start()
    for j in range(PARTS):
        out_ref[:, columns(j)] = product(first, second, j)
    for j in range(PARTS):
        f_copy(second, j).wait_recv()
        g_copy(j).wait_recv()
        out_ref[:, columns(j)] += first_in[second, :, columns(j)].astype(jnp.float32) + second_in[
            :, columns(j)
        ].astype(jnp.float32)
    for j in range(PARTS):
        g_copy(j).wait_send()
        for sec in range(2):
            f_copy(sec, j).wait_send()


def branch_near(mixed, weight, collective_id):
    tokens, depth = mixed.shape[0] // 4, weight.shape[1]
    dma = pltpu.SemaphoreType.DMA
    inside = pl.BlockSpec(memory_space=pltpu.VMEM)
    low = lambda *shape: pltpu.VMEM((*shape, tokens, depth), jnp.bfloat16)
    return pl.pallas_call(
        branch_body,
        in_specs=[inside] * 2,
        out_specs=inside,
        out_shape=jax.ShapeDtypeStruct((tokens, depth), jnp.float32),
        scratch_shapes=[
            low(2), low(), low(2), low(), dma((2, PARTS)), dma((2, PARTS)), dma((PARTS,)), dma((PARTS,))
        ],
        compiler_params=pltpu.CompilerParams(
            collective_id=collective_id, has_side_effects=True, vmem_limit_bytes=40 * 1024 * 1024
        ),
    )(mixed, weight)


def causal_scores(query_rows, key_rows):
    scores = outer_cols(query_rows, key_rows) * HD ** (-0.5)
    count, length = scores.shape
    position = lax.broadcasted_iota(jnp.int32, scores.shape, 0) + (length - count)
    return jnp.where(position >= lax.broadcasted_iota(jnp.int32, scores.shape, 1), scores, MASKED)


def attend_body(q_raw, k_raw, v_ref, q_rs, k_rs, q_gain, k_gain, cos_ref, sin_ref,
                mixed_ref, q_out, k_out, v_out, lse_ref):
    length = v_ref.shape[0]
    block = min(256, length)
    v_out[...] = v_ref[...].astype(jnp.bfloat16)
    for raw, scale, gain, out in ((q_raw, q_rs, q_gain, q_out), (k_raw, k_rs, k_gain, k_out)):
        normed = raw[...] * scale[...] * gain[...]
        turned = normed * cos_ref[...] + pltpu.roll(normed, HD // 2, 1) * sin_ref[...]
        out[...] = turned.astype(jnp.bfloat16)
    for start in range(0, length, block):
        here, seen = pl.ds(start, block), pl.ds(0, start + block)
        scores = causal_scores(q_out[here], k_out[seen])
        row_top = jnp.max(scores, axis=-1, keepdims=True)
        exponent = jnp.exp(scores - row_top)
        row_total = jnp.sum(exponent, axis=-1, keepdims=True)
        weights = (exponent / row_total).astype(jnp.bfloat16)
        mixed_ref[here] = wide_dot(weights, v_out[seen]).astype(jnp.bfloat16)
        lse_ref[0, here] = row_top + jnp.log(row_total)


def three_slabs(length, heads):
    return [pl.BlockSpec((length, HD), lambda h, at=at: (0, at * heads + h)) for at in range(3)]


def attend(raw, q_rs, k_rs, q_gain, k_gain, cosine, sine):
    length, width = raw.shape[0], raw.shape[1] // 3
    heads = width // HD
    slab = pl.BlockSpec((length, HD), lambda h: (0, h))
    thin = pl.BlockSpec((length, 1), lambda h: (0, 0))
    line = pl.BlockSpec((1, HD), lambda h: (0, h))
    table = pl.BlockSpec((length, HD), lambda h: (0, 0))
    low = jax.ShapeDtypeStruct((length, width), jnp.bfloat16)
    return pl.pallas_call(
        attend_body,
        grid=(heads,),
        in_specs=three_slabs(length, heads) + [thin, thin, line, line, table, table],
        out_specs=[slab, slab, slab, slab, pl.BlockSpec((1, length, 1), lambda h: (h, 0, 0))],
        out_shape=[low, low, low, low, jax.ShapeDtypeStruct((heads, length, 1), jnp.float32)],
        cost_estimate=pl.CostEstimate(
            flops=4 * heads * length * length * HD, bytes_accessed=8 << 20, transcendentals=heads * length * length
        ),
    )(raw, raw, raw, q_rs, k_rs, q_gain[None], k_gain[None], cosine, sine)


def attend_back_body(count, *refs):
    (q_ref, k_ref, v_ref, grad_ref, lse_ref, q_raw, k_raw, q_rs, k_rs, q_gain, k_gain, cos_ref, sin_ref) = refs[:13]
    v_grad, q_grad, k_grad, q_term, k_term, q_inner, k_inner = refs[13 + count : 20 + count]
    dq, dk, dv = refs[20 + 2 * count :]
    for low, wide in zip(refs[13 : 13 + count], refs[20 + count : 20 + 2 * count]):
        wide[...] = low[...].astype(jnp.float32)
    length = v_ref.shape[0]
    block = min(256, length)
    dk[...] = jnp.zeros_like(dk)
    dv[...] = jnp.zeros_like(dv)
    for start in range(0, length, block):
        here, seen = pl.ds(start, block), pl.ds(0, start + block)
        query_rows, key_rows, grads = q_ref[here], k_ref[seen], grad_ref[here]
        probs = jnp.exp(causal_scores(query_rows, key_rows) - lse_ref[0, here])
        dv[seen] += inner_rows(probs.astype(jnp.bfloat16), grads)
        weights = outer_cols(grads, v_ref[seen])
        delta = jnp.sum(probs * weights, axis=-1, keepdims=True)
        scores = (probs * (weights - delta)).astype(jnp.bfloat16)
        dq[here] = wide_dot(scores, key_rows) * HD ** (-0.5)
        dk[seen] += inner_rows(scores, query_rows) * HD ** (-0.5)
    v_grad[...] = dv[...].astype(jnp.bfloat16)
    for raw, scale, gain, grad, out, term, inner in (
        (q_raw, q_rs, q_gain, dq, q_grad, q_term, q_inner),
        (k_raw, k_rs, k_gain, dk, k_grad, k_term, k_inner),
    ):
        field, value = raw[...], grad[...]
        normed = value * cos_ref[...] + pltpu.roll(value * sin_ref[...], HD // 2, 1)
        weighted = normed * gain[...]
        out[...] = weighted
        term[...] = jnp.sum(normed * field * scale[...], axis=0, keepdims=True)
        inner[0] = jnp.sum(weighted * field, axis=-1, keepdims=True)


def attend_back(lows, queries, keys, values, grads, lse, raw, q_rs, k_rs, q_gain, k_gain, cosine, sine):
    length, width = raw.shape[0], raw.shape[1] // 3
    heads = width // HD
    slab = pl.BlockSpec((length, HD), lambda h: (0, h))
    thin = pl.BlockSpec((length, 1), lambda h: (0, 0))
    line = pl.BlockSpec((1, HD), lambda h: (0, h))
    table = pl.BlockSpec((length, HD), lambda h: (0, 0))
    column = pl.BlockSpec((1, length, 1), lambda h: (h, 0, 0))
    wide = jax.ShapeDtypeStruct((length, width), jnp.float32)
    slices = [
        pl.BlockSpec((low.shape[0] // heads, *low.shape[1:]), lambda h: (h, 0, 0)) for low in lows
    ]
    outs = pl.pallas_call(
        functools.partial(attend_back_body, len(lows)),
        grid=(heads,),
        in_specs=[slab] * 4 + [column] + three_slabs(length, heads)[:2] + [thin, thin, line, line, table, table] + slices,
        out_specs=[slab, slab, slab, line, line, column, column] + slices,
        out_shape=[
            jax.ShapeDtypeStruct((length, width), jnp.bfloat16),
            wide,
            wide,
            jax.ShapeDtypeStruct((1, width), jnp.float32),
            jax.ShapeDtypeStruct((1, width), jnp.float32),
            jax.ShapeDtypeStruct((heads, length, 1), jnp.float32),
            jax.ShapeDtypeStruct((heads, length, 1), jnp.float32),
        ]
        + [jax.ShapeDtypeStruct(low.shape, jnp.float32) for low in lows],
        compiler_params=pltpu.CompilerParams(vmem_limit_bytes=60 * 1024 * 1024),
        scratch_shapes=[pltpu.VMEM((length, HD), jnp.float32)] * 3,
        cost_estimate=pl.CostEstimate(
            flops=10 * heads * length * length * HD, bytes_accessed=16 << 20, transcendentals=heads * length * length
        ),
    )(queries, keys, values, grads, lse, raw, raw, q_rs, k_rs, q_gain[None], k_gain[None], cosine, sine, *lows)
    return outs[:7], outs[7:]


def local(
    layer_input,
    cotangent,
    expert_index,
    attention_gain,
    query_gain,
    key_gain,
    query_weight,
    key_weight,
    value_weight,
    output_weight,
    feed_gain,
    router_weight,
    gate_weight,
    up_weight,
    down_weight,
):
    tokens = layer_input.shape[0]
    rows_count = lax.axis_size("row")
    near = rows_count == 4 and lax.axis_size("col") == 8
    if near:
        head_part = query_gain.shape[0]
        slice_width = attention_gain.shape[0]
        pack = jnp.concatenate(
            [attention_gain, feed_gain, query_gain, key_gain, router_weight.reshape(-1)]
        )
        pack = jnp.pad(pack, (0, PACK_ROWS * 128 - pack.shape[0])).reshape(PACK_ROWS, 128)
        (
            sequence, qkv_full, output_full, pack_all, cotangent_all, index_all
        ) = start_near(
            layer_input,
            [query_weight, key_weight, value_weight, output_weight],
            pack,
            cotangent,
            expert_index.T,
            1,
        )
        index_all = jnp.swapaxes(index_all, 1, 2)
        pack_all = pack_all.reshape(8, -1)
        ends = [slice_width, 2 * slice_width, 2 * slice_width + head_part, 2 * slice_width + 2 * head_part]
        attention_full = pack_all[:, : ends[0]].reshape(-1)
        feed_full = pack_all[:, ends[0] : ends[1]].reshape(-1)
        query_scale_w = pack_all[:, ends[1] : ends[2]].reshape(-1)
        key_scale_w = pack_all[:, ends[2] : ends[3]].reshape(-1)
        router_full = pack_all[:, ends[3] : ends[3] + router_weight.size].reshape(
            -1, router_weight.shape[1]
        )
    else:
        (
            attention_full,
            query_scale_w,
            key_scale_w,
            query_full,
            key_full,
            value_full,
            output_full,
            feed_full,
            router_full,
        ) = (
            lax.all_gather(attention_gain, "col", axis=0, tiled=True),
            lax.all_gather(query_gain, "col", axis=0, tiled=True),
            lax.all_gather(key_gain, "col", axis=0, tiled=True),
            lax.all_gather(query_weight, "col", axis=0, tiled=True),
            lax.all_gather(key_weight, "col", axis=0, tiled=True),
            lax.all_gather(value_weight, "col", axis=0, tiled=True),
            lax.all_gather(output_weight, "col", axis=1, tiled=True),
            lax.all_gather(feed_gain, "col", axis=0, tiled=True),
            lax.all_gather(router_weight, "col", axis=0, tiled=True),
        )
        qkv_full = jnp.concatenate([query_full, key_full, value_full], axis=1)
        sequence = lax.all_gather(layer_input, "row", axis=0, tiled=True)
    length = sequence.shape[0]
    model_width = sequence.shape[1]
    local_width = qkv_full.shape[1] // 3
    seq_float = sequence.astype(jnp.float32)
    seq_scale = rms_scale(seq_float)
    attention_float = attention_full.astype(jnp.float32)
    normed = (seq_float * seq_scale * attention_float).astype(jnp.bfloat16)
    raw = wide_dot(normed, qkv_full)
    query_raw, key_raw = raw[:, :local_width], raw[:, local_width : 2 * local_width]
    query_total, key_total = lax.psum(
        (jnp.sum(query_raw * query_raw, axis=-1), jnp.sum(key_raw * key_raw, axis=-1)), "row"
    )
    query_rs = lax.rsqrt(query_total / model_width + EPS)[:, None]
    key_rs = lax.rsqrt(key_total / model_width + EPS)[:, None]
    query_gain_f = query_scale_w.astype(jnp.float32)
    key_gain_f = key_scale_w.astype(jnp.float32)
    cosine, sine_table = rope_tables(length)
    mixed_heads, queries, keys_rotated, values, lse_all = attend(
        raw, query_rs, key_rs, query_gain_f, key_gain_f, cosine, sine_table
    )
    if near:
        branch = branch_near(mixed_heads, output_full, 5)
    else:
        branch = lax.psum_scatter(
            wide_dot(mixed_heads, output_full).astype(jnp.bfloat16), "row", scatter_dimension=0, tiled=True
        ).astype(jnp.float32)
    hidden = layer_input.astype(jnp.float32) + branch
    feed_scale = rms_scale(hidden)
    feed_float = feed_full.astype(jnp.float32)
    feed_normed = (hidden * feed_scale * feed_float).astype(jnp.bfloat16)
    logits = wide_dot(feed_normed, router_full)
    logit_top = jnp.max(logits, axis=-1, keepdims=True)
    logit_exp = jnp.exp(logits - logit_top)
    router_probs = logit_exp / jnp.sum(logit_exp, axis=-1, keepdims=True)
    experts = router_full.shape[1]
    experts_local = gate_weight.shape[0]
    ranks = lax.axis_size("col") * rows_count
    gate_hits = expert_index[:, :, None] == jnp.arange(experts, dtype=jnp.int32)
    gate_probs = jnp.sum(jnp.where(gate_hits, router_probs[:, None, :], 0.0), axis=-1)

    if not near:
        index_all = lax.all_gather(expert_index, ("col", "row"), axis=0, tiled=True)
    own = (index_all - lax.axis_index("col") * experts_local).reshape(ranks, tokens, -1)
    matches = own[..., None] == jnp.arange(experts_local, dtype=jnp.int32)
    hit = jnp.sum(matches.astype(jnp.float32), axis=2)
    earlier = jnp.tril(jnp.ones((tokens, tokens), jnp.bfloat16), -1)
    rank = jnp.einsum(
        "tu,sue->ste", earlier, hit.astype(jnp.bfloat16), preferred_element_type=jnp.float32
    )
    slot = jnp.where(hit > 0, rank, -1.0)
    places = jnp.arange(SLOTS, dtype=jnp.float32)
    slot_t = jnp.swapaxes(slot, 1, 2)
    width = experts_local * SLOTS
    picked = slot_t[:, :, None, :] == places[None, None, :, None]
    pick = picked.astype(jnp.bfloat16).reshape(ranks, width, tokens)
    lanes = jnp.arange(width, dtype=jnp.int32)
    widen = (lanes[None, :] // SLOTS == jnp.arange(experts_local)[:, None]).astype(jnp.bfloat16)
    spread = jnp.einsum(
        "ste,ew->stw", slot.astype(jnp.bfloat16), widen, preferred_element_type=jnp.float32
    ) == (lanes % SLOTS).astype(jnp.float32)
    spread_plain = spread.astype(jnp.bfloat16)

    def weigh(probs_all):
        probs_own = jnp.sum(
            jnp.where(matches, probs_all.reshape(ranks, tokens, -1, 1), 0.0), axis=2
        )
        probs_wide = jnp.einsum(
            "ste,ew->stw", probs_own.astype(jnp.bfloat16), widen, preferred_element_type=jnp.float32
        )
        spread_probs = jnp.where(spread, probs_wide, 0.0).astype(jnp.bfloat16)
        probs_t = jnp.swapaxes(probs_own, 1, 2)
        row_probs = jnp.sum(jnp.where(picked, probs_t[:, :, None, :], 0.0), axis=-1)
        row_probs = jnp.swapaxes(row_probs, 0, 1).reshape(experts_local, ranks * SLOTS, 1)
        return spread_probs, row_probs

    if near:
        expert_grads, plain_act, feed_all, probs_all = grads_in(
            pick, cotangent_all, down_weight, feed_normed, gate_probs.T, 2
        )
        spread_probs, row_probs = weigh(jnp.swapaxes(probs_all, 1, 2))
        expert_rows, activated, weighted_act, grad_gate, grad_up, row_gates = feed_in(
            pick, feed_all, gate_weight, up_weight, plain_act, row_probs
        )
    else:
        probs_all = lax.all_gather(gate_probs, ("col", "row"), axis=0, tiled=True)
        spread_probs, row_probs = weigh(probs_all)
        expert_grads = gather_rows(pick, cotangent)
        expert_rows = gather_rows(pick, feed_normed)
        gate_val = jnp.einsum(
            "erd,edf->erf", expert_rows, gate_weight, preferred_element_type=jnp.float32
        )
        up_val = jnp.einsum(
            "erd,edf->erf", expert_rows, up_weight, preferred_element_type=jnp.float32
        )
        plain_act = jnp.einsum(
            "erd,efd->erf", expert_grads, down_weight, preferred_element_type=jnp.float32
        )
        sigmoid_val = jax.nn.sigmoid(gate_val)
        silu_val = gate_val * sigmoid_val
        activated = silu_val * up_val
        grad_act = plain_act * row_probs
        grad_up = (grad_act * silu_val).astype(jnp.bfloat16)
        grad_gate = (
            grad_act * up_val * sigmoid_val * (1.0 + gate_val * (1.0 - sigmoid_val))
        ).astype(jnp.bfloat16)
        row_gates = jnp.sum(activated * plain_act, axis=-1)
        weighted_act = (activated * row_probs).astype(jnp.bfloat16)
        activated = activated.astype(jnp.bfloat16)
    row_gates = jnp.swapaxes(row_gates.reshape(experts_local, ranks, SLOTS), 0, 1)
    own_gates = jnp.sum(jnp.where(picked, row_gates[..., None], 0.0), axis=2)
    if near:
        grad_feed_part = restore(
            spread_plain, [grad_gate, grad_up], [gate_weight, up_weight], (True, True)
        )
        grad_feed, gates_in, grad_gate_weight, grad_up_weight, grad_down_weight = feed_back(
            grad_feed_part, own_gates, expert_rows, grad_gate, grad_up, weighted_act, expert_grads, 3
        )
        expert_terms = [grad_gate_weight, grad_up_weight, grad_down_weight]
        gates_in = jnp.sum(gates_in.reshape(-1, rows_count, experts_local, tokens), axis=1)
        grad_probs = gates_in.reshape(experts, tokens).T
    else:
        own_gates = lax.psum_scatter(
            jnp.swapaxes(own_gates, 1, 2).reshape(-1, rows_count, tokens, experts_local),
            "row",
            scatter_dimension=1,
        )
        grad_probs = lax.all_to_all(own_gates, "col", split_axis=0, concat_axis=2, tiled=True)[0]
        back_rows = (
            jnp.einsum("erf,edf->erd", grad_gate, gate_weight, preferred_element_type=jnp.float32)
            + jnp.einsum("erf,edf->erd", grad_up, up_weight, preferred_element_type=jnp.float32)
        ).astype(jnp.bfloat16)
        grad_feed = return_rows(spread_plain, back_rows).astype(jnp.float32)
        out_rows = jnp.einsum(
            "erf,efd->erd", activated, down_weight, preferred_element_type=jnp.float32
        ).astype(jnp.bfloat16)
        mixture = return_rows(spread_probs, out_rows).astype(jnp.float32)
        grad_gate_weight = jnp.einsum(
            "erd,erf->edf", expert_rows, grad_gate, preferred_element_type=jnp.float32
        )
        grad_up_weight = jnp.einsum(
            "erd,erf->edf", expert_rows, grad_up, preferred_element_type=jnp.float32
        )
        grad_down_weight = jnp.einsum(
            "erf,erd->efd", weighted_act, expert_grads, preferred_element_type=jnp.float32
        )
    grad_out = cotangent.astype(jnp.float32)
    grad_logits = (
        router_probs * (grad_probs - jnp.sum(router_probs * grad_probs, axis=-1, keepdims=True))
    ).astype(jnp.bfloat16)
    router_grad = inner_rows(feed_normed, grad_logits)
    grad_feed = grad_feed + outer_cols(grad_logits, router_full)
    feed_gain_term = jnp.sum(grad_feed * hidden * feed_scale, axis=0)
    feed_weighted = grad_feed * feed_float
    grad_hidden = (
        grad_out
        + feed_scale * feed_weighted
        - hidden * feed_scale**3 * jnp.mean(feed_weighted * hidden, axis=-1, keepdims=True)
    )
    if near:
        mixture_part, grad_branch = restore_out(
            spread_probs, activated, down_weight, grad_hidden.astype(jnp.bfloat16), 6
        )
    else:
        grad_branch = lax.all_gather(grad_hidden.astype(jnp.bfloat16), "row", axis=0, tiled=True)
    output_grad = inner_rows(mixed_heads, grad_branch)
    grad_mixed = outer_cols(grad_branch, output_full).astype(jnp.bfloat16)
    (
        grad_value_low, query_weighted, key_weighted, query_gain_term, key_gain_term, query_inner, key_inner
    ), widened = attend_back(
        expert_terms if near else [],
        queries, keys_rotated, values, grad_mixed, lse_all, raw, query_rs, key_rs,
        query_gain_f, key_gain_f, cosine, sine_table,
    )
    query_gain_term, key_gain_term = query_gain_term.reshape(-1), key_gain_term.reshape(-1)
    if near:
        grad_gate_weight, grad_up_weight, grad_down_weight = widened
    query_inner, key_inner = (
        lax.psum(jnp.sum(query_inner, axis=(0, 2)), "row"),
        lax.psum(jnp.sum(key_inner, axis=(0, 2)), "row"),
    )
    grad_query_raw = (
        query_rs * query_weighted - query_raw * query_rs**3 * (query_inner / model_width)[:, None]
    ).astype(jnp.bfloat16)
    grad_key_raw = (
        key_rs * key_weighted - key_raw * key_rs**3 * (key_inner / model_width)[:, None]
    ).astype(jnp.bfloat16)
    raw_grads = jnp.concatenate([grad_query_raw, grad_key_raw, grad_value_low], axis=1)
    qkv_grad = inner_rows(normed, raw_grads)
    grad_normed = outer_cols(raw_grads, qkv_full)
    attention_weighted = grad_normed * attention_float
    grad_seq_part = seq_scale * attention_weighted - seq_float * seq_scale**3 * jnp.mean(
        attention_weighted * seq_float, axis=-1, keepdims=True
    )
    attention_gain_term = jnp.sum(grad_normed * seq_float * seq_scale, axis=0)
    if near:
        cols = lax.axis_size("col")
        pack = jnp.concatenate(
            [
                attention_gain_term.reshape(cols, -1),
                feed_gain_term.reshape(cols, -1),
                query_gain_term.reshape(cols, -1),
                key_gain_term.reshape(cols, -1),
                router_grad.reshape(cols, -1),
            ],
            axis=1,
        )
        pack = jnp.pad(pack, ((0, 0), (0, PACK_ROWS * 128 - pack.shape[1])))
        pack = pack.astype(jnp.bfloat16).reshape(cols, PACK_ROWS, 128)
        (
            mixture, summed, grad_query_weight, grad_key_weight, grad_value_weight, grad_output_weight, packs
        ) = finish_near(
            mixture_part,
            grad_seq_part.astype(jnp.bfloat16).reshape(rows_count, tokens, model_width),
            [grad.astype(jnp.bfloat16) for grad in (qkv_grad, output_grad)],
            pack,
            4,
        )
        input_grad = grad_hidden + summed
        packs = packs.reshape(cols, rows_count, -1).astype(jnp.float32)
        whole = jnp.sum(packs, axis=(0, 1))
        heads_sum = jnp.sum(
            lax.dynamic_index_in_dim(packs, lax.axis_index("row"), 1, keepdims=False), axis=0
        )
        grad_attention_gain = whole[: ends[0]]
        grad_feed_gain = whole[ends[0] : ends[1]]
        grad_query_gain = heads_sum[ends[1] : ends[2]]
        grad_key_gain = heads_sum[ends[2] : ends[3]]
        grad_router_weight = whole[ends[3] : ends[3] + router_weight.size].reshape(router_weight.shape)
    else:
        stacked = jnp.concatenate(
            [
                grad_seq_part.reshape(rows_count, tokens, model_width),
                jnp.broadcast_to(attention_gain_term[None, None, :], (rows_count, 1, model_width)),
            ],
            axis=1,
        ).reshape(rows_count * (tokens + 1), model_width)
        summed = lax.psum_scatter(
            stacked.astype(jnp.bfloat16), "row", scatter_dimension=0, tiled=True
        ).astype(jnp.float32)
        input_grad = grad_hidden + summed[:tokens]
        attention_gain_total = summed[tokens]
        query_grad, key_grad, value_grad = jnp.split(qkv_grad, 3, axis=1)
        feed_gain_total, router_total = (
            lax.psum(feed_gain_term.astype(jnp.bfloat16), "row").astype(jnp.float32),
            lax.psum(router_grad.astype(jnp.bfloat16), "row").astype(jnp.float32),
        )
        (
            grad_attention_gain,
            grad_query_gain,
            grad_key_gain,
            grad_query_weight,
            grad_key_weight,
            grad_value_weight,
            grad_output_weight,
            grad_feed_gain,
            grad_router_weight,
        ) = (
            lax.psum_scatter(
                attention_gain_total.astype(jnp.bfloat16), "col", scatter_dimension=0, tiled=True
            ).astype(jnp.float32),
            lax.psum_scatter(
                query_gain_term.astype(jnp.bfloat16), "col", scatter_dimension=0, tiled=True
            ).astype(jnp.float32),
            lax.psum_scatter(
                key_gain_term.astype(jnp.bfloat16), "col", scatter_dimension=0, tiled=True
            ).astype(jnp.float32),
            lax.psum_scatter(
                query_grad.astype(jnp.bfloat16), "col", scatter_dimension=0, tiled=True
            ).astype(jnp.float32),
            lax.psum_scatter(
                key_grad.astype(jnp.bfloat16), "col", scatter_dimension=0, tiled=True
            ).astype(jnp.float32),
            lax.psum_scatter(
                value_grad.astype(jnp.bfloat16), "col", scatter_dimension=0, tiled=True
            ).astype(jnp.float32),
            lax.psum_scatter(
                output_grad.astype(jnp.bfloat16), "col", scatter_dimension=1, tiled=True
            ).astype(jnp.float32),
            lax.psum_scatter(
                feed_gain_total.astype(jnp.bfloat16), "col", scatter_dimension=0, tiled=True
            ).astype(jnp.float32),
            lax.psum_scatter(
                router_total.astype(jnp.bfloat16), "col", scatter_dimension=0, tiled=True
            ).astype(jnp.float32),
        )
    layer_output = hidden + mixture
    return (
        layer_output,
        input_grad,
        grad_attention_gain,
        grad_query_gain,
        grad_key_gain,
        grad_query_weight,
        grad_key_weight,
        grad_value_weight,
        grad_output_weight,
        grad_feed_gain,
        grad_router_weight,
        grad_gate_weight,
        grad_up_weight,
        grad_down_weight,
    )


def solution(mesh):
    placed = (
        P(("col", "row"), None),
        P(("col", "row"), None),
        P(("col", "row"), None),
        P("col"),
        P(("row", "col")),
        P(("row", "col")),
        P("col", "row"),
        P("col", "row"),
        P("col", "row"),
        P("row", "col"),
        P("col"),
        P("col", None),
        P("col", None, "row"),
        P("col", None, "row"),
        P("col", "row", None),
    )
    return jax.shard_map(
        local,
        mesh=mesh,
        in_specs=placed,
        out_specs=(
            P(("col", "row"), None),
            P(("col", "row"), None),
            P("col"),
            P(("row", "col")),
            P(("row", "col")),
            P("col", "row"),
            P("col", "row"),
            P("col", "row"),
            P("row", "col"),
            P("col"),
            P("col", None),
            P("col", None, "row"),
            P("col", None, "row"),
            P("col", "row", None),
        ),
        check_vma=False,
    )
```
